16 devices in a mesh: dp: 4 (over z, y), cp: 4 (over x, core).
Axes of the slice: x: 2, y: 2, z: 2, core: 2. Of those that a mesh axis runs over, the one named last changes fastest.
Arguments:
- q_tokens: bfloat16 [4096, 32, 128], P(('dp', 'cp')), parts along dimension 0
- k_tokens: bfloat16 [4096, 8, 128], P(('dp', 'cp')), parts along dimension 0
- v_tokens: bfloat16 [4096, 8, 128], P(('dp', 'cp')), parts along dimension 0
- d_out: bfloat16 [4096, 32, 128], P(('dp', 'cp')), parts along dimension 0
- key_valid: int32 [4096], P(('dp', 'cp')), parts along dimension 0
- cu_seqlens: int32 [12], P('dp'), parts along dimension 0
Outputs:
- output 1: bfloat16 [4096, 32, 128], P(('dp', 'cp')), parts along dimension 0
- output 2: float32 [4096, 32], P(('dp', 'cp')), parts along dimension 0
- output 3: bfloat16 [4096, 32, 128], P(('dp', 'cp')), parts along dimension 0
- output 4: bfloat16 [4096, 8, 128], P(('dp', 'cp')), parts along dimension 0
- output 5: bfloat16 [4096, 8, 128], P(('dp', 'cp')), parts along dimension 0
There are 4 independent parts. The reference program is written for one: setup_inputs(seed, part) draws one part's arguments, and reference() takes and returns one part's arrays. A program takes and returns all parts, laid end to end along the dimension named above; each array names one.
All inputs are finite; a program needn't handle non-finite values.
Results may differ from the reference program's by a relative error of at most 0.00877425.
Values are sent between devices in bfloat16 or wider.
A program may use at most 1 GiB of HBM per device.

```python
import jax
import jax.numpy as jnp
from jax import lax

HEADS = 32
KV_HEADS = 8
HEAD = 128
TOK_DEV = 256
DOCS = 2
CP = 4
TOKENS = TOK_DEV * CP
GROUP = HEADS // KV_HEADS
Q_BLOCK = min(32, TOKENS)
MASK_FILL = -1.0e30


def token_coords(cu_seqlens, rank_ids, local_ids):
    starts = cu_seqlens[:-1] // CP
    doc_id = jnp.sum((local_ids[..., None] >= starts).astype(jnp.int32), axis=-1) - 1
    seg_start = cu_seqlens[doc_id]
    piece_len = (cu_seqlens[doc_id + 1] - seg_start) // (2 * CP)
    within = local_ids - seg_start // CP
    in_upper = (within >= piece_len).astype(jnp.int32)
    piece_idx = rank_ids + in_upper * (2 * CP - 1 - 2 * rank_ids)
    position = seg_start + piece_idx * piece_len + within - in_upper * piece_len
    return doc_id, position


def draw_layout(layout_key):
    key_cut, key_pad = jax.random.split(layout_key)
    unit_count = TOKENS // (2 * CP)
    cut_points = jnp.sort(jax.random.permutation(key_cut, unit_count - 1)[:DOCS - 1] + 1)
    bounds = jnp.concatenate([jnp.zeros((1,), jnp.int32), cut_points.astype(jnp.int32), jnp.full((1,), unit_count, jnp.int32)]) * (2 * CP)
    pad_len = jax.random.randint(key_pad, (DOCS,), 0, 2 * CP)
    tok_index = jnp.arange(TOKENS)
    doc_id, position = token_coords(bounds, tok_index // TOK_DEV, tok_index % TOK_DEV)
    key_valid = (position < bounds[doc_id + 1] - pad_len[doc_id]).astype(jnp.int32)
    return bounds, key_valid


def setup_inputs(seed: int = 0, part: int = 0) -> dict:
    part_key = jax.random.fold_in(jax.random.key(seed), part)
    key_list = jax.random.split(part_key, 5)
    cu_seqlens, key_valid = draw_layout(key_list[0])
    q_tokens = jax.random.normal(key_list[1], (TOKENS, HEADS, HEAD), jnp.float32).astype(jnp.bfloat16)
    k_tokens = jax.random.normal(key_list[2], (TOKENS, KV_HEADS, HEAD), jnp.float32).astype(jnp.bfloat16)
    v_tokens = jax.random.normal(key_list[3], (TOKENS, KV_HEADS, HEAD), jnp.float32).astype(jnp.bfloat16)
    d_out = jax.random.normal(key_list[4], (TOKENS, HEADS, HEAD), jnp.float32).astype(jnp.bfloat16)
    return {'q_tokens': q_tokens, 'k_tokens': k_tokens, 'v_tokens': v_tokens, 'd_out': d_out, 'key_valid': key_valid, 'cu_seqlens': cu_seqlens}


def reference(q_tokens, k_tokens, v_tokens, d_out, key_valid, cu_seqlens):
    tok_index = jnp.arange(TOKENS)
    doc_id, position = token_coords(cu_seqlens, tok_index // TOK_DEV, tok_index % TOK_DEV)
    key_ok = key_valid > 0
    score_scale = HEAD ** -0.5
    k_full = k_tokens.astype(jnp.float32)
    v_full = v_tokens.astype(jnp.float32)
    n_blocks = TOKENS // Q_BLOCK
    q_blocks = q_tokens.reshape(n_blocks, Q_BLOCK, KV_HEADS, GROUP, HEAD)
    do_blocks = d_out.reshape(n_blocks, Q_BLOCK, KV_HEADS, GROUP, HEAD)
    doc_blocks = doc_id.reshape(n_blocks, Q_BLOCK)
    pos_blocks = position.reshape(n_blocks, Q_BLOCK)

    def block_scores(q_blk, doc_q, pos_q):
        scores = jnp.einsum('qhgd,khd->hgqk', q_blk.astype(jnp.float32), k_full) * score_scale
        allowed = (doc_q[:, None] == doc_id[None, :]) & (position[None, :] <= pos_q[:, None]) & key_ok[None, :]
        return jnp.where(allowed, scores, MASK_FILL), allowed

    def forward_block(inputs):
        q_blk, doc_q, pos_q = inputs
        scores, allowed = block_scores(q_blk, doc_q, pos_q)
        row_max = jnp.max(scores, axis=-1)
        weights = jnp.where(allowed, jnp.exp(scores - row_max[..., None]), 0.0)
        row_sum = jnp.sum(weights, axis=-1)
        has_key = row_sum > 0
        safe_den = jnp.where(has_key, row_sum, 1.0)
        acc_out = jnp.einsum('hgqk,khd->qhgd', weights, v_full)
        inv_den = jnp.where(has_key, 1.0 / safe_den, 0.0)
        out_blk = acc_out * jnp.transpose(inv_den, (2, 0, 1))[..., None]
        lse_blk = jnp.where(has_key, row_max + jnp.log(safe_den), 0.0)
        return out_blk.astype(jnp.bfloat16), jnp.transpose(lse_blk, (2, 0, 1))

    out_blocks, lse_blocks = lax.map(forward_block, (q_blocks, doc_blocks, pos_blocks))

    def backward_block(grad_acc, inputs):
        dk_acc, dv_acc = grad_acc
        q_blk, do_blk, out_blk, lse_blk, doc_q, pos_q = inputs
        scores, allowed = block_scores(q_blk, doc_q, pos_q)
        lse_hgq = jnp.transpose(lse_blk, (1, 2, 0))
        weights = jnp.where(allowed, jnp.exp(scores - lse_hgq[..., None]), 0.0)
        do_full = do_blk.astype(jnp.float32)
        row_delta = jnp.transpose(jnp.sum(do_full * out_blk.astype(jnp.float32), axis=-1), (1, 2, 0))
        d_prob = jnp.einsum('qhgd,khd->hgqk', do_full, v_full)
        d_score = weights * (d_prob - row_delta[..., None])
        dq_blk = jnp.einsum('hgqk,khd->qhgd', d_score, k_full) * score_scale
        dk_acc = dk_acc + jnp.einsum('hgqk,qhgd->khd', d_score, q_blk.astype(jnp.float32)) * score_scale
        dv_acc = dv_acc + jnp.einsum('hgqk,qhgd->khd', weights, do_full)
        return (dk_acc, dv_acc), dq_blk.astype(jnp.bfloat16)

    zero_acc = jnp.zeros((TOKENS, KV_HEADS, HEAD), jnp.float32)
    grad_sums, dq_blocks = lax.scan(backward_block, (zero_acc, zero_acc), (q_blocks, do_blocks, out_blocks, lse_blocks, doc_blocks, pos_blocks))
    attn_out = out_blocks.reshape(TOKENS, HEADS, HEAD)
    log_sumexp = lse_blocks.reshape(TOKENS, HEADS)
    d_query = dq_blocks.reshape(TOKENS, HEADS, HEAD)
    return attn_out, log_sumexp, d_query, grad_sums[0].astype(jnp.bfloat16), grad_sums[1].astype(jnp.bfloat16)
```

```python
import functools
import math

import jax
import jax.numpy as jnp
from jax import lax
from jax.experimental import pallas as pl
from jax.experimental.pallas import tpu as pltpu
from jax.sharding import PartitionSpec as P

MESH = pl.DeviceIdType.MESH
FILL = -1.0e30
BIG = 3.0e38
HEAD = 128
SLOT = 128
TILE = 512
GROUP = 4
HC = 4
SCALE = HEAD ** -0.5
C2 = SCALE * math.log2(math.e)
NT = (((1,), (1,)), ((), ()))
NN = (((1,), (0,)), ((), ()))
F32 = jnp.float32
BF16 = jnp.bfloat16

TILES = ((0, 0), (1, 0), (1, 1), (0, 1))


def slot_of(chip, ti):
    oc, up = TILES[ti]
    r = 2 * chip + oc
    return 7 - r if up else r


def mm(a, b, dims):
    return lax.dot_general(a, b, dims, preferred_element_type=F32)


def src_row(up, t, l0):
    if up:
        return jnp.where(t < l0, t + l0, t + SLOT)
    return jnp.where(t < l0, t, t + l0)


def attn_kernel(cu, valid, q, k, v, do, o_out, dq_out, dkv_out, lse_out,
                raw_q, raw_do, far_q, far_do, raw_k, raw_v, kv_hm, kv_all, kt, vt, qh, doh, st, pb, db,
                dkv_acc, dkv_in, o_st, dq_st, dkv_st, lse_st, caps, valid_all,
                in_sem, raw_ssem, raw_rsem, val_ssem, val_rsem, kv_ssem, kv_rsem,
                part_ssem, part_rsem, out_sem, out_rsem, lse_sem, lse_rsem):
    r = lax.axis_index("cp")
    chip = r // 2
    c = r % 2
    pc = 1 - c
    partner = chip * 2 + pc
    cross = (1 - chip) * 2 + c
    cross_o = (1 - chip) * 2 + pc
    l0 = lax.shift_right_logical(cu[1], 3)

    def remote(src, dst, ssem, rsem, dev):
        return pltpu.make_async_remote_copy(src_ref=src, dst_ref=dst, send_sem=ssem, recv_sem=rsem,
                                            device_id={"cp": dev}, device_id_type=MESH)

    own_heads = pl.ds(pl.multiple_of(16 * c, 16), 16)
    oth_heads = pl.ds(pl.multiple_of(16 * pc, 16), 16)
    ld_k = pltpu.make_async_copy(k, raw_k, in_sem.at[0])
    ld_v = pltpu.make_async_copy(v, raw_v, in_sem.at[1])
    ld_q = pltpu.make_async_copy(q.at[:, own_heads, :], raw_q, in_sem.at[2])
    ld_do = pltpu.make_async_copy(do.at[:, own_heads, :], raw_do, in_sem.at[3])
    ld_val = pltpu.make_async_copy(valid, valid_all.at[r], in_sem.at[4])
    for cp in (ld_k, ld_v, ld_q, ld_do, ld_val):
        cp.start()

    barrier = pltpu.get_barrier_semaphore()
    for dev in (partner, cross, cross_o):
        pl.semaphore_signal(barrier, inc=1, device_id={"cp": dev}, device_id_type=MESH)
    pl.semaphore_wait(barrier, 3)

    peers = (partner, cross, cross_o)
    push_q = remote(q.at[:, oth_heads, :], far_q, raw_ssem.at[0], raw_rsem.at[0], partner)
    push_do = remote(do.at[:, oth_heads, :], far_do, raw_ssem.at[1], raw_rsem.at[1], partner)
    push_val = [remote(valid, valid_all.at[r], val_ssem.at[i], val_rsem.at[r], dev) for i, dev in enumerate(peers)]

    def kv_relayout(up):
        def body(i, _):
            t0 = i * 16
            for which, raw in ((0, raw_k), (1, raw_v)):
                rows = jnp.stack([raw[src_row(up, t0 + j, l0)] for j in range(16)])
                kv_hm[:, up, which, pl.ds(pl.multiple_of(t0, 16), 16), :] = jnp.transpose(rows, (1, 0, 2))
            return 0
        lax.fori_loop(0, SLOT // 16, body, 0)

    my_slot = (r, 7 - r)

    def kv_push(h, up, to):
        head = (4 * c if to == 1 else 4 * pc) + h
        dev = (partner, cross, cross_o)[to]
        return remote(kv_hm.at[head, up], kv_all.at[h, my_slot[up]], kv_ssem.at[to, h, up],
                      kv_rsem.at[h, my_slot[up]], dev)

    ld_k.wait()
    ld_v.wait()
    kv_relayout(0)
    for h in range(HC):
        kv_push(h, 0, 1).start()
        kv_push(h, 0, 2).start()
    kv_relayout(1)

    @pl.when(chip == 1)
    def _():
        for h in range(HC):
            kv_push(h, 1, 1).start()
            kv_push(h, 1, 2).start()

    for h in range(HC):
        kv_push(h, 0, 0).start()
        kv_push(h, 1, 0).start()
    push_q.start()
    push_do.start()
    ld_val.wait()
    for cp in push_val:
        cp.start()

    def copy_own(h, _):
        for up in range(2):
            kv_all[h, my_slot[up]] = kv_hm[4 * c + h, up]
        return 0
    lax.fori_loop(0, HC, copy_own, 0)

    def q_relayout(oc, from_q, from_do):
        for up, ti in ((0, oc), (1, 3 - oc)):
            def body(i, _):
                t0 = i * 16
                at = pl.ds(pl.multiple_of(t0, 16), 16)
                for raw, dst in ((from_q, qh), (from_do, doh)):
                    rows = jnp.stack([raw[src_row(up, t0 + j, l0)] for j in range(16)])
                    dst[:, ti, :, at, :] = jnp.transpose(rows, (1, 0, 2)).reshape(HC, GROUP, 16, HEAD)
                return 0
            lax.fori_loop(0, SLOT // 16, body, 0)

    ld_q.wait()
    ld_do.wait()
    q_relayout(c, raw_q, raw_do)

    for i in range(3):
        remote(valid, valid_all.at[peers[i]], val_ssem.at[i], val_rsem.at[peers[i]], peers[i]).wait_recv()
    lane = lax.broadcasted_iota(jnp.int32, (SLOT, SLOT), 1)
    sub = lax.broadcasted_iota(jnp.int32, (SLOT, SLOT), 0)
    lane2 = lax.broadcasted_iota(jnp.int32, (SLOT, 2 * SLOT), 1)
    sub2 = lax.broadcasted_iota(jnp.int32, (SLOT, 2 * SLOT), 0)
    same_doc = (lane < l0) == (sub < l0)
    doc_f = jnp.where(lane < l0, 1.0, 0.0)
    doc_s = jnp.where(sub < l0, 1.0, 0.0)
    same_f = jnp.where(doc_f == doc_s, 1.0, 0.0)
    del same_doc

    def cap_body(s, _):
        owner = jnp.where(s < 4, s, 7 - s)
        off = jnp.where(s < 4, 0, 1)
        src_lo = jnp.where(sub2 < l0, sub2, sub2 + l0)
        src_hi = jnp.where(sub2 < l0, sub2 + l0, sub2 + SLOT)
        src = jnp.where(off == 1, src_hi, src_lo)
        row = jnp.broadcast_to(valid_all[owner].astype(F32), (SLOT, 2 * SLOT))
        ok = jnp.sum(jnp.where(src == lane2, row, 0.0), axis=1, keepdims=True)
        caps[s] = jnp.where(same_f * ok > 0.5, BIG, FILL)
        return 0
    lax.fori_loop(0, 8, cap_body, 0)
    for ti in range(4):
        oc, up = TILES[ti]
        s = (7 - (2 * chip + oc)) if up else 2 * chip + oc
        caps[8 + ti] = jnp.where(sub <= lane, caps[s], FILL)

    push_q.wait_recv()
    push_do.wait_recv()
    q_relayout(pc, far_q, far_do)

    def part_copy(h, i, slot):
        return remote(dkv_acc.at[h, slot], dkv_in.at[h, i], part_ssem.at[h, i], part_rsem.at[h, i], cross)

    def out_copies(h, ti, which):
        stage, out = ((o_st, o_out), (dq_st, dq_out), (dkv_st, dkv_out))[which]
        oc, up = TILES[ti]
        dst = out.at[4 * c + h, up]
        src = stage.at[h, ti]
        return (pltpu.make_async_copy(src, dst, out_sem.at[which, h, ti]),
                remote(src, dst, out_sem.at[which, h, ti], out_rsem.at[which, h, up], partner))

    def out_start(h, ti, which):
        local, far = out_copies(h, ti, which)
        oc = TILES[ti][0]

        @pl.when(c == oc)
        def _():
            local.start()

        @pl.when(c != oc)
        def _():
            far.start()

    lse_local = pltpu.make_async_copy(lse_st.at[c], lse_out.at[:, own_heads, :], lse_sem.at[0])
    lse_far = remote(lse_st.at[pc], lse_out.at[:, own_heads, :], lse_sem.at[1], lse_rsem, partner)

    def run_chip(ch):
        slots = [slot_of(ch, ti) for ti in range(4)]
        sent = [0, 1] if ch == 1 else [2, 3, 4, 5]
        kept = [0, 1] if ch == 0 else [2, 3, 4, 5]
        order = [0, 1, 2, 3]

        def transposes(s):
            for src, dst in ((0, kt), (1, vt)):
                dst[:, s * SLOT:(s + 1) * SLOT] = jnp.transpose(kv_all[h_ref[0], s, src])

        h_ref = [None]

        def head(h, _):
            h_ref[0] = h
            seen = set()
            ready = set()

            def wait_slot(s):
                if s in ready:
                    return
                ready.add(s)
                if s in slots:
                    @pl.when(jnp.logical_and(r != s, 7 - r != s))
                    def _():
                        remote(kv_hm.at[0, 0], kv_all.at[h, s], kv_ssem.at[0, h, 0], kv_rsem.at[h, s], partner).wait_recv()
                else:
                    remote(kv_hm.at[0, 0], kv_all.at[h, s], kv_ssem.at[0, h, 0], kv_rsem.at[h, s], partner).wait_recv()
                transposes(s)

            for ti in order:
                s = slots[ti]
                nk = s + 1
                for u in range(nk):
                    wait_slot(u)
                qt = qh[h, ti].reshape(TILE, HEAD)
                dt = doh[h, ti].reshape(TILE, HEAD)
                m8 = [None] * GROUP
                for a in range(0, nk, 2):
                    n = min(2, nk - a)
                    kb = kv_all[h, a:a + n, 0].reshape(n * SLOT, HEAD)
                    sc = mm(kb, qt, NT)
                    for j in range(n):
                        cap = caps[8 + ti] if a + j == s else caps[a + j]
                        for g in range(GROUP):
                            x = jnp.minimum(sc[j * SLOT:(j + 1) * SLOT, g * SLOT:(g + 1) * SLOT], cap)
                            st[(a + j) * SLOT:(a + j + 1) * SLOT, g * SLOT:(g + 1) * SLOT] = x
                            top = jnp.max(x.reshape(SLOT // 8, 8, SLOT), axis=0)
                            m8[g] = top if m8[g] is None else jnp.maximum(m8[g], top)
                m = [jnp.max(x, axis=0, keepdims=True) for x in m8]
                mc = [x * C2 for x in m]
                l8 = [None] * GROUP
                for a in range(nk):
                    for g in range(GROUP):
                        at = (slice(a * SLOT, (a + 1) * SLOT), slice(g * SLOT, (g + 1) * SLOT))
                        e = jnp.exp2(st[at] * C2 - mc[g])
                        st[at] = e
                        pb[at] = e.astype(BF16)
                        tot = jnp.sum(e.reshape(SLOT // 8, 8, SLOT), axis=0)
                        l8[g] = tot if l8[g] is None else l8[g] + tot
                ot = mm(vt[:, :nk * SLOT], pb[:nk * SLOT, :], NN)
                inv, dd = [], []
                oc, up = TILES[ti]
                for g in range(GROUP):
                    l = jnp.sum(l8[g], axis=0, keepdims=True)
                    has = m[g] > 0.5 * FILL
                    safe = jnp.where(has, l, 1.0)
                    i_l = jnp.where(has, 1.0 / safe, 0.0)
                    lse = jnp.where(has, m[g] * SCALE + jnp.log(safe), 0.0)
                    lse_st[oc, up, pl.ds(h * GROUP + g, 1), :] = lse
                    og = (ot[:, g * SLOT:(g + 1) * SLOT] * i_l).astype(BF16)
                    dog = jnp.transpose(dt[g * SLOT:(g + 1) * SLOT, :])
                    dd.append(jnp.sum(og.astype(F32) * dog.astype(F32), axis=0, keepdims=True))
                    inv.append(i_l)
                    o_st[h, ti, g * SLOT:(g + 1) * SLOT, :] = jnp.transpose(og)
                out_start(h, ti, 0)

                first = [u for u in range(nk) if u in sent] if (ch == 0 and ti >= 2) else []
                rest = [u for u in range(nk) if u not in first]
                dqt = None
                for part in (first, rest):
                    runs = []
                    for u in part:
                        if runs and runs[-1][1] == u and u - runs[-1][0] < 2:
                            runs[-1][1] = u + 1
                        else:
                            runs.append([u, u + 1])
                    for a, b in runs:
                        n = b - a
                        vb = kv_all[h, a:b, 1].reshape(n * SLOT, HEAD)
                        dp = mm(vb, dt, NT)
                        for j in range(n):
                            for g in range(GROUP):
                                at = (slice((a + j) * SLOT, (a + j + 1) * SLOT), slice(g * SLOT, (g + 1) * SLOT))
                                p = st[at] * inv[g]
                                pb[at] = p.astype(BF16)
                                ds = p * (dp[j * SLOT:(j + 1) * SLOT, g * SLOT:(g + 1) * SLOT] - dd[g])
                                db[at] = ds.astype(BF16)
                        dsb = db[a * SLOT:b * SLOT, :]
                        dv = mm(pb[a * SLOT:b * SLOT, :], dt, NN)
                        dk = mm(dsb, qt, NN) * SCALE
                        dq = mm(kt[:, a * SLOT:b * SLOT], dsb, NN)
                        dqt = dq if dqt is None else dqt + dq
                        for j in range(n):
                            u = a + j
                            new = (dk[j * SLOT:(j + 1) * SLOT], dv[j * SLOT:(j + 1) * SLOT])
                            for w in range(2):
                                dkv_acc[h, u, w] = dkv_acc[h, u, w] + new[w] if u in seen else new[w]
                            seen.add(u)
                    if part is first and ti == 3 and ch == 0:
                        for i, u in enumerate(sent):
                            part_copy(h, i, u).start()
                for g in range(GROUP):
                    dqg = (dqt[:, g * SLOT:(g + 1) * SLOT] * SCALE).astype(BF16)
                    dq_st[h, ti, g * SLOT:(g + 1) * SLOT, :] = jnp.transpose(dqg)
                out_start(h, ti, 1)
            if ch == 1:
                for i, u in enumerate(sent):
                    part_copy(h, i, u).start()
            else:
                for ti in (2, 3):
                    for w in range(2):
                        dkv_st[h, ti, w] = dkv_acc[h, slots[ti], w].astype(BF16)
                    out_start(h, ti, 2)
            return 0

        lax.fori_loop(0, HC, head, 0)

        lse_local.start()
        lse_far.start()

        def tail(h, _):
            for i, u in enumerate(kept):
                ti = slots.index(u)
                part_copy(h, i, u).wait_recv()
                for w in range(2):
                    dkv_st[h, ti, w] = (dkv_acc[h, u, w] + dkv_in[h, i, w]).astype(BF16)
                out_start(h, ti, 2)
            return 0
        lax.fori_loop(0, HC, tail, 0)

        def drain(h, _):
            for i, u in enumerate(sent):
                part_copy(h, i, u).wait_send()
            return 0
        lax.fori_loop(0, HC, drain, 0)

    pl.when(chip == 0)(functools.partial(run_chip, 0))
    pl.when(chip == 1)(functools.partial(run_chip, 1))

    push_q.wait_send()
    push_do.wait_send()
    for cp in push_val:
        cp.wait_send()

    def drain(h, _):
        for up in range(2):
            kv_push(h, up, 0).wait_send()
        for to in (1, 2):
            kv_push(h, 0, to).wait_send()

        @pl.when(chip == 1)
        def _():
            for to in (1, 2):
                kv_push(h, 1, to).wait_send()
        for which in range(3):
            for ti in range(4):
                local, far = out_copies(h, ti, which)
                oc = TILES[ti][0]

                @pl.when(c == oc)
                def _():
                    local.wait()

                @pl.when(c != oc)
                def _():
                    far.wait_send()
            for up in range(2):
                stage, out = ((o_st, o_out), (dq_st, dq_out), (dkv_st, dkv_out))[which]
                remote(stage.at[h, 0], out.at[4 * pc + h, up], out_sem.at[which, h, 0],
                       out_rsem.at[which, h, up], partner).wait_recv()
        return 0
    lax.fori_loop(0, HC, drain, 0)
    lse_local.wait()
    lse_far.wait_send()
    remote(lse_st.at[0], lse_out.at[:, oth_heads, :], lse_sem.at[1], lse_rsem, partner).wait_recv()


def attn_call(cu, valid, q, k, v, do):
    any_spec = pl.BlockSpec(memory_space=pl.ANY)
    dma = pltpu.SemaphoreType.DMA
    return pl.pallas_call(
        attn_kernel,
        out_shape=(
            jax.ShapeDtypeStruct((8, 2, GROUP * SLOT, HEAD), BF16),
            jax.ShapeDtypeStruct((8, 2, GROUP * SLOT, HEAD), BF16),
            jax.ShapeDtypeStruct((8, 2, 2, SLOT, HEAD), BF16),
            jax.ShapeDtypeStruct((2, 32, SLOT), F32),
        ),
        in_specs=[pl.BlockSpec(memory_space=pltpu.SMEM)] + [any_spec] * 5,
        out_specs=(any_spec,) * 4,
        scratch_shapes=[
            pltpu.VMEM((256, 16, HEAD), BF16),
            pltpu.VMEM((256, 16, HEAD), BF16),
            pltpu.VMEM((256, 16, HEAD), BF16),
            pltpu.VMEM((256, 16, HEAD), BF16),
            pltpu.VMEM((256, 8, HEAD), BF16),
            pltpu.VMEM((256, 8, HEAD), BF16),
            pltpu.VMEM((8, 2, 2, SLOT, HEAD), BF16),
            pltpu.VMEM((HC, 8, 2, SLOT, HEAD), BF16),
            pltpu.VMEM((HEAD, 8 * SLOT), BF16),
            pltpu.VMEM((HEAD, 8 * SLOT), BF16),
            pltpu.VMEM((HC, 4, GROUP, SLOT, HEAD), BF16),
            pltpu.VMEM((HC, 4, GROUP, SLOT, HEAD), BF16),
            pltpu.VMEM((8 * SLOT, TILE), F32),
            pltpu.VMEM((8 * SLOT, TILE), BF16),
            pltpu.VMEM((8 * SLOT, TILE), BF16),
            pltpu.VMEM((HC, 8, 2, SLOT, HEAD), F32),
            pltpu.VMEM((HC, 4, 2, SLOT, HEAD), F32),
            pltpu.VMEM((HC, 4, TILE, HEAD), BF16),
            pltpu.VMEM((HC, 4, TILE, HEAD), BF16),
            pltpu.VMEM((HC, 4, 2, SLOT, HEAD), BF16),
            pltpu.VMEM((2, 2, 16, SLOT), F32),
            pltpu.VMEM((12, SLOT, SLOT), F32),
            pltpu.VMEM((4, 1, 2 * SLOT), jnp.int32),
            dma((5,)),
            dma((2,)), dma((2,)),
            dma((3,)), dma((4,)),
            dma((3, HC, 2)), dma((HC, 8)),
            dma((HC, 4)), dma((HC, 4)),
            dma((3, HC, 4)), dma((3, HC, 2)),
            dma((2,)), dma,
        ],
        compiler_params=pltpu.CompilerParams(collective_id=0, has_side_effects=True, vmem_limit_bytes=60 * 1024 * 1024),
        name="attn",
    )(cu, valid, q, k, v, do)


def finish_kernel(cu, o_in, dq_in, dkv_in, lse_in, o_out, dq_out, dk_out, dv_out, lse_out):
    l0 = lax.shift_right_logical(cu[1], 3)

    def put(get, out):
        for up in range(2):
            def body(i, _):
                t0 = i * 16
                x = get(up, pl.ds(pl.multiple_of(t0, 16), 16))
                y = jnp.transpose(x, (1, 0, 2))
                for j in range(16):
                    out[src_row(up, t0 + j, l0)] = y[j]
                return 0
            lax.fori_loop(0, SLOT // 16, body, 0)

    put(lambda up, at: o_in[:, up, :, at, :].reshape(8, 16, HEAD), o_out)
    put(lambda up, at: dq_in[:, up, :, at, :].reshape(8, 16, HEAD), dq_out)

    @pl.when(pl.program_id(0) == 0)
    def _():
        put(lambda up, at: dkv_in[:, up, 0, at, :], dk_out)
        put(lambda up, at: dkv_in[:, up, 1, at, :], dv_out)
        row = lax.broadcasted_iota(jnp.int32, (2 * SLOT, SLOT), 0)
        col = lax.broadcasted_iota(jnp.int32, (2 * SLOT, SLOT), 1)
        acc = None
        for up in range(2):
            if up:
                src = jnp.where(col < l0, col + l0, col + SLOT)
            else:
                src = jnp.where(col < l0, col, col + l0)
            pick = jnp.where(row == src, 1.0, 0.0)
            part = lax.dot_general(pick, lse_in[up], NT, precision=lax.Precision.HIGHEST, preferred_element_type=F32)
            acc = part if acc is None else acc + part
        lse_out[...] = acc


def finish_call(cu, o_hm, dq_hm, dkv_hm, lse_hm):
    return pl.pallas_call(
        finish_kernel,
        grid=(4,),
        out_shape=(
            jax.ShapeDtypeStruct((256, 32, HEAD), BF16),
            jax.ShapeDtypeStruct((256, 32, HEAD), BF16),
            jax.ShapeDtypeStruct((256, 8, HEAD), BF16),
            jax.ShapeDtypeStruct((256, 8, HEAD), BF16),
            jax.ShapeDtypeStruct((256, 32), F32),
        ),
        in_specs=[
            pl.BlockSpec(memory_space=pltpu.SMEM),
            pl.BlockSpec((2, 2, GROUP, SLOT, HEAD), lambda i: (i, 0, 0, 0, 0)),
            pl.BlockSpec((2, 2, GROUP, SLOT, HEAD), lambda i: (i, 0, 0, 0, 0)),
            pl.BlockSpec((8, 2, 2, SLOT, HEAD), lambda i: (0, 0, 0, 0, 0)),
            pl.BlockSpec((2, 32, SLOT), lambda i: (0, 0, 0)),
        ],
        out_specs=(
            pl.BlockSpec((256, 8, HEAD), lambda i: (0, i, 0)),
            pl.BlockSpec((256, 8, HEAD), lambda i: (0, i, 0)),
            pl.BlockSpec((256, 8, HEAD), lambda i: (0, 0, 0)),
            pl.BlockSpec((256, 8, HEAD), lambda i: (0, 0, 0)),
            pl.BlockSpec((256, 32), lambda i: (0, 0)),
        ),
        compiler_params=pltpu.CompilerParams(dimension_semantics=("arbitrary",), vmem_limit_bytes=40 * 1024 * 1024),
        name="finish",
    )(cu, o_hm.reshape(8, 2, GROUP, SLOT, HEAD), dq_hm.reshape(8, 2, GROUP, SLOT, HEAD), dkv_hm, lse_hm)


def solution(mesh):
    tok_spec = P(("dp", "cp"), None, None)
    lse_spec = P(("dp", "cp"), None)

    def local(q, k, v, do, valid, cu):
        o_hm, dq_hm, dkv_hm, lse_hm = attn_call(cu, valid.reshape(1, 256), q, k, v, do)
        o, dq, dk, dv, lse = finish_call(cu, o_hm, dq_hm, dkv_hm, lse_hm)
        return o, lse, dq, dk, dv

    return jax.shard_map(local, mesh=mesh, in_specs=(tok_spec,) * 4 + (P(("dp", "cp")), P("dp")),
                         out_specs=(tok_spec, lse_spec, tok_spec, tok_spec, tok_spec), check_vma=False)
```

```python
import functools
import math

import jax
import jax.numpy as jnp
from jax import lax
from jax.experimental import pallas as pl
from jax.experimental.pallas import tpu as pltpu
from jax.sharding import PartitionSpec as P

MESH = pl.DeviceIdType.MESH
FILL = -1.0e30
BIG = 3.0e38
HEAD = 128
SLOT = 128
TILE = 512
GROUP = 4
HC = 4
SCALE = HEAD ** -0.5
C2 = SCALE * math.log2(math.e)
NT = (((1,), (1,)), ((), ()))
NN = (((1,), (0,)), ((), ()))
F32 = jnp.float32
BF16 = jnp.bfloat16

TILES = ((0, 0), (1, 0), (1, 1), (0, 1))


def slot_of(chip, ti):
    oc, up = TILES[ti]
    r = 2 * chip + oc
    return 7 - r if up else r


def mm(a, b, dims):
    return lax.dot_general(a, b, dims, preferred_element_type=F32)


def src_row(up, t, l0):
    if up:
        return jnp.where(t < l0, t + l0, t + SLOT)
    return jnp.where(t < l0, t, t + l0)


def attn_kernel(cu, valid, q, k, v, do, o_out, dq_out, dkv_out, lse_out,
                raw_q, raw_do, far_q, far_do, raw_k, raw_v, kv_hm, kv_all, kt, vt, qh, doh, st, pb, db,
                dkv_acc, dkv_in, o_st, dq_st, dkv_st, lse_st, caps, valid_all,
                in_sem, raw_ssem, raw_rsem, val_ssem, val_rsem, kv_ssem, kv_rsem,
                part_ssem, part_rsem, out_sem, out_rsem, lse_sem, lse_rsem):
    r = lax.axis_index("cp")
    chip = r // 2
    c = r % 2
    pc = 1 - c
    partner = chip * 2 + pc
    cross = (1 - chip) * 2 + c
    cross_o = (1 - chip) * 2 + pc
    l0 = lax.shift_right_logical(cu[1], 3)

    def remote(src, dst, ssem, rsem, dev):
        return pltpu.make_async_remote_copy(src_ref=src, dst_ref=dst, send_sem=ssem, recv_sem=rsem,
                                            device_id={"cp": dev}, device_id_type=MESH)

    own_heads = pl.ds(pl.multiple_of(16 * c, 16), 16)
    oth_heads = pl.ds(pl.multiple_of(16 * pc, 16), 16)
    ld_k = pltpu.make_async_copy(k, raw_k, in_sem.at[0])
    ld_v = pltpu.make_async_copy(v, raw_v, in_sem.at[1])
    ld_q = pltpu.make_async_copy(q.at[:, own_heads, :], raw_q, in_sem.at[2])
    ld_do = pltpu.make_async_copy(do.at[:, own_heads, :], raw_do, in_sem.at[3])
    ld_val = pltpu.make_async_copy(valid, valid_all.at[r], in_sem.at[4])
    for cp in (ld_k, ld_v, ld_q, ld_do, ld_val):
        cp.start()

    barrier = pltpu.get_barrier_semaphore()
    for dev in (partner, cross, cross_o):
        pl.semaphore_signal(barrier, inc=1, device_id={"cp": dev}, device_id_type=MESH)
    pl.semaphore_wait(barrier, 3)

    peers = (partner, cross, cross_o)
    push_q = remote(q.at[:, oth_heads, :], far_q, raw_ssem.at[0], raw_rsem.at[0], partner)
    push_do = remote(do.at[:, oth_heads, :], far_do, raw_ssem.at[1], raw_rsem.at[1], partner)
    push_val = [remote(valid, valid_all.at[r], val_ssem.at[i], val_rsem.at[r], dev) for i, dev in enumerate(peers)]

    def kv_relayout(up):
        def body(i, _):
            t0 = i * 16
            for which, raw in ((0, raw_k), (1, raw_v)):
                rows = jnp.stack([raw[src_row(up, t0 + j, l0)] for j in range(16)])
                kv_hm[:, up, which, pl.ds(pl.multiple_of(t0, 16), 16), :] = jnp.transpose(rows, (1, 0, 2))
            return 0
        lax.fori_loop(0, SLOT // 16, body, 0)

    def kv_push(h, to, both):
        head = (4 * c if to == 1 else 4 * pc) + h
        dev = (partner, cross, cross_o)[to]
        ups = pl.ds(0, 2 if both else 1)
        return remote(kv_hm.at[head, ups], kv_all.at[h, r, ups], kv_ssem.at[to, h], kv_rsem.at[h, r], dev)

    def kv_wait(h, owner, both):
        ups = pl.ds(0, 2 if both else 1)
        remote(kv_hm.at[0, ups], kv_all.at[h, owner, ups], kv_ssem.at[0, h], kv_rsem.at[h, owner], partner).wait_recv()

    ld_k.wait()
    ld_v.wait()
    kv_relayout(0)

    @pl.when(chip == 0)
    def _():
        for h in range(HC):
            kv_push(h, 1, False).start()
            kv_push(h, 2, False).start()

    kv_relayout(1)

    @pl.when(chip == 1)
    def _():
        for h in range(HC):
            kv_push(h, 1, True).start()
            kv_push(h, 2, True).start()

    for h in range(HC):
        kv_push(h, 0, True).start()
    push_q.start()
    push_do.start()
    ld_val.wait()
    for cp in push_val:
        cp.start()

    def copy_own(h, _):
        for up in range(2):
            kv_all[h, r, up] = kv_hm[4 * c + h, up]
        return 0
    lax.fori_loop(0, HC, copy_own, 0)

    def q_relayout(oc, from_q, from_do):
        for up, ti in ((0, oc), (1, 3 - oc)):
            def body(i, _):
                t0 = i * 16
                at = pl.ds(pl.multiple_of(t0, 16), 16)
                for raw, dst in ((from_q, qh), (from_do, doh)):
                    rows = jnp.stack([raw[src_row(up, t0 + j, l0)] for j in range(16)])
                    dst[:, ti, :, at, :] = jnp.transpose(rows, (1, 0, 2)).reshape(HC, GROUP, 16, HEAD)
                return 0
            lax.fori_loop(0, SLOT // 16, body, 0)

    ld_q.wait()
    ld_do.wait()
    q_relayout(c, raw_q, raw_do)

    for i in range(3):
        remote(valid, valid_all.at[peers[i]], val_ssem.at[i], val_rsem.at[peers[i]], peers[i]).wait_recv()
    lane = lax.broadcasted_iota(jnp.int32, (SLOT, SLOT), 1)
    sub = lax.broadcasted_iota(jnp.int32, (SLOT, SLOT), 0)
    lane2 = lax.broadcasted_iota(jnp.int32, (SLOT, 2 * SLOT), 1)
    sub2 = lax.broadcasted_iota(jnp.int32, (SLOT, 2 * SLOT), 0)
    same_doc = (lane < l0) == (sub < l0)
    doc_f = jnp.where(lane < l0, 1.0, 0.0)
    doc_s = jnp.where(sub < l0, 1.0, 0.0)
    same_f = jnp.where(doc_f == doc_s, 1.0, 0.0)
    del same_doc

    def cap_body(s, _):
        owner = jnp.where(s < 4, s, 7 - s)
        off = jnp.where(s < 4, 0, 1)
        src_lo = jnp.where(sub2 < l0, sub2, sub2 + l0)
        src_hi = jnp.where(sub2 < l0, sub2 + l0, sub2 + SLOT)
        src = jnp.where(off == 1, src_hi, src_lo)
        row = jnp.broadcast_to(valid_all[owner].astype(F32), (SLOT, 2 * SLOT))
        ok = jnp.sum(jnp.where(src == lane2, row, 0.0), axis=1, keepdims=True)
        caps[s] = jnp.where(same_f * ok > 0.5, BIG, FILL)
        return 0
    lax.fori_loop(0, 8, cap_body, 0)
    for ti in range(4):
        oc, up = TILES[ti]
        s = (7 - (2 * chip + oc)) if up else 2 * chip + oc
        caps[8 + ti] = jnp.where(sub <= lane, caps[s], FILL)

    push_q.wait_recv()
    push_do.wait_recv()
    q_relayout(pc, far_q, far_do)

    def part_copy(h, i, n):
        return remote(dkv_acc.at[h, pl.ds(i, n)], dkv_in.at[h, pl.ds(0, n)], part_ssem.at[h], part_rsem.at[h], cross)

    def out_copies(h, ti, which):
        stage, out = ((o_st, o_out), (dq_st, dq_out), (dkv_st, dkv_out))[which]
        oc, up = TILES[ti]
        dst = out.at[4 * c + h, up]
        src = stage.at[h, ti]
        return (pltpu.make_async_copy(src, dst, out_sem.at[which, h, ti]),
                remote(src, dst, out_sem.at[which, h, ti], out_rsem.at[which, h, up], partner))

    def out_start(h, ti, which):
        local, far = out_copies(h, ti, which)
        oc = TILES[ti][0]

        @pl.when(c == oc)
        def _():
            local.start()

        @pl.when(c != oc)
        def _():
            far.start()

    lse_local = pltpu.make_async_copy(lse_st.at[c], lse_out.at[:, own_heads, :], lse_sem.at[0])
    lse_far = remote(lse_st.at[pc], lse_out.at[:, own_heads, :], lse_sem.at[1], lse_rsem, partner)

    def kv_slot(h, s, which):
        return kv_all[h, min(s, 7 - s), int(s > 3), which]

    def kv_slots(h, a, b, which):
        return jnp.concatenate([kv_slot(h, s, which) for s in range(a, b)], axis=0)

    def run_chip(ch):
        slots = [slot_of(ch, ti) for ti in range(4)]
        sent = [0, 1] if ch == 1 else [2, 3, 4, 5]
        kept = [0, 1] if ch == 0 else [2, 3, 4, 5]
        order = [0, 1, 2, 3]

        def transposes(s):
            for src, dst in ((0, kt), (1, vt)):
                dst[:, s * SLOT:(s + 1) * SLOT] = jnp.transpose(kv_slot(h_ref[0], s, src))

        h_ref = [None]

        def head(h, _):
            h_ref[0] = h
            seen = set()
            ready = set()

            def wait_slot(s):
                if s in ready:
                    return
                if s in slots:
                    kv_wait(h, partner, True)
                    new = slots
                elif ch == 1:
                    for owner in (0, 1):
                        kv_wait(h, owner, False)
                    new = [0, 1]
                else:
                    for owner in (2, 3):
                        kv_wait(h, owner, True)
                    new = [2, 3, 4, 5]
                for u in new:
                    ready.add(u)
                    transposes(u)

            for ti in order:
                s = slots[ti]
                nk = s + 1
                for u in range(nk):
                    wait_slot(u)
                qt = qh[h, ti].reshape(TILE, HEAD)
                dt = doh[h, ti].reshape(TILE, HEAD)
                m8 = [None] * GROUP
                for a in range(0, nk, 2):
                    n = min(2, nk - a)
                    kb = kv_slots(h, a, a + n, 0)
                    sc = mm(kb, qt, NT)
                    for j in range(n):
                        cap = caps[8 + ti] if a + j == s else caps[a + j]
                        for g in range(GROUP):
                            x = jnp.minimum(sc[j * SLOT:(j + 1) * SLOT, g * SLOT:(g + 1) * SLOT], cap)
                            st[(a + j) * SLOT:(a + j + 1) * SLOT, g * SLOT:(g + 1) * SLOT] = x
                            top = jnp.max(x.reshape(SLOT // 8, 8, SLOT), axis=0)
                            m8[g] = top if m8[g] is None else jnp.maximum(m8[g], top)
                m = [jnp.max(x, axis=0, keepdims=True) for x in m8]
                mc = [x * C2 for x in m]
                l8 = [None] * GROUP
                for a in range(nk):
                    for g in range(GROUP):
                        at = (slice(a * SLOT, (a + 1) * SLOT), slice(g * SLOT, (g + 1) * SLOT))
                        e = jnp.exp2(st[at] * C2 - mc[g])
                        st[at] = e
                        pb[at] = e.astype(BF16)
                        tot = jnp.sum(e.reshape(SLOT // 8, 8, SLOT), axis=0)
                        l8[g] = tot if l8[g] is None else l8[g] + tot
                ot = mm(vt[:, :nk * SLOT], pb[:nk * SLOT, :], NN)
                inv, dd = [], []
                oc, up = TILES[ti]
                for g in range(GROUP):
                    l = jnp.sum(l8[g], axis=0, keepdims=True)
                    has = m[g] > 0.5 * FILL
                    safe = jnp.where(has, l, 1.0)
                    i_l = jnp.where(has, 1.0 / safe, 0.0)
                    lse = jnp.where(has, m[g] * SCALE + jnp.log(safe), 0.0)
                    lse_st[oc, up, pl.ds(h * GROUP + g, 1), :] = lse
                    og = (ot[:, g * SLOT:(g + 1) * SLOT] * i_l).astype(BF16)
                    dog = jnp.transpose(dt[g * SLOT:(g + 1) * SLOT, :])
                    dd.append(jnp.sum(og.astype(F32) * dog.astype(F32), axis=0, keepdims=True))
                    inv.append(i_l)
                    o_st[h, ti, g * SLOT:(g + 1) * SLOT, :] = jnp.transpose(og)
                out_start(h, ti, 0)

                first = [u for u in range(nk) if u in sent] if (ch == 0 and ti >= 2) else []
                rest = [u for u in range(nk) if u not in first]
                dqt = None
                for part in (first, rest):
                    runs = []
                    for u in part:
                        if runs and runs[-1][1] == u and u - runs[-1][0] < 2:
                            runs[-1][1] = u + 1
                        else:
                            runs.append([u, u + 1])
                    for a, b in runs:
                        n = b - a
                        vb = kv_slots(h, a, b, 1)
                        dp = mm(vb, dt, NT)
                        for j in range(n):
                            for g in range(GROUP):
                                at = (slice((a + j) * SLOT, (a + j + 1) * SLOT), slice(g * SLOT, (g + 1) * SLOT))
                                p = st[at] * inv[g]
                                pb[at] = p.astype(BF16)
                                ds = p * (dp[j * SLOT:(j + 1) * SLOT, g * SLOT:(g + 1) * SLOT] - dd[g])
                                db[at] = ds.astype(BF16)
                        dsb = db[a * SLOT:b * SLOT, :]
                        dv = mm(pb[a * SLOT:b * SLOT, :], dt, NN)
                        dk = mm(dsb, qt, NN) * SCALE
                        dq = mm(kt[:, a * SLOT:b * SLOT], dsb, NN)
                        dqt = dq if dqt is None else dqt + dq
                        for j in range(n):
                            u = a + j
                            new = (dk[j * SLOT:(j + 1) * SLOT], dv[j * SLOT:(j + 1) * SLOT])
                            for w in range(2):
                                dkv_acc[h, u, w] = dkv_acc[h, u, w] + new[w] if u in seen else new[w]
                            seen.add(u)
                    if part is first and ti == 3 and ch == 0:
                        part_copy(h, sent[0], len(sent)).start()
                for g in range(GROUP):
                    dqg = (dqt[:, g * SLOT:(g + 1) * SLOT] * SCALE).astype(BF16)
                    dq_st[h, ti, g * SLOT:(g + 1) * SLOT, :] = jnp.transpose(dqg)
                out_start(h, ti, 1)
            if ch == 1:
                part_copy(h, sent[0], len(sent)).start()
            else:
                for ti in (2, 3):
                    for w in range(2):
                        dkv_st[h, ti, w] = dkv_acc[h, slots[ti], w].astype(BF16)
                    out_start(h, ti, 2)
            return 0

        lax.fori_loop(0, HC, head, 0)

        lse_local.start()
        lse_far.start()

        def tail(h, _):
            part_copy(h, kept[0], len(kept)).wait_recv()
            for i, u in enumerate(kept):
                ti = slots.index(u)
                for w in range(2):
                    dkv_st[h, ti, w] = (dkv_acc[h, u, w] + dkv_in[h, i, w]).astype(BF16)
                out_start(h, ti, 2)
            return 0
        lax.fori_loop(0, HC, tail, 0)

        def drain(h, _):
            part_copy(h, sent[0], len(sent)).wait_send()
            return 0
        lax.fori_loop(0, HC, drain, 0)

    pl.when(chip == 0)(functools.partial(run_chip, 0))
    pl.when(chip == 1)(functools.partial(run_chip, 1))

    push_q.wait_send()
    push_do.wait_send()
    for cp in push_val:
        cp.wait_send()

    def drain(h, _):
        kv_push(h, 0, True).wait_send()
        for ch in range(2):
            @pl.when(chip == ch)
            def _():
                for to in (1, 2):
                    kv_push(h, to, ch == 1).wait_send()
        for which in range(3):
            for ti in range(4):
                local, far = out_copies(h, ti, which)
                oc = TILES[ti][0]

                @pl.when(c == oc)
                def _():
                    local.wait()

                @pl.when(c != oc)
                def _():
                    far.wait_send()
            for up in range(2):
                stage, out = ((o_st, o_out), (dq_st, dq_out), (dkv_st, dkv_out))[which]
                remote(stage.at[h, 0], out.at[4 * pc + h, up], out_sem.at[which, h, 0],
                       out_rsem.at[which, h, up], partner).wait_recv()
        return 0
    lax.fori_loop(0, HC, drain, 0)
    lse_local.wait()
    lse_far.wait_send()
    remote(lse_st.at[0], lse_out.at[:, oth_heads, :], lse_sem.at[1], lse_rsem, partner).wait_recv()


def attn_call(cu, valid, q, k, v, do):
    any_spec = pl.BlockSpec(memory_space=pl.ANY)
    dma = pltpu.SemaphoreType.DMA
    return pl.pallas_call(
        attn_kernel,
        out_shape=(
            jax.ShapeDtypeStruct((8, 2, GROUP * SLOT, HEAD), BF16),
            jax.ShapeDtypeStruct((8, 2, GROUP * SLOT, HEAD), BF16),
            jax.ShapeDtypeStruct((8, 2, 2, SLOT, HEAD), BF16),
            jax.ShapeDtypeStruct((2, 32, SLOT), F32),
        ),
        in_specs=[pl.BlockSpec(memory_space=pltpu.SMEM)] + [any_spec] * 5,
        out_specs=(any_spec,) * 4,
        scratch_shapes=[
            pltpu.VMEM((256, 16, HEAD), BF16),
            pltpu.VMEM((256, 16, HEAD), BF16),
            pltpu.VMEM((256, 16, HEAD), BF16),
            pltpu.VMEM((256, 16, HEAD), BF16),
            pltpu.VMEM((256, 8, HEAD), BF16),
            pltpu.VMEM((256, 8, HEAD), BF16),
            pltpu.VMEM((8, 2, 2, SLOT, HEAD), BF16),
            pltpu.VMEM((HC, 4, 2, 2, SLOT, HEAD), BF16),
            pltpu.VMEM((HEAD, 8 * SLOT), BF16),
            pltpu.VMEM((HEAD, 8 * SLOT), BF16),
            pltpu.VMEM((HC, 4, GROUP, SLOT, HEAD), BF16),
            pltpu.VMEM((HC, 4, GROUP, SLOT, HEAD), BF16),
            pltpu.VMEM((8 * SLOT, TILE), F32),
            pltpu.VMEM((8 * SLOT, TILE), BF16),
            pltpu.VMEM((8 * SLOT, TILE), BF16),
            pltpu.VMEM((HC, 8, 2, SLOT, HEAD), F32),
            pltpu.VMEM((HC, 4, 2, SLOT, HEAD), F32),
            pltpu.VMEM((HC, 4, TILE, HEAD), BF16),
            pltpu.VMEM((HC, 4, TILE, HEAD), BF16),
            pltpu.VMEM((HC, 4, 2, SLOT, HEAD), BF16),
            pltpu.VMEM((2, 2, 16, SLOT), F32),
            pltpu.VMEM((12, SLOT, SLOT), F32),
            pltpu.VMEM((4, 1, 2 * SLOT), jnp.int32),
            dma((5,)),
            dma((2,)), dma((2,)),
            dma((3,)), dma((4,)),
            dma((3, HC)), dma((HC, 4)),
            dma((HC,)), dma((HC,)),
            dma((3, HC, 4)), dma((3, HC, 2)),
            dma((2,)), dma,
        ],
        compiler_params=pltpu.CompilerParams(collective_id=0, has_side_effects=True, vmem_limit_bytes=60 * 1024 * 1024),
        name="attn",
    )(cu, valid, q, k, v, do)


def finish_kernel(cu, o_in, dq_in, dkv_in, lse_in, o_out, dq_out, dk_out, dv_out, lse_out):
    l0 = lax.shift_right_logical(cu[1], 3)

    def put(get, out):
        for up in range(2):
            def body(i, _):
                t0 = i * 16
                x = get(up, pl.ds(pl.multiple_of(t0, 16), 16))
                y = jnp.transpose(x, (1, 0, 2))
                for j in range(16):
                    out[src_row(up, t0 + j, l0)] = y[j]
                return 0
            lax.fori_loop(0, SLOT // 16, body, 0)

    put(lambda up, at: o_in[:, up, :, at, :].reshape(8, 16, HEAD), o_out)
    put(lambda up, at: dq_in[:, up, :, at, :].reshape(8, 16, HEAD), dq_out)

    @pl.when(pl.program_id(0) == 0)
    def _():
        put(lambda up, at: dkv_in[:, up, 0, at, :], dk_out)
        put(lambda up, at: dkv_in[:, up, 1, at, :], dv_out)
        row = lax.broadcasted_iota(jnp.int32, (2 * SLOT, SLOT), 0)
        col = lax.broadcasted_iota(jnp.int32, (2 * SLOT, SLOT), 1)
        acc = None
        for up in range(2):
            if up:
                src = jnp.where(col < l0, col + l0, col + SLOT)
            else:
                src = jnp.where(col < l0, col, col + l0)
            pick = jnp.where(row == src, 1.0, 0.0)
            part = lax.dot_general(pick, lse_in[up], NT, precision=lax.Precision.HIGHEST, preferred_element_type=F32)
            acc = part if acc is None else acc + part
        lse_out[...] = acc


def finish_call(cu, o_hm, dq_hm, dkv_hm, lse_hm):
    return pl.pallas_call(
        finish_kernel,
        grid=(4,),
        out_shape=(
            jax.ShapeDtypeStruct((256, 32, HEAD), BF16),
            jax.ShapeDtypeStruct((256, 32, HEAD), BF16),
            jax.ShapeDtypeStruct((256, 8, HEAD), BF16),
            jax.ShapeDtypeStruct((256, 8, HEAD), BF16),
            jax.ShapeDtypeStruct((256, 32), F32),
        ),
        in_specs=[
            pl.BlockSpec(memory_space=pltpu.SMEM),
            pl.BlockSpec((2, 2, GROUP, SLOT, HEAD), lambda i: (i, 0, 0, 0, 0)),
            pl.BlockSpec((2, 2, GROUP, SLOT, HEAD), lambda i: (i, 0, 0, 0, 0)),
            pl.BlockSpec((8, 2, 2, SLOT, HEAD), lambda i: (0, 0, 0, 0, 0)),
            pl.BlockSpec((2, 32, SLOT), lambda i: (0, 0, 0)),
        ],
        out_specs=(
            pl.BlockSpec((256, 8, HEAD), lambda i: (0, i, 0)),
            pl.BlockSpec((256, 8, HEAD), lambda i: (0, i, 0)),
            pl.BlockSpec((256, 8, HEAD), lambda i: (0, 0, 0)),
            pl.BlockSpec((256, 8, HEAD), lambda i: (0, 0, 0)),
            pl.BlockSpec((256, 32), lambda i: (0, 0)),
        ),
        compiler_params=pltpu.CompilerParams(dimension_semantics=("arbitrary",), vmem_limit_bytes=40 * 1024 * 1024),
        name="finish",
    )(cu, o_hm.reshape(8, 2, GROUP, SLOT, HEAD), dq_hm.reshape(8, 2, GROUP, SLOT, HEAD), dkv_hm, lse_hm)


def solution(mesh):
    tok_spec = P(("dp", "cp"), None, None)
    lse_spec = P(("dp", "cp"), None)

    def local(q, k, v, do, valid, cu):
        o_hm, dq_hm, dkv_hm, lse_hm = attn_call(cu, valid.reshape(1, 256), q, k, v, do)
        o, dq, dk, dv, lse = finish_call(cu, o_hm, dq_hm, dkv_hm, lse_hm)
        return o, lse, dq, dk, dv

    return jax.shard_map(local, mesh=mesh, in_specs=(tok_spec,) * 4 + (P(("dp", "cp")), P("dp")),
                         out_specs=(tok_spec, lse_spec, tok_spec, tok_spec, tok_spec), check_vma=False)
```

```python
import functools
import math

import jax
import jax.numpy as jnp
from jax import lax
from jax.experimental import pallas as pl
from jax.experimental.pallas import tpu as pltpu
from jax.sharding import PartitionSpec as P

MESH = pl.DeviceIdType.MESH
FILL = -1.0e30
BIG = 3.0e38
HEAD = 128
SLOT = 128
TILE = 512
GROUP = 4
HC = 4
SCALE = HEAD ** -0.5
C2 = SCALE * math.log2(math.e)
NT = (((1,), (1,)), ((), ()))
NN = (((1,), (0,)), ((), ()))
F32 = jnp.float32
BF16 = jnp.bfloat16

TILES = ((0, 0), (1, 0), (1, 1), (0, 1))


def slot_of(chip, ti):
    oc, up = TILES[ti]
    r = 2 * chip + oc
    return 7 - r if up else r


def mm(a, b, dims):
    return lax.dot_general(a, b, dims, preferred_element_type=F32)


def src_row(up, t, l0):
    if up:
        return jnp.where(t < l0, t + l0, t + SLOT)
    return jnp.where(t < l0, t, t + l0)


def attn_kernel(cu, valid, q, k, v, do, o_out, dq_out, dkv_out, lse_out,
                raw_q, raw_do, far_q, far_do, raw_k, raw_v, kv_hm, kv_all, kt, vt, qh, doh, st, pb, db,
                dkv_acc, dkv_in, o_st, dq_st, dkv_st, lse_st, caps, valid_all,
                in_sem, raw_ssem, raw_rsem, val_ssem, val_rsem, kv_ssem, kv_rsem,
                part_ssem, part_rsem, out_sem, out_rsem, lse_sem, lse_rsem):
    r = lax.axis_index("cp")
    chip = r // 2
    c = r % 2
    pc = 1 - c
    partner = chip * 2 + pc
    cross = (1 - chip) * 2 + c
    cross_o = (1 - chip) * 2 + pc
    l0 = lax.shift_right_logical(cu[1], 3)

    def remote(src, dst, ssem, rsem, dev):
        return pltpu.make_async_remote_copy(src_ref=src, dst_ref=dst, send_sem=ssem, recv_sem=rsem,
                                            device_id={"cp": dev}, device_id_type=MESH)

    own_heads = pl.ds(pl.multiple_of(16 * c, 16), 16)
    oth_heads = pl.ds(pl.multiple_of(16 * pc, 16), 16)
    ld_k = pltpu.make_async_copy(k, raw_k, in_sem.at[0])
    ld_v = pltpu.make_async_copy(v, raw_v, in_sem.at[1])
    ld_q = pltpu.make_async_copy(q.at[:, own_heads, :], raw_q, in_sem.at[2])
    ld_do = pltpu.make_async_copy(do.at[:, own_heads, :], raw_do, in_sem.at[3])
    ld_val = pltpu.make_async_copy(valid, valid_all.at[r], in_sem.at[4])
    for cp in (ld_k, ld_v, ld_q, ld_do, ld_val):
        cp.start()

    barrier = pltpu.get_barrier_semaphore()
    for dev in (partner, cross, cross_o):
        pl.semaphore_signal(barrier, inc=1, device_id={"cp": dev}, device_id_type=MESH)
    pl.semaphore_wait(barrier, 3)

    peers = (partner, cross, cross_o)
    push_q = remote(q.at[:, oth_heads, :], far_q, raw_ssem.at[0], raw_rsem.at[0], partner)
    push_do = remote(do.at[:, oth_heads, :], far_do, raw_ssem.at[1], raw_rsem.at[1], partner)
    push_val = [remote(valid, valid_all.at[r], val_ssem.at[i], val_rsem.at[r], dev) for i, dev in enumerate(peers)]

    push_q.start()
    push_do.start()

    def kv_relayout(up):
        def body(i, _):
            t0 = i * 16
            for which, raw in ((0, raw_k), (1, raw_v)):
                rows = jnp.stack([raw[src_row(up, t0 + j, l0)] for j in range(16)])
                kv_hm[:, up, which, pl.ds(pl.multiple_of(t0, 16), 16), :] = jnp.transpose(rows, (1, 0, 2))
            return 0
        lax.fori_loop(0, SLOT // 16, body, 0)

    def kv_push(h, to, both):
        head = (4 * c if to == 1 else 4 * pc) + h
        dev = (partner, cross, cross_o)[to]
        ups = pl.ds(0, 2 if both else 1)
        return remote(kv_hm.at[head, ups], kv_all.at[h, r, ups], kv_ssem.at[to, h], kv_rsem.at[h, r], dev)

    def kv_wait(h, owner, both):
        ups = pl.ds(0, 2 if both else 1)
        remote(kv_hm.at[0, ups], kv_all.at[h, owner, ups], kv_ssem.at[0, h], kv_rsem.at[h, owner], partner).wait_recv()

    ld_k.wait()
    ld_v.wait()
    kv_relayout(0)

    @pl.when(chip == 0)
    def _():
        for h in range(HC):
            kv_push(h, 1, False).start()
            kv_push(h, 2, False).start()

    kv_relayout(1)

    @pl.when(chip == 1)
    def _():
        for h in range(HC):
            kv_push(h, 1, True).start()
            kv_push(h, 2, True).start()

    for h in range(HC):
        kv_push(h, 0, True).start()
    ld_val.wait()
    for cp in push_val:
        cp.start()

    def copy_own(h, _):
        for up in range(2):
            kv_all[h, r, up] = kv_hm[4 * c + h, up]
        return 0
    lax.fori_loop(0, HC, copy_own, 0)

    def q_relayout(oc, from_q, from_do):
        for up, ti in ((0, oc), (1, 3 - oc)):
            def body(i, _):
                t0 = i * 16
                at = pl.ds(pl.multiple_of(t0, 16), 16)
                for raw, dst in ((from_q, qh), (from_do, doh)):
                    rows = jnp.stack([raw[src_row(up, t0 + j, l0)] for j in range(16)])
                    dst[:, ti, :, at, :] = jnp.transpose(rows, (1, 0, 2)).reshape(HC, GROUP, 16, HEAD)
                return 0
            lax.fori_loop(0, SLOT // 16, body, 0)

    ld_q.wait()
    ld_do.wait()
    q_relayout(c, raw_q, raw_do)

    for i in range(3):
        remote(valid, valid_all.at[peers[i]], val_ssem.at[i], val_rsem.at[peers[i]], peers[i]).wait_recv()
    lane = lax.broadcasted_iota(jnp.int32, (SLOT, SLOT), 1)
    sub = lax.broadcasted_iota(jnp.int32, (SLOT, SLOT), 0)
    lane2 = lax.broadcasted_iota(jnp.int32, (SLOT, 2 * SLOT), 1)
    sub2 = lax.broadcasted_iota(jnp.int32, (SLOT, 2 * SLOT), 0)
    same_doc = (lane < l0) == (sub < l0)
    doc_f = jnp.where(lane < l0, 1.0, 0.0)
    doc_s = jnp.where(sub < l0, 1.0, 0.0)
    same_f = jnp.where(doc_f == doc_s, 1.0, 0.0)
    del same_doc

    def cap_body(s, _):
        owner = jnp.where(s < 4, s, 7 - s)
        off = jnp.where(s < 4, 0, 1)
        src_lo = jnp.where(sub2 < l0, sub2, sub2 + l0)
        src_hi = jnp.where(sub2 < l0, sub2 + l0, sub2 + SLOT)
        src = jnp.where(off == 1, src_hi, src_lo)
        row = jnp.broadcast_to(valid_all[owner].astype(F32), (SLOT, 2 * SLOT))
        ok = jnp.sum(jnp.where(src == lane2, row, 0.0), axis=1, keepdims=True)
        caps[s] = jnp.where(same_f * ok > 0.5, BIG, FILL)
        return 0
    lax.fori_loop(0, 8, cap_body, 0)
    for ti in range(4):
        oc, up = TILES[ti]
        s = (7 - (2 * chip + oc)) if up else 2 * chip + oc
        caps[8 + ti] = jnp.where(sub <= lane, caps[s], FILL)

    push_q.wait_recv()
    push_do.wait_recv()
    q_relayout(pc, far_q, far_do)

    def part_copy(h, i, n):
        return remote(dkv_acc.at[h, pl.ds(i, n)], dkv_in.at[h, pl.ds(0, n)], part_ssem.at[h], part_rsem.at[h], cross)

    def out_copies(h, ti, which):
        stage, out = ((o_st, o_out), (dq_st, dq_out), (dkv_st, dkv_out))[which]
        oc, up = TILES[ti]
        dst = out.at[4 * c + h, up]
        src = stage.at[h, ti]
        return (pltpu.make_async_copy(src, dst, out_sem.at[which, h, ti]),
                remote(src, dst, out_sem.at[which, h, ti], out_rsem.at[which, h, up], partner))

    def out_start(h, ti, which):
        local, far = out_copies(h, ti, which)
        oc = TILES[ti][0]

        @pl.when(c == oc)
        def _():
            local.start()

        @pl.when(c != oc)
        def _():
            far.start()

    lse_local = pltpu.make_async_copy(lse_st.at[c], lse_out.at[:, own_heads, :], lse_sem.at[0])
    lse_far = remote(lse_st.at[pc], lse_out.at[:, own_heads, :], lse_sem.at[1], lse_rsem, partner)

    def kv_slot(h, s, which):
        return kv_all[h, min(s, 7 - s), int(s > 3), which]

    def kv_slots(h, a, b, which):
        return jnp.concatenate([kv_slot(h, s, which) for s in range(a, b)], axis=0)

    def run_chip(ch):
        slots = [slot_of(ch, ti) for ti in range(4)]
        sent = [0, 1] if ch == 1 else [2, 3, 4, 5]
        kept = [0, 1] if ch == 0 else [2, 3, 4, 5]
        order = [0, 1, 2, 3]

        def transposes(s):
            for src, dst in ((0, kt), (1, vt)):
                dst[:, s * SLOT:(s + 1) * SLOT] = jnp.transpose(kv_slot(h_ref[0], s, src))

        h_ref = [None]

        def head(h, _):
            h_ref[0] = h
            seen = set()
            ready = set()

            def wait_slot(s):
                if s in ready:
                    return
                if s in slots:
                    kv_wait(h, partner, True)
                    new = slots
                elif ch == 1:
                    for owner in (0, 1):
                        kv_wait(h, owner, False)
                    new = [0, 1]
                else:
                    for owner in (2, 3):
                        kv_wait(h, owner, True)
                    new = [2, 3, 4, 5]
                for u in new:
                    ready.add(u)
                    transposes(u)

            for ti in order:
                s = slots[ti]
                nk = s + 1
                for u in range(nk):
                    wait_slot(u)
                qt = qh[h, ti].reshape(TILE, HEAD)
                dt = doh[h, ti].reshape(TILE, HEAD)
                m8 = [None] * GROUP
                for a in range(0, nk, 2):
                    n = min(2, nk - a)
                    kb = kv_slots(h, a, a + n, 0)
                    sc = mm(kb, qt, NT)
                    for j in range(n):
                        cap = caps[8 + ti] if a + j == s else caps[a + j]
                        for g in range(GROUP):
                            x = jnp.minimum(sc[j * SLOT:(j + 1) * SLOT, g * SLOT:(g + 1) * SLOT], cap)
                            st[(a + j) * SLOT:(a + j + 1) * SLOT, g * SLOT:(g + 1) * SLOT] = x
                            top = jnp.max(x.reshape(SLOT // 8, 8, SLOT), axis=0)
                            m8[g] = top if m8[g] is None else jnp.maximum(m8[g], top)
                m = [jnp.max(x, axis=0, keepdims=True) for x in m8]
                mc = [x * C2 for x in m]
                l8 = [None] * GROUP
                for a in range(nk):
                    for g in range(GROUP):
                        at = (slice(a * SLOT, (a + 1) * SLOT), slice(g * SLOT, (g + 1) * SLOT))
                        e = jnp.exp2(st[at] * C2 - mc[g])
                        st[at] = e
                        pb[at] = e.astype(BF16)
                        tot = jnp.sum(e.reshape(SLOT // 8, 8, SLOT), axis=0)
                        l8[g] = tot if l8[g] is None else l8[g] + tot
                ot = mm(vt[:, :nk * SLOT], pb[:nk * SLOT, :], NN)
                inv, dd = [], []
                oc, up = TILES[ti]
                for g in range(GROUP):
                    l = jnp.sum(l8[g], axis=0, keepdims=True)
                    has = m[g] > 0.5 * FILL
                    safe = jnp.where(has, l, 1.0)
                    i_l = jnp.where(has, 1.0 / safe, 0.0)
                    lse = jnp.where(has, m[g] * SCALE + jnp.log(safe), 0.0)
                    lse_st[oc, up, pl.ds(h * GROUP + g, 1), :] = lse
                    og = (ot[:, g * SLOT:(g + 1) * SLOT] * i_l).astype(BF16)
                    dog = jnp.transpose(dt[g * SLOT:(g + 1) * SLOT, :])
                    dd.append(jnp.sum(og.astype(F32) * dog.astype(F32), axis=0, keepdims=True))
                    inv.append(i_l)
                    o_st[h, ti, g * SLOT:(g + 1) * SLOT, :] = jnp.transpose(og)
                out_start(h, ti, 0)

                first = [u for u in range(nk) if u in sent] if (ch == 0 and ti >= 2) else []
                rest = [u for u in range(nk) if u not in first]
                dqt = None
                for part in (first, rest):
                    runs = []
                    for u in part:
                        if runs and runs[-1][1] == u and u - runs[-1][0] < 2:
                            runs[-1][1] = u + 1
                        else:
                            runs.append([u, u + 1])
                    for a, b in runs:
                        n = b - a
                        vb = kv_slots(h, a, b, 1)
                        dp = mm(vb, dt, NT)
                        for j in range(n):
                            for g in range(GROUP):
                                at = (slice((a + j) * SLOT, (a + j + 1) * SLOT), slice(g * SLOT, (g + 1) * SLOT))
                                p = st[at] * inv[g]
                                pb[at] = p.astype(BF16)
                                ds = p * (dp[j * SLOT:(j + 1) * SLOT, g * SLOT:(g + 1) * SLOT] - dd[g])
                                db[at] = ds.astype(BF16)
                        dsb = db[a * SLOT:b * SLOT, :]
                        dv = mm(pb[a * SLOT:b * SLOT, :], dt, NN)
                        dk = mm(dsb, qt, NN) * SCALE
                        dq = mm(kt[:, a * SLOT:b * SLOT], dsb, NN)
                        dqt = dq if dqt is None else dqt + dq
                        for j in range(n):
                            u = a + j
                            new = (dk[j * SLOT:(j + 1) * SLOT], dv[j * SLOT:(j + 1) * SLOT])
                            for w in range(2):
                                dkv_acc[h, u, w] = dkv_acc[h, u, w] + new[w] if u in seen else new[w]
                            seen.add(u)
                    if part is first and ti == 3 and ch == 0:
                        part_copy(h, sent[0], len(sent)).start()
                for g in range(GROUP):
                    dqg = (dqt[:, g * SLOT:(g + 1) * SLOT] * SCALE).astype(BF16)
                    dq_st[h, ti, g * SLOT:(g + 1) * SLOT, :] = jnp.transpose(dqg)
                out_start(h, ti, 1)
            if ch == 1:
                part_copy(h, sent[0], len(sent)).start()
            else:
                for ti in (2, 3):
                    for w in range(2):
                        dkv_st[h, ti, w] = dkv_acc[h, slots[ti], w].astype(BF16)
                    out_start(h, ti, 2)
            return 0

        lax.fori_loop(0, HC, head, 0)

        lse_local.start()
        lse_far.start()

        def tail(h, _):
            part_copy(h, kept[0], len(kept)).wait_recv()
            for i, u in enumerate(kept):
                ti = slots.index(u)
                for w in range(2):
                    dkv_st[h, ti, w] = (dkv_acc[h, u, w] + dkv_in[h, i, w]).astype(BF16)
                out_start(h, ti, 2)
            return 0
        lax.fori_loop(0, HC, tail, 0)

        def drain(h, _):
            part_copy(h, sent[0], len(sent)).wait_send()
            return 0
        lax.fori_loop(0, HC, drain, 0)

    pl.when(chip == 0)(functools.partial(run_chip, 0))
    pl.when(chip == 1)(functools.partial(run_chip, 1))

    push_q.wait_send()
    push_do.wait_send()
    for cp in push_val:
        cp.wait_send()

    def drain(h, _):
        kv_push(h, 0, True).wait_send()
        for ch in range(2):
            @pl.when(chip == ch)
            def _():
                for to in (1, 2):
                    kv_push(h, to, ch == 1).wait_send()
        for which in range(3):
            for ti in range(4):
                local, far = out_copies(h, ti, which)
                oc = TILES[ti][0]

                @pl.when(c == oc)
                def _():
                    local.wait()

                @pl.when(c != oc)
                def _():
                    far.wait_send()
            for up in range(2):
                stage, out = ((o_st, o_out), (dq_st, dq_out), (dkv_st, dkv_out))[which]
                remote(stage.at[h, 0], out.at[4 * pc + h, up], out_sem.at[which, h, 0],
                       out_rsem.at[which, h, up], partner).wait_recv()
        return 0
    lax.fori_loop(0, HC, drain, 0)
    lse_local.wait()
    lse_far.wait_send()
    remote(lse_st.at[0], lse_out.at[:, oth_heads, :], lse_sem.at[1], lse_rsem, partner).wait_recv()


def attn_call(cu, valid, q, k, v, do):
    any_spec = pl.BlockSpec(memory_space=pl.ANY)
    dma = pltpu.SemaphoreType.DMA
    return pl.pallas_call(
        attn_kernel,
        out_shape=(
            jax.ShapeDtypeStruct((8, 2, GROUP * SLOT, HEAD), BF16),
            jax.ShapeDtypeStruct((8, 2, GROUP * SLOT, HEAD), BF16),
            jax.ShapeDtypeStruct((8, 2, 2, SLOT, HEAD), BF16),
            jax.ShapeDtypeStruct((2, 32, SLOT), F32),
        ),
        in_specs=[pl.BlockSpec(memory_space=pltpu.SMEM)] + [any_spec] * 5,
        out_specs=(any_spec,) * 4,
        scratch_shapes=[
            pltpu.VMEM((256, 16, HEAD), BF16),
            pltpu.VMEM((256, 16, HEAD), BF16),
            pltpu.VMEM((256, 16, HEAD), BF16),
            pltpu.VMEM((256, 16, HEAD), BF16),
            pltpu.VMEM((256, 8, HEAD), BF16),
            pltpu.VMEM((256, 8, HEAD), BF16),
            pltpu.VMEM((8, 2, 2, SLOT, HEAD), BF16),
            pltpu.VMEM((HC, 4, 2, 2, SLOT, HEAD), BF16),
            pltpu.VMEM((HEAD, 8 * SLOT), BF16),
            pltpu.VMEM((HEAD, 8 * SLOT), BF16),
            pltpu.VMEM((HC, 4, GROUP, SLOT, HEAD), BF16),
            pltpu.VMEM((HC, 4, GROUP, SLOT, HEAD), BF16),
            pltpu.VMEM((8 * SLOT, TILE), F32),
            pltpu.VMEM((8 * SLOT, TILE), BF16),
            pltpu.VMEM((8 * SLOT, TILE), BF16),
            pltpu.VMEM((HC, 8, 2, SLOT, HEAD), F32),
            pltpu.VMEM((HC, 4, 2, SLOT, HEAD), F32),
            pltpu.VMEM((HC, 4, TILE, HEAD), BF16),
            pltpu.VMEM((HC, 4, TILE, HEAD), BF16),
            pltpu.VMEM((HC, 4, 2, SLOT, HEAD), BF16),
            pltpu.VMEM((2, 2, 16, SLOT), F32),
            pltpu.VMEM((12, SLOT, SLOT), F32),
            pltpu.VMEM((4, 1, 2 * SLOT), jnp.int32),
            dma((5,)),
            dma((2,)), dma((2,)),
            dma((3,)), dma((4,)),
            dma((3, HC)), dma((HC, 4)),
            dma((HC,)), dma((HC,)),
            dma((3, HC, 4)), dma((3, HC, 2)),
            dma((2,)), dma,
        ],
        compiler_params=pltpu.CompilerParams(collective_id=0, has_side_effects=True, vmem_limit_bytes=60 * 1024 * 1024),
        name="attn",
    )(cu, valid, q, k, v, do)


def finish_kernel(cu, o_in, dq_in, dkv_in, lse_in, o_out, dq_out, dk_out, dv_out, lse_out):
    l0 = lax.shift_right_logical(cu[1], 3)

    def put(get, out):
        for up in range(2):
            def body(i, _):
                t0 = i * 16
                x = get(up, pl.ds(pl.multiple_of(t0, 16), 16))
                y = jnp.transpose(x, (1, 0, 2))
                for j in range(16):
                    out[src_row(up, t0 + j, l0)] = y[j]
                return 0
            lax.fori_loop(0, SLOT // 16, body, 0)

    put(lambda up, at: o_in[:, up, :, at, :].reshape(8, 16, HEAD), o_out)
    put(lambda up, at: dq_in[:, up, :, at, :].reshape(8, 16, HEAD), dq_out)

    @pl.when(pl.program_id(0) == 0)
    def _():
        put(lambda up, at: dkv_in[:, up, 0, at, :], dk_out)
        put(lambda up, at: dkv_in[:, up, 1, at, :], dv_out)
        row = lax.broadcasted_iota(jnp.int32, (2 * SLOT, SLOT), 0)
        col = lax.broadcasted_iota(jnp.int32, (2 * SLOT, SLOT), 1)
        acc = None
        for up in range(2):
            if up:
                src = jnp.where(col < l0, col + l0, col + SLOT)
            else:
                src = jnp.where(col < l0, col, col + l0)
            pick = jnp.where(row == src, 1.0, 0.0)
            part = lax.dot_general(pick, lse_in[up], NT, precision=lax.Precision.HIGHEST, preferred_element_type=F32)
            acc = part if acc is None else acc + part
        lse_out[...] = acc


def finish_call(cu, o_hm, dq_hm, dkv_hm, lse_hm):
    return pl.pallas_call(
        finish_kernel,
        grid=(4,),
        out_shape=(
            jax.ShapeDtypeStruct((256, 32, HEAD), BF16),
            jax.ShapeDtypeStruct((256, 32, HEAD), BF16),
            jax.ShapeDtypeStruct((256, 8, HEAD), BF16),
            jax.ShapeDtypeStruct((256, 8, HEAD), BF16),
            jax.ShapeDtypeStruct((256, 32), F32),
        ),
        in_specs=[
            pl.BlockSpec(memory_space=pltpu.SMEM),
            pl.BlockSpec((2, 2, GROUP, SLOT, HEAD), lambda i: (i, 0, 0, 0, 0)),
            pl.BlockSpec((2, 2, GROUP, SLOT, HEAD), lambda i: (i, 0, 0, 0, 0)),
            pl.BlockSpec((8, 2, 2, SLOT, HEAD), lambda i: (0, 0, 0, 0, 0)),
            pl.BlockSpec((2, 32, SLOT), lambda i: (0, 0, 0)),
        ],
        out_specs=(
            pl.BlockSpec((256, 8, HEAD), lambda i: (0, i, 0)),
            pl.BlockSpec((256, 8, HEAD), lambda i: (0, i, 0)),
            pl.BlockSpec((256, 8, HEAD), lambda i: (0, 0, 0)),
            pl.BlockSpec((256, 8, HEAD), lambda i: (0, 0, 0)),
            pl.BlockSpec((256, 32), lambda i: (0, 0)),
        ),
        compiler_params=pltpu.CompilerParams(dimension_semantics=("arbitrary",), vmem_limit_bytes=40 * 1024 * 1024),
        name="finish",
    )(cu, o_hm.reshape(8, 2, GROUP, SLOT, HEAD), dq_hm.reshape(8, 2, GROUP, SLOT, HEAD), dkv_hm, lse_hm)


def solution(mesh):
    tok_spec = P(("dp", "cp"), None, None)
    lse_spec = P(("dp", "cp"), None)

    def local(q, k, v, do, valid, cu):
        o_hm, dq_hm, dkv_hm, lse_hm = attn_call(cu, valid.reshape(1, 256), q, k, v, do)
        o, dq, dk, dv, lse = finish_call(cu, o_hm, dq_hm, dkv_hm, lse_hm)
        return o, lse, dq, dk, dv

    return jax.shard_map(local, mesh=mesh, in_specs=(tok_spec,) * 4 + (P(("dp", "cp")), P("dp")),
                         out_specs=(tok_spec, lse_spec, tok_spec, tok_spec, tok_spec), check_vma=False)
```

```python
import functools
import math

import jax
import jax.numpy as jnp
from jax import lax
from jax.experimental import pallas as pl
from jax.experimental.pallas import tpu as pltpu
from jax.sharding import PartitionSpec as P

MESH = pl.DeviceIdType.MESH
FILL = -1.0e30
BIG = 3.0e38
HEAD = 128
SLOT = 128
TILE = 512
GROUP = 4
HC = 4
SCALE = HEAD ** -0.5
C2 = SCALE * math.log2(math.e)
NT = (((1,), (1,)), ((), ()))
NN = (((1,), (0,)), ((), ()))
F32 = jnp.float32
BF16 = jnp.bfloat16

TILES = ((0, 0), (1, 0), (1, 1), (0, 1))


def slot_of(chip, ti):
    oc, up = TILES[ti]
    r = 2 * chip + oc
    return 7 - r if up else r


def mm(a, b, dims):
    return lax.dot_general(a, b, dims, preferred_element_type=F32)


def src_row(up, t, l0):
    if up:
        return jnp.where(t < l0, t + l0, t + SLOT)
    return jnp.where(t < l0, t, t + l0)


def attn_kernel(cu, valid, q, k, v, do, o_out, dq_out, dkv_out, lse_out,
                raw_q, raw_do, far_q, far_do, raw_k, raw_v, kv_hm, kv_all, kt, vt, qh, doh, st, pb, db,
                dkv_acc, dkv_in, o_st, dq_st, dkv_st, lse_st, caps, valid_all,
                in_sem, raw_ssem, raw_rsem, val_ssem, val_rsem, kv_ssem, kv_rsem,
                part_ssem, part_rsem, out_sem, out_rsem, lse_sem, lse_rsem):
    r = lax.axis_index("cp")
    chip = r // 2
    c = r % 2
    pc = 1 - c
    partner = chip * 2 + pc
    cross = (1 - chip) * 2 + c
    cross_o = (1 - chip) * 2 + pc
    l0 = lax.shift_right_logical(cu[1], 3)

    def remote(src, dst, ssem, rsem, dev):
        return pltpu.make_async_remote_copy(src_ref=src, dst_ref=dst, send_sem=ssem, recv_sem=rsem,
                                            device_id={"cp": dev}, device_id_type=MESH)

    own_heads = pl.ds(pl.multiple_of(16 * c, 16), 16)
    oth_heads = pl.ds(pl.multiple_of(16 * pc, 16), 16)
    ld_k = pltpu.make_async_copy(k, raw_k, in_sem.at[0])
    ld_v = pltpu.make_async_copy(v, raw_v, in_sem.at[1])
    ld_q = pltpu.make_async_copy(q.at[:, own_heads, :], raw_q, in_sem.at[2])
    ld_do = pltpu.make_async_copy(do.at[:, own_heads, :], raw_do, in_sem.at[3])
    ld_val = pltpu.make_async_copy(valid, valid_all.at[r], in_sem.at[4])
    for cp in (ld_k, ld_v, ld_q, ld_do, ld_val):
        cp.start()

    barrier = pltpu.get_barrier_semaphore()
    for dev in (partner, cross, cross_o):
        pl.semaphore_signal(barrier, inc=1, device_id={"cp": dev}, device_id_type=MESH)
    pl.semaphore_wait(barrier, 3)

    peers = (partner, cross, cross_o)
    push_q = remote(q.at[:, oth_heads, :], far_q, raw_ssem.at[0], raw_rsem.at[0], partner)
    push_do = remote(do.at[:, oth_heads, :], far_do, raw_ssem.at[1], raw_rsem.at[1], partner)
    push_val = [remote(valid, valid_all.at[r], val_ssem.at[i], val_rsem.at[r], dev) for i, dev in enumerate(peers)]

    push_q.start()
    push_do.start()

    def kv_relayout(up):
        def body(i, _):
            t0 = i * 16
            for which, raw in ((0, raw_k), (1, raw_v)):
                rows = jnp.stack([raw[src_row(up, t0 + j, l0)] for j in range(16)])
                kv_hm[:, up, which, pl.ds(pl.multiple_of(t0, 16), 16), :] = jnp.transpose(rows, (1, 0, 2))
            return 0
        lax.fori_loop(0, SLOT // 16, body, 0)

    def kv_push(h, to, both):
        head = (4 * c if to == 1 else 4 * pc) + h
        dev = (partner, cross, cross_o)[to]
        ups = pl.ds(0, 2 if both else 1)
        return remote(kv_hm.at[head, ups], kv_all.at[h, r, ups], kv_ssem.at[to, h], kv_rsem.at[h, r], dev)

    def kv_wait(h, owner, both):
        ups = pl.ds(0, 2 if both else 1)
        remote(kv_hm.at[0, ups], kv_all.at[h, owner, ups], kv_ssem.at[0, h], kv_rsem.at[h, owner], partner).wait_recv()

    ld_k.wait()
    ld_v.wait()
    kv_relayout(0)

    def cross_next(ch, h):
        @pl.when(chip == ch)
        def _():
            for to in (1, 2):
                if h > 0:
                    kv_push(h - 1, to, ch == 1).wait_send()
            for to in (1, 2):
                kv_push(h, to, ch == 1).start()

    cross_next(0, 0)
    kv_relayout(1)
    cross_next(1, 0)
    for h in range(HC):
        kv_push(h, 0, True).start()
    ld_val.wait()
    for cp in push_val:
        cp.start()

    def copy_own(h, _):
        for up in range(2):
            kv_all[h, r, up] = kv_hm[4 * c + h, up]
        return 0
    lax.fori_loop(0, HC, copy_own, 0)

    def q_relayout(oc, from_q, from_do):
        for up, ti in ((0, oc), (1, 3 - oc)):
            def body(i, _):
                t0 = i * 16
                at = pl.ds(pl.multiple_of(t0, 16), 16)
                for raw, dst in ((from_q, qh), (from_do, doh)):
                    rows = jnp.stack([raw[src_row(up, t0 + j, l0)] for j in range(16)])
                    dst[:, ti, :, at, :] = jnp.transpose(rows, (1, 0, 2)).reshape(HC, GROUP, 16, HEAD)
                return 0
            lax.fori_loop(0, SLOT // 16, body, 0)

    ld_q.wait()
    ld_do.wait()
    cross_next(0, 1)
    q_relayout(c, raw_q, raw_do)

    cross_next(0, 2)
    for i in range(3):
        remote(valid, valid_all.at[peers[i]], val_ssem.at[i], val_rsem.at[peers[i]], peers[i]).wait_recv()
    lane = lax.broadcasted_iota(jnp.int32, (SLOT, SLOT), 1)
    sub = lax.broadcasted_iota(jnp.int32, (SLOT, SLOT), 0)
    lane2 = lax.broadcasted_iota(jnp.int32, (SLOT, 2 * SLOT), 1)
    sub2 = lax.broadcasted_iota(jnp.int32, (SLOT, 2 * SLOT), 0)
    same_doc = (lane < l0) == (sub < l0)
    doc_f = jnp.where(lane < l0, 1.0, 0.0)
    doc_s = jnp.where(sub < l0, 1.0, 0.0)
    same_f = jnp.where(doc_f == doc_s, 1.0, 0.0)
    del same_doc

    def cap_body(s, _):
        owner = jnp.where(s < 4, s, 7 - s)
        off = jnp.where(s < 4, 0, 1)
        src_lo = jnp.where(sub2 < l0, sub2, sub2 + l0)
        src_hi = jnp.where(sub2 < l0, sub2 + l0, sub2 + SLOT)
        src = jnp.where(off == 1, src_hi, src_lo)
        row = jnp.broadcast_to(valid_all[owner].astype(F32), (SLOT, 2 * SLOT))
        ok = jnp.sum(jnp.where(src == lane2, row, 0.0), axis=1, keepdims=True)
        caps[s] = jnp.where(same_f * ok > 0.5, BIG, FILL)
        return 0
    lax.fori_loop(0, 8, cap_body, 0)
    for ti in range(4):
        oc, up = TILES[ti]
        s = (7 - (2 * chip + oc)) if up else 2 * chip + oc
        caps[8 + ti] = jnp.where(sub <= lane, caps[s], FILL)

    cross_next(0, 3)
    cross_next(1, 1)
    push_q.wait_recv()
    push_do.wait_recv()
    q_relayout(pc, far_q, far_do)

    def part_copy(h, i, n):
        return remote(dkv_acc.at[h, pl.ds(i, n)], dkv_in.at[h, pl.ds(0, n)], part_ssem.at[h], part_rsem.at[h], cross)

    def out_copies(h, ti, which):
        stage, out = ((o_st, o_out), (dq_st, dq_out), (dkv_st, dkv_out))[which]
        oc, up = TILES[ti]
        dst = out.at[4 * c + h, up]
        src = stage.at[h, ti]
        return (pltpu.make_async_copy(src, dst, out_sem.at[which, h, ti]),
                remote(src, dst, out_sem.at[which, h, ti], out_rsem.at[which, h, up], partner))

    def out_start(h, ti, which):
        local, far = out_copies(h, ti, which)
        oc = TILES[ti][0]

        @pl.when(c == oc)
        def _():
            local.start()

        @pl.when(c != oc)
        def _():
            far.start()

    lse_local = pltpu.make_async_copy(lse_st.at[c], lse_out.at[:, own_heads, :], lse_sem.at[0])
    lse_far = remote(lse_st.at[pc], lse_out.at[:, own_heads, :], lse_sem.at[1], lse_rsem, partner)

    def kv_slot(h, s, which):
        return kv_all[h, min(s, 7 - s), int(s > 3), which]

    def kv_slots(h, a, b, which):
        return jnp.concatenate([kv_slot(h, s, which) for s in range(a, b)], axis=0)

    def run_chip(ch):
        slots = [slot_of(ch, ti) for ti in range(4)]
        sent = [0, 1] if ch == 1 else [2, 3, 4, 5]
        kept = [0, 1] if ch == 0 else [2, 3, 4, 5]
        order = [0, 1, 2, 3]

        def transposes(s):
            for src, dst in ((0, kt), (1, vt)):
                dst[:, s * SLOT:(s + 1) * SLOT] = jnp.transpose(kv_slot(h_ref[0], s, src))

        h_ref = [None]

        def head(h, _):
            h_ref[0] = h
            seen = set()
            ready = set()

            def wait_slot(s):
                if s in ready:
                    return
                if s in slots:
                    kv_wait(h, partner, True)
                    new = slots
                elif ch == 1:
                    for owner in (0, 1):
                        kv_wait(h, owner, False)
                    new = [0, 1]
                else:
                    for owner in (2, 3):
                        kv_wait(h, owner, True)
                    new = [2, 3, 4, 5]
                for u in new:
                    ready.add(u)
                    transposes(u)

            for ti in order:
                s = slots[ti]
                nk = s + 1
                if ch == 1 and ti == 1:
                    for nxt in (2, 3):
                        pl.when(h == nxt - 2)(functools.partial(cross_next, 1, nxt))
                for u in range(nk):
                    wait_slot(u)
                qt = qh[h, ti].reshape(TILE, HEAD)
                dt = doh[h, ti].reshape(TILE, HEAD)
                m8 = [None] * GROUP
                for a in range(0, nk, 2):
                    n = min(2, nk - a)
                    kb = kv_slots(h, a, a + n, 0)
                    sc = mm(kb, qt, NT)
                    for j in range(n):
                        cap = caps[8 + ti] if a + j == s else caps[a + j]
                        for g in range(GROUP):
                            x = jnp.minimum(sc[j * SLOT:(j + 1) * SLOT, g * SLOT:(g + 1) * SLOT], cap)
                            st[(a + j) * SLOT:(a + j + 1) * SLOT, g * SLOT:(g + 1) * SLOT] = x
                            top = jnp.max(x.reshape(SLOT // 8, 8, SLOT), axis=0)
                            m8[g] = top if m8[g] is None else jnp.maximum(m8[g], top)
                m = [jnp.max(x, axis=0, keepdims=True) for x in m8]
                mc = [x * C2 for x in m]
                l8 = [None] * GROUP
                for a in range(nk):
                    for g in range(GROUP):
                        at = (slice(a * SLOT, (a + 1) * SLOT), slice(g * SLOT, (g + 1) * SLOT))
                        e = jnp.exp2(st[at] * C2 - mc[g])
                        st[at] = e
                        pb[at] = e.astype(BF16)
                        tot = jnp.sum(e.reshape(SLOT // 8, 8, SLOT), axis=0)
                        l8[g] = tot if l8[g] is None else l8[g] + tot
                ot = mm(vt[:, :nk * SLOT], pb[:nk * SLOT, :], NN)
                inv, dd = [], []
                oc, up = TILES[ti]
                for g in range(GROUP):
                    l = jnp.sum(l8[g], axis=0, keepdims=True)
                    has = m[g] > 0.5 * FILL
                    safe = jnp.where(has, l, 1.0)
                    i_l = jnp.where(has, 1.0 / safe, 0.0)
                    lse = jnp.where(has, m[g] * SCALE + jnp.log(safe), 0.0)
                    lse_st[oc, up, pl.ds(h * GROUP + g, 1), :] = lse
                    og = (ot[:, g * SLOT:(g + 1) * SLOT] * i_l).astype(BF16)
                    dog = jnp.transpose(dt[g * SLOT:(g + 1) * SLOT, :])
                    dd.append(jnp.sum(og.astype(F32) * dog.astype(F32), axis=0, keepdims=True))
                    inv.append(i_l)
                    o_st[h, ti, g * SLOT:(g + 1) * SLOT, :] = jnp.transpose(og)
                out_start(h, ti, 0)

                first = [u for u in range(nk) if u in sent] if (ch == 0 and ti >= 2) else []
                rest = [u for u in range(nk) if u not in first]
                dqt = None
                for part in (first, rest):
                    runs = []
                    for u in part:
                        if runs and runs[-1][1] == u and u - runs[-1][0] < 2:
                            runs[-1][1] = u + 1
                        else:
                            runs.append([u, u + 1])
                    for a, b in runs:
                        n = b - a
                        vb = kv_slots(h, a, b, 1)
                        dp = mm(vb, dt, NT)
                        for j in range(n):
                            for g in range(GROUP):
                                at = (slice((a + j) * SLOT, (a + j + 1) * SLOT), slice(g * SLOT, (g + 1) * SLOT))
                                p = st[at] * inv[g]
                                pb[at] = p.astype(BF16)
                                ds = p * (dp[j * SLOT:(j + 1) * SLOT, g * SLOT:(g + 1) * SLOT] - dd[g])
                                db[at] = ds.astype(BF16)
                        dsb = db[a * SLOT:b * SLOT, :]
                        dv = mm(pb[a * SLOT:b * SLOT, :], dt, NN)
                        dk = mm(dsb, qt, NN) * SCALE
                        dq = mm(kt[:, a * SLOT:b * SLOT], dsb, NN)
                        dqt = dq if dqt is None else dqt + dq
                        for j in range(n):
                            u = a + j
                            new = (dk[j * SLOT:(j + 1) * SLOT], dv[j * SLOT:(j + 1) * SLOT])
                            for w in range(2):
                                dkv_acc[h, u, w] = dkv_acc[h, u, w] + new[w] if u in seen else new[w]
                            seen.add(u)
                    if part is first and ti == 3 and ch == 0:
                        part_copy(h, sent[0], len(sent)).start()
                for g in range(GROUP):
                    dqg = (dqt[:, g * SLOT:(g + 1) * SLOT] * SCALE).astype(BF16)
                    dq_st[h, ti, g * SLOT:(g + 1) * SLOT, :] = jnp.transpose(dqg)
                out_start(h, ti, 1)
            if ch == 1:
                part_copy(h, sent[0], len(sent)).start()
            else:
                for ti in (2, 3):
                    for w in range(2):
                        dkv_st[h, ti, w] = dkv_acc[h, slots[ti], w].astype(BF16)
                    out_start(h, ti, 2)
            return 0

        lax.fori_loop(0, HC, head, 0)

        lse_local.start()
        lse_far.start()

        def tail(h, _):
            part_copy(h, kept[0], len(kept)).wait_recv()
            for i, u in enumerate(kept):
                ti = slots.index(u)
                for w in range(2):
                    dkv_st[h, ti, w] = (dkv_acc[h, u, w] + dkv_in[h, i, w]).astype(BF16)
                out_start(h, ti, 2)
            return 0
        lax.fori_loop(0, HC, tail, 0)

        def drain(h, _):
            part_copy(h, sent[0], len(sent)).wait_send()
            return 0
        lax.fori_loop(0, HC, drain, 0)

    pl.when(chip == 0)(functools.partial(run_chip, 0))
    pl.when(chip == 1)(functools.partial(run_chip, 1))

    push_q.wait_send()
    push_do.wait_send()
    for cp in push_val:
        cp.wait_send()

    def drain(h, _):
        kv_push(h, 0, True).wait_send()
        for ch in range(2):
            @pl.when(chip == ch)
            def _():
                for to in (1, 2):
                    pl.when(h == HC - 1)(kv_push(h, to, ch == 1).wait_send)
        for which in range(3):
            for ti in range(4):
                local, far = out_copies(h, ti, which)
                oc = TILES[ti][0]

                @pl.when(c == oc)
                def _():
                    local.wait()

                @pl.when(c != oc)
                def _():
                    far.wait_send()
            for up in range(2):
                stage, out = ((o_st, o_out), (dq_st, dq_out), (dkv_st, dkv_out))[which]
                remote(stage.at[h, 0], out.at[4 * pc + h, up], out_sem.at[which, h, 0],
                       out_rsem.at[which, h, up], partner).wait_recv()
        return 0
    lax.fori_loop(0, HC, drain, 0)
    lse_local.wait()
    lse_far.wait_send()
    remote(lse_st.at[0], lse_out.at[:, oth_heads, :], lse_sem.at[1], lse_rsem, partner).wait_recv()


def attn_call(cu, valid, q, k, v, do):
    any_spec = pl.BlockSpec(memory_space=pl.ANY)
    dma = pltpu.SemaphoreType.DMA
    return pl.pallas_call(
        attn_kernel,
        out_shape=(
            jax.ShapeDtypeStruct((8, 2, GROUP * SLOT, HEAD), BF16),
            jax.ShapeDtypeStruct((8, 2, GROUP * SLOT, HEAD), BF16),
            jax.ShapeDtypeStruct((8, 2, 2, SLOT, HEAD), BF16),
            jax.ShapeDtypeStruct((2, 32, SLOT), F32),
        ),
        in_specs=[pl.BlockSpec(memory_space=pltpu.SMEM)] + [any_spec] * 5,
        out_specs=(any_spec,) * 4,
        scratch_shapes=[
            pltpu.VMEM((256, 16, HEAD), BF16),
            pltpu.VMEM((256, 16, HEAD), BF16),
            pltpu.VMEM((256, 16, HEAD), BF16),
            pltpu.VMEM((256, 16, HEAD), BF16),
            pltpu.VMEM((256, 8, HEAD), BF16),
            pltpu.VMEM((256, 8, HEAD), BF16),
            pltpu.VMEM((8, 2, 2, SLOT, HEAD), BF16),
            pltpu.VMEM((HC, 4, 2, 2, SLOT, HEAD), BF16),
            pltpu.VMEM((HEAD, 8 * SLOT), BF16),
            pltpu.VMEM((HEAD, 8 * SLOT), BF16),
            pltpu.VMEM((HC, 4, GROUP, SLOT, HEAD), BF16),
            pltpu.VMEM((HC, 4, GROUP, SLOT, HEAD), BF16),
            pltpu.VMEM((8 * SLOT, TILE), F32),
            pltpu.VMEM((8 * SLOT, TILE), BF16),
            pltpu.VMEM((8 * SLOT, TILE), BF16),
            pltpu.VMEM((HC, 8, 2, SLOT, HEAD), F32),
            pltpu.VMEM((HC, 4, 2, SLOT, HEAD), F32),
            pltpu.VMEM((HC, 4, TILE, HEAD), BF16),
            pltpu.VMEM((HC, 4, TILE, HEAD), BF16),
            pltpu.VMEM((HC, 4, 2, SLOT, HEAD), BF16),
            pltpu.VMEM((2, 2, 16, SLOT), F32),
            pltpu.VMEM((12, SLOT, SLOT), F32),
            pltpu.VMEM((4, 1, 2 * SLOT), jnp.int32),
            dma((5,)),
            dma((2,)), dma((2,)),
            dma((3,)), dma((4,)),
            dma((3, HC)), dma((HC, 4)),
            dma((HC,)), dma((HC,)),
            dma((3, HC, 4)), dma((3, HC, 2)),
            dma((2,)), dma,
        ],
        compiler_params=pltpu.CompilerParams(collective_id=0, has_side_effects=True, vmem_limit_bytes=60 * 1024 * 1024),
        name="attn",
    )(cu, valid, q, k, v, do)


def finish_kernel(cu, o_in, dq_in, dkv_in, lse_in, o_out, dq_out, dk_out, dv_out, lse_out):
    l0 = lax.shift_right_logical(cu[1], 3)

    def put(get, out):
        for up in range(2):
            def body(i, _):
                t0 = i * 16
                x = get(up, pl.ds(pl.multiple_of(t0, 16), 16))
                y = jnp.transpose(x, (1, 0, 2))
                for j in range(16):
                    out[src_row(up, t0 + j, l0)] = y[j]
                return 0
            lax.fori_loop(0, SLOT // 16, body, 0)

    put(lambda up, at: o_in[:, up, :, at, :].reshape(8, 16, HEAD), o_out)
    put(lambda up, at: dq_in[:, up, :, at, :].reshape(8, 16, HEAD), dq_out)

    @pl.when(pl.program_id(0) == 0)
    def _():
        put(lambda up, at: dkv_in[:, up, 0, at, :], dk_out)
        put(lambda up, at: dkv_in[:, up, 1, at, :], dv_out)
        row = lax.broadcasted_iota(jnp.int32, (2 * SLOT, SLOT), 0)
        col = lax.broadcasted_iota(jnp.int32, (2 * SLOT, SLOT), 1)
        acc = None
        for up in range(2):
            if up:
                src = jnp.where(col < l0, col + l0, col + SLOT)
            else:
                src = jnp.where(col < l0, col, col + l0)
            pick = jnp.where(row == src, 1.0, 0.0)
            part = lax.dot_general(pick, lse_in[up], NT, precision=lax.Precision.HIGHEST, preferred_element_type=F32)
            acc = part if acc is None else acc + part
        lse_out[...] = acc


def finish_call(cu, o_hm, dq_hm, dkv_hm, lse_hm):
    return pl.pallas_call(
        finish_kernel,
        grid=(4,),
        out_shape=(
            jax.ShapeDtypeStruct((256, 32, HEAD), BF16),
            jax.ShapeDtypeStruct((256, 32, HEAD), BF16),
            jax.ShapeDtypeStruct((256, 8, HEAD), BF16),
            jax.ShapeDtypeStruct((256, 8, HEAD), BF16),
            jax.ShapeDtypeStruct((256, 32), F32),
        ),
        in_specs=[
            pl.BlockSpec(memory_space=pltpu.SMEM),
            pl.BlockSpec((2, 2, GROUP, SLOT, HEAD), lambda i: (i, 0, 0, 0, 0)),
            pl.BlockSpec((2, 2, GROUP, SLOT, HEAD), lambda i: (i, 0, 0, 0, 0)),
            pl.BlockSpec((8, 2, 2, SLOT, HEAD), lambda i: (0, 0, 0, 0, 0)),
            pl.BlockSpec((2, 32, SLOT), lambda i: (0, 0, 0)),
        ],
        out_specs=(
            pl.BlockSpec((256, 8, HEAD), lambda i: (0, i, 0)),
            pl.BlockSpec((256, 8, HEAD), lambda i: (0, i, 0)),
            pl.BlockSpec((256, 8, HEAD), lambda i: (0, 0, 0)),
            pl.BlockSpec((256, 8, HEAD), lambda i: (0, 0, 0)),
            pl.BlockSpec((256, 32), lambda i: (0, 0)),
        ),
        compiler_params=pltpu.CompilerParams(dimension_semantics=("arbitrary",), vmem_limit_bytes=40 * 1024 * 1024),
        name="finish",
    )(cu, o_hm.reshape(8, 2, GROUP, SLOT, HEAD), dq_hm.reshape(8, 2, GROUP, SLOT, HEAD), dkv_hm, lse_hm)


def solution(mesh):
    tok_spec = P(("dp", "cp"), None, None)
    lse_spec = P(("dp", "cp"), None)

    def local(q, k, v, do, valid, cu):
        o_hm, dq_hm, dkv_hm, lse_hm = attn_call(cu, valid.reshape(1, 256), q, k, v, do)
        o, dq, dk, dv, lse = finish_call(cu, o_hm, dq_hm, dkv_hm, lse_hm)
        return o, lse, dq, dk, dv

    return jax.shard_map(local, mesh=mesh, in_specs=(tok_spec,) * 4 + (P(("dp", "cp")), P("dp")),
                         out_specs=(tok_spec, lse_spec, tok_spec, tok_spec, tok_spec), check_vma=False)
```

```python
import functools
import math

import jax
import jax.numpy as jnp
from jax import lax
from jax.experimental import pallas as pl
from jax.experimental.pallas import tpu as pltpu
from jax.sharding import PartitionSpec as P

MESH = pl.DeviceIdType.MESH
FILL = -1.0e30
BIG = 3.0e38
HEAD = 128
SLOT = 128
TILE = 512
GROUP = 4
HC = 4
SCALE = HEAD ** -0.5
C2 = SCALE * math.log2(math.e)
NT = (((1,), (1,)), ((), ()))
NN = (((1,), (0,)), ((), ()))
F32 = jnp.float32
BF16 = jnp.bfloat16

TILES = ((0, 0), (1, 0), (1, 1), (0, 1))


def slot_of(chip, ti):
    oc, up = TILES[ti]
    r = 2 * chip + oc
    return 7 - r if up else r


def mm(a, b, dims):
    return lax.dot_general(a, b, dims, preferred_element_type=F32)


def src_row(up, t, l0):
    if up:
        return jnp.where(t < l0, t + l0, t + SLOT)
    return jnp.where(t < l0, t, t + l0)


def attn_kernel(cu, valid, q, k, v, do, o_out, dq_out, dkv_out, lse_out,
                raw_q, raw_do, far_q, far_do, raw_k, raw_v, kv_hm, kv_all, kt, vt, qh, doh, st, pb, db,
                dkv_acc, dkv_in, o_st, dq_st, o_far, dq_far, dkv_st, lse_st, caps, valid_all,
                in_sem, raw_ssem, raw_rsem, val_ssem, val_rsem, kv_ssem, kv_rsem,
                part_ssem, part_rsem, res_ssem, res_rsem, dkv_ssem, dkv_rsem, lse_sem, lse_rsem):
    r = lax.axis_index("cp")
    chip = r // 2
    c = r % 2
    pc = 1 - c
    partner = chip * 2 + pc
    cross = (1 - chip) * 2 + c
    cross_o = (1 - chip) * 2 + pc
    l0 = lax.shift_right_logical(cu[1], 3)

    def remote(src, dst, ssem, rsem, dev):
        return pltpu.make_async_remote_copy(src_ref=src, dst_ref=dst, send_sem=ssem, recv_sem=rsem,
                                            device_id={"cp": dev}, device_id_type=MESH)

    own_heads = pl.ds(pl.multiple_of(16 * c, 16), 16)
    oth_heads = pl.ds(pl.multiple_of(16 * pc, 16), 16)
    ld_k = pltpu.make_async_copy(k, raw_k, in_sem.at[0])
    ld_v = pltpu.make_async_copy(v, raw_v, in_sem.at[1])
    ld_q = pltpu.make_async_copy(q.at[:, own_heads, :], raw_q, in_sem.at[2])
    ld_do = pltpu.make_async_copy(do.at[:, own_heads, :], raw_do, in_sem.at[3])
    ld_val = pltpu.make_async_copy(valid, valid_all.at[r], in_sem.at[4])
    for cp in (ld_k, ld_v, ld_q, ld_do, ld_val):
        cp.start()

    barrier = pltpu.get_barrier_semaphore()
    for dev in (partner, cross, cross_o):
        pl.semaphore_signal(barrier, inc=1, device_id={"cp": dev}, device_id_type=MESH)
    pl.semaphore_wait(barrier, 3)

    peers = (partner, cross, cross_o)
    push_q = remote(q.at[:, oth_heads, :], far_q, raw_ssem.at[0], raw_rsem.at[0], partner)
    push_do = remote(do.at[:, oth_heads, :], far_do, raw_ssem.at[1], raw_rsem.at[1], partner)
    push_val = [remote(valid, valid_all.at[r], val_ssem.at[i], val_rsem.at[r], dev) for i, dev in enumerate(peers)]

    push_q.start()
    push_do.start()

    def kv_relayout(up):
        def body(i, _):
            t0 = i * 16
            for which, raw in ((0, raw_k), (1, raw_v)):
                rows = jnp.stack([raw[src_row(up, t0 + j, l0)] for j in range(16)])
                kv_hm[:, up, which, pl.ds(pl.multiple_of(t0, 16), 16), :] = jnp.transpose(rows, (1, 0, 2))
            return 0
        lax.fori_loop(0, SLOT // 16, body, 0)

    def kv_push(h, to, both):
        head = (4 * c if to == 1 else 4 * pc) + h
        dev = (partner, cross, cross_o)[to]
        ups = pl.ds(0, 2 if both else 1)
        return remote(kv_hm.at[head, ups], kv_all.at[h, r, ups], kv_ssem.at[to, h], kv_rsem.at[h, r], dev)

    def kv_wait(h, owner, both):
        ups = pl.ds(0, 2 if both else 1)
        remote(kv_hm.at[0, ups], kv_all.at[h, owner, ups], kv_ssem.at[0, h], kv_rsem.at[h, owner], partner).wait_recv()

    ld_k.wait()
    ld_v.wait()
    kv_relayout(0)

    def cross_next(ch, h):
        @pl.when(chip == ch)
        def _():
            for to in (1, 2):
                if h > 0:
                    kv_push(h - 1, to, ch == 1).wait_send()
            for to in (1, 2):
                kv_push(h, to, ch == 1).start()

    cross_next(0, 0)
    kv_relayout(1)
    cross_next(1, 0)
    for h in range(HC):
        kv_push(h, 0, True).start()
    ld_val.wait()
    for cp in push_val:
        cp.start()

    def copy_own(h, _):
        for up in range(2):
            kv_all[h, r, up] = kv_hm[4 * c + h, up]
        return 0
    lax.fori_loop(0, HC, copy_own, 0)

    def q_relayout(oc, from_q, from_do):
        for up, ti in ((0, oc), (1, 3 - oc)):
            def body(i, _):
                t0 = i * 16
                at = pl.ds(pl.multiple_of(t0, 16), 16)
                for raw, dst in ((from_q, qh), (from_do, doh)):
                    rows = jnp.stack([raw[src_row(up, t0 + j, l0)] for j in range(16)])
                    dst[:, ti, :, at, :] = jnp.transpose(rows, (1, 0, 2)).reshape(HC, GROUP, 16, HEAD)
                return 0
            lax.fori_loop(0, SLOT // 16, body, 0)

    ld_q.wait()
    ld_do.wait()
    cross_next(0, 1)
    q_relayout(c, raw_q, raw_do)

    cross_next(0, 2)
    for i in range(3):
        remote(valid, valid_all.at[peers[i]], val_ssem.at[i], val_rsem.at[peers[i]], peers[i]).wait_recv()
    lane = lax.broadcasted_iota(jnp.int32, (SLOT, SLOT), 1)
    sub = lax.broadcasted_iota(jnp.int32, (SLOT, SLOT), 0)
    lane2 = lax.broadcasted_iota(jnp.int32, (SLOT, 2 * SLOT), 1)
    sub2 = lax.broadcasted_iota(jnp.int32, (SLOT, 2 * SLOT), 0)
    same_doc = (lane < l0) == (sub < l0)
    doc_f = jnp.where(lane < l0, 1.0, 0.0)
    doc_s = jnp.where(sub < l0, 1.0, 0.0)
    same_f = jnp.where(doc_f == doc_s, 1.0, 0.0)
    del same_doc

    def cap_body(s, _):
        owner = jnp.where(s < 4, s, 7 - s)
        off = jnp.where(s < 4, 0, 1)
        src_lo = jnp.where(sub2 < l0, sub2, sub2 + l0)
        src_hi = jnp.where(sub2 < l0, sub2 + l0, sub2 + SLOT)
        src = jnp.where(off == 1, src_hi, src_lo)
        row = jnp.broadcast_to(valid_all[owner].astype(F32), (SLOT, 2 * SLOT))
        ok = jnp.sum(jnp.where(src == lane2, row, 0.0), axis=1, keepdims=True)
        caps[s] = jnp.where(same_f * ok > 0.5, BIG, FILL)
        return 0
    lax.fori_loop(0, 8, cap_body, 0)
    for ti in range(4):
        oc, up = TILES[ti]
        s = (7 - (2 * chip + oc)) if up else 2 * chip + oc
        caps[8 + ti] = jnp.where(sub <= lane, caps[s], FILL)

    cross_next(0, 3)
    cross_next(1, 1)
    push_q.wait_recv()
    push_do.wait_recv()
    q_relayout(pc, far_q, far_do)

    def part_copy(h, i, n):
        return remote(dkv_acc.at[h, pl.ds(i, n)], dkv_in.at[h, pl.ds(0, n)], part_ssem.at[h], part_rsem.at[h], cross)

    def res_copy(p, ti, which):
        stage, out = ((o_far, o_out), (dq_far, dq_out))[which]
        dst = out.at[TILES[ti][1], :, pl.ds(pl.multiple_of(16 * c + 8 * p, 8), 8), :]
        return remote(stage.at[p, ti], dst, res_ssem.at[which, p, ti], res_rsem.at[which, p, TILES[ti][1]], partner)

    def dkv_copy(h, ti):
        up = TILES[ti][1]
        return remote(dkv_st.at[h, ti], dkv_out.at[4 * c + h, up], dkv_ssem.at[h, ti], dkv_rsem.at[h, up], partner)

    def res_put(p):
        heads = pl.ds(pl.multiple_of(16 * c + 8 * p, 8), 8)
        for ti, (oc, up) in enumerate(TILES):
            def body(i, _, keep):
                at = pl.ds(pl.multiple_of(i * 16, 16), 16)
                for stage, far, out in ((o_st, o_far, o_out), (dq_st, dq_far, dq_out)):
                    x = jnp.concatenate([stage[e, ti, pl.ds(pl.multiple_of(g * SLOT + i * 16, 16), 16), :][None]
                                         for e in range(2) for g in range(GROUP)], axis=0)
                    y = jnp.transpose(x, (1, 0, 2))
                    if keep:
                        out[up, at, heads, :] = y
                    else:
                        far[p, ti, at, :, :] = y
                return 0

            @pl.when(c == oc)
            def _():
                lax.fori_loop(0, SLOT // 16, functools.partial(body, keep=True), 0)

            @pl.when(c != oc)
            def _():
                lax.fori_loop(0, SLOT // 16, functools.partial(body, keep=False), 0)
                for which in range(2):
                    res_copy(p, ti, which).start()

    def dkv_put(h, ti, parts):
        oc, up = TILES[ti]

        @pl.when(c == oc)
        def _():
            for w in range(2):
                dkv_out[4 * c + h, up, w] = parts(w).astype(BF16)

        @pl.when(c != oc)
        def _():
            for w in range(2):
                dkv_st[h, ti, w] = parts(w).astype(BF16)
            dkv_copy(h, ti).start()

    lse_far = remote(lse_st.at[pc], lse_out.at[:, own_heads, :], lse_sem, lse_rsem, partner)

    def kv_slot(h, s, which):
        return kv_all[h, min(s, 7 - s), int(s > 3), which]

    def kv_slots(h, a, b, which):
        return jnp.concatenate([kv_slot(h, s, which) for s in range(a, b)], axis=0)

    def run_chip(ch):
        slots = [slot_of(ch, ti) for ti in range(4)]
        sent = [0, 1] if ch == 1 else [2, 3, 4, 5]
        kept = [0, 1] if ch == 0 else [2, 3, 4, 5]
        order = [0, 1, 2, 3]

        def transposes(s):
            for src, dst in ((0, kt), (1, vt)):
                dst[:, s * SLOT:(s + 1) * SLOT] = jnp.transpose(kv_slot(h_ref[0], s, src))

        h_ref = [None]

        def head(h, _):
            h_ref[0] = h
            seen = set()
            ready = set()

            def wait_slot(s):
                if s in ready:
                    return
                if s in slots:
                    kv_wait(h, partner, True)
                    new = slots
                elif ch == 1:
                    for owner in (0, 1):
                        kv_wait(h, owner, False)
                    new = [0, 1]
                else:
                    for owner in (2, 3):
                        kv_wait(h, owner, True)
                    new = [2, 3, 4, 5]
                for u in new:
                    ready.add(u)
                    transposes(u)

            for ti in order:
                s = slots[ti]
                nk = s + 1
                if ch == 1 and ti == 1:
                    for nxt in (2, 3):
                        pl.when(h == nxt - 2)(functools.partial(cross_next, 1, nxt))
                for u in range(nk):
                    wait_slot(u)
                qt = qh[h, ti].reshape(TILE, HEAD)
                dt = doh[h, ti].reshape(TILE, HEAD)
                m8 = [None] * GROUP
                for a in range(0, nk, 2):
                    n = min(2, nk - a)
                    kb = kv_slots(h, a, a + n, 0)
                    sc = mm(kb, qt, NT)
                    for j in range(n):
                        cap = caps[8 + ti] if a + j == s else caps[a + j]
                        for g in range(GROUP):
                            x = jnp.minimum(sc[j * SLOT:(j + 1) * SLOT, g * SLOT:(g + 1) * SLOT], cap)
                            st[(a + j) * SLOT:(a + j + 1) * SLOT, g * SLOT:(g + 1) * SLOT] = x
                            top = jnp.max(x.reshape(SLOT // 8, 8, SLOT), axis=0)
                            m8[g] = top if m8[g] is None else jnp.maximum(m8[g], top)
                m = [jnp.max(x, axis=0, keepdims=True) for x in m8]
                mc = [x * C2 for x in m]
                l8 = [None] * GROUP
                for a in range(nk):
                    for g in range(GROUP):
                        at = (slice(a * SLOT, (a + 1) * SLOT), slice(g * SLOT, (g + 1) * SLOT))
                        e = jnp.exp2(st[at] * C2 - mc[g])
                        st[at] = e
                        pb[at] = e.astype(BF16)
                        tot = jnp.sum(e.reshape(SLOT // 8, 8, SLOT), axis=0)
                        l8[g] = tot if l8[g] is None else l8[g] + tot
                ot = mm(vt[:, :nk * SLOT], pb[:nk * SLOT, :], NN)
                inv, dd = [], []
                oc, up = TILES[ti]
                for g in range(GROUP):
                    l = jnp.sum(l8[g], axis=0, keepdims=True)
                    has = m[g] > 0.5 * FILL
                    safe = jnp.where(has, l, 1.0)
                    i_l = jnp.where(has, 1.0 / safe, 0.0)
                    lse = jnp.where(has, m[g] * SCALE + jnp.log(safe), 0.0)
                    lse_st[oc, up, pl.ds(h * GROUP + g, 1), :] = lse
                    og = (ot[:, g * SLOT:(g + 1) * SLOT] * i_l).astype(BF16)
                    dog = jnp.transpose(dt[g * SLOT:(g + 1) * SLOT, :])
                    dd.append(jnp.sum(og.astype(F32) * dog.astype(F32), axis=0, keepdims=True))
                    inv.append(i_l)
                    o_st[h % 2, ti, g * SLOT:(g + 1) * SLOT, :] = jnp.transpose(og)

                first = [u for u in range(nk) if u in sent] if (ch == 0 and ti >= 2) else []
                rest = [u for u in range(nk) if u not in first]
                dqt = None
                for part in (first, rest):
                    runs = []
                    for u in part:
                        if runs and runs[-1][1] == u and u - runs[-1][0] < 2:
                            runs[-1][1] = u + 1
                        else:
                            runs.append([u, u + 1])
                    for a, b in runs:
                        n = b - a
                        vb = kv_slots(h, a, b, 1)
                        dp = mm(vb, dt, NT)
                        for j in range(n):
                            for g in range(GROUP):
                                at = (slice((a + j) * SLOT, (a + j + 1) * SLOT), slice(g * SLOT, (g + 1) * SLOT))
                                p = st[at] * inv[g]
                                pb[at] = p.astype(BF16)
                                ds = p * (dp[j * SLOT:(j + 1) * SLOT, g * SLOT:(g + 1) * SLOT] - dd[g])
                                db[at] = ds.astype(BF16)
                        dsb = db[a * SLOT:b * SLOT, :]
                        dv = mm(pb[a * SLOT:b * SLOT, :], dt, NN)
                        dk = mm(dsb, qt, NN) * SCALE
                        dq = mm(kt[:, a * SLOT:b * SLOT], dsb, NN)
                        dqt = dq if dqt is None else dqt + dq
                        for j in range(n):
                            u = a + j
                            new = (dk[j * SLOT:(j + 1) * SLOT], dv[j * SLOT:(j + 1) * SLOT])
                            for w in range(2):
                                dkv_acc[h, u, w] = dkv_acc[h, u, w] + new[w] if u in seen else new[w]
                            seen.add(u)
                    if part is first and ti == 3 and ch == 0:
                        part_copy(h, sent[0], len(sent)).start()
                for g in range(GROUP):
                    dqg = (dqt[:, g * SLOT:(g + 1) * SLOT] * SCALE).astype(BF16)
                    dq_st[h % 2, ti, g * SLOT:(g + 1) * SLOT, :] = jnp.transpose(dqg)
            if ch == 1:
                part_copy(h, sent[0], len(sent)).start()
            else:
                for ti in (2, 3):
                    dkv_put(h, ti, lambda w, ti=ti: dkv_acc[h, slots[ti], w])
            pl.when(h % 2 == 1)(lambda: res_put(h // 2))
            return 0

        lax.fori_loop(0, HC, head, 0)

        lse_out[:, own_heads, :] = lse_st[c]
        lse_far.start()

        def tail(h, _):
            part_copy(h, kept[0], len(kept)).wait_recv()
            for i, u in enumerate(kept):
                ti = slots.index(u)
                dkv_put(h, ti, lambda w, u=u, i=i: dkv_acc[h, u, w] + dkv_in[h, i, w])
            return 0
        lax.fori_loop(0, HC, tail, 0)

        def drain(h, _):
            part_copy(h, sent[0], len(sent)).wait_send()
            return 0
        lax.fori_loop(0, HC, drain, 0)

    pl.when(chip == 0)(functools.partial(run_chip, 0))
    pl.when(chip == 1)(functools.partial(run_chip, 1))

    push_q.wait_send()
    push_do.wait_send()
    for cp in push_val:
        cp.wait_send()

    def drain(h, _):
        kv_push(h, 0, True).wait_send()
        for ch in range(2):
            @pl.when(chip == ch)
            def _():
                for to in (1, 2):
                    pl.when(h == HC - 1)(kv_push(h, to, ch == 1).wait_send)
        for ti in range(4):
            pl.when(c != TILES[ti][0])(dkv_copy(h, ti).wait_send)
        for up in range(2):
            remote(dkv_st.at[h, 0], dkv_out.at[4 * pc + h, up], dkv_ssem.at[h, 0], dkv_rsem.at[h, up], partner).wait_recv()
        return 0
    lax.fori_loop(0, HC, drain, 0)

    for p in range(2):
        for which in range(2):
            stage, out = ((o_far, o_out), (dq_far, dq_out))[which]
            for ti in range(4):
                pl.when(c != TILES[ti][0])(res_copy(p, ti, which).wait_send)
            for up in range(2):
                dst = out.at[up, :, pl.ds(pl.multiple_of(16 * pc + 8 * p, 8), 8), :]
                remote(stage.at[p, 0], dst, res_ssem.at[which, p, 0], res_rsem.at[which, p, up], partner).wait_recv()
    lse_far.wait_send()
    remote(lse_st.at[0], lse_out.at[:, oth_heads, :], lse_sem, lse_rsem, partner).wait_recv()


def attn_call(cu, valid, q, k, v, do):
    any_spec = pl.BlockSpec(memory_space=pl.ANY)
    dma = pltpu.SemaphoreType.DMA
    return pl.pallas_call(
        attn_kernel,
        out_shape=(
            pltpu.VMEM((2, SLOT, 32, HEAD), BF16),
            pltpu.VMEM((2, SLOT, 32, HEAD), BF16),
            pltpu.VMEM((8, 2, 2, SLOT, HEAD), BF16),
            pltpu.VMEM((2, 32, SLOT), F32),
        ),
        in_specs=[pl.BlockSpec(memory_space=pltpu.SMEM)] + [any_spec] * 5,
        out_specs=(pl.BlockSpec(memory_space=pltpu.VMEM),) * 4,
        scratch_shapes=[
            pltpu.VMEM((256, 16, HEAD), BF16),
            pltpu.VMEM((256, 16, HEAD), BF16),
            pltpu.VMEM((256, 16, HEAD), BF16),
            pltpu.VMEM((256, 16, HEAD), BF16),
            pltpu.VMEM((256, 8, HEAD), BF16),
            pltpu.VMEM((256, 8, HEAD), BF16),
            pltpu.VMEM((8, 2, 2, SLOT, HEAD), BF16),
            pltpu.VMEM((HC, 4, 2, 2, SLOT, HEAD), BF16),
            pltpu.VMEM((HEAD, 8 * SLOT), BF16),
            pltpu.VMEM((HEAD, 8 * SLOT), BF16),
            pltpu.VMEM((HC, 4, GROUP, SLOT, HEAD), BF16),
            pltpu.VMEM((HC, 4, GROUP, SLOT, HEAD), BF16),
            pltpu.VMEM((8 * SLOT, TILE), F32),
            pltpu.VMEM((8 * SLOT, TILE), BF16),
            pltpu.VMEM((8 * SLOT, TILE), BF16),
            pltpu.VMEM((HC, 8, 2, SLOT, HEAD), F32),
            pltpu.VMEM((HC, 4, 2, SLOT, HEAD), F32),
            pltpu.VMEM((2, 4, TILE, HEAD), BF16),
            pltpu.VMEM((2, 4, TILE, HEAD), BF16),
            pltpu.VMEM((2, 4, SLOT, 8, HEAD), BF16),
            pltpu.VMEM((2, 4, SLOT, 8, HEAD), BF16),
            pltpu.VMEM((HC, 4, 2, SLOT, HEAD), BF16),
            pltpu.VMEM((2, 2, 16, SLOT), F32),
            pltpu.VMEM((12, SLOT, SLOT), F32),
            pltpu.VMEM((4, 1, 2 * SLOT), jnp.int32),
            dma((5,)),
            dma((2,)), dma((2,)),
            dma((3,)), dma((4,)),
            dma((3, HC)), dma((HC, 4)),
            dma((HC,)), dma((HC,)),
            dma((2, 2, 4)), dma((2, 2, 2)),
            dma((HC, 4)), dma((HC, 2)),
            dma, dma,
        ],
        compiler_params=pltpu.CompilerParams(collective_id=0, has_side_effects=True, vmem_limit_bytes=44 * 1024 * 1024),
        name="attn",
    )(cu, valid, q, k, v, do)


def finish_kernel(cu, o_in, dq_in, dkv_in, lse_in, o_out, dq_out, dk_out, dv_out, lse_out, dk_t, dv_t, sem):
    l0 = lax.shift_right_logical(cu[1], 3)
    rest = SLOT - l0

    def copies(i, x, out):
        runs = ((0, 0, 0, l0), (1, 0, l0, l0), (0, l0, 2 * l0, rest), (1, l0, SLOT + l0, rest))
        return [pltpu.make_async_copy(x.at[up, pl.ds(at, n)], out.at[pl.ds(to, n)], sem.at[i, j])
                for j, (up, at, to, n) in enumerate(runs)]

    moves = copies(0, o_in, o_out) + copies(1, dq_in, dq_out)
    for cp in moves:
        cp.start()

    for w, dst in ((0, dk_t), (1, dv_t)):
        for up in range(2):
            def body(i, _):
                at = pl.ds(pl.multiple_of(i * 16, 16), 16)
                dst[up, at] = jnp.transpose(dkv_in[:, up, w, at, :], (1, 0, 2))
                return 0
            lax.fori_loop(0, SLOT // 16, body, 0)
        more = copies(2 + w, dst, (dk_out, dv_out)[w])
        for cp in more:
            cp.start()
        moves += more

    row = lax.broadcasted_iota(jnp.int32, (2 * SLOT, SLOT), 0)
    col = lax.broadcasted_iota(jnp.int32, (2 * SLOT, SLOT), 1)
    acc = None
    for up in range(2):
        if up:
            src = jnp.where(col < l0, col + l0, col + SLOT)
        else:
            src = jnp.where(col < l0, col, col + l0)
        pick = jnp.where(row == src, 1.0, 0.0)
        part = lax.dot_general(lse_in[up], pick, NT, precision=lax.Precision.HIGHEST, preferred_element_type=F32)
        acc = part if acc is None else acc + part
    lse_out[...] = acc
    for cp in moves:
        cp.wait()


def finish_call(cu, o_t, dq_t, dkv_hm, lse_hm):
    any_spec = pl.BlockSpec(memory_space=pl.ANY)
    vmem = pl.BlockSpec(memory_space=pltpu.VMEM)
    return pl.pallas_call(
        finish_kernel,
        out_shape=(
            jax.ShapeDtypeStruct((256, 32, HEAD), BF16),
            jax.ShapeDtypeStruct((256, 32, HEAD), BF16),
            jax.ShapeDtypeStruct((256, 8, HEAD), BF16),
            jax.ShapeDtypeStruct((256, 8, HEAD), BF16),
            jax.ShapeDtypeStruct((32, 256), F32),
        ),
        in_specs=[pl.BlockSpec(memory_space=pltpu.SMEM)] + [vmem] * 4,
        out_specs=(any_spec,) * 4 + (vmem,),
        scratch_shapes=[
            pltpu.VMEM((2, SLOT, 8, HEAD), BF16),
            pltpu.VMEM((2, SLOT, 8, HEAD), BF16),
            pltpu.SemaphoreType.DMA((4, 4)),
        ],
        compiler_params=pltpu.CompilerParams(vmem_limit_bytes=16 * 1024 * 1024),
        name="finish",
    )(cu, o_t, dq_t, dkv_hm, lse_hm)


def solution(mesh):
    tok_spec = P(("dp", "cp"), None, None)
    lse_spec = P(("dp", "cp"), None)

    def local(q, k, v, do, valid, cu):
        res = attn_call(cu, valid.reshape(1, 256), q, k, v, do)
        o, dq, dk, dv, lse = finish_call(cu, *res)
        return o, lse.T, dq, dk, dv

    return jax.shard_map(local, mesh=mesh, in_specs=(tok_spec,) * 4 + (P(("dp", "cp")), P("dp")),
                         out_specs=(tok_spec, lse_spec, tok_spec, tok_spec, tok_spec), check_vma=False)
```

```python
import functools
import math

import jax
import jax.numpy as jnp
from jax import lax
from jax.experimental import pallas as pl
from jax.experimental.pallas import tpu as pltpu
from jax.sharding import PartitionSpec as P

MESH = pl.DeviceIdType.MESH
FILL = -1.0e30
BIG = 3.0e38
HEAD = 128
SLOT = 128
TILE = 512
GROUP = 4
HC = 4
SCALE = HEAD ** -0.5
C2 = SCALE * math.log2(math.e)
NT = (((1,), (1,)), ((), ()))
NN = (((1,), (0,)), ((), ()))
F32 = jnp.float32
BF16 = jnp.bfloat16

TILES = ((0, 0), (1, 0), (1, 1), (0, 1))


def slot_of(chip, ti):
    oc, up = TILES[ti]
    r = 2 * chip + oc
    return 7 - r if up else r


def mm(a, b, dims):
    return lax.dot_general(a, b, dims, preferred_element_type=F32)


def src_row(up, t, l0):
    if up:
        return jnp.where(t < l0, t + l0, t + SLOT)
    return jnp.where(t < l0, t, t + l0)


def attn_kernel(cu, valid, q, k, v, do, o_out, dq_out, dkv_out, lse_out,
                raw_q, raw_do, far_q, far_do, raw_k, raw_v, kv_hm, kv_all, kt, vt, qh, doh, st, pb, db,
                dkv_acc, dkv_in, o_st, dq_st, o_far, dq_far, dkv_st, lse_st, caps, valid_all,
                in_sem, raw_ssem, raw_rsem, val_ssem, val_rsem, kv_ssem, kv_rsem,
                part_ssem, part_rsem, res_ssem, res_rsem, dkv_ssem, dkv_rsem, lse_sem, lse_rsem):
    r = lax.axis_index("cp")
    chip = r // 2
    c = r % 2
    pc = 1 - c
    partner = chip * 2 + pc
    cross = (1 - chip) * 2 + c
    cross_o = (1 - chip) * 2 + pc
    l0 = lax.shift_right_logical(cu[1], 3)

    def remote(src, dst, ssem, rsem, dev):
        return pltpu.make_async_remote_copy(src_ref=src, dst_ref=dst, send_sem=ssem, recv_sem=rsem,
                                            device_id={"cp": dev}, device_id_type=MESH)

    own_heads = pl.ds(pl.multiple_of(16 * c, 16), 16)
    oth_heads = pl.ds(pl.multiple_of(16 * pc, 16), 16)
    ld_k = pltpu.make_async_copy(k, raw_k, in_sem.at[0])
    ld_v = pltpu.make_async_copy(v, raw_v, in_sem.at[1])
    ld_q = pltpu.make_async_copy(q.at[:, own_heads, :], raw_q, in_sem.at[2])
    ld_do = pltpu.make_async_copy(do.at[:, own_heads, :], raw_do, in_sem.at[3])
    ld_val = pltpu.make_async_copy(valid, valid_all.at[r], in_sem.at[4])
    for cp in (ld_k, ld_v, ld_q, ld_do, ld_val):
        cp.start()

    barrier = pltpu.get_barrier_semaphore()
    for dev in (partner, cross, cross_o):
        pl.semaphore_signal(barrier, inc=1, device_id={"cp": dev}, device_id_type=MESH)
    pl.semaphore_wait(barrier, 3)

    peers = (partner, cross, cross_o)
    push_q = remote(q.at[:, oth_heads, :], far_q, raw_ssem.at[0], raw_rsem.at[0], partner)
    push_do = remote(do.at[:, oth_heads, :], far_do, raw_ssem.at[1], raw_rsem.at[1], partner)
    push_val = [remote(valid, valid_all.at[r], val_ssem.at[i], val_rsem.at[r], dev) for i, dev in enumerate(peers)]

    push_q.start()
    push_do.start()

    def kv_relayout(up):
        def body(i, _):
            t0 = i * 16
            for which, raw in ((0, raw_k), (1, raw_v)):
                rows = jnp.stack([raw[src_row(up, t0 + j, l0)] for j in range(16)])
                kv_hm[:, up, which, pl.ds(pl.multiple_of(t0, 16), 16), :] = jnp.transpose(rows, (1, 0, 2))
            return 0
        lax.fori_loop(0, SLOT // 16, body, 0)

    def kv_push(h, to, both):
        head = (4 * c if to == 1 else 4 * pc) + h
        dev = (partner, cross, cross_o)[to]
        ups = pl.ds(0, 2 if both else 1)
        return remote(kv_hm.at[head, ups], kv_all.at[h, r, ups], kv_ssem.at[to, h], kv_rsem.at[h, r], dev)

    def kv_wait(h, owner, both):
        ups = pl.ds(0, 2 if both else 1)
        remote(kv_hm.at[0, ups], kv_all.at[h, owner, ups], kv_ssem.at[0, h], kv_rsem.at[h, owner], partner).wait_recv()

    ld_k.wait()
    ld_v.wait()
    kv_relayout(0)

    def cross_next(ch, h):
        @pl.when(chip == ch)
        def _():
            for to in (1, 2):
                if h > 0:
                    kv_push(h - 1, to, ch == 1).wait_send()
            for to in (1, 2):
                kv_push(h, to, ch == 1).start()

    cross_next(0, 0)
    kv_relayout(1)
    cross_next(1, 0)
    for h in range(HC):
        kv_push(h, 0, True).start()
    ld_val.wait()
    for cp in push_val:
        cp.start()

    def copy_own(h, _):
        for up in range(2):
            kv_all[h, r, up] = kv_hm[4 * c + h, up]
        return 0
    lax.fori_loop(0, HC, copy_own, 0)

    def q_relayout(oc, from_q, from_do):
        for up, ti in ((0, oc), (1, 3 - oc)):
            def body(i, _):
                t0 = i * 16
                at = pl.ds(pl.multiple_of(t0, 16), 16)
                for raw, dst in ((from_q, qh), (from_do, doh)):
                    rows = jnp.stack([raw[src_row(up, t0 + j, l0)] for j in range(16)])
                    dst[:, ti, :, at, :] = jnp.transpose(rows, (1, 0, 2)).reshape(HC, GROUP, 16, HEAD)
                return 0
            lax.fori_loop(0, SLOT // 16, body, 0)

    ld_q.wait()
    ld_do.wait()
    cross_next(0, 1)
    q_relayout(c, raw_q, raw_do)

    cross_next(0, 2)
    for i in range(3):
        remote(valid, valid_all.at[peers[i]], val_ssem.at[i], val_rsem.at[peers[i]], peers[i]).wait_recv()
    lane = lax.broadcasted_iota(jnp.int32, (SLOT, SLOT), 1)
    sub = lax.broadcasted_iota(jnp.int32, (SLOT, SLOT), 0)
    lane2 = lax.broadcasted_iota(jnp.int32, (SLOT, 2 * SLOT), 1)
    sub2 = lax.broadcasted_iota(jnp.int32, (SLOT, 2 * SLOT), 0)
    same_doc = (lane < l0) == (sub < l0)
    doc_f = jnp.where(lane < l0, 1.0, 0.0)
    doc_s = jnp.where(sub < l0, 1.0, 0.0)
    same_f = jnp.where(doc_f == doc_s, 1.0, 0.0)
    del same_doc

    def cap_body(s, _):
        owner = jnp.where(s < 4, s, 7 - s)
        off = jnp.where(s < 4, 0, 1)
        src_lo = jnp.where(sub2 < l0, sub2, sub2 + l0)
        src_hi = jnp.where(sub2 < l0, sub2 + l0, sub2 + SLOT)
        src = jnp.where(off == 1, src_hi, src_lo)
        row = jnp.broadcast_to(valid_all[owner].astype(F32), (SLOT, 2 * SLOT))
        ok = jnp.sum(jnp.where(src == lane2, row, 0.0), axis=1, keepdims=True)
        caps[s] = jnp.where(same_f * ok > 0.5, BIG, FILL)
        return 0
    lax.fori_loop(0, 8, cap_body, 0)
    for ti in range(4):
        oc, up = TILES[ti]
        s = (7 - (2 * chip + oc)) if up else 2 * chip + oc
        caps[8 + ti] = jnp.where(sub <= lane, caps[s], FILL)

    cross_next(0, 3)
    cross_next(1, 1)
    push_q.wait_recv()
    push_do.wait_recv()
    q_relayout(pc, far_q, far_do)

    def part_copy(h, i, n):
        return remote(dkv_acc.at[h, pl.ds(i, n)], dkv_in.at[h, pl.ds(0, n)], part_ssem.at[h], part_rsem.at[h], cross)

    def res_copy(p, ti, which):
        stage, out = ((o_far, o_out), (dq_far, dq_out))[which]
        dst = out.at[TILES[ti][1], :, pl.ds(pl.multiple_of(16 * c + 8 * p, 8), 8), :]
        return remote(stage.at[p, ti], dst, res_ssem.at[which, p, ti], res_rsem.at[which, p, TILES[ti][1]], partner)

    def dkv_copy(h, ti):
        up = TILES[ti][1]
        return remote(dkv_st.at[h, ti], dkv_out.at[4 * c + h, up], dkv_ssem.at[h, ti], dkv_rsem.at[h, up], partner)

    def res_put(p):
        heads = pl.ds(pl.multiple_of(16 * c + 8 * p, 8), 8)
        for ti, (oc, up) in enumerate(TILES):
            def body(i, _, keep):
                at = pl.ds(pl.multiple_of(i * 16, 16), 16)
                for stage, far, out in ((o_st, o_far, o_out), (dq_st, dq_far, dq_out)):
                    x = jnp.concatenate([stage[e, ti, pl.ds(pl.multiple_of(g * SLOT + i * 16, 16), 16), :][None]
                                         for e in range(2) for g in range(GROUP)], axis=0)
                    y = jnp.transpose(x, (1, 0, 2))
                    if keep:
                        out[up, at, heads, :] = y
                    else:
                        far[p, ti, at, :, :] = y
                return 0

            @pl.when(c == oc)
            def _():
                lax.fori_loop(0, SLOT // 16, functools.partial(body, keep=True), 0)

            @pl.when(c != oc)
            def _():
                lax.fori_loop(0, SLOT // 16, functools.partial(body, keep=False), 0)
                for which in range(2):
                    res_copy(p, ti, which).start()

    def dkv_put(h, ti, parts):
        oc, up = TILES[ti]

        @pl.when(c == oc)
        def _():
            for w in range(2):
                dkv_out[4 * c + h, up, w] = parts(w).astype(BF16)

        @pl.when(c != oc)
        def _():
            for w in range(2):
                dkv_st[h, ti, w] = parts(w).astype(BF16)
            dkv_copy(h, ti).start()

    lse_far = remote(lse_st.at[pc], lse_out.at[:, own_heads, :], lse_sem, lse_rsem, partner)

    def kv_slot(h, s, which):
        return kv_all[h, min(s, 7 - s), int(s > 3), which]

    def kv_slots(h, a, b, which):
        return jnp.concatenate([kv_slot(h, s, which) for s in range(a, b)], axis=0)

    def run_chip(ch):
        slots = [slot_of(ch, ti) for ti in range(4)]
        sent = [0, 1] if ch == 1 else [2, 3, 4, 5]
        kept = [0, 1] if ch == 0 else [2, 3, 4, 5]
        order = [0, 1, 2, 3]

        def transposes(s):
            for src, dst in ((0, kt), (1, vt)):
                dst[:, s * SLOT:(s + 1) * SLOT] = jnp.transpose(kv_slot(h_ref[0], s, src))

        h_ref = [None]

        def head(h, _):
            h_ref[0] = h
            seen = set()
            ready = set()

            def wait_slot(s):
                if s in ready:
                    return
                if s in slots:
                    kv_wait(h, partner, True)
                    new = slots
                elif ch == 1:
                    for owner in (0, 1):
                        kv_wait(h, owner, False)
                    new = [0, 1]
                else:
                    for owner in (2, 3):
                        kv_wait(h, owner, True)
                    new = [2, 3, 4, 5]
                for u in new:
                    ready.add(u)
                    transposes(u)

            for ti in order:
                s = slots[ti]
                nk = s + 1
                if ch == 1 and ti == 1:
                    for nxt in (2, 3):
                        pl.when(h == nxt - 2)(functools.partial(cross_next, 1, nxt))
                for u in range(nk):
                    wait_slot(u)
                qt = qh[h, ti].reshape(TILE, HEAD)
                dt = doh[h, ti].reshape(TILE, HEAD)
                m8 = [None] * GROUP
                for a in range(0, nk, 2):
                    n = min(2, nk - a)
                    kb = kv_slots(h, a, a + n, 0)
                    sc = mm(kb, qt, NT)
                    for j in range(n):
                        cap = caps[8 + ti] if a + j == s else caps[a + j]
                        for g in range(GROUP):
                            x = jnp.minimum(sc[j * SLOT:(j + 1) * SLOT, g * SLOT:(g + 1) * SLOT], cap)
                            st[(a + j) * SLOT:(a + j + 1) * SLOT, g * SLOT:(g + 1) * SLOT] = x
                            top = jnp.max(x.reshape(SLOT // 8, 8, SLOT), axis=0)
                            m8[g] = top if m8[g] is None else jnp.maximum(m8[g], top)
                m = [jnp.max(x, axis=0, keepdims=True) for x in m8]
                mc = [x * C2 for x in m]
                l8 = [None] * GROUP
                for a in range(nk):
                    for g in range(GROUP):
                        at = (slice(a * SLOT, (a + 1) * SLOT), slice(g * SLOT, (g + 1) * SLOT))
                        e = jnp.exp2(st[at] * C2 - mc[g])
                        st[at] = e
                        pb[at] = e.astype(BF16)
                        tot = jnp.sum(e.reshape(SLOT // 8, 8, SLOT), axis=0)
                        l8[g] = tot if l8[g] is None else l8[g] + tot
                ot = mm(vt[:, :nk * SLOT], pb[:nk * SLOT, :], NN)
                inv, dd = [], []
                oc, up = TILES[ti]
                for g in range(GROUP):
                    l = jnp.sum(l8[g], axis=0, keepdims=True)
                    has = m[g] > 0.5 * FILL
                    safe = jnp.where(has, l, 1.0)
                    i_l = jnp.where(has, 1.0 / safe, 0.0)
                    lse = jnp.where(has, m[g] * SCALE + jnp.log(safe), 0.0)
                    lse_st[oc, up, pl.ds(h * GROUP + g, 1), :] = lse
                    og = (ot[:, g * SLOT:(g + 1) * SLOT] * i_l).astype(BF16)
                    dog = jnp.transpose(dt[g * SLOT:(g + 1) * SLOT, :])
                    dd.append(jnp.sum(og.astype(F32) * dog.astype(F32), axis=0, keepdims=True))
                    inv.append(i_l)
                    o_st[h % 2, ti, g * SLOT:(g + 1) * SLOT, :] = jnp.transpose(og)

                first = [u for u in range(nk) if u in sent] if (ch == 0 and ti >= 2) else []
                rest = [u for u in range(nk) if u not in first]
                dqt = None
                for part in (first, rest):
                    runs = []
                    for u in part:
                        if runs and runs[-1][1] == u and u - runs[-1][0] < 2:
                            runs[-1][1] = u + 1
                        else:
                            runs.append([u, u + 1])
                    for a, b in runs:
                        n = b - a
                        vb = kv_slots(h, a, b, 1)
                        dp = mm(vb, dt, NT)
                        for j in range(n):
                            for g in range(GROUP):
                                at = (slice((a + j) * SLOT, (a + j + 1) * SLOT), slice(g * SLOT, (g + 1) * SLOT))
                                p = st[at] * inv[g]
                                pb[at] = p.astype(BF16)
                                ds = p * (dp[j * SLOT:(j + 1) * SLOT, g * SLOT:(g + 1) * SLOT] - dd[g])
                                db[at] = ds.astype(BF16)
                        dsb = db[a * SLOT:b * SLOT, :]
                        dv = mm(pb[a * SLOT:b * SLOT, :], dt, NN)
                        dk = mm(dsb, qt, NN) * SCALE
                        dq = mm(kt[:, a * SLOT:b * SLOT], dsb, NN)
                        dqt = dq if dqt is None else dqt + dq
                        for j in range(n):
                            u = a + j
                            new = (dk[j * SLOT:(j + 1) * SLOT], dv[j * SLOT:(j + 1) * SLOT])
                            for w in range(2):
                                dkv_acc[h, u, w] = dkv_acc[h, u, w] + new[w] if u in seen else new[w]
                            seen.add(u)
                    if part is first and ti == 3 and ch == 0:
                        part_copy(h, sent[0], len(sent)).start()
                for g in range(GROUP):
                    dqg = (dqt[:, g * SLOT:(g + 1) * SLOT] * SCALE).astype(BF16)
                    dq_st[h % 2, ti, g * SLOT:(g + 1) * SLOT, :] = jnp.transpose(dqg)
            if ch == 1:
                part_copy(h, sent[0], len(sent)).start()
            else:
                for ti in (2, 3):
                    dkv_put(h, ti, lambda w, ti=ti: dkv_acc[h, slots[ti], w])
            pl.when(h % 2 == 1)(lambda: res_put(h // 2))
            return 0

        lax.fori_loop(0, HC, head, 0)

        lse_out[:, own_heads, :] = lse_st[c]
        lse_far.start()

        def tail(h, _):
            part_copy(h, kept[0], len(kept)).wait_recv()
            for i, u in enumerate(kept):
                ti = slots.index(u)
                dkv_put(h, ti, lambda w, u=u, i=i: dkv_acc[h, u, w] + dkv_in[h, i, w])
            return 0
        lax.fori_loop(0, HC, tail, 0)

        def drain(h, _):
            part_copy(h, sent[0], len(sent)).wait_send()
            return 0
        lax.fori_loop(0, HC, drain, 0)

    pl.when(chip == 0)(functools.partial(run_chip, 0))
    pl.when(chip == 1)(functools.partial(run_chip, 1))

    push_q.wait_send()
    push_do.wait_send()
    for cp in push_val:
        cp.wait_send()

    def drain(h, _):
        kv_push(h, 0, True).wait_send()
        for ch in range(2):
            @pl.when(chip == ch)
            def _():
                for to in (1, 2):
                    pl.when(h == HC - 1)(kv_push(h, to, ch == 1).wait_send)
        for ti in range(4):
            pl.when(c != TILES[ti][0])(dkv_copy(h, ti).wait_send)
        for up in range(2):
            remote(dkv_st.at[h, 0], dkv_out.at[4 * pc + h, up], dkv_ssem.at[h, 0], dkv_rsem.at[h, up], partner).wait_recv()
        return 0
    lax.fori_loop(0, HC, drain, 0)

    for p in range(2):
        for which in range(2):
            stage, out = ((o_far, o_out), (dq_far, dq_out))[which]
            for ti in range(4):
                pl.when(c != TILES[ti][0])(res_copy(p, ti, which).wait_send)
            for up in range(2):
                dst = out.at[up, :, pl.ds(pl.multiple_of(16 * pc + 8 * p, 8), 8), :]
                remote(stage.at[p, 0], dst, res_ssem.at[which, p, 0], res_rsem.at[which, p, up], partner).wait_recv()
    lse_far.wait_send()
    remote(lse_st.at[0], lse_out.at[:, oth_heads, :], lse_sem, lse_rsem, partner).wait_recv()


def attn_call(cu, valid, q, k, v, do):
    any_spec = pl.BlockSpec(memory_space=pl.ANY)
    dma = pltpu.SemaphoreType.DMA
    return pl.pallas_call(
        attn_kernel,
        out_shape=(
            pltpu.VMEM((2, SLOT, 32, HEAD), BF16),
            pltpu.VMEM((2, SLOT, 32, HEAD), BF16),
            pltpu.VMEM((8, 2, 2, SLOT, HEAD), BF16),
            pltpu.VMEM((2, 32, SLOT), F32),
        ),
        in_specs=[pl.BlockSpec(memory_space=pltpu.SMEM)] + [any_spec] * 5,
        out_specs=(pl.BlockSpec(memory_space=pltpu.VMEM),) * 4,
        scratch_shapes=[
            pltpu.VMEM((256, 16, HEAD), BF16),
            pltpu.VMEM((256, 16, HEAD), BF16),
            pltpu.VMEM((256, 16, HEAD), BF16),
            pltpu.VMEM((256, 16, HEAD), BF16),
            pltpu.VMEM((256, 8, HEAD), BF16),
            pltpu.VMEM((256, 8, HEAD), BF16),
            pltpu.VMEM((8, 2, 2, SLOT, HEAD), BF16),
            pltpu.VMEM((HC, 4, 2, 2, SLOT, HEAD), BF16),
            pltpu.VMEM((HEAD, 8 * SLOT), BF16),
            pltpu.VMEM((HEAD, 8 * SLOT), BF16),
            pltpu.VMEM((HC, 4, GROUP, SLOT, HEAD), BF16),
            pltpu.VMEM((HC, 4, GROUP, SLOT, HEAD), BF16),
            pltpu.VMEM((8 * SLOT, TILE), F32),
            pltpu.VMEM((8 * SLOT, TILE), BF16),
            pltpu.VMEM((8 * SLOT, TILE), BF16),
            pltpu.VMEM((HC, 8, 2, SLOT, HEAD), F32),
            pltpu.VMEM((HC, 4, 2, SLOT, HEAD), F32),
            pltpu.VMEM((2, 4, TILE, HEAD), BF16),
            pltpu.VMEM((2, 4, TILE, HEAD), BF16),
            pltpu.VMEM((2, 4, SLOT, 8, HEAD), BF16),
            pltpu.VMEM((2, 4, SLOT, 8, HEAD), BF16),
            pltpu.VMEM((HC, 4, 2, SLOT, HEAD), BF16),
            pltpu.VMEM((2, 2, 16, SLOT), F32),
            pltpu.VMEM((12, SLOT, SLOT), F32),
            pltpu.VMEM((4, 1, 2 * SLOT), jnp.int32),
            dma((5,)),
            dma((2,)), dma((2,)),
            dma((3,)), dma((4,)),
            dma((3, HC)), dma((HC, 4)),
            dma((HC,)), dma((HC,)),
            dma((2, 2, 4)), dma((2, 2, 2)),
            dma((HC, 4)), dma((HC, 2)),
            dma, dma,
        ],
        compiler_params=pltpu.CompilerParams(collective_id=0, has_side_effects=True, vmem_limit_bytes=61300000),
        name="attn",
    )(cu, valid, q, k, v, do)


def finish_kernel(cu, o_in, dq_in, dkv_in, lse_in, o_out, dq_out, dk_out, dv_out, lse_out, dk_t, dv_t, sem):
    l0 = lax.shift_right_logical(cu[1], 3)
    rest = SLOT - l0

    def copies(i, x, out):
        runs = ((0, 0, 0, l0), (1, 0, l0, l0), (0, l0, 2 * l0, rest), (1, l0, SLOT + l0, rest))
        return [pltpu.make_async_copy(x.at[up, pl.ds(at, n)], out.at[pl.ds(to, n)], sem.at[i, j])
                for j, (up, at, to, n) in enumerate(runs)]

    moves = copies(0, o_in, o_out) + copies(1, dq_in, dq_out)
    for cp in moves:
        cp.start()

    for w, dst in ((0, dk_t), (1, dv_t)):
        for up in range(2):
            def body(i, _):
                at = pl.ds(pl.multiple_of(i * 16, 16), 16)
                dst[up, at] = jnp.transpose(dkv_in[:, up, w, at, :], (1, 0, 2))
                return 0
            lax.fori_loop(0, SLOT // 16, body, 0)
        more = copies(2 + w, dst, (dk_out, dv_out)[w])
        for cp in more:
            cp.start()
        moves += more

    row = lax.broadcasted_iota(jnp.int32, (2 * SLOT, SLOT), 0)
    col = lax.broadcasted_iota(jnp.int32, (2 * SLOT, SLOT), 1)
    acc = None
    for up in range(2):
        if up:
            src = jnp.where(col < l0, col + l0, col + SLOT)
        else:
            src = jnp.where(col < l0, col, col + l0)
        pick = jnp.where(row == src, 1.0, 0.0)
        part = lax.dot_general(lse_in[up], pick, NT, precision=lax.Precision.HIGHEST, preferred_element_type=F32)
        acc = part if acc is None else acc + part
    lse_out[...] = acc
    for cp in moves:
        cp.wait()


def finish_call(cu, o_t, dq_t, dkv_hm, lse_hm):
    any_spec = pl.BlockSpec(memory_space=pl.ANY)
    vmem = pl.BlockSpec(memory_space=pltpu.VMEM)
    return pl.pallas_call(
        finish_kernel,
        out_shape=(
            jax.ShapeDtypeStruct((256, 32, HEAD), BF16),
            jax.ShapeDtypeStruct((256, 32, HEAD), BF16),
            jax.ShapeDtypeStruct((256, 8, HEAD), BF16),
            jax.ShapeDtypeStruct((256, 8, HEAD), BF16),
            jax.ShapeDtypeStruct((32, 256), F32),
        ),
        in_specs=[pl.BlockSpec(memory_space=pltpu.SMEM)] + [vmem] * 4,
        out_specs=(any_spec,) * 4 + (vmem,),
        scratch_shapes=[
            pltpu.VMEM((2, SLOT, 8, HEAD), BF16),
            pltpu.VMEM((2, SLOT, 8, HEAD), BF16),
            pltpu.SemaphoreType.DMA((4, 4)),
        ],
        compiler_params=pltpu.CompilerParams(vmem_limit_bytes=16 * 1024 * 1024),
        name="finish",
    )(cu, o_t, dq_t, dkv_hm, lse_hm)


def solution(mesh):
    tok_spec = P(("dp", "cp"), None, None)
    lse_spec = P(("dp", "cp"), None)

    def local(q, k, v, do, valid, cu):
        res = attn_call(cu, valid.reshape(1, 256), q, k, v, do)
        o, dq, dk, dv, lse = finish_call(cu, *res)
        return o, lse.T, dq, dk, dv

    return jax.shard_map(local, mesh=mesh, in_specs=(tok_spec,) * 4 + (P(("dp", "cp")), P("dp")),
                         out_specs=(tok_spec, lse_spec, tok_spec, tok_spec, tok_spec), check_vma=False)
```

```python
import functools
import math

import jax
import jax.numpy as jnp
from jax import lax
from jax.experimental import pallas as pl
from jax.experimental.pallas import tpu as pltpu
from jax.sharding import PartitionSpec as P

MESH = pl.DeviceIdType.MESH
FILL = -1.0e30
BIG = 3.0e38
HEAD = 128
SLOT = 128
TILE = 512
GROUP = 4
HC = 4
SWAP = 2
SCALE = HEAD ** -0.5
C2 = SCALE * math.log2(math.e)
NT = (((1,), (1,)), ((), ()))
NN = (((1,), (0,)), ((), ()))
F32 = jnp.float32
BF16 = jnp.bfloat16

TILES = ((0, 0), (1, 0), (1, 1), (0, 1))


def slot_of(chip, ti):
    oc, up = TILES[ti]
    r = 2 * chip + oc
    return 7 - r if up else r


def mm(a, b, dims):
    return lax.dot_general(a, b, dims, preferred_element_type=F32)


def src_row(up, t, l0):
    if up:
        return jnp.where(t < l0, t + l0, t + SLOT)
    return jnp.where(t < l0, t, t + l0)


def attn_kernel(cu, valid, q, k, v, do, o_out, dq_out, dkv_out, lse_out,
                raw_q, raw_do, far_q, far_do, raw_k, raw_v, kv_hm, kv_all, kt, vt, qh, doh, st, pb, db,
                dkv_acc, dkv_in, o_st, dq_st, o_far, dq_far, dkv_st, back_st, lse_st, caps, valid_all,
                in_sem, raw_ssem, raw_rsem, val_ssem, val_rsem, kv_ssem, kv_rsem,
                part_ssem, part_rsem, swap_ssem, swap_rsem, back_ssem, back_rsem, res_ssem, res_rsem, dkv_ssem, dkv_rsem, lse_sem, lse_rsem):
    r = lax.axis_index("cp")
    chip = r // 2
    c = r % 2
    pc = 1 - c
    partner = chip * 2 + pc
    cross = (1 - chip) * 2 + c
    cross_o = (1 - chip) * 2 + pc
    l0 = lax.shift_right_logical(cu[1], 3)

    def remote(src, dst, ssem, rsem, dev):
        return pltpu.make_async_remote_copy(src_ref=src, dst_ref=dst, send_sem=ssem, recv_sem=rsem,
                                            device_id={"cp": dev}, device_id_type=MESH)

    own_heads = pl.ds(pl.multiple_of(16 * c, 16), 16)
    oth_heads = pl.ds(pl.multiple_of(16 * pc, 16), 16)
    ld_k = pltpu.make_async_copy(k, raw_k, in_sem.at[0])
    ld_v = pltpu.make_async_copy(v, raw_v, in_sem.at[1])
    ld_q = pltpu.make_async_copy(q.at[:, own_heads, :], raw_q, in_sem.at[2])
    ld_do = pltpu.make_async_copy(do.at[:, own_heads, :], raw_do, in_sem.at[3])
    ld_val = pltpu.make_async_copy(valid, valid_all.at[r], in_sem.at[4])
    for cp in (ld_k, ld_v, ld_q, ld_do, ld_val):
        cp.start()

    barrier = pltpu.get_barrier_semaphore()
    for dev in (partner, cross, cross_o):
        pl.semaphore_signal(barrier, inc=1, device_id={"cp": dev}, device_id_type=MESH)
    pl.semaphore_wait(barrier, 3)

    peers = (partner, cross, cross_o)
    push_q = remote(q.at[:, oth_heads, :], far_q, raw_ssem.at[0], raw_rsem.at[0], partner)
    push_do = remote(do.at[:, oth_heads, :], far_do, raw_ssem.at[1], raw_rsem.at[1], partner)
    push_val = [remote(valid, valid_all.at[r], val_ssem.at[i], val_rsem.at[r], dev) for i, dev in enumerate(peers)]

    push_q.start()
    push_do.start()

    def kv_relayout(up):
        def body(i, _):
            t0 = i * 16
            for which, raw in ((0, raw_k), (1, raw_v)):
                rows = jnp.stack([raw[src_row(up, t0 + j, l0)] for j in range(16)])
                kv_hm[:, up, which, pl.ds(pl.multiple_of(t0, 16), 16), :] = jnp.transpose(rows, (1, 0, 2))
            return 0
        lax.fori_loop(0, SLOT // 16, body, 0)

    def kv_push(h, to, both):
        head = (4 * c if to == 1 else 4 * pc) + h
        dev = (partner, cross, cross_o)[to]
        ups = pl.ds(0, 2 if both else 1)
        return remote(kv_hm.at[head, ups], kv_all.at[h, r, ups], kv_ssem.at[to, h], kv_rsem.at[h, r], dev)

    def kv_wait(h, owner, both):
        ups = pl.ds(0, 2 if both else 1)
        remote(kv_hm.at[0, ups], kv_all.at[h, owner, ups], kv_ssem.at[0, h], kv_rsem.at[h, owner], partner).wait_recv()

    ld_k.wait()
    ld_v.wait()
    kv_relayout(0)

    def cross_next(ch, h, upto=None):
        @pl.when(chip == ch)
        def _():
            for to in (1, 2):
                if h > 0:
                    kv_push(h - 1, to, ch == 1).wait_send()
            for e in range(h, upto or h + 1):
                for to in (1, 2):
                    kv_push(e, to, ch == 1).start()

    cross_next(0, 0)
    kv_relayout(1)
    cross_next(1, 0)
    for h in range(HC):
        kv_push(h, 0, True).start()
    ld_val.wait()
    for cp in push_val:
        cp.start()

    def copy_own(h, _):
        for up in range(2):
            kv_all[h, r, up] = kv_hm[4 * c + h, up]
        return 0
    lax.fori_loop(0, HC, copy_own, 0)

    def q_relayout(oc, from_q, from_do):
        for up, ti in ((0, oc), (1, 3 - oc)):
            def body(i, _):
                t0 = i * 16
                at = pl.ds(pl.multiple_of(t0, 16), 16)
                for raw, dst in ((from_q, qh), (from_do, doh)):
                    rows = jnp.stack([raw[src_row(up, t0 + j, l0)] for j in range(16)])
                    dst[:, ti, :, at, :] = jnp.transpose(rows, (1, 0, 2)).reshape(HC, GROUP, 16, HEAD)
                return 0
            lax.fori_loop(0, SLOT // 16, body, 0)

    ld_q.wait()
    ld_do.wait()
    cross_next(0, 1, HC)
    q_relayout(c, raw_q, raw_do)

    for i in range(3):
        remote(valid, valid_all.at[peers[i]], val_ssem.at[i], val_rsem.at[peers[i]], peers[i]).wait_recv()
    lane = lax.broadcasted_iota(jnp.int32, (SLOT, SLOT), 1)
    sub = lax.broadcasted_iota(jnp.int32, (SLOT, SLOT), 0)
    lane2 = lax.broadcasted_iota(jnp.int32, (SLOT, 2 * SLOT), 1)
    sub2 = lax.broadcasted_iota(jnp.int32, (SLOT, 2 * SLOT), 0)
    same_doc = (lane < l0) == (sub < l0)
    doc_f = jnp.where(lane < l0, 1.0, 0.0)
    doc_s = jnp.where(sub < l0, 1.0, 0.0)
    same_f = jnp.where(doc_f == doc_s, 1.0, 0.0)
    del same_doc

    def cap_body(s, _):
        owner = jnp.where(s < 4, s, 7 - s)
        off = jnp.where(s < 4, 0, 1)
        src_lo = jnp.where(sub2 < l0, sub2, sub2 + l0)
        src_hi = jnp.where(sub2 < l0, sub2 + l0, sub2 + SLOT)
        src = jnp.where(off == 1, src_hi, src_lo)
        row = jnp.broadcast_to(valid_all[owner].astype(F32), (SLOT, 2 * SLOT))
        ok = jnp.sum(jnp.where(src == lane2, row, 0.0), axis=1, keepdims=True)
        caps[s] = jnp.where(same_f * ok > 0.5, BIG, FILL)
        return 0
    lax.fori_loop(0, 8, cap_body, 0)
    for ti in range(4):
        oc, up = TILES[ti]
        s = (7 - (2 * chip + oc)) if up else 2 * chip + oc
        caps[8 + ti] = jnp.where(sub <= lane, caps[s], FILL)

    cross_next(1, 1)
    push_q.wait_recv()
    push_do.wait_recv()
    q_relayout(pc, far_q, far_do)

    def part_copy(h, i, n):
        return remote(dkv_acc.at[h, pl.ds(i, n)], dkv_in.at[h, pl.ds(0, n)], part_ssem.at[h], part_rsem.at[h], cross)

    def part_run(ch, h, act):
        if ch == 1:
            act(part_copy(h, 0, 2))
        else:
            pl.when(h < SWAP)(lambda: act(part_copy(h, 2, 3)))
            pl.when(h >= SWAP)(lambda: act(part_copy(h, 2, 4)))

    def swap_copy(h):
        return remote(dkv_acc.at[h, 5], dkv_in.at[h, 2], swap_ssem.at[h], swap_rsem.at[h], cross)

    def swap_back(h):
        return remote(back_st.at[h], dkv_out.at[4 * c + h, 1], back_ssem.at[h], back_rsem.at[4 * c + h], 2)

    def res_copy(p, ti, which):
        stage, out = ((o_far, o_out), (dq_far, dq_out))[which]
        dst = out.at[TILES[ti][1], :, pl.ds(pl.multiple_of(16 * c + 8 * p, 8), 8), :]
        return remote(stage.at[p, ti], dst, res_ssem.at[which, p, ti], res_rsem.at[which, p, TILES[ti][1]], partner)

    def dkv_copy(h, ti):
        up = TILES[ti][1]
        return remote(dkv_st.at[h, ti], dkv_out.at[4 * c + h, up], dkv_ssem.at[h, ti], dkv_rsem.at[h, up], partner)

    def res_put(p):
        heads = pl.ds(pl.multiple_of(16 * c + 8 * p, 8), 8)
        for ti, (oc, up) in enumerate(TILES):
            def body(i, _, keep):
                at = pl.ds(pl.multiple_of(i * 16, 16), 16)
                for stage, far, out in ((o_st, o_far, o_out), (dq_st, dq_far, dq_out)):
                    x = jnp.concatenate([stage[e, ti, pl.ds(pl.multiple_of(g * SLOT + i * 16, 16), 16), :][None]
                                         for e in range(2) for g in range(GROUP)], axis=0)
                    y = jnp.transpose(x, (1, 0, 2))
                    if keep:
                        out[up, at, heads, :] = y
                    else:
                        far[p, ti, at, :, :] = y
                return 0

            @pl.when(c == oc)
            def _():
                lax.fori_loop(0, SLOT // 16, functools.partial(body, keep=True), 0)

            @pl.when(c != oc)
            def _():
                lax.fori_loop(0, SLOT // 16, functools.partial(body, keep=False), 0)
                for which in range(2):
                    res_copy(p, ti, which).start()

    def dkv_put(h, ti, parts):
        oc, up = TILES[ti]

        @pl.when(c == oc)
        def _():
            for w in range(2):
                dkv_out[4 * c + h, up, w] = parts(w).astype(BF16)

        @pl.when(c != oc)
        def _():
            for w in range(2):
                dkv_st[h, ti, w] = parts(w).astype(BF16)
            dkv_copy(h, ti).start()

    lse_far = remote(lse_st.at[pc], lse_out.at[:, own_heads, :], lse_sem, lse_rsem, partner)

    def kv_slot(h, s, which):
        return kv_all[h, min(s, 7 - s), int(s > 3), which]

    def kv_slots(h, a, b, which):
        return jnp.concatenate([kv_slot(h, s, which) for s in range(a, b)], axis=0)

    def run_chip(ch):
        slots = [slot_of(ch, ti) for ti in range(4)]
        sent = [0, 1] if ch == 1 else [2, 3, 4, 5]
        kept = [0, 1] if ch == 0 else [2, 3, 4, 5]
        order = [0, 1, 2, 3]

        def transposes(s):
            for src, dst in ((0, kt), (1, vt)):
                dst[:, s * SLOT:(s + 1) * SLOT] = jnp.transpose(kv_slot(h_ref[0], s, src))

        h_ref = [None]

        def head(h, _):
            h_ref[0] = h
            seen = set()
            ready = set()

            def wait_slot(s):
                if s in ready:
                    return
                if s in slots:
                    kv_wait(h, partner, True)
                    new = slots
                elif ch == 1:
                    for owner in (0, 1):
                        kv_wait(h, owner, False)
                    new = [0, 1]
                else:
                    for owner in (2, 3):
                        kv_wait(h, owner, True)
                    new = [2, 3, 4, 5]
                for u in new:
                    ready.add(u)
                    transposes(u)

            for ti in order:
                s = slots[ti]
                nk = s + 1
                if ch == 1 and ti == 1:
                    for nxt in (2, 3):
                        pl.when(h == nxt - 2)(functools.partial(cross_next, 1, nxt))
                for u in range(nk):
                    wait_slot(u)
                qt = qh[h, ti].reshape(TILE, HEAD)
                dt = doh[h, ti].reshape(TILE, HEAD)
                m8 = [None] * GROUP
                for a in range(0, nk, 2):
                    n = min(2, nk - a)
                    kb = kv_slots(h, a, a + n, 0)
                    sc = mm(kb, qt, NT)
                    for j in range(n):
                        cap = caps[8 + ti] if a + j == s else caps[a + j]
                        for g in range(GROUP):
                            x = jnp.minimum(sc[j * SLOT:(j + 1) * SLOT, g * SLOT:(g + 1) * SLOT], cap)
                            st[(a + j) * SLOT:(a + j + 1) * SLOT, g * SLOT:(g + 1) * SLOT] = x
                            top = jnp.max(x.reshape(SLOT // 8, 8, SLOT), axis=0)
                            m8[g] = top if m8[g] is None else jnp.maximum(m8[g], top)
                m = [jnp.max(x, axis=0, keepdims=True) for x in m8]
                mc = [x * C2 for x in m]
                l8 = [None] * GROUP
                for a in range(nk):
                    for g in range(GROUP):
                        at = (slice(a * SLOT, (a + 1) * SLOT), slice(g * SLOT, (g + 1) * SLOT))
                        e = jnp.exp2(st[at] * C2 - mc[g])
                        st[at] = e
                        pb[at] = e.astype(BF16)
                        tot = jnp.sum(e.reshape(SLOT // 8, 8, SLOT), axis=0)
                        l8[g] = tot if l8[g] is None else l8[g] + tot
                ot = mm(vt[:, :nk * SLOT], pb[:nk * SLOT, :], NN)
                inv, dd = [], []
                oc, up = TILES[ti]
                for g in range(GROUP):
                    l = jnp.sum(l8[g], axis=0, keepdims=True)
                    has = m[g] > 0.5 * FILL
                    safe = jnp.where(has, l, 1.0)
                    i_l = jnp.where(has, 1.0 / safe, 0.0)
                    lse = jnp.where(has, m[g] * SCALE + jnp.log(safe), 0.0)
                    lse_st[oc, up, pl.ds(h * GROUP + g, 1), :] = lse
                    og = (ot[:, g * SLOT:(g + 1) * SLOT] * i_l).astype(BF16)
                    dog = jnp.transpose(dt[g * SLOT:(g + 1) * SLOT, :])
                    dd.append(jnp.sum(og.astype(F32) * dog.astype(F32), axis=0, keepdims=True))
                    inv.append(i_l)
                    o_st[h % 2, ti, g * SLOT:(g + 1) * SLOT, :] = jnp.transpose(og)

                first = [u for u in range(nk) if u in sent] if (ch == 0 and ti >= 2) else []
                rest = [u for u in range(nk) if u not in first]
                dqt = None
                for part in (first, rest):
                    runs = []
                    for u in part:
                        if runs and runs[-1][1] == u and u - runs[-1][0] < 2:
                            runs[-1][1] = u + 1
                        else:
                            runs.append([u, u + 1])
                    for a, b in runs:
                        n = b - a
                        vb = kv_slots(h, a, b, 1)
                        dp = mm(vb, dt, NT)
                        for j in range(n):
                            for g in range(GROUP):
                                at = (slice((a + j) * SLOT, (a + j + 1) * SLOT), slice(g * SLOT, (g + 1) * SLOT))
                                p = st[at] * inv[g]
                                pb[at] = p.astype(BF16)
                                ds = p * (dp[j * SLOT:(j + 1) * SLOT, g * SLOT:(g + 1) * SLOT] - dd[g])
                                db[at] = ds.astype(BF16)
                        dsb = db[a * SLOT:b * SLOT, :]
                        dv = mm(pb[a * SLOT:b * SLOT, :], dt, NN)
                        dk = mm(dsb, qt, NN) * SCALE
                        dq = mm(kt[:, a * SLOT:b * SLOT], dsb, NN)
                        dqt = dq if dqt is None else dqt + dq
                        for j in range(n):
                            u = a + j
                            new = (dk[j * SLOT:(j + 1) * SLOT], dv[j * SLOT:(j + 1) * SLOT])
                            for w in range(2):
                                dkv_acc[h, u, w] = dkv_acc[h, u, w] + new[w] if u in seen else new[w]
                            seen.add(u)
                    if part is first and ti == 3 and ch == 0:
                        part_run(0, h, lambda cp: cp.start())
                for g in range(GROUP):
                    dqg = (dqt[:, g * SLOT:(g + 1) * SLOT] * SCALE).astype(BF16)
                    dq_st[h % 2, ti, g * SLOT:(g + 1) * SLOT, :] = jnp.transpose(dqg)
            if ch == 1:
                part_run(1, h, lambda cp: cp.start())
                pl.when(h < SWAP)(lambda: swap_copy(h).start())
            else:
                for ti in (2, 3):
                    dkv_put(h, ti, lambda w, ti=ti: dkv_acc[h, slots[ti], w])
            pl.when(h % 2 == 1)(lambda: res_put(h // 2))
            return 0

        lax.fori_loop(0, HC, head, 0)

        lse_out[:, own_heads, :] = lse_st[c]
        lse_far.start()

        if ch == 0:
            def swapped(h, _):
                swap_copy(h).wait_recv()
                for w in range(2):
                    back_st[h, w] = (dkv_in[h, 2, w] + dkv_acc[h, 5, w]).astype(BF16)
                swap_back(h).start()
                return 0
            lax.fori_loop(0, SWAP, swapped, 0)

        def tail(h, _):
            part_run(1 - ch, h, lambda cp: cp.wait_recv())
            for i, u in enumerate(kept):
                ti = slots.index(u)
                put = functools.partial(dkv_put, h, ti, lambda w, u=u, i=i: dkv_acc[h, u, w] + dkv_in[h, i, w])
                if u == 5:
                    pl.when(h >= SWAP)(put)
                else:
                    put()
            return 0
        lax.fori_loop(0, HC, tail, 0)

        def drain(h, _):
            part_run(ch, h, lambda cp: cp.wait_send())
            return 0
        lax.fori_loop(0, HC, drain, 0)

        def drain_swap(h, _):
            if ch == 0:
                swap_back(h).wait_send()
            else:
                swap_copy(h).wait_send()
            return 0
        lax.fori_loop(0, SWAP, drain_swap, 0)

        if ch == 1:
            @pl.when(c == 0)
            def _():
                for core in range(2):
                    for h in range(SWAP):
                        remote(back_st.at[h], dkv_out.at[4 * core + h, 1], back_ssem.at[h], back_rsem.at[4 * core + h], 2).wait_recv()

    pl.when(chip == 0)(functools.partial(run_chip, 0))
    pl.when(chip == 1)(functools.partial(run_chip, 1))

    push_q.wait_send()
    push_do.wait_send()
    for cp in push_val:
        cp.wait_send()

    def drain(h, _):
        kv_push(h, 0, True).wait_send()
        for ch in range(2):
            @pl.when(chip == ch)
            def _():
                for to in (1, 2):
                    pl.when((h == HC - 1) if ch == 1 else (h > 0))(kv_push(h, to, ch == 1).wait_send)
        far = jnp.logical_and(chip == 1, h < SWAP)
        for ti in range(4):
            sent = c != TILES[ti][0]
            pl.when(jnp.logical_and(sent, jnp.logical_not(far)) if ti == 3 else sent)(dkv_copy(h, ti).wait_send)
        for up in range(2):
            come = remote(dkv_st.at[h, 0], dkv_out.at[4 * pc + h, up], dkv_ssem.at[h, 0], dkv_rsem.at[h, up], partner)
            if up:
                pl.when(jnp.logical_not(jnp.logical_and(far, c == 0)))(come.wait_recv)
            else:
                come.wait_recv()
        return 0
    lax.fori_loop(0, HC, drain, 0)

    for p in range(2):
        for which in range(2):
            stage, out = ((o_far, o_out), (dq_far, dq_out))[which]
            for ti in range(4):
                pl.when(c != TILES[ti][0])(res_copy(p, ti, which).wait_send)
            for up in range(2):
                dst = out.at[up, :, pl.ds(pl.multiple_of(16 * pc + 8 * p, 8), 8), :]
                remote(stage.at[p, 0], dst, res_ssem.at[which, p, 0], res_rsem.at[which, p, up], partner).wait_recv()
    lse_far.wait_send()
    remote(lse_st.at[0], lse_out.at[:, oth_heads, :], lse_sem, lse_rsem, partner).wait_recv()


def attn_call(cu, valid, q, k, v, do):
    any_spec = pl.BlockSpec(memory_space=pl.ANY)
    dma = pltpu.SemaphoreType.DMA
    return pl.pallas_call(
        attn_kernel,
        out_shape=(
            pltpu.VMEM((2, SLOT, 32, HEAD), BF16),
            pltpu.VMEM((2, SLOT, 32, HEAD), BF16),
            pltpu.VMEM((8, 2, 2, SLOT, HEAD), BF16),
            pltpu.VMEM((2, 32, SLOT), F32),
        ),
        in_specs=[pl.BlockSpec(memory_space=pltpu.SMEM)] + [any_spec] * 5,
        out_specs=(pl.BlockSpec(memory_space=pltpu.VMEM),) * 4,
        scratch_shapes=[
            pltpu.VMEM((256, 16, HEAD), BF16),
            pltpu.VMEM((256, 16, HEAD), BF16),
            pltpu.VMEM((256, 16, HEAD), BF16),
            pltpu.VMEM((256, 16, HEAD), BF16),
            pltpu.VMEM((256, 8, HEAD), BF16),
            pltpu.VMEM((256, 8, HEAD), BF16),
            pltpu.VMEM((8, 2, 2, SLOT, HEAD), BF16),
            pltpu.VMEM((HC, 4, 2, 2, SLOT, HEAD), BF16),
            pltpu.VMEM((HEAD, 8 * SLOT), BF16),
            pltpu.VMEM((HEAD, 8 * SLOT), BF16),
            pltpu.VMEM((HC, 4, GROUP, SLOT, HEAD), BF16),
            pltpu.VMEM((HC, 4, GROUP, SLOT, HEAD), BF16),
            pltpu.VMEM((8 * SLOT, TILE), F32),
            pltpu.VMEM((8 * SLOT, TILE), BF16),
            pltpu.VMEM((8 * SLOT, TILE), BF16),
            pltpu.VMEM((HC, 8, 2, SLOT, HEAD), F32),
            pltpu.VMEM((HC, 4, 2, SLOT, HEAD), F32),
            pltpu.VMEM((2, 4, TILE, HEAD), BF16),
            pltpu.VMEM((2, 4, TILE, HEAD), BF16),
            pltpu.VMEM((2, 4, SLOT, 8, HEAD), BF16),
            pltpu.VMEM((2, 4, SLOT, 8, HEAD), BF16),
            pltpu.VMEM((HC, 4, 2, SLOT, HEAD), BF16),
            pltpu.VMEM((HC, 2, SLOT, HEAD), BF16),
            pltpu.VMEM((2, 2, 16, SLOT), F32),
            pltpu.VMEM((12, SLOT, SLOT), F32),
            pltpu.VMEM((4, 1, 2 * SLOT), jnp.int32),
            dma((5,)),
            dma((2,)), dma((2,)),
            dma((3,)), dma((4,)),
            dma((3, HC)), dma((HC, 4)),
            dma((HC,)), dma((HC,)),
            dma((HC,)), dma((HC,)), dma((HC,)), dma((8,)),
            dma((2, 2, 4)), dma((2, 2, 2)),
            dma((HC, 4)), dma((HC, 2)),
            dma, dma,
        ],
        compiler_params=pltpu.CompilerParams(collective_id=0, has_side_effects=True, vmem_limit_bytes=61300000),
        name="attn",
    )(cu, valid, q, k, v, do)


def finish_kernel(cu, o_in, dq_in, dkv_in, lse_in, o_out, dq_out, dk_out, dv_out, lse_out, dk_t, dv_t, sem):
    l0 = lax.shift_right_logical(cu[1], 3)
    rest = SLOT - l0

    def copies(i, x, out):
        runs = ((0, 0, 0, l0), (1, 0, l0, l0), (0, l0, 2 * l0, rest), (1, l0, SLOT + l0, rest))
        return [pltpu.make_async_copy(x.at[up, pl.ds(at, n)], out.at[pl.ds(to, n)], sem.at[i, j])
                for j, (up, at, to, n) in enumerate(runs)]

    moves = copies(0, o_in, o_out) + copies(1, dq_in, dq_out)
    for cp in moves:
        cp.start()

    for w, dst in ((0, dk_t), (1, dv_t)):
        for up in range(2):
            def body(i, _):
                at = pl.ds(pl.multiple_of(i * 16, 16), 16)
                dst[up, at] = jnp.transpose(dkv_in[:, up, w, at, :], (1, 0, 2))
                return 0
            lax.fori_loop(0, SLOT // 16, body, 0)
        more = copies(2 + w, dst, (dk_out, dv_out)[w])
        for cp in more:
            cp.start()
        moves += more

    row = lax.broadcasted_iota(jnp.int32, (2 * SLOT, SLOT), 0)
    col = lax.broadcasted_iota(jnp.int32, (2 * SLOT, SLOT), 1)
    acc = None
    for up in range(2):
        if up:
            src = jnp.where(col < l0, col + l0, col + SLOT)
        else:
            src = jnp.where(col < l0, col, col + l0)
        pick = jnp.where(row == src, 1.0, 0.0)
        part = lax.dot_general(lse_in[up], pick, NT, precision=lax.Precision.HIGHEST, preferred_element_type=F32)
        acc = part if acc is None else acc + part
    lse_out[...] = acc
    for cp in moves:
        cp.wait()


def finish_call(cu, o_t, dq_t, dkv_hm, lse_hm):
    any_spec = pl.BlockSpec(memory_space=pl.ANY)
    vmem = pl.BlockSpec(memory_space=pltpu.VMEM)
    return pl.pallas_call(
        finish_kernel,
        out_shape=(
            jax.ShapeDtypeStruct((256, 32, HEAD), BF16),
            jax.ShapeDtypeStruct((256, 32, HEAD), BF16),
            jax.ShapeDtypeStruct((256, 8, HEAD), BF16),
            jax.ShapeDtypeStruct((256, 8, HEAD), BF16),
            jax.ShapeDtypeStruct((32, 256), F32),
        ),
        in_specs=[pl.BlockSpec(memory_space=pltpu.SMEM)] + [vmem] * 4,
        out_specs=(any_spec,) * 4 + (vmem,),
        scratch_shapes=[
            pltpu.VMEM((2, SLOT, 8, HEAD), BF16),
            pltpu.VMEM((2, SLOT, 8, HEAD), BF16),
            pltpu.SemaphoreType.DMA((4, 4)),
        ],
        compiler_params=pltpu.CompilerParams(vmem_limit_bytes=16 * 1024 * 1024),
        name="finish",
    )(cu, o_t, dq_t, dkv_hm, lse_hm)


def solution(mesh):
    tok_spec = P(("dp", "cp"), None, None)
    lse_spec = P(("dp", "cp"), None)

    def local(q, k, v, do, valid, cu):
        res = attn_call(cu, valid.reshape(1, 256), q, k, v, do)
        o, dq, dk, dv, lse = finish_call(cu, *res)
        return o, lse.T, dq, dk, dv

    return jax.shard_map(local, mesh=mesh, in_specs=(tok_spec,) * 4 + (P(("dp", "cp")), P("dp")),
                         out_specs=(tok_spec, lse_spec, tok_spec, tok_spec, tok_spec), check_vma=False)
```

```python
import functools
import math

import jax
import jax.numpy as jnp
from jax import lax
from jax.experimental import pallas as pl
from jax.experimental.pallas import tpu as pltpu
from jax.sharding import PartitionSpec as P

MESH = pl.DeviceIdType.MESH
FILL = -1.0e30
BIG = 3.0e38
HEAD = 128
SLOT = 128
TILE = 512
GROUP = 4
HC = 4
SWAP = 3
SCALE = HEAD ** -0.5
C2 = SCALE * math.log2(math.e)
NT = (((1,), (1,)), ((), ()))
NN = (((1,), (0,)), ((), ()))
F32 = jnp.float32
BF16 = jnp.bfloat16

TILES = ((0, 0), (1, 0), (1, 1), (0, 1))


def slot_of(chip, ti):
    oc, up = TILES[ti]
    r = 2 * chip + oc
    return 7 - r if up else r


def mm(a, b, dims):
    return lax.dot_general(a, b, dims, preferred_element_type=F32)


def src_row(up, t, l0):
    if up:
        return jnp.where(t < l0, t + l0, t + SLOT)
    return jnp.where(t < l0, t, t + l0)


def attn_kernel(cu, valid, q, k, v, do, o_out, dq_out, dkv_out, lse_out,
                raw_q, raw_do, far_q, far_do, raw_k, raw_v, kv_hm, kv_all, kt, vt, qh, doh, st, pb, db,
                dkv_acc, dkv_in, o_st, dq_st, o_far, dq_far, dkv_st, back_st, lse_st, caps, valid_all,
                in_sem, raw_ssem, raw_rsem, val_ssem, val_rsem, kv_ssem, kv_rsem,
                part_ssem, part_rsem, swap_ssem, swap_rsem, back_ssem, back_rsem, res_ssem, res_rsem, dkv_ssem, dkv_rsem, lse_sem, lse_rsem):
    r = lax.axis_index("cp")
    chip = r // 2
    c = r % 2
    pc = 1 - c
    partner = chip * 2 + pc
    cross = (1 - chip) * 2 + c
    cross_o = (1 - chip) * 2 + pc
    l0 = lax.shift_right_logical(cu[1], 3)

    def remote(src, dst, ssem, rsem, dev):
        return pltpu.make_async_remote_copy(src_ref=src, dst_ref=dst, send_sem=ssem, recv_sem=rsem,
                                            device_id={"cp": dev}, device_id_type=MESH)

    own_heads = pl.ds(pl.multiple_of(16 * c, 16), 16)
    oth_heads = pl.ds(pl.multiple_of(16 * pc, 16), 16)
    ld_k = pltpu.make_async_copy(k, raw_k, in_sem.at[0])
    ld_v = pltpu.make_async_copy(v, raw_v, in_sem.at[1])
    ld_q = pltpu.make_async_copy(q.at[:, own_heads, :], raw_q, in_sem.at[2])
    ld_do = pltpu.make_async_copy(do.at[:, own_heads, :], raw_do, in_sem.at[3])
    ld_val = pltpu.make_async_copy(valid, valid_all.at[r], in_sem.at[4])
    for cp in (ld_k, ld_v, ld_q, ld_do, ld_val):
        cp.start()

    barrier = pltpu.get_barrier_semaphore()
    for dev in (partner, cross, cross_o):
        pl.semaphore_signal(barrier, inc=1, device_id={"cp": dev}, device_id_type=MESH)
    pl.semaphore_wait(barrier, 3)

    peers = (partner, cross, cross_o)
    push_q = remote(q.at[:, oth_heads, :], far_q, raw_ssem.at[0], raw_rsem.at[0], partner)
    push_do = remote(do.at[:, oth_heads, :], far_do, raw_ssem.at[1], raw_rsem.at[1], partner)
    push_val = [remote(valid, valid_all.at[r], val_ssem.at[i], val_rsem.at[r], dev) for i, dev in enumerate(peers)]

    push_q.start()
    push_do.start()

    def kv_relayout(up):
        def body(i, _):
            t0 = i * 16
            for which, raw in ((0, raw_k), (1, raw_v)):
                rows = jnp.stack([raw[src_row(up, t0 + j, l0)] for j in range(16)])
                kv_hm[:, up, which, pl.ds(pl.multiple_of(t0, 16), 16), :] = jnp.transpose(rows, (1, 0, 2))
            return 0
        lax.fori_loop(0, SLOT // 16, body, 0)

    def kv_push(h, to, both):
        head = (4 * c if to == 1 else 4 * pc) + h
        dev = (partner, cross, cross_o)[to]
        ups = pl.ds(0, 2 if both else 1)
        return remote(kv_hm.at[head, ups], kv_all.at[h, r, ups], kv_ssem.at[to, h], kv_rsem.at[h, r], dev)

    def kv_wait(h, owner, both):
        ups = pl.ds(0, 2 if both else 1)
        remote(kv_hm.at[0, ups], kv_all.at[h, owner, ups], kv_ssem.at[0, h], kv_rsem.at[h, owner], partner).wait_recv()

    ld_k.wait()
    ld_v.wait()
    kv_relayout(0)

    def cross_next(ch, h, upto=None):
        @pl.when(chip == ch)
        def _():
            for to in (1, 2):
                if h > 0:
                    kv_push(h - 1, to, ch == 1).wait_send()
            for e in range(h, upto or h + 1):
                for to in (1, 2):
                    kv_push(e, to, ch == 1).start()

    cross_next(0, 0)
    kv_relayout(1)
    cross_next(1, 0)
    for h in range(HC):
        kv_push(h, 0, True).start()
    ld_val.wait()
    for cp in push_val:
        cp.start()

    def copy_own(h, _):
        for up in range(2):
            kv_all[h, r, up] = kv_hm[4 * c + h, up]
        return 0
    lax.fori_loop(0, HC, copy_own, 0)

    def q_relayout(oc, from_q, from_do):
        for up, ti in ((0, oc), (1, 3 - oc)):
            def body(i, _):
                t0 = i * 16
                at = pl.ds(pl.multiple_of(t0, 16), 16)
                for raw, dst in ((from_q, qh), (from_do, doh)):
                    rows = jnp.stack([raw[src_row(up, t0 + j, l0)] for j in range(16)])
                    dst[:, ti, :, at, :] = jnp.transpose(rows, (1, 0, 2)).reshape(HC, GROUP, 16, HEAD)
                return 0
            lax.fori_loop(0, SLOT // 16, body, 0)

    ld_q.wait()
    ld_do.wait()
    cross_next(0, 1, HC)
    q_relayout(c, raw_q, raw_do)

    for i in range(3):
        remote(valid, valid_all.at[peers[i]], val_ssem.at[i], val_rsem.at[peers[i]], peers[i]).wait_recv()
    lane = lax.broadcasted_iota(jnp.int32, (SLOT, SLOT), 1)
    sub = lax.broadcasted_iota(jnp.int32, (SLOT, SLOT), 0)
    lane2 = lax.broadcasted_iota(jnp.int32, (SLOT, 2 * SLOT), 1)
    sub2 = lax.broadcasted_iota(jnp.int32, (SLOT, 2 * SLOT), 0)
    same_doc = (lane < l0) == (sub < l0)
    doc_f = jnp.where(lane < l0, 1.0, 0.0)
    doc_s = jnp.where(sub < l0, 1.0, 0.0)
    same_f = jnp.where(doc_f == doc_s, 1.0, 0.0)
    del same_doc

    def cap_body(s, _):
        owner = jnp.where(s < 4, s, 7 - s)
        off = jnp.where(s < 4, 0, 1)
        src_lo = jnp.where(sub2 < l0, sub2, sub2 + l0)
        src_hi = jnp.where(sub2 < l0, sub2 + l0, sub2 + SLOT)
        src = jnp.where(off == 1, src_hi, src_lo)
        row = jnp.broadcast_to(valid_all[owner].astype(F32), (SLOT, 2 * SLOT))
        ok = jnp.sum(jnp.where(src == lane2, row, 0.0), axis=1, keepdims=True)
        caps[s] = jnp.where(same_f * ok > 0.5, BIG, FILL)
        return 0
    lax.fori_loop(0, 8, cap_body, 0)
    for ti in range(4):
        oc, up = TILES[ti]
        s = (7 - (2 * chip + oc)) if up else 2 * chip + oc
        caps[8 + ti] = jnp.where(sub <= lane, caps[s], FILL)

    cross_next(1, 1)
    push_q.wait_recv()
    push_do.wait_recv()
    q_relayout(pc, far_q, far_do)

    def part_copy(h, i, n):
        return remote(dkv_acc.at[h, pl.ds(i, n)], dkv_in.at[h, pl.ds(0, n)], part_ssem.at[h], part_rsem.at[h], cross)

    def part_run(ch, h, act):
        if ch == 1:
            act(part_copy(h, 0, 2))
        else:
            pl.when(h < SWAP)(lambda: act(part_copy(h, 2, 3)))
            pl.when(h >= SWAP)(lambda: act(part_copy(h, 2, 4)))

    def swap_copy(h):
        return remote(dkv_acc.at[h, 5], dkv_in.at[h, 2], swap_ssem.at[h], swap_rsem.at[h], cross)

    def swap_back(h):
        return remote(back_st.at[h], dkv_out.at[4 * c + h, 1], back_ssem.at[h], back_rsem.at[4 * c + h], 2)

    def res_copy(p, ti, which):
        stage, out = ((o_far, o_out), (dq_far, dq_out))[which]
        dst = out.at[TILES[ti][1], :, pl.ds(pl.multiple_of(16 * c + 8 * p, 8), 8), :]
        return remote(stage.at[p, ti], dst, res_ssem.at[which, p, ti], res_rsem.at[which, p, TILES[ti][1]], partner)

    def dkv_copy(h, ti):
        up = TILES[ti][1]
        return remote(dkv_st.at[h, ti], dkv_out.at[4 * c + h, up], dkv_ssem.at[h, ti], dkv_rsem.at[h, up], partner)

    def res_put(p):
        heads = pl.ds(pl.multiple_of(16 * c + 8 * p, 8), 8)
        for ti, (oc, up) in enumerate(TILES):
            def body(i, _, keep):
                at = pl.ds(pl.multiple_of(i * 16, 16), 16)
                for stage, far, out in ((o_st, o_far, o_out), (dq_st, dq_far, dq_out)):
                    x = jnp.concatenate([stage[e, ti, pl.ds(pl.multiple_of(g * SLOT + i * 16, 16), 16), :][None]
                                         for e in range(2) for g in range(GROUP)], axis=0)
                    y = jnp.transpose(x, (1, 0, 2))
                    if keep:
                        out[up, at, heads, :] = y
                    else:
                        far[p, ti, at, :, :] = y
                return 0

            @pl.when(c == oc)
            def _():
                lax.fori_loop(0, SLOT // 16, functools.partial(body, keep=True), 0)

            @pl.when(c != oc)
            def _():
                lax.fori_loop(0, SLOT // 16, functools.partial(body, keep=False), 0)
                for which in range(2):
                    res_copy(p, ti, which).start()

    def dkv_put(h, ti, parts):
        oc, up = TILES[ti]

        @pl.when(c == oc)
        def _():
            for w in range(2):
                dkv_out[4 * c + h, up, w] = parts(w).astype(BF16)

        @pl.when(c != oc)
        def _():
            for w in range(2):
                dkv_st[h, ti, w] = parts(w).astype(BF16)
            dkv_copy(h, ti).start()

    lse_far = remote(lse_st.at[pc], lse_out.at[:, own_heads, :], lse_sem, lse_rsem, partner)

    def kv_slot(h, s, which):
        return kv_all[h, min(s, 7 - s), int(s > 3), which]

    def kv_slots(h, a, b, which):
        return jnp.concatenate([kv_slot(h, s, which) for s in range(a, b)], axis=0)

    def run_chip(ch):
        slots = [slot_of(ch, ti) for ti in range(4)]
        sent = [0, 1] if ch == 1 else [2, 3, 4, 5]
        kept = [0, 1] if ch == 0 else [2, 3, 4, 5]
        order = [0, 1, 2, 3]

        def transposes(s):
            for src, dst in ((0, kt), (1, vt)):
                dst[:, s * SLOT:(s + 1) * SLOT] = jnp.transpose(kv_slot(h_ref[0], s, src))

        h_ref = [None]

        def head(h, _):
            h_ref[0] = h
            seen = set()
            ready = set()

            def wait_slot(s):
                if s in ready:
                    return
                if s in slots:
                    kv_wait(h, partner, True)
                    new = slots
                elif ch == 1:
                    for owner in (0, 1):
                        kv_wait(h, owner, False)
                    new = [0, 1]
                else:
                    for owner in (2, 3):
                        kv_wait(h, owner, True)
                    new = [2, 3, 4, 5]
                for u in new:
                    ready.add(u)
                    transposes(u)

            for ti in order:
                s = slots[ti]
                nk = s + 1
                if ch == 1 and ti == 1:
                    for nxt in (2, 3):
                        pl.when(h == nxt - 2)(functools.partial(cross_next, 1, nxt))
                for u in range(nk):
                    wait_slot(u)
                qt = qh[h, ti].reshape(TILE, HEAD)
                dt = doh[h, ti].reshape(TILE, HEAD)
                m8 = [None] * GROUP
                for a in range(0, nk, 2):
                    n = min(2, nk - a)
                    kb = kv_slots(h, a, a + n, 0)
                    sc = mm(kb, qt, NT)
                    for j in range(n):
                        cap = caps[8 + ti] if a + j == s else caps[a + j]
                        for g in range(GROUP):
                            x = jnp.minimum(sc[j * SLOT:(j + 1) * SLOT, g * SLOT:(g + 1) * SLOT], cap)
                            st[(a + j) * SLOT:(a + j + 1) * SLOT, g * SLOT:(g + 1) * SLOT] = x
                            top = jnp.max(x.reshape(SLOT // 8, 8, SLOT), axis=0)
                            m8[g] = top if m8[g] is None else jnp.maximum(m8[g], top)
                m = [jnp.max(x, axis=0, keepdims=True) for x in m8]
                mc = [x * C2 for x in m]
                l8 = [None] * GROUP
                for a in range(nk):
                    for g in range(GROUP):
                        at = (slice(a * SLOT, (a + 1) * SLOT), slice(g * SLOT, (g + 1) * SLOT))
                        e = jnp.exp2(st[at] * C2 - mc[g])
                        st[at] = e
                        pb[at] = e.astype(BF16)
                        tot = jnp.sum(e.reshape(SLOT // 8, 8, SLOT), axis=0)
                        l8[g] = tot if l8[g] is None else l8[g] + tot
                ot = mm(vt[:, :nk * SLOT], pb[:nk * SLOT, :], NN)
                inv, dd = [], []
                oc, up = TILES[ti]
                for g in range(GROUP):
                    l = jnp.sum(l8[g], axis=0, keepdims=True)
                    has = m[g] > 0.5 * FILL
                    safe = jnp.where(has, l, 1.0)
                    i_l = jnp.where(has, 1.0 / safe, 0.0)
                    lse = jnp.where(has, m[g] * SCALE + jnp.log(safe), 0.0)
                    lse_st[oc, up, pl.ds(h * GROUP + g, 1), :] = lse
                    og = (ot[:, g * SLOT:(g + 1) * SLOT] * i_l).astype(BF16)
                    dog = jnp.transpose(dt[g * SLOT:(g + 1) * SLOT, :])
                    dd.append(jnp.sum(og.astype(F32) * dog.astype(F32), axis=0, keepdims=True))
                    inv.append(i_l)
                    o_st[h % 2, ti, g * SLOT:(g + 1) * SLOT, :] = jnp.transpose(og)

                first = [u for u in range(nk) if u in sent] if (ch == 0 and ti >= 2) else []
                rest = [u for u in range(nk) if u not in first]
                dqt = None
                for part in (first, rest):
                    runs = []
                    for u in part:
                        if runs and runs[-1][1] == u and u - runs[-1][0] < 2:
                            runs[-1][1] = u + 1
                        else:
                            runs.append([u, u + 1])
                    for a, b in runs:
                        n = b - a
                        vb = kv_slots(h, a, b, 1)
                        dp = mm(vb, dt, NT)
                        for j in range(n):
                            for g in range(GROUP):
                                at = (slice((a + j) * SLOT, (a + j + 1) * SLOT), slice(g * SLOT, (g + 1) * SLOT))
                                p = st[at] * inv[g]
                                pb[at] = p.astype(BF16)
                                ds = p * (dp[j * SLOT:(j + 1) * SLOT, g * SLOT:(g + 1) * SLOT] - dd[g])
                                db[at] = ds.astype(BF16)
                        dsb = db[a * SLOT:b * SLOT, :]
                        dv = mm(pb[a * SLOT:b * SLOT, :], dt, NN)
                        dk = mm(dsb, qt, NN) * SCALE
                        dq = mm(kt[:, a * SLOT:b * SLOT], dsb, NN)
                        dqt = dq if dqt is None else dqt + dq
                        for j in range(n):
                            u = a + j
                            new = (dk[j * SLOT:(j + 1) * SLOT], dv[j * SLOT:(j + 1) * SLOT])
                            for w in range(2):
                                dkv_acc[h, u, w] = dkv_acc[h, u, w] + new[w] if u in seen else new[w]
                            seen.add(u)
                    if part is first and ti == 3 and ch == 0:
                        part_run(0, h, lambda cp: cp.start())
                for g in range(GROUP):
                    dqg = (dqt[:, g * SLOT:(g + 1) * SLOT] * SCALE).astype(BF16)
                    dq_st[h % 2, ti, g * SLOT:(g + 1) * SLOT, :] = jnp.transpose(dqg)
            if ch == 1:
                part_run(1, h, lambda cp: cp.start())
                pl.when(h < SWAP)(lambda: swap_copy(h).start())
            else:
                for ti in (2, 3):
                    dkv_put(h, ti, lambda w, ti=ti: dkv_acc[h, slots[ti], w])
            pl.when(h % 2 == 1)(lambda: res_put(h // 2))
            return 0

        lax.fori_loop(0, HC, head, 0)

        lse_out[:, own_heads, :] = lse_st[c]
        lse_far.start()

        if ch == 0:
            def swapped(h, _):
                swap_copy(h).wait_recv()
                for w in range(2):
                    back_st[h, w] = (dkv_in[h, 2, w] + dkv_acc[h, 5, w]).astype(BF16)
                swap_back(h).start()
                return 0
            lax.fori_loop(0, SWAP, swapped, 0)

        def tail(h, _):
            part_run(1 - ch, h, lambda cp: cp.wait_recv())
            for i, u in enumerate(kept):
                ti = slots.index(u)
                put = functools.partial(dkv_put, h, ti, lambda w, u=u, i=i: dkv_acc[h, u, w] + dkv_in[h, i, w])
                if u == 5:
                    pl.when(h >= SWAP)(put)
                else:
                    put()
            return 0
        lax.fori_loop(0, HC, tail, 0)

        def drain(h, _):
            part_run(ch, h, lambda cp: cp.wait_send())
            return 0
        lax.fori_loop(0, HC, drain, 0)

        def drain_swap(h, _):
            if ch == 0:
                swap_back(h).wait_send()
            else:
                swap_copy(h).wait_send()
            return 0
        lax.fori_loop(0, SWAP, drain_swap, 0)

        if ch == 1:
            @pl.when(c == 0)
            def _():
                for core in range(2):
                    for h in range(SWAP):
                        remote(back_st.at[h], dkv_out.at[4 * core + h, 1], back_ssem.at[h], back_rsem.at[4 * core + h], 2).wait_recv()

    pl.when(chip == 0)(functools.partial(run_chip, 0))
    pl.when(chip == 1)(functools.partial(run_chip, 1))

    push_q.wait_send()
    push_do.wait_send()
    for cp in push_val:
        cp.wait_send()

    def drain(h, _):
        kv_push(h, 0, True).wait_send()
        for ch in range(2):
            @pl.when(chip == ch)
            def _():
                for to in (1, 2):
                    pl.when((h == HC - 1) if ch == 1 else (h > 0))(kv_push(h, to, ch == 1).wait_send)
        far = jnp.logical_and(chip == 1, h < SWAP)
        for ti in range(4):
            sent = c != TILES[ti][0]
            pl.when(jnp.logical_and(sent, jnp.logical_not(far)) if ti == 3 else sent)(dkv_copy(h, ti).wait_send)
        for up in range(2):
            come = remote(dkv_st.at[h, 0], dkv_out.at[4 * pc + h, up], dkv_ssem.at[h, 0], dkv_rsem.at[h, up], partner)
            if up:
                pl.when(jnp.logical_not(jnp.logical_and(far, c == 0)))(come.wait_recv)
            else:
                come.wait_recv()
        return 0
    lax.fori_loop(0, HC, drain, 0)

    for p in range(2):
        for which in range(2):
            stage, out = ((o_far, o_out), (dq_far, dq_out))[which]
            for ti in range(4):
                pl.when(c != TILES[ti][0])(res_copy(p, ti, which).wait_send)
            for up in range(2):
                dst = out.at[up, :, pl.ds(pl.multiple_of(16 * pc + 8 * p, 8), 8), :]
                remote(stage.at[p, 0], dst, res_ssem.at[which, p, 0], res_rsem.at[which, p, up], partner).wait_recv()
    lse_far.wait_send()
    remote(lse_st.at[0], lse_out.at[:, oth_heads, :], lse_sem, lse_rsem, partner).wait_recv()


def attn_call(cu, valid, q, k, v, do):
    any_spec = pl.BlockSpec(memory_space=pl.ANY)
    dma = pltpu.SemaphoreType.DMA
    return pl.pallas_call(
        attn_kernel,
        out_shape=(
            pltpu.VMEM((2, SLOT, 32, HEAD), BF16),
            pltpu.VMEM((2, SLOT, 32, HEAD), BF16),
            pltpu.VMEM((8, 2, 2, SLOT, HEAD), BF16),
            pltpu.VMEM((2, 32, SLOT), F32),
        ),
        in_specs=[pl.BlockSpec(memory_space=pltpu.SMEM)] + [any_spec] * 5,
        out_specs=(pl.BlockSpec(memory_space=pltpu.VMEM),) * 4,
        scratch_shapes=[
            pltpu.VMEM((256, 16, HEAD), BF16),
            pltpu.VMEM((256, 16, HEAD), BF16),
            pltpu.VMEM((256, 16, HEAD), BF16),
            pltpu.VMEM((256, 16, HEAD), BF16),
            pltpu.VMEM((256, 8, HEAD), BF16),
            pltpu.VMEM((256, 8, HEAD), BF16),
            pltpu.VMEM((8, 2, 2, SLOT, HEAD), BF16),
            pltpu.VMEM((HC, 4, 2, 2, SLOT, HEAD), BF16),
            pltpu.VMEM((HEAD, 8 * SLOT), BF16),
            pltpu.VMEM((HEAD, 8 * SLOT), BF16),
            pltpu.VMEM((HC, 4, GROUP, SLOT, HEAD), BF16),
            pltpu.VMEM((HC, 4, GROUP, SLOT, HEAD), BF16),
            pltpu.VMEM((8 * SLOT, TILE), F32),
            pltpu.VMEM((8 * SLOT, TILE), BF16),
            pltpu.VMEM((8 * SLOT, TILE), BF16),
            pltpu.VMEM((HC, 8, 2, SLOT, HEAD), F32),
            pltpu.VMEM((HC, 4, 2, SLOT, HEAD), F32),
            pltpu.VMEM((2, 4, TILE, HEAD), BF16),
            pltpu.VMEM((2, 4, TILE, HEAD), BF16),
            pltpu.VMEM((2, 4, SLOT, 8, HEAD), BF16),
            pltpu.VMEM((2, 4, SLOT, 8, HEAD), BF16),
            pltpu.VMEM((HC, 4, 2, SLOT, HEAD), BF16),
            pltpu.VMEM((HC, 2, SLOT, HEAD), BF16),
            pltpu.VMEM((2, 2, 16, SLOT), F32),
            pltpu.VMEM((12, SLOT, SLOT), F32),
            pltpu.VMEM((4, 1, 2 * SLOT), jnp.int32),
            dma((5,)),
            dma((2,)), dma((2,)),
            dma((3,)), dma((4,)),
            dma((3, HC)), dma((HC, 4)),
            dma((HC,)), dma((HC,)),
            dma((HC,)), dma((HC,)), dma((HC,)), dma((8,)),
            dma((2, 2, 4)), dma((2, 2, 2)),
            dma((HC, 4)), dma((HC, 2)),
            dma, dma,
        ],
        compiler_params=pltpu.CompilerParams(collective_id=0, has_side_effects=True, vmem_limit_bytes=61300000),
        name="attn",
    )(cu, valid, q, k, v, do)


def finish_kernel(cu, o_in, dq_in, dkv_in, lse_in, o_out, dq_out, dk_out, dv_out, lse_out, dk_t, dv_t, sem):
    l0 = lax.shift_right_logical(cu[1], 3)
    rest = SLOT - l0

    def copies(i, x, out):
        runs = ((0, 0, 0, l0), (1, 0, l0, l0), (0, l0, 2 * l0, rest), (1, l0, SLOT + l0, rest))
        return [pltpu.make_async_copy(x.at[up, pl.ds(at, n)], out.at[pl.ds(to, n)], sem.at[i, j])
                for j, (up, at, to, n) in enumerate(runs)]

    moves = copies(0, o_in, o_out) + copies(1, dq_in, dq_out)
    for cp in moves:
        cp.start()

    for w, dst in ((0, dk_t), (1, dv_t)):
        for up in range(2):
            def body(i, _):
                at = pl.ds(pl.multiple_of(i * 16, 16), 16)
                dst[up, at] = jnp.transpose(dkv_in[:, up, w, at, :], (1, 0, 2))
                return 0
            lax.fori_loop(0, SLOT // 16, body, 0)
        more = copies(2 + w, dst, (dk_out, dv_out)[w])
        for cp in more:
            cp.start()
        moves += more

    row = lax.broadcasted_iota(jnp.int32, (2 * SLOT, SLOT), 0)
    col = lax.broadcasted_iota(jnp.int32, (2 * SLOT, SLOT), 1)
    acc = None
    for up in range(2):
        if up:
            src = jnp.where(col < l0, col + l0, col + SLOT)
        else:
            src = jnp.where(col < l0, col, col + l0)
        pick = jnp.where(row == src, 1.0, 0.0)
        part = lax.dot_general(lse_in[up], pick, NT, precision=lax.Precision.HIGHEST, preferred_element_type=F32)
        acc = part if acc is None else acc + part
    lse_out[...] = acc
    for cp in moves:
        cp.wait()


def finish_call(cu, o_t, dq_t, dkv_hm, lse_hm):
    any_spec = pl.BlockSpec(memory_space=pl.ANY)
    vmem = pl.BlockSpec(memory_space=pltpu.VMEM)
    return pl.pallas_call(
        finish_kernel,
        out_shape=(
            jax.ShapeDtypeStruct((256, 32, HEAD), BF16),
            jax.ShapeDtypeStruct((256, 32, HEAD), BF16),
            jax.ShapeDtypeStruct((256, 8, HEAD), BF16),
            jax.ShapeDtypeStruct((256, 8, HEAD), BF16),
            jax.ShapeDtypeStruct((32, 256), F32),
        ),
        in_specs=[pl.BlockSpec(memory_space=pltpu.SMEM)] + [vmem] * 4,
        out_specs=(any_spec,) * 4 + (vmem,),
        scratch_shapes=[
            pltpu.VMEM((2, SLOT, 8, HEAD), BF16),
            pltpu.VMEM((2, SLOT, 8, HEAD), BF16),
            pltpu.SemaphoreType.DMA((4, 4)),
        ],
        compiler_params=pltpu.CompilerParams(vmem_limit_bytes=16 * 1024 * 1024),
        name="finish",
    )(cu, o_t, dq_t, dkv_hm, lse_hm)


def solution(mesh):
    tok_spec = P(("dp", "cp"), None, None)
    lse_spec = P(("dp", "cp"), None)

    def local(q, k, v, do, valid, cu):
        res = attn_call(cu, valid.reshape(1, 256), q, k, v, do)
        o, dq, dk, dv, lse = finish_call(cu, *res)
        return o, lse.T, dq, dk, dv

    return jax.shard_map(local, mesh=mesh, in_specs=(tok_spec,) * 4 + (P(("dp", "cp")), P("dp")),
                         out_specs=(tok_spec, lse_spec, tok_spec, tok_spec, tok_spec), check_vma=False)
```

```python
import functools
import math

import jax
import jax.numpy as jnp
from jax import lax
from jax.experimental import pallas as pl
from jax.experimental.pallas import tpu as pltpu
from jax.sharding import PartitionSpec as P

MESH = pl.DeviceIdType.MESH
FILL = -1.0e30
BIG = 3.0e38
HEAD = 128
SLOT = 128
TILE = 512
GROUP = 4
HC = 4
SWAP = 3
SCALE = HEAD ** -0.5
C2 = SCALE * math.log2(math.e)
NT = (((1,), (1,)), ((), ()))
NN = (((1,), (0,)), ((), ()))
F32 = jnp.float32
BF16 = jnp.bfloat16

TILES = ((0, 0), (1, 0), (1, 1), (0, 1))


def slot_of(chip, ti):
    oc, up = TILES[ti]
    r = 2 * chip + oc
    return 7 - r if up else r


def mm(a, b, dims):
    return lax.dot_general(a, b, dims, preferred_element_type=F32)


def src_row(up, t, l0):
    if up:
        return jnp.where(t < l0, t + l0, t + SLOT)
    return jnp.where(t < l0, t, t + l0)


def attn_kernel(cu_hbm, valid, q, k, v, do, o_out, dq_out, dkv_out, lse_out, cu,
                raw_q, raw_do, far_q, far_do, raw_k, raw_v, kv_hm, kv_all, kt, vt, qh, doh, st, pb, db,
                dkv_acc, dkv_in, o_st, dq_st, o_far, dq_far, dkv_st, back_st, lse_st, caps, valid_all,
                in_sem, raw_ssem, raw_rsem, val_ssem, val_rsem, kv_ssem, kv_rsem,
                part_ssem, part_rsem, swap_ssem, swap_rsem, back_ssem, back_rsem, res_ssem, res_rsem, dkv_ssem, dkv_rsem, lse_sem, lse_rsem):
    r = lax.axis_index("cp")
    chip = r // 2
    c = r % 2
    pc = 1 - c
    partner = chip * 2 + pc
    cross = (1 - chip) * 2 + c
    cross_o = (1 - chip) * 2 + pc

    def remote(src, dst, ssem, rsem, dev):
        return pltpu.make_async_remote_copy(src_ref=src, dst_ref=dst, send_sem=ssem, recv_sem=rsem,
                                            device_id={"cp": dev}, device_id_type=MESH)

    own_heads = pl.ds(pl.multiple_of(16 * c, 16), 16)
    oth_heads = pl.ds(pl.multiple_of(16 * pc, 16), 16)
    ld_k = pltpu.make_async_copy(k, raw_k, in_sem.at[0])
    ld_v = pltpu.make_async_copy(v, raw_v, in_sem.at[1])
    ld_q = pltpu.make_async_copy(q.at[:, own_heads, :], raw_q, in_sem.at[2])
    ld_do = pltpu.make_async_copy(do.at[:, own_heads, :], raw_do, in_sem.at[3])
    ld_val = pltpu.make_async_copy(valid, valid_all.at[r], in_sem.at[4])
    ld_cu = pltpu.make_async_copy(cu_hbm, cu, in_sem.at[5])
    for cp in (ld_cu, ld_k, ld_v, ld_q, ld_do, ld_val):
        cp.start()

    barrier = pltpu.get_barrier_semaphore()
    for dev in (partner, cross, cross_o):
        pl.semaphore_signal(barrier, inc=1, device_id={"cp": dev}, device_id_type=MESH)
    pl.semaphore_wait(barrier, 3)
    ld_cu.wait()
    l0 = lax.shift_right_logical(cu[1], 3)

    peers = (partner, cross, cross_o)
    push_q = remote(q.at[:, oth_heads, :], far_q, raw_ssem.at[0], raw_rsem.at[0], partner)
    push_do = remote(do.at[:, oth_heads, :], far_do, raw_ssem.at[1], raw_rsem.at[1], partner)
    push_val = [remote(valid, valid_all.at[r], val_ssem.at[i], val_rsem.at[r], dev) for i, dev in enumerate(peers)]

    push_q.start()
    push_do.start()

    def kv_relayout(up):
        def body(i, _):
            t0 = i * 16
            for which, raw in ((0, raw_k), (1, raw_v)):
                rows = jnp.stack([raw[src_row(up, t0 + j, l0)] for j in range(16)])
                kv_hm[:, up, which, pl.ds(pl.multiple_of(t0, 16), 16), :] = jnp.transpose(rows, (1, 0, 2))
            return 0
        lax.fori_loop(0, SLOT // 16, body, 0)

    def kv_push(h, to, both):
        head = (4 * c if to == 1 else 4 * pc) + h
        dev = (partner, cross, cross_o)[to]
        ups = pl.ds(0, 2 if both else 1)
        return remote(kv_hm.at[head, ups], kv_all.at[h, r, ups], kv_ssem.at[to, h], kv_rsem.at[h, r], dev)

    def kv_wait(h, owner, both):
        ups = pl.ds(0, 2 if both else 1)
        remote(kv_hm.at[0, ups], kv_all.at[h, owner, ups], kv_ssem.at[0, h], kv_rsem.at[h, owner], partner).wait_recv()

    ld_k.wait()
    ld_v.wait()
    kv_relayout(0)

    def cross_send(ch, h):
        @pl.when(chip == ch)
        def _():
            for to in (1, 2):
                kv_push(h, to, ch == 1).start()

    cross_send(0, 0)
    kv_relayout(1)
    cross_send(1, 0)
    for h in range(HC):
        kv_push(h, 0, True).start()
    ld_val.wait()
    for cp in push_val:
        cp.start()

    def copy_own(h, _):
        for up in range(2):
            kv_all[h, r, up] = kv_hm[4 * c + h, up]
        return 0
    lax.fori_loop(0, HC, copy_own, 0)

    def q_relayout(oc, from_q, from_do):
        for up, ti in ((0, oc), (1, 3 - oc)):
            def body(i, _):
                t0 = i * 16
                at = pl.ds(pl.multiple_of(t0, 16), 16)
                for raw, dst in ((from_q, qh), (from_do, doh)):
                    rows = jnp.stack([raw[src_row(up, t0 + j, l0)] for j in range(16)])
                    dst[:, ti, :, at, :] = jnp.transpose(rows, (1, 0, 2)).reshape(HC, GROUP, 16, HEAD)
                return 0
            lax.fori_loop(0, SLOT // 16, body, 0)

    ld_q.wait()
    ld_do.wait()
    cross_send(0, 1)
    q_relayout(c, raw_q, raw_do)

    cross_send(0, 2)
    for i in range(3):
        remote(valid, valid_all.at[peers[i]], val_ssem.at[i], val_rsem.at[peers[i]], peers[i]).wait_recv()
    lane = lax.broadcasted_iota(jnp.int32, (SLOT, SLOT), 1)
    sub = lax.broadcasted_iota(jnp.int32, (SLOT, SLOT), 0)
    lane2 = lax.broadcasted_iota(jnp.int32, (SLOT, 2 * SLOT), 1)
    sub2 = lax.broadcasted_iota(jnp.int32, (SLOT, 2 * SLOT), 0)
    same_doc = (lane < l0) == (sub < l0)
    doc_f = jnp.where(lane < l0, 1.0, 0.0)
    doc_s = jnp.where(sub < l0, 1.0, 0.0)
    same_f = jnp.where(doc_f == doc_s, 1.0, 0.0)
    del same_doc

    def cap_body(s, _):
        owner = jnp.where(s < 4, s, 7 - s)
        off = jnp.where(s < 4, 0, 1)
        src_lo = jnp.where(sub2 < l0, sub2, sub2 + l0)
        src_hi = jnp.where(sub2 < l0, sub2 + l0, sub2 + SLOT)
        src = jnp.where(off == 1, src_hi, src_lo)
        row = jnp.broadcast_to(valid_all[owner].astype(F32), (SLOT, 2 * SLOT))
        ok = jnp.sum(jnp.where(src == lane2, row, 0.0), axis=1, keepdims=True)
        caps[s] = jnp.where(same_f * ok > 0.5, BIG, FILL)
        return 0
    lax.fori_loop(0, 8, cap_body, 0)
    for ti in range(4):
        oc, up = TILES[ti]
        s = (7 - (2 * chip + oc)) if up else 2 * chip + oc
        caps[8 + ti] = jnp.where(sub <= lane, caps[s], FILL)

    cross_send(0, 3)
    cross_send(1, 1)
    push_q.wait_recv()
    push_do.wait_recv()
    q_relayout(pc, far_q, far_do)

    def part_copy(h, i, n):
        return remote(dkv_acc.at[h, pl.ds(i, n)], dkv_in.at[h, pl.ds(0, n)], part_ssem.at[h], part_rsem.at[h], cross)

    def part_run(ch, h, act):
        if ch == 1:
            act(part_copy(h, 0, 2))
        else:
            pl.when(h < SWAP)(lambda: act(part_copy(h, 2, 3)))
            pl.when(h >= SWAP)(lambda: act(part_copy(h, 2, 4)))

    def swap_copy(h):
        return remote(dkv_acc.at[h, 5], dkv_in.at[h, 2], swap_ssem.at[h], swap_rsem.at[h], cross)

    def swap_back(h):
        return remote(back_st.at[h], dkv_out.at[4 * c + h, 1], back_ssem.at[h], back_rsem.at[4 * c + h], 2)

    def res_copy(p, ti, which):
        stage, out = ((o_far, o_out), (dq_far, dq_out))[which]
        dst = out.at[TILES[ti][1], :, pl.ds(pl.multiple_of(16 * c + 8 * p, 8), 8), :]
        return remote(stage.at[p, ti], dst, res_ssem.at[which, p, ti], res_rsem.at[which, p, TILES[ti][1]], partner)

    def dkv_copy(h, ti):
        up = TILES[ti][1]
        return remote(dkv_st.at[h, ti], dkv_out.at[4 * c + h, up], dkv_ssem.at[h, ti], dkv_rsem.at[h, up], partner)

    def res_put(p):
        heads = pl.ds(pl.multiple_of(16 * c + 8 * p, 8), 8)
        for ti, (oc, up) in enumerate(TILES):
            def body(i, _, keep):
                at = pl.ds(pl.multiple_of(i * 16, 16), 16)
                for stage, far, out in ((o_st, o_far, o_out), (dq_st, dq_far, dq_out)):
                    x = jnp.concatenate([stage[e, ti, pl.ds(pl.multiple_of(g * SLOT + i * 16, 16), 16), :][None]
                                         for e in range(2) for g in range(GROUP)], axis=0)
                    y = jnp.transpose(x, (1, 0, 2))
                    if keep:
                        out[up, at, heads, :] = y
                    else:
                        far[p, ti, at, :, :] = y
                return 0

            @pl.when(c == oc)
            def _():
                lax.fori_loop(0, SLOT // 16, functools.partial(body, keep=True), 0)

            @pl.when(c != oc)
            def _():
                lax.fori_loop(0, SLOT // 16, functools.partial(body, keep=False), 0)
                for which in range(2):
                    res_copy(p, ti, which).start()

    def dkv_put(h, ti, parts):
        oc, up = TILES[ti]

        @pl.when(c == oc)
        def _():
            for w in range(2):
                dkv_out[4 * c + h, up, w] = parts(w).astype(BF16)

        @pl.when(c != oc)
        def _():
            for w in range(2):
                dkv_st[h, ti, w] = parts(w).astype(BF16)
            dkv_copy(h, ti).start()

    lse_far = remote(lse_st.at[pc], lse_out.at[:, own_heads, :], lse_sem, lse_rsem, partner)

    def kv_slot(h, s, which):
        return kv_all[h, min(s, 7 - s), int(s > 3), which]

    def kv_slots(h, a, b, which):
        return jnp.concatenate([kv_slot(h, s, which) for s in range(a, b)], axis=0)

    def run_chip(ch):
        slots = [slot_of(ch, ti) for ti in range(4)]
        sent = [0, 1] if ch == 1 else [2, 3, 4, 5]
        kept = [0, 1] if ch == 0 else [2, 3, 4, 5]
        order = [0, 1, 2, 3]

        def transposes(s):
            for src, dst in ((0, kt), (1, vt)):
                dst[:, s * SLOT:(s + 1) * SLOT] = jnp.transpose(kv_slot(h_ref[0], s, src))

        h_ref = [None]

        def head(h, _):
            h_ref[0] = h
            seen = set()
            ready = set()

            def wait_slot(s):
                if s in ready:
                    return
                if s in slots:
                    kv_wait(h, partner, True)
                    new = slots
                elif ch == 1:
                    for owner in (0, 1):
                        kv_wait(h, owner, False)
                    new = [0, 1]
                else:
                    for owner in (2, 3):
                        kv_wait(h, owner, True)
                    new = [2, 3, 4, 5]
                for u in new:
                    ready.add(u)
                    transposes(u)

            for ti in order:
                s = slots[ti]
                nk = s + 1
                for u in range(nk):
                    wait_slot(u)
                qt = qh[h, ti].reshape(TILE, HEAD)
                dt = doh[h, ti].reshape(TILE, HEAD)
                m8 = [None] * GROUP
                for a in range(0, nk, 2):
                    n = min(2, nk - a)
                    kb = kv_slots(h, a, a + n, 0)
                    sc = mm(kb, qt, NT)
                    for j in range(n):
                        cap = caps[8 + ti] if a + j == s else caps[a + j]
                        for g in range(GROUP):
                            x = jnp.minimum(sc[j * SLOT:(j + 1) * SLOT, g * SLOT:(g + 1) * SLOT], cap)
                            st[(a + j) * SLOT:(a + j + 1) * SLOT, g * SLOT:(g + 1) * SLOT] = x
                            top = jnp.max(x.reshape(SLOT // 8, 8, SLOT), axis=0)
                            m8[g] = top if m8[g] is None else jnp.maximum(m8[g], top)
                m = [jnp.max(x, axis=0, keepdims=True) for x in m8]
                mc = [x * C2 for x in m]
                l8 = [None] * GROUP
                for a in range(nk):
                    for g in range(GROUP):
                        at = (slice(a * SLOT, (a + 1) * SLOT), slice(g * SLOT, (g + 1) * SLOT))
                        e = jnp.exp2(st[at] * C2 - mc[g])
                        st[at] = e
                        pb[at] = e.astype(BF16)
                        tot = jnp.sum(e.reshape(SLOT // 8, 8, SLOT), axis=0)
                        l8[g] = tot if l8[g] is None else l8[g] + tot
                ot = mm(vt[:, :nk * SLOT], pb[:nk * SLOT, :], NN)
                inv, dd = [], []
                oc, up = TILES[ti]
                for g in range(GROUP):
                    l = jnp.sum(l8[g], axis=0, keepdims=True)
                    has = m[g] > 0.5 * FILL
                    safe = jnp.where(has, l, 1.0)
                    i_l = jnp.where(has, 1.0 / safe, 0.0)
                    lse = jnp.where(has, m[g] * SCALE + jnp.log(safe), 0.0)
                    lse_st[oc, up, pl.ds(h * GROUP + g, 1), :] = lse
                    og = (ot[:, g * SLOT:(g + 1) * SLOT] * i_l).astype(BF16)
                    dog = jnp.transpose(dt[g * SLOT:(g + 1) * SLOT, :])
                    dd.append(jnp.sum(og.astype(F32) * dog.astype(F32), axis=0, keepdims=True))
                    inv.append(i_l)
                    o_st[h % 2, ti, g * SLOT:(g + 1) * SLOT, :] = jnp.transpose(og)

                first = [u for u in range(nk) if u in sent] if (ch == 0 and ti >= 2) else []
                rest = [u for u in range(nk) if u not in first]
                dqt = None
                for part in (first, rest):
                    runs = []
                    for u in part:
                        if runs and runs[-1][1] == u and u - runs[-1][0] < 2:
                            runs[-1][1] = u + 1
                        else:
                            runs.append([u, u + 1])
                    for a, b in runs:
                        n = b - a
                        vb = kv_slots(h, a, b, 1)
                        dp = mm(vb, dt, NT)
                        for j in range(n):
                            for g in range(GROUP):
                                at = (slice((a + j) * SLOT, (a + j + 1) * SLOT), slice(g * SLOT, (g + 1) * SLOT))
                                p = st[at] * inv[g]
                                pb[at] = p.astype(BF16)
                                ds = p * (dp[j * SLOT:(j + 1) * SLOT, g * SLOT:(g + 1) * SLOT] - dd[g])
                                db[at] = ds.astype(BF16)
                        dsb = db[a * SLOT:b * SLOT, :]
                        dv = mm(pb[a * SLOT:b * SLOT, :], dt, NN)
                        dk = mm(dsb, qt, NN) * SCALE
                        dq = mm(kt[:, a * SLOT:b * SLOT], dsb, NN)
                        dqt = dq if dqt is None else dqt + dq
                        for j in range(n):
                            u = a + j
                            new = (dk[j * SLOT:(j + 1) * SLOT], dv[j * SLOT:(j + 1) * SLOT])
                            for w in range(2):
                                dkv_acc[h, u, w] = dkv_acc[h, u, w] + new[w] if u in seen else new[w]
                            seen.add(u)
                    if part is first and ti == 3 and ch == 0:
                        part_run(0, h, lambda cp: cp.start())
                for g in range(GROUP):
                    dqg = (dqt[:, g * SLOT:(g + 1) * SLOT] * SCALE).astype(BF16)
                    dq_st[h % 2, ti, g * SLOT:(g + 1) * SLOT, :] = jnp.transpose(dqg)
            if ch == 1:
                @pl.when(h < HC - 2)
                def _():
                    for to in (1, 2):
                        kv_push(h + 2, to, True).start()

                @pl.when(h == HC - 2)
                def _():
                    for e in range(SWAP):
                        swap_copy(e).start()

                @pl.when(h == HC - 1)
                def _():
                    for e in range(HC):
                        part_copy(e, 0, 2).start()
            else:
                for ti in (2, 3):
                    dkv_put(h, ti, lambda w, ti=ti: dkv_acc[h, slots[ti], w])
            pl.when(h % 2 == 1)(lambda: res_put(h // 2))
            return 0

        lax.fori_loop(0, HC, head, 0)

        lse_out[:, own_heads, :] = lse_st[c]
        lse_far.start()

        if ch == 0:
            def swapped(h, _):
                swap_copy(h).wait_recv()
                for w in range(2):
                    back_st[h, w] = (dkv_in[h, 2, w] + dkv_acc[h, 5, w]).astype(BF16)
                swap_back(h).start()
                return 0
            lax.fori_loop(0, SWAP, swapped, 0)

        def tail(h, _):
            part_run(1 - ch, h, lambda cp: cp.wait_recv())
            for i, u in enumerate(kept):
                ti = slots.index(u)
                put = functools.partial(dkv_put, h, ti, lambda w, u=u, i=i: dkv_acc[h, u, w] + dkv_in[h, i, w])
                if u == 5:
                    pl.when(h >= SWAP)(put)
                else:
                    put()
            return 0
        lax.fori_loop(0, HC, tail, 0)

        def drain(h, _):
            part_run(ch, h, lambda cp: cp.wait_send())
            return 0
        lax.fori_loop(0, HC, drain, 0)

        def drain_swap(h, _):
            if ch == 0:
                swap_back(h).wait_send()
            else:
                swap_copy(h).wait_send()
            return 0
        lax.fori_loop(0, SWAP, drain_swap, 0)

        if ch == 1:
            @pl.when(c == 0)
            def _():
                for core in range(2):
                    for h in range(SWAP):
                        remote(back_st.at[h], dkv_out.at[4 * core + h, 1], back_ssem.at[h], back_rsem.at[4 * core + h], 2).wait_recv()

    pl.when(chip == 0)(functools.partial(run_chip, 0))
    pl.when(chip == 1)(functools.partial(run_chip, 1))

    push_q.wait_send()
    push_do.wait_send()
    for cp in push_val:
        cp.wait_send()

    def drain(h, _):
        kv_push(h, 0, True).wait_send()
        for ch in range(2):
            @pl.when(chip == ch)
            def _():
                for to in (1, 2):
                    kv_push(h, to, ch == 1).wait_send()
        far = jnp.logical_and(chip == 1, h < SWAP)
        for ti in range(4):
            sent = c != TILES[ti][0]
            pl.when(jnp.logical_and(sent, jnp.logical_not(far)) if ti == 3 else sent)(dkv_copy(h, ti).wait_send)
        for up in range(2):
            come = remote(dkv_st.at[h, 0], dkv_out.at[4 * pc + h, up], dkv_ssem.at[h, 0], dkv_rsem.at[h, up], partner)
            if up:
                pl.when(jnp.logical_not(jnp.logical_and(far, c == 0)))(come.wait_recv)
            else:
                come.wait_recv()
        return 0
    lax.fori_loop(0, HC, drain, 0)

    for p in range(2):
        for which in range(2):
            stage, out = ((o_far, o_out), (dq_far, dq_out))[which]
            for ti in range(4):
                pl.when(c != TILES[ti][0])(res_copy(p, ti, which).wait_send)
            for up in range(2):
                dst = out.at[up, :, pl.ds(pl.multiple_of(16 * pc + 8 * p, 8), 8), :]
                remote(stage.at[p, 0], dst, res_ssem.at[which, p, 0], res_rsem.at[which, p, up], partner).wait_recv()
    lse_far.wait_send()
    remote(lse_st.at[0], lse_out.at[:, oth_heads, :], lse_sem, lse_rsem, partner).wait_recv()


def attn_call(cu, valid, q, k, v, do):
    any_spec = pl.BlockSpec(memory_space=pl.ANY)
    dma = pltpu.SemaphoreType.DMA
    return pl.pallas_call(
        attn_kernel,
        out_shape=(
            pltpu.VMEM((2, SLOT, 32, HEAD), BF16),
            pltpu.VMEM((2, SLOT, 32, HEAD), BF16),
            pltpu.VMEM((8, 2, 2, SLOT, HEAD), BF16),
            pltpu.VMEM((2, 32, SLOT), F32),
            pltpu.SMEM((3,), jnp.int32),
        ),
        in_specs=[any_spec] * 6,
        out_specs=(pl.BlockSpec(memory_space=pltpu.VMEM),) * 4 + (pl.BlockSpec(memory_space=pltpu.SMEM),),
        scratch_shapes=[
            pltpu.VMEM((256, 16, HEAD), BF16),
            pltpu.VMEM((256, 16, HEAD), BF16),
            pltpu.VMEM((256, 16, HEAD), BF16),
            pltpu.VMEM((256, 16, HEAD), BF16),
            pltpu.VMEM((256, 8, HEAD), BF16),
            pltpu.VMEM((256, 8, HEAD), BF16),
            pltpu.VMEM((8, 2, 2, SLOT, HEAD), BF16),
            pltpu.VMEM((HC, 4, 2, 2, SLOT, HEAD), BF16),
            pltpu.VMEM((HEAD, 8 * SLOT), BF16),
            pltpu.VMEM((HEAD, 8 * SLOT), BF16),
            pltpu.VMEM((HC, 4, GROUP, SLOT, HEAD), BF16),
            pltpu.VMEM((HC, 4, GROUP, SLOT, HEAD), BF16),
            pltpu.VMEM((8 * SLOT, TILE), F32),
            pltpu.VMEM((8 * SLOT, TILE), BF16),
            pltpu.VMEM((8 * SLOT, TILE), BF16),
            pltpu.VMEM((HC, 8, 2, SLOT, HEAD), F32),
            pltpu.VMEM((HC, 4, 2, SLOT, HEAD), F32),
            pltpu.VMEM((2, 4, TILE, HEAD), BF16),
            pltpu.VMEM((2, 4, TILE, HEAD), BF16),
            pltpu.VMEM((2, 4, SLOT, 8, HEAD), BF16),
            pltpu.VMEM((2, 4, SLOT, 8, HEAD), BF16),
            pltpu.VMEM((HC, 4, 2, SLOT, HEAD), BF16),
            pltpu.VMEM((HC, 2, SLOT, HEAD), BF16),
            pltpu.VMEM((2, 2, 16, SLOT), F32),
            pltpu.VMEM((12, SLOT, SLOT), F32),
            pltpu.VMEM((4, 1, 2 * SLOT), jnp.int32),
            dma((6,)),
            dma((2,)), dma((2,)),
            dma((3,)), dma((4,)),
            dma((3, HC)), dma((HC, 4)),
            dma((HC,)), dma((HC,)),
            dma((HC,)), dma((HC,)), dma((HC,)), dma((8,)),
            dma((2, 2, 4)), dma((2, 2, 2)),
            dma((HC, 4)), dma((HC, 2)),
            dma, dma,
        ],
        compiler_params=pltpu.CompilerParams(collective_id=0, has_side_effects=True, vmem_limit_bytes=61300000),
        name="attn",
    )(cu, valid, q, k, v, do)


def finish_kernel(o_in, dq_in, dkv_in, lse_in, cu, o_out, dq_out, dk_out, dv_out, lse_out, dk_t, dv_t, lse_t, sem, lse_sem):
    l0 = lax.shift_right_logical(cu[1], 3)
    rest = SLOT - l0

    def copies(i, x, out):
        runs = ((0, 0, 0, l0), (1, 0, l0, l0), (0, l0, 2 * l0, rest), (1, l0, SLOT + l0, rest))
        return [pltpu.make_async_copy(x.at[up, pl.ds(at, n)], out.at[pl.ds(to, n)], sem.at[i, j])
                for j, (up, at, to, n) in enumerate(runs)]

    moves = copies(0, o_in, o_out) + copies(1, dq_in, dq_out)
    for cp in moves:
        cp.start()

    for w, dst in ((0, dk_t), (1, dv_t)):
        for up in range(2):
            def body(i, _):
                at = pl.ds(pl.multiple_of(i * 16, 16), 16)
                dst[up, at] = jnp.transpose(dkv_in[:, up, w, at, :], (1, 0, 2))
                return 0
            lax.fori_loop(0, SLOT // 16, body, 0)
        more = copies(2 + w, dst, (dk_out, dv_out)[w])
        for cp in more:
            cp.start()
        moves += more

    row = lax.broadcasted_iota(jnp.int32, (2 * SLOT, SLOT), 0)
    col = lax.broadcasted_iota(jnp.int32, (2 * SLOT, SLOT), 1)
    acc = None
    for up in range(2):
        if up:
            src = jnp.where(col < l0, col + l0, col + SLOT)
        else:
            src = jnp.where(col < l0, col, col + l0)
        pick = jnp.where(row == src, 1.0, 0.0)
        part = lax.dot_general(lse_in[up], pick, NT, precision=lax.Precision.HIGHEST, preferred_element_type=F32)
        acc = part if acc is None else acc + part
    lse_t[...] = acc
    lse_move = pltpu.make_async_copy(lse_t, lse_out, lse_sem)
    lse_move.start()
    for cp in moves + [lse_move]:
        cp.wait()


def finish_call(o_t, dq_t, dkv_hm, lse_hm, cu):
    any_spec = pl.BlockSpec(memory_space=pl.ANY)
    vmem = pl.BlockSpec(memory_space=pltpu.VMEM)
    return pl.pallas_call(
        finish_kernel,
        out_shape=(
            jax.ShapeDtypeStruct((256, 32, HEAD), BF16),
            jax.ShapeDtypeStruct((256, 32, HEAD), BF16),
            jax.ShapeDtypeStruct((256, 8, HEAD), BF16),
            jax.ShapeDtypeStruct((256, 8, HEAD), BF16),
            jax.ShapeDtypeStruct((32, 256), F32),
        ),
        in_specs=[vmem] * 4 + [pl.BlockSpec(memory_space=pltpu.SMEM)],
        out_specs=(any_spec,) * 5,
        scratch_shapes=[
            pltpu.VMEM((2, SLOT, 8, HEAD), BF16),
            pltpu.VMEM((2, SLOT, 8, HEAD), BF16),
            pltpu.VMEM((32, 256), F32),
            pltpu.SemaphoreType.DMA((4, 4)),
            pltpu.SemaphoreType.DMA,
        ],
        compiler_params=pltpu.CompilerParams(vmem_limit_bytes=16 * 1024 * 1024),
        name="finish",
    )(o_t, dq_t, dkv_hm, lse_hm, cu)


def solution(mesh):
    tok_spec = P(("dp", "cp"), None, None)
    lse_spec = P(("dp", "cp"), None)

    def local(q, k, v, do, valid, cu):
        res = attn_call(cu, valid.reshape(1, 256), q, k, v, do)
        o, dq, dk, dv, lse = finish_call(*res)
        return o, lse.T, dq, dk, dv

    return jax.shard_map(local, mesh=mesh, in_specs=(tok_spec,) * 4 + (P(("dp", "cp")), P("dp")),
                         out_specs=(tok_spec, lse_spec, tok_spec, tok_spec, tok_spec), check_vma=False)
```

```python
import functools
import math

import jax
import jax.numpy as jnp
from jax import lax
from jax.experimental import pallas as pl
from jax.experimental.pallas import tpu as pltpu
from jax.sharding import PartitionSpec as P

MESH = pl.DeviceIdType.MESH
FILL = -1.0e30
BIG = 3.0e38
HEAD = 128
SLOT = 128
TILE = 512
GROUP = 4
HC = 4
SWAP = 3
SCALE = HEAD ** -0.5
C2 = SCALE * math.log2(math.e)
NT = (((1,), (1,)), ((), ()))
NN = (((1,), (0,)), ((), ()))
F32 = jnp.float32
BF16 = jnp.bfloat16

TILES = ((0, 0), (1, 0), (1, 1), (0, 1))


def slot_of(chip, ti):
    oc, up = TILES[ti]
    r = 2 * chip + oc
    return 7 - r if up else r


def mm(a, b, dims):
    return lax.dot_general(a, b, dims, preferred_element_type=F32)


def src_row(up, t, l0):
    if up:
        return jnp.where(t < l0, t + l0, t + SLOT)
    return jnp.where(t < l0, t, t + l0)


def attn_kernel(cu_hbm, valid, q, k, v, do, o_out, dq_out, dkv_out, lse_out, cu,
                raw_q, raw_do, far_q, far_do, raw_k, raw_v, kv_hm, kv_all, kt, vt, qh, doh, st0, st1, pb, db,
                dkv_acc, dkv_in, o_st, dq_st, o_far, dq_far, dkv_st, back_st, lse_st, caps, valid_all,
                in_sem, raw_ssem, raw_rsem, val_ssem, val_rsem, kv_ssem, kv_rsem,
                part_ssem, part_rsem, swap_ssem, swap_rsem, back_ssem, back_rsem, res_ssem, res_rsem, dkv_ssem, dkv_rsem, lse_sem, lse_rsem):
    r = lax.axis_index("cp")
    chip = r // 2
    c = r % 2
    pc = 1 - c
    partner = chip * 2 + pc
    cross = (1 - chip) * 2 + c
    cross_o = (1 - chip) * 2 + pc

    def remote(src, dst, ssem, rsem, dev):
        return pltpu.make_async_remote_copy(src_ref=src, dst_ref=dst, send_sem=ssem, recv_sem=rsem,
                                            device_id={"cp": dev}, device_id_type=MESH)

    own_heads = pl.ds(pl.multiple_of(16 * c, 16), 16)
    oth_heads = pl.ds(pl.multiple_of(16 * pc, 16), 16)
    ld_k = pltpu.make_async_copy(k, raw_k, in_sem.at[0])
    ld_v = pltpu.make_async_copy(v, raw_v, in_sem.at[1])
    ld_q = pltpu.make_async_copy(q.at[:, own_heads, :], raw_q, in_sem.at[2])
    ld_do = pltpu.make_async_copy(do.at[:, own_heads, :], raw_do, in_sem.at[3])
    ld_val = pltpu.make_async_copy(valid, valid_all.at[r], in_sem.at[4])
    ld_cu = pltpu.make_async_copy(cu_hbm, cu, in_sem.at[5])
    for cp in (ld_cu, ld_k, ld_v, ld_q, ld_do, ld_val):
        cp.start()

    barrier = pltpu.get_barrier_semaphore()
    for dev in (partner, cross, cross_o):
        pl.semaphore_signal(barrier, inc=1, device_id={"cp": dev}, device_id_type=MESH)
    pl.semaphore_wait(barrier, 3)
    ld_cu.wait()
    l0 = lax.shift_right_logical(cu[1], 3)

    peers = (partner, cross, cross_o)
    push_q = remote(q.at[:, oth_heads, :], far_q, raw_ssem.at[0], raw_rsem.at[0], partner)
    push_do = remote(do.at[:, oth_heads, :], far_do, raw_ssem.at[1], raw_rsem.at[1], partner)
    push_val = [remote(valid, valid_all.at[r], val_ssem.at[i], val_rsem.at[r], dev) for i, dev in enumerate(peers)]

    push_q.start()
    push_do.start()

    def kv_relayout(up):
        def body(i, _):
            t0 = i * 16
            for which, raw in ((0, raw_k), (1, raw_v)):
                rows = jnp.stack([raw[src_row(up, t0 + j, l0)] for j in range(16)])
                kv_hm[:, up, which, pl.ds(pl.multiple_of(t0, 16), 16), :] = jnp.transpose(rows, (1, 0, 2))
            return 0
        lax.fori_loop(0, SLOT // 16, body, 0)

    def kv_push(h, to, both):
        head = (4 * c if to == 1 else 4 * pc) + h
        dev = (partner, cross, cross_o)[to]
        ups = pl.ds(0, 2 if both else 1)
        return remote(kv_hm.at[head, ups], kv_all.at[h, r, ups], kv_ssem.at[to, h], kv_rsem.at[h, r], dev)

    def kv_wait(h, owner, both):
        ups = pl.ds(0, 2 if both else 1)
        remote(kv_hm.at[0, ups], kv_all.at[h, owner, ups], kv_ssem.at[0, h], kv_rsem.at[h, owner], partner).wait_recv()

    ld_k.wait()
    ld_v.wait()
    kv_relayout(0)

    def cross_send(ch, h):
        @pl.when(chip == ch)
        def _():
            for to in (1, 2):
                kv_push(h, to, ch == 1).start()

    cross_send(0, 0)
    kv_relayout(1)
    cross_send(1, 0)
    for h in range(HC):
        kv_push(h, 0, True).start()
    ld_val.wait()
    for cp in push_val:
        cp.start()

    def copy_own(h, _):
        for up in range(2):
            kv_all[h, r, up] = kv_hm[4 * c + h, up]
        return 0
    lax.fori_loop(0, HC, copy_own, 0)

    def q_relayout(oc, from_q, from_do):
        for up, ti in ((0, oc), (1, 3 - oc)):
            def body(i, _):
                t0 = i * 16
                at = pl.ds(pl.multiple_of(t0, 16), 16)
                for raw, dst in ((from_q, qh), (from_do, doh)):
                    rows = jnp.stack([raw[src_row(up, t0 + j, l0)] for j in range(16)])
                    dst[:, ti, :, at, :] = jnp.transpose(rows, (1, 0, 2)).reshape(HC, GROUP, 16, HEAD)
                return 0
            lax.fori_loop(0, SLOT // 16, body, 0)

    ld_q.wait()
    ld_do.wait()
    cross_send(0, 1)
    q_relayout(c, raw_q, raw_do)

    cross_send(0, 2)
    for i in range(3):
        remote(valid, valid_all.at[peers[i]], val_ssem.at[i], val_rsem.at[peers[i]], peers[i]).wait_recv()
    lane = lax.broadcasted_iota(jnp.int32, (SLOT, SLOT), 1)
    sub = lax.broadcasted_iota(jnp.int32, (SLOT, SLOT), 0)
    lane2 = lax.broadcasted_iota(jnp.int32, (SLOT, 2 * SLOT), 1)
    sub2 = lax.broadcasted_iota(jnp.int32, (SLOT, 2 * SLOT), 0)
    same_doc = (lane < l0) == (sub < l0)
    doc_f = jnp.where(lane < l0, 1.0, 0.0)
    doc_s = jnp.where(sub < l0, 1.0, 0.0)
    same_f = jnp.where(doc_f == doc_s, 1.0, 0.0)
    del same_doc

    def cap_body(s, _):
        owner = jnp.where(s < 4, s, 7 - s)
        off = jnp.where(s < 4, 0, 1)
        src_lo = jnp.where(sub2 < l0, sub2, sub2 + l0)
        src_hi = jnp.where(sub2 < l0, sub2 + l0, sub2 + SLOT)
        src = jnp.where(off == 1, src_hi, src_lo)
        row = jnp.broadcast_to(valid_all[owner].astype(F32), (SLOT, 2 * SLOT))
        ok = jnp.sum(jnp.where(src == lane2, row, 0.0), axis=1, keepdims=True)
        caps[s] = jnp.where(same_f * ok > 0.5, BIG, FILL)
        return 0
    lax.fori_loop(0, 8, cap_body, 0)
    for ti in range(4):
        oc, up = TILES[ti]
        s = (7 - (2 * chip + oc)) if up else 2 * chip + oc
        caps[8 + ti] = jnp.where(sub <= lane, caps[s], FILL)

    cross_send(0, 3)
    cross_send(1, 1)
    push_q.wait_recv()
    push_do.wait_recv()
    q_relayout(pc, far_q, far_do)

    def part_copy(h, i, n):
        return remote(dkv_acc.at[h, pl.ds(i, n)], dkv_in.at[h, pl.ds(0, n)], part_ssem.at[h], part_rsem.at[h], cross)

    def part_run(ch, h, act):
        if ch == 1:
            act(part_copy(h, 0, 2))
        else:
            pl.when(h < SWAP)(lambda: act(part_copy(h, 2, 3)))
            pl.when(h >= SWAP)(lambda: act(part_copy(h, 2, 4)))

    def swap_copy(h):
        return remote(dkv_acc.at[h, 5], dkv_in.at[h, 2], swap_ssem.at[h], swap_rsem.at[h], cross)

    def swap_back(h):
        return remote(back_st.at[h], dkv_out.at[4 * c + h, 1], back_ssem.at[h], back_rsem.at[4 * c + h], 2)

    def res_copy(p, ti, which):
        stage, out = ((o_far, o_out), (dq_far, dq_out))[which]
        dst = out.at[TILES[ti][1], :, pl.ds(pl.multiple_of(16 * c + 8 * p, 8), 8), :]
        return remote(stage.at[p, ti], dst, res_ssem.at[which, p, ti], res_rsem.at[which, p, TILES[ti][1]], partner)

    def dkv_copy(h, ti):
        up = TILES[ti][1]
        return remote(dkv_st.at[h, ti], dkv_out.at[4 * c + h, up], dkv_ssem.at[h, ti], dkv_rsem.at[h, up], partner)

    def res_put(p):
        heads = pl.ds(pl.multiple_of(16 * c + 8 * p, 8), 8)
        for ti, (oc, up) in enumerate(TILES):
            def body(i, _, keep):
                at = pl.ds(pl.multiple_of(i * 16, 16), 16)
                for stage, far, out in ((o_st, o_far, o_out), (dq_st, dq_far, dq_out)):
                    x = jnp.concatenate([stage[e, ti, pl.ds(pl.multiple_of(g * SLOT + i * 16, 16), 16), :][None]
                                         for e in range(2) for g in range(GROUP)], axis=0)
                    y = jnp.transpose(x, (1, 0, 2))
                    if keep:
                        out[up, at, heads, :] = y
                    else:
                        far[p, ti, at, :, :] = y
                return 0

            @pl.when(c == oc)
            def _():
                lax.fori_loop(0, SLOT // 16, functools.partial(body, keep=True), 0)

            @pl.when(c != oc)
            def _():
                lax.fori_loop(0, SLOT // 16, functools.partial(body, keep=False), 0)
                for which in range(2):
                    res_copy(p, ti, which).start()

    def dkv_put(h, ti, parts):
        oc, up = TILES[ti]

        @pl.when(c == oc)
        def _():
            for w in range(2):
                dkv_out[4 * c + h, up, w] = parts(w).astype(BF16)

        @pl.when(c != oc)
        def _():
            for w in range(2):
                dkv_st[h, ti, w] = parts(w).astype(BF16)
            dkv_copy(h, ti).start()

    lse_far = remote(lse_st.at[pc], lse_out.at[:, own_heads, :], lse_sem, lse_rsem, partner)

    def kv_slot(h, s, which):
        return kv_all[h, min(s, 7 - s), int(s > 3), which]

    def kv_slots(h, a, b, which):
        return jnp.concatenate([kv_slot(h, s, which) for s in range(a, b)], axis=0)

    def run_chip(ch):
        slots = [slot_of(ch, ti) for ti in range(4)]
        sent = [0, 1] if ch == 1 else [2, 3, 4, 5]
        kept = [0, 1] if ch == 0 else [2, 3, 4, 5]

        def transposes(s):
            for src, dst in ((0, kt), (1, vt)):
                dst[:, s * SLOT:(s + 1) * SLOT] = jnp.transpose(kv_slot(h_ref[0], s, src))

        h_ref = [None]
        sts = (st0, st1)

        def point(h, where):
            if ch == 0:
                return
            kv = {(0, 3): 2, (1, 2): 3}
            swaps = {(1, 4): (0, 1), (2, 4): (2,)}
            parts = {(2, 2): (0,), (2, 4): (1,), (3, 4): (2, 3)}
            for at in range(HC):
                if not any((at, where) in d for d in (kv, swaps, parts)):
                    continue

                @pl.when(h == at)
                def _():
                    if (at, where) in kv:
                        for to in (1, 2):
                            kv_push(kv[at, where], to, True).start()
                    for e in swaps.get((at, where), ()):
                        swap_copy(e).start()
                    for e in parts.get((at, where), ()):
                        part_copy(e, 0, 2).start()

        def head(h, _):
            h_ref[0] = h
            seen = set()
            ready = set()

            def wait_slot(s):
                if s in ready:
                    return
                if s in slots:
                    kv_wait(h, partner, True)
                    new = slots
                elif ch == 1:
                    for owner in (0, 1):
                        kv_wait(h, owner, False)
                    new = [0, 1]
                else:
                    for owner in (2, 3):
                        kv_wait(h, owner, True)
                    new = [2, 3, 4, 5]
                for u in new:
                    ready.add(u)
                    transposes(u)

            state = {}

            def forward(ti):
                point(h, ti)
                s = slots[ti]
                nk = s + 1
                for u in range(nk):
                    wait_slot(u)
                st = sts[ti % 2]
                qt = qh[h, ti].reshape(TILE, HEAD)
                dt = doh[h, ti].reshape(TILE, HEAD)
                m8 = [None] * GROUP
                for a in range(0, nk, 2):
                    n = min(2, nk - a)
                    kb = kv_slots(h, a, a + n, 0)
                    sc = mm(kb, qt, NT)
                    for j in range(n):
                        cap = caps[8 + ti] if a + j == s else caps[a + j]
                        for g in range(GROUP):
                            x = jnp.minimum(sc[j * SLOT:(j + 1) * SLOT, g * SLOT:(g + 1) * SLOT], cap)
                            st[(a + j) * SLOT:(a + j + 1) * SLOT, g * SLOT:(g + 1) * SLOT] = x
                            top = jnp.max(x.reshape(SLOT // 8, 8, SLOT), axis=0)
                            m8[g] = top if m8[g] is None else jnp.maximum(m8[g], top)
                m = [jnp.max(x, axis=0, keepdims=True) for x in m8]
                mc = [x * C2 for x in m]
                l8 = [None] * GROUP
                for a in range(nk):
                    for g in range(GROUP):
                        at = (slice(a * SLOT, (a + 1) * SLOT), slice(g * SLOT, (g + 1) * SLOT))
                        e = jnp.exp2(st[at] * C2 - mc[g])
                        st[at] = e
                        pb[at] = e.astype(BF16)
                        tot = jnp.sum(e.reshape(SLOT // 8, 8, SLOT), axis=0)
                        l8[g] = tot if l8[g] is None else l8[g] + tot
                ot = mm(vt[:, :nk * SLOT], pb[:nk * SLOT, :], NN)
                inv, dd = [], []
                oc, up = TILES[ti]
                for g in range(GROUP):
                    l = jnp.sum(l8[g], axis=0, keepdims=True)
                    has = m[g] > 0.5 * FILL
                    safe = jnp.where(has, l, 1.0)
                    i_l = jnp.where(has, 1.0 / safe, 0.0)
                    lse = jnp.where(has, m[g] * SCALE + jnp.log(safe), 0.0)
                    lse_st[oc, up, pl.ds(h * GROUP + g, 1), :] = lse
                    og = (ot[:, g * SLOT:(g + 1) * SLOT] * i_l).astype(BF16)
                    dog = jnp.transpose(dt[g * SLOT:(g + 1) * SLOT, :])
                    dd.append(jnp.sum(og.astype(F32) * dog.astype(F32), axis=0, keepdims=True))
                    inv.append(i_l)
                    o_st[h % 2, ti, g * SLOT:(g + 1) * SLOT, :] = jnp.transpose(og)

                state[ti] = [inv, dd, None]

            def backward(ti, part):
                inv, dd, dqt = state[ti]
                qt = qh[h, ti].reshape(TILE, HEAD)
                dt = doh[h, ti].reshape(TILE, HEAD)
                st = sts[ti % 2]
                runs = []
                for u in part:
                    if runs and runs[-1][1] == u and u - runs[-1][0] < 2:
                        runs[-1][1] = u + 1
                    else:
                        runs.append([u, u + 1])
                for a, b in runs:
                    n = b - a
                    vb = kv_slots(h, a, b, 1)
                    dp = mm(vb, dt, NT)
                    for j in range(n):
                        for g in range(GROUP):
                            at = (slice((a + j) * SLOT, (a + j + 1) * SLOT), slice(g * SLOT, (g + 1) * SLOT))
                            p = st[at] * inv[g]
                            pb[at] = p.astype(BF16)
                            ds = p * (dp[j * SLOT:(j + 1) * SLOT, g * SLOT:(g + 1) * SLOT] - dd[g])
                            db[at] = ds.astype(BF16)
                    dsb = db[a * SLOT:b * SLOT, :]
                    dv = mm(pb[a * SLOT:b * SLOT, :], dt, NN)
                    dk = mm(dsb, qt, NN) * SCALE
                    dq = mm(kt[:, a * SLOT:b * SLOT], dsb, NN)
                    dqt = dq if dqt is None else dqt + dq
                    for j in range(n):
                        u = a + j
                        new = (dk[j * SLOT:(j + 1) * SLOT], dv[j * SLOT:(j + 1) * SLOT])
                        for w in range(2):
                            dkv_acc[h, u, w] = dkv_acc[h, u, w] + new[w] if u in seen else new[w]
                        seen.add(u)
                state[ti][2] = dqt

            def finish(ti):
                dqt = state[ti][2]
                for g in range(GROUP):
                    dqg = (dqt[:, g * SLOT:(g + 1) * SLOT] * SCALE).astype(BF16)
                    dq_st[h % 2, ti, g * SLOT:(g + 1) * SLOT, :] = jnp.transpose(dqg)

            if ch == 0:
                for ti in (0, 1):
                    forward(ti)
                    backward(ti, range(slots[ti] + 1))
                    finish(ti)
                for ti in (2, 3):
                    forward(ti)
                    backward(ti, sent)
                part_run(0, h, lambda cp: cp.start())
                for ti in (2, 3):
                    backward(ti, [u for u in range(slots[ti] + 1) if u not in sent])
                    finish(ti)
            else:
                for ti in range(4):
                    forward(ti)
                    backward(ti, range(slots[ti] + 1))
                    finish(ti)
            if ch == 1:
                point(h, 4)
            else:
                for ti in (2, 3):
                    dkv_put(h, ti, lambda w, ti=ti: dkv_acc[h, slots[ti], w])
            pl.when(h % 2 == 1)(lambda: res_put(h // 2))
            return 0

        lax.fori_loop(0, HC, head, 0)

        lse_out[:, own_heads, :] = lse_st[c]
        lse_far.start()

        if ch == 0:
            def swapped(h, _):
                swap_copy(h).wait_recv()
                for w in range(2):
                    back_st[h, w] = (dkv_in[h, 2, w] + dkv_acc[h, 5, w]).astype(BF16)
                swap_back(h).start()
                return 0
            lax.fori_loop(0, SWAP, swapped, 0)

        def tail(h, _):
            part_run(1 - ch, h, lambda cp: cp.wait_recv())
            for i, u in enumerate(kept):
                ti = slots.index(u)
                put = functools.partial(dkv_put, h, ti, lambda w, u=u, i=i: dkv_acc[h, u, w] + dkv_in[h, i, w])
                if u == 5:
                    pl.when(h >= SWAP)(put)
                else:
                    put()
            return 0
        lax.fori_loop(0, HC, tail, 0)

        def drain(h, _):
            part_run(ch, h, lambda cp: cp.wait_send())
            return 0
        lax.fori_loop(0, HC, drain, 0)

        def drain_swap(h, _):
            if ch == 0:
                swap_back(h).wait_send()
            else:
                swap_copy(h).wait_send()
            return 0
        lax.fori_loop(0, SWAP, drain_swap, 0)

        if ch == 1:
            @pl.when(c == 0)
            def _():
                for core in range(2):
                    for h in range(SWAP):
                        remote(back_st.at[h], dkv_out.at[4 * core + h, 1], back_ssem.at[h], back_rsem.at[4 * core + h], 2).wait_recv()

    pl.when(chip == 0)(functools.partial(run_chip, 0))
    pl.when(chip == 1)(functools.partial(run_chip, 1))

    push_q.wait_send()
    push_do.wait_send()
    for cp in push_val:
        cp.wait_send()

    def drain(h, _):
        kv_push(h, 0, True).wait_send()
        for ch in range(2):
            @pl.when(chip == ch)
            def _():
                for to in (1, 2):
                    kv_push(h, to, ch == 1).wait_send()
        far = jnp.logical_and(chip == 1, h < SWAP)
        for ti in range(4):
            sent = c != TILES[ti][0]
            pl.when(jnp.logical_and(sent, jnp.logical_not(far)) if ti == 3 else sent)(dkv_copy(h, ti).wait_send)
        for up in range(2):
            come = remote(dkv_st.at[h, 0], dkv_out.at[4 * pc + h, up], dkv_ssem.at[h, 0], dkv_rsem.at[h, up], partner)
            if up:
                pl.when(jnp.logical_not(jnp.logical_and(far, c == 0)))(come.wait_recv)
            else:
                come.wait_recv()
        return 0
    lax.fori_loop(0, HC, drain, 0)

    for p in range(2):
        for which in range(2):
            stage, out = ((o_far, o_out), (dq_far, dq_out))[which]
            for ti in range(4):
                pl.when(c != TILES[ti][0])(res_copy(p, ti, which).wait_send)
            for up in range(2):
                dst = out.at[up, :, pl.ds(pl.multiple_of(16 * pc + 8 * p, 8), 8), :]
                remote(stage.at[p, 0], dst, res_ssem.at[which, p, 0], res_rsem.at[which, p, up], partner).wait_recv()
    lse_far.wait_send()
    remote(lse_st.at[0], lse_out.at[:, oth_heads, :], lse_sem, lse_rsem, partner).wait_recv()


def attn_call(cu, valid, q, k, v, do):
    any_spec = pl.BlockSpec(memory_space=pl.ANY)
    dma = pltpu.SemaphoreType.DMA
    return pl.pallas_call(
        attn_kernel,
        out_shape=(
            pltpu.VMEM((2, SLOT, 32, HEAD), BF16),
            pltpu.VMEM((2, SLOT, 32, HEAD), BF16),
            pltpu.VMEM((8, 2, 2, SLOT, HEAD), BF16),
            pltpu.VMEM((2, 32, SLOT), F32),
            pltpu.SMEM((3,), jnp.int32),
        ),
        in_specs=[any_spec] * 6,
        out_specs=(pl.BlockSpec(memory_space=pltpu.VMEM),) * 4 + (pl.BlockSpec(memory_space=pltpu.SMEM),),
        scratch_shapes=[
            pltpu.VMEM((256, 16, HEAD), BF16),
            pltpu.VMEM((256, 16, HEAD), BF16),
            pltpu.VMEM((256, 16, HEAD), BF16),
            pltpu.VMEM((256, 16, HEAD), BF16),
            pltpu.VMEM((256, 8, HEAD), BF16),
            pltpu.VMEM((256, 8, HEAD), BF16),
            pltpu.VMEM((8, 2, 2, SLOT, HEAD), BF16),
            pltpu.VMEM((HC, 4, 2, 2, SLOT, HEAD), BF16),
            pltpu.VMEM((HEAD, 8 * SLOT), BF16),
            pltpu.VMEM((HEAD, 8 * SLOT), BF16),
            pltpu.VMEM((HC, 4, GROUP, SLOT, HEAD), BF16),
            pltpu.VMEM((HC, 4, GROUP, SLOT, HEAD), BF16),
            pltpu.VMEM((8 * SLOT, TILE), F32),
            pltpu.VMEM((8 * SLOT, TILE), F32),
            pltpu.VMEM((8 * SLOT, TILE), BF16),
            pltpu.VMEM((8 * SLOT, TILE), BF16),
            pltpu.VMEM((HC, 8, 2, SLOT, HEAD), F32),
            pltpu.VMEM((HC, 4, 2, SLOT, HEAD), F32),
            pltpu.VMEM((2, 4, TILE, HEAD), BF16),
            pltpu.VMEM((2, 4, TILE, HEAD), BF16),
            pltpu.VMEM((2, 4, SLOT, 8, HEAD), BF16),
            pltpu.VMEM((2, 4, SLOT, 8, HEAD), BF16),
            pltpu.VMEM((HC, 4, 2, SLOT, HEAD), BF16),
            pltpu.VMEM((HC, 2, SLOT, HEAD), BF16),
            pltpu.VMEM((2, 2, 16, SLOT), F32),
            pltpu.VMEM((12, SLOT, SLOT), F32),
            pltpu.VMEM((4, 1, 2 * SLOT), jnp.int32),
            dma((6,)),
            dma((2,)), dma((2,)),
            dma((3,)), dma((4,)),
            dma((3, HC)), dma((HC, 4)),
            dma((HC,)), dma((HC,)),
            dma((HC,)), dma((HC,)), dma((HC,)), dma((8,)),
            dma((2, 2, 4)), dma((2, 2, 2)),
            dma((HC, 4)), dma((HC, 2)),
            dma, dma,
        ],
        compiler_params=pltpu.CompilerParams(collective_id=0, has_side_effects=True, vmem_limit_bytes=61300000),
        name="attn",
    )(cu, valid, q, k, v, do)


def finish_kernel(o_in, dq_in, dkv_in, lse_in, cu, o_out, dq_out, dk_out, dv_out, lse_out, dk_t, dv_t, lse_t, sem, lse_sem):
    l0 = lax.shift_right_logical(cu[1], 3)
    rest = SLOT - l0

    def copies(i, x, out):
        runs = ((0, 0, 0, l0), (1, 0, l0, l0), (0, l0, 2 * l0, rest), (1, l0, SLOT + l0, rest))
        return [pltpu.make_async_copy(x.at[up, pl.ds(at, n)], out.at[pl.ds(to, n)], sem.at[i, j])
                for j, (up, at, to, n) in enumerate(runs)]

    moves = copies(0, o_in, o_out) + copies(1, dq_in, dq_out)
    for cp in moves:
        cp.start()

    for w, dst in ((0, dk_t), (1, dv_t)):
        for up in range(2):
            def body(i, _):
                at = pl.ds(pl.multiple_of(i * 16, 16), 16)
                dst[up, at] = jnp.transpose(dkv_in[:, up, w, at, :], (1, 0, 2))
                return 0
            lax.fori_loop(0, SLOT // 16, body, 0)
        more = copies(2 + w, dst, (dk_out, dv_out)[w])
        for cp in more:
            cp.start()
        moves += more

    row = lax.broadcasted_iota(jnp.int32, (2 * SLOT, SLOT), 0)
    col = lax.broadcasted_iota(jnp.int32, (2 * SLOT, SLOT), 1)
    acc = None
    for up in range(2):
        if up:
            src = jnp.where(col < l0, col + l0, col + SLOT)
        else:
            src = jnp.where(col < l0, col, col + l0)
        pick = jnp.where(row == src, 1.0, 0.0)
        part = lax.dot_general(lse_in[up], pick, NT, precision=lax.Precision.HIGHEST, preferred_element_type=F32)
        acc = part if acc is None else acc + part
    lse_t[...] = acc
    lse_move = pltpu.make_async_copy(lse_t, lse_out, lse_sem)
    lse_move.start()
    for cp in moves + [lse_move]:
        cp.wait()


def finish_call(o_t, dq_t, dkv_hm, lse_hm, cu):
    any_spec = pl.BlockSpec(memory_space=pl.ANY)
    vmem = pl.BlockSpec(memory_space=pltpu.VMEM)
    return pl.pallas_call(
        finish_kernel,
        out_shape=(
            jax.ShapeDtypeStruct((256, 32, HEAD), BF16),
            jax.ShapeDtypeStruct((256, 32, HEAD), BF16),
            jax.ShapeDtypeStruct((256, 8, HEAD), BF16),
            jax.ShapeDtypeStruct((256, 8, HEAD), BF16),
            jax.ShapeDtypeStruct((32, 256), F32),
        ),
        in_specs=[vmem] * 4 + [pl.BlockSpec(memory_space=pltpu.SMEM)],
        out_specs=(any_spec,) * 5,
        scratch_shapes=[
            pltpu.VMEM((2, SLOT, 8, HEAD), BF16),
            pltpu.VMEM((2, SLOT, 8, HEAD), BF16),
            pltpu.VMEM((32, 256), F32),
            pltpu.SemaphoreType.DMA((4, 4)),
            pltpu.SemaphoreType.DMA,
        ],
        compiler_params=pltpu.CompilerParams(vmem_limit_bytes=16 * 1024 * 1024),
        name="finish",
    )(o_t, dq_t, dkv_hm, lse_hm, cu)


def solution(mesh):
    tok_spec = P(("dp", "cp"), None, None)
    lse_spec = P(("dp", "cp"), None)

    def local(q, k, v, do, valid, cu):
        res = attn_call(cu, valid.reshape(1, 256), q, k, v, do)
        o, dq, dk, dv, lse = finish_call(*res)
        return o, lse.T, dq, dk, dv

    return jax.shard_map(local, mesh=mesh, in_specs=(tok_spec,) * 4 + (P(("dp", "cp")), P("dp")),
                         out_specs=(tok_spec, lse_spec, tok_spec, tok_spec, tok_spec), check_vma=False)
```

```python
import functools
import math

import jax
import jax.numpy as jnp
from jax import lax
from jax.experimental import pallas as pl
from jax.experimental.pallas import tpu as pltpu
from jax.sharding import PartitionSpec as P

MESH = pl.DeviceIdType.MESH
FILL = -1.0e30
BIG = 3.0e38
HEAD = 128
SLOT = 128
TILE = 512
GROUP = 4
HC = 4
SW = (2, 2, 1, 0)
SCALE = HEAD ** -0.5
C2 = SCALE * math.log2(math.e)
NT = (((1,), (1,)), ((), ()))
NN = (((1,), (0,)), ((), ()))
F32 = jnp.float32
BF16 = jnp.bfloat16

TILES = ((0, 0), (1, 0), (1, 1), (0, 1))


def slot_of(chip, ti):
    oc, up = TILES[ti]
    r = 2 * chip + oc
    return 7 - r if up else r


def mm(a, b, dims):
    return lax.dot_general(a, b, dims, preferred_element_type=F32)


def src_row(up, t, l0):
    if up:
        return jnp.where(t < l0, t + l0, t + SLOT)
    return jnp.where(t < l0, t, t + l0)


def attn_kernel(cu_hbm, valid, q, k, v, do, o_out, dq_out, dkv_out, lse_out, cu,
                raw_q, raw_do, far_q, far_do, raw_k, raw_v, kv_hm, kv_all, kt, vt, qh, doh, st0, st1, pb, db,
                dkv_acc, cross_in, near_in, swap_in, o_st, dq_st, o_far, dq_far, dkv_st, back_st, lse_st, caps, valid_all,
                in_sem, raw_ssem, raw_rsem, val_ssem, val_rsem, kv_ssem, kv_rsem,
                part_ssem, part_rsem, near_ssem, near_rsem, swap_ssem, swap_rsem, back_ssem, back_rsem, res_ssem, res_rsem, dkv_ssem, dkv_rsem, lse_sem, lse_rsem):
    r = lax.axis_index("cp")
    chip = r // 2
    c = r % 2
    pc = 1 - c
    partner = chip * 2 + pc
    cross = (1 - chip) * 2 + c
    cross_o = (1 - chip) * 2 + pc

    def remote(src, dst, ssem, rsem, dev):
        return pltpu.make_async_remote_copy(src_ref=src, dst_ref=dst, send_sem=ssem, recv_sem=rsem,
                                            device_id={"cp": dev}, device_id_type=MESH)

    own_heads = pl.ds(pl.multiple_of(16 * c, 16), 16)
    oth_heads = pl.ds(pl.multiple_of(16 * pc, 16), 16)
    ld_k = pltpu.make_async_copy(k, raw_k, in_sem.at[0])
    ld_v = pltpu.make_async_copy(v, raw_v, in_sem.at[1])
    ld_q = pltpu.make_async_copy(q.at[:, own_heads, :], raw_q, in_sem.at[2])
    ld_do = pltpu.make_async_copy(do.at[:, own_heads, :], raw_do, in_sem.at[3])
    ld_val = pltpu.make_async_copy(valid, valid_all.at[r], in_sem.at[4])
    ld_cu = pltpu.make_async_copy(cu_hbm, cu, in_sem.at[5])
    for cp in (ld_cu, ld_k, ld_v, ld_q, ld_do, ld_val):
        cp.start()

    barrier = pltpu.get_barrier_semaphore()
    for dev in (partner, cross, cross_o):
        pl.semaphore_signal(barrier, inc=1, device_id={"cp": dev}, device_id_type=MESH)
    pl.semaphore_wait(barrier, 3)
    ld_cu.wait()
    l0 = lax.shift_right_logical(cu[1], 3)

    peers = (partner, cross, cross_o)
    push_q = remote(q.at[:, oth_heads, :], far_q, raw_ssem.at[0], raw_rsem.at[0], partner)
    push_do = remote(do.at[:, oth_heads, :], far_do, raw_ssem.at[1], raw_rsem.at[1], partner)
    push_val = [remote(valid, valid_all.at[r], val_ssem.at[i], val_rsem.at[r], dev) for i, dev in enumerate(peers)]

    push_q.start()
    push_do.start()

    def kv_relayout(up):
        def body(i, _):
            t0 = i * 16
            for which, raw in ((0, raw_k), (1, raw_v)):
                rows = jnp.stack([raw[src_row(up, t0 + j, l0)] for j in range(16)])
                kv_hm[:, up, which, pl.ds(pl.multiple_of(t0, 16), 16), :] = jnp.transpose(rows, (1, 0, 2))
            return 0
        lax.fori_loop(0, SLOT // 16, body, 0)

    def kv_push(h, to, both):
        head = (4 * c if to == 1 else 4 * pc) + h
        dev = (partner, cross, cross_o)[to]
        ups = pl.ds(0, 2 if both else 1)
        return remote(kv_hm.at[head, ups], kv_all.at[h, r, ups], kv_ssem.at[to, h], kv_rsem.at[h, r], dev)

    def kv_wait(h, owner, both):
        ups = pl.ds(0, 2 if both else 1)
        remote(kv_hm.at[0, ups], kv_all.at[h, owner, ups], kv_ssem.at[0, h], kv_rsem.at[h, owner], partner).wait_recv()

    ld_k.wait()
    ld_v.wait()
    kv_relayout(0)

    def cross_send(ch, h):
        @pl.when(chip == ch)
        def _():
            for to in (1, 2):
                kv_push(h, to, ch == 1).start()

    cross_send(0, 0)
    kv_relayout(1)
    cross_send(1, 0)
    for h in range(HC):
        kv_push(h, 0, True).start()
    ld_val.wait()
    for cp in push_val:
        cp.start()

    def copy_own(h, _):
        for up in range(2):
            kv_all[h, r, up] = kv_hm[4 * c + h, up]
        return 0
    lax.fori_loop(0, HC, copy_own, 0)

    def q_relayout(oc, from_q, from_do):
        for up, ti in ((0, oc), (1, 3 - oc)):
            def body(i, _):
                t0 = i * 16
                at = pl.ds(pl.multiple_of(t0, 16), 16)
                for raw, dst in ((from_q, qh), (from_do, doh)):
                    rows = jnp.stack([raw[src_row(up, t0 + j, l0)] for j in range(16)])
                    dst[:, ti, :, at, :] = jnp.transpose(rows, (1, 0, 2)).reshape(HC, GROUP, 16, HEAD)
                return 0
            lax.fori_loop(0, SLOT // 16, body, 0)

    ld_q.wait()
    ld_do.wait()
    cross_send(0, 1)
    q_relayout(c, raw_q, raw_do)

    cross_send(0, 2)
    for i in range(3):
        remote(valid, valid_all.at[peers[i]], val_ssem.at[i], val_rsem.at[peers[i]], peers[i]).wait_recv()
    lane = lax.broadcasted_iota(jnp.int32, (SLOT, SLOT), 1)
    sub = lax.broadcasted_iota(jnp.int32, (SLOT, SLOT), 0)
    lane2 = lax.broadcasted_iota(jnp.int32, (SLOT, 2 * SLOT), 1)
    sub2 = lax.broadcasted_iota(jnp.int32, (SLOT, 2 * SLOT), 0)
    same_doc = (lane < l0) == (sub < l0)
    doc_f = jnp.where(lane < l0, 1.0, 0.0)
    doc_s = jnp.where(sub < l0, 1.0, 0.0)
    same_f = jnp.where(doc_f == doc_s, 1.0, 0.0)
    del same_doc

    def cap_body(s, _):
        owner = jnp.where(s < 4, s, 7 - s)
        off = jnp.where(s < 4, 0, 1)
        src_lo = jnp.where(sub2 < l0, sub2, sub2 + l0)
        src_hi = jnp.where(sub2 < l0, sub2 + l0, sub2 + SLOT)
        src = jnp.where(off == 1, src_hi, src_lo)
        row = jnp.broadcast_to(valid_all[owner].astype(F32), (SLOT, 2 * SLOT))
        ok = jnp.sum(jnp.where(src == lane2, row, 0.0), axis=1, keepdims=True)
        caps[s] = jnp.where(same_f * ok > 0.5, BIG, FILL)
        return 0
    lax.fori_loop(0, 8, cap_body, 0)
    for ti in range(4):
        oc, up = TILES[ti]
        s = (7 - (2 * chip + oc)) if up else 2 * chip + oc
        caps[8 + ti] = jnp.where(sub <= lane, caps[s], FILL)

    cross_send(0, 3)
    cross_send(1, 1)
    push_q.wait_recv()
    push_do.wait_recv()
    q_relayout(pc, far_q, far_do)

    def part_copy(h, u, n=2):
        up = int(u > 3)
        i = u if u < 2 else u - 2
        return remote(dkv_acc.at[h, pl.ds(2 * u, n)], cross_in.at[4 * c + h, up, pl.ds(0, n)], part_ssem.at[h, i],
                      part_rsem.at[4 * c + h, up], min(u, 7 - u))

    def part_wait(j, up, n=2):
        remote(dkv_acc.at[0, pl.ds(0, n)], cross_in.at[j, up, pl.ds(0, n)], part_ssem.at[0, 0],
               part_rsem.at[j, up], partner).wait_recv()

    def near_copy(h, up, slot, n=2):
        return remote(dkv_acc.at[h, pl.ds(2 * slot, n)], near_in.at[h, up, pl.ds(0, n)], near_ssem.at[h, up],
                      near_rsem.at[h, up], partner)

    def near_run(ch, h, act):
        act(near_copy(h, 0, 2 * ch + pc))
        if ch == 1:
            pl.when(c == 0)(lambda: act(near_copy(h, 1, 4)))
            if SW[h] < 2:
                pl.when(c == 1)(lambda: act(near_copy(h, 1, 5, 2 - SW[h])))

    def near_wait(h, up, n=2):
        near_copy(h, up, 0, n).wait_recv()

    def swap_copy(h):
        n = SW[h]
        return remote(dkv_acc.at[h, pl.ds(12 - n, n)], swap_in.at[h, pl.ds(2 - n, n)], swap_ssem.at[h], swap_rsem.at[h], cross)

    def swap_back(h, core):
        at = pl.ds(2 - SW[h], SW[h])
        j = 4 * core + h
        return remote(back_st.at[h, at], dkv_out.at[j, 1, at], back_ssem.at[h], back_rsem.at[j], 2)

    def res_copy(p, ti, which):
        stage, out = ((o_far, o_out), (dq_far, dq_out))[which]
        dst = out.at[TILES[ti][1], :, pl.ds(pl.multiple_of(16 * c + 8 * p, 8), 8), :]
        return remote(stage.at[p, ti], dst, res_ssem.at[which, p, ti], res_rsem.at[which, p, TILES[ti][1]], partner)

    def dkv_copy(h, ti):
        up = TILES[ti][1]
        return remote(dkv_st.at[h, ti], dkv_out.at[4 * c + h, up], dkv_ssem.at[h, ti], dkv_rsem.at[h, up], partner)

    def res_put(p):
        heads = pl.ds(pl.multiple_of(16 * c + 8 * p, 8), 8)
        for ti, (oc, up) in enumerate(TILES):
            def body(i, _, keep):
                at = pl.ds(pl.multiple_of(i * 16, 16), 16)
                for stage, far, out in ((o_st, o_far, o_out), (dq_st, dq_far, dq_out)):
                    x = jnp.concatenate([stage[e, ti, pl.ds(pl.multiple_of(g * SLOT + i * 16, 16), 16), :][None]
                                         for e in range(2) for g in range(GROUP)], axis=0)
                    y = jnp.transpose(x, (1, 0, 2))
                    if keep:
                        out[up, at, heads, :] = y
                    else:
                        far[p, ti, at, :, :] = y
                return 0

            @pl.when(c == oc)
            def _():
                lax.fori_loop(0, SLOT // 16, functools.partial(body, keep=True), 0)

            @pl.when(c != oc)
            def _():
                lax.fori_loop(0, SLOT // 16, functools.partial(body, keep=False), 0)
                for which in range(2):
                    res_copy(p, ti, which).start()

    def dkv_put(h, ti, parts):
        oc, up = TILES[ti]

        @pl.when(c == oc)
        def _():
            for w in range(2):
                dkv_out[4 * c + h, up, w] = parts(w).astype(BF16)

        @pl.when(c != oc)
        def _():
            for w in range(2):
                dkv_st[h, ti, w] = parts(w).astype(BF16)
            dkv_copy(h, ti).start()

    lse_far = remote(lse_st.at[pc], lse_out.at[:, own_heads, :], lse_sem, lse_rsem, partner)

    def kv_slot(h, s, which):
        return kv_all[h, min(s, 7 - s), int(s > 3), which]

    def kv_slots(h, a, b, which):
        return jnp.concatenate([kv_slot(h, s, which) for s in range(a, b)], axis=0)

    def run_chip(ch):
        slots = [slot_of(ch, ti) for ti in range(4)]
        sent = [0, 1] if ch == 1 else [2, 3, 4, 5]

        def transposes(s):
            for src, dst in ((0, kt), (1, vt)):
                dst[:, s * SLOT:(s + 1) * SLOT] = jnp.transpose(kv_slot(h_ref[0], s, src))

        h_ref = [None]
        sts = (st0, st1)

        def point(h, where):
            if ch == 0:
                return
            kv = {(0, 3): 2, (1, 2): 3}
            swaps = {(1, 4): (0, 1), (2, 4): (2,)}
            parts = {(2, 2): (0,), (2, 4): (1,), (3, 4): (2, 3)}
            for at in range(HC):
                if not any((at, where) in d for d in (kv, swaps, parts)):
                    continue

                @pl.when(h == at)
                def _():
                    if (at, where) in kv:
                        for to in (1, 2):
                            kv_push(kv[at, where], to, True).start()
                    for e in swaps.get((at, where), ()):
                        swap_copy(e).start()
                    for e in parts.get((at, where), ()):
                        for u in (0, 1):
                            part_copy(e, u).start()

        def head(h, _):
            h_ref[0] = h
            seen = set()
            ready = set()

            def wait_slot(s):
                if s in ready:
                    return
                if s in slots:
                    kv_wait(h, partner, True)
                    new = slots
                elif ch == 1:
                    for owner in (0, 1):
                        kv_wait(h, owner, False)
                    new = [0, 1]
                else:
                    for owner in (2, 3):
                        kv_wait(h, owner, True)
                    new = [2, 3, 4, 5]
                for u in new:
                    ready.add(u)
                    transposes(u)

            state = {}

            def forward(ti):
                point(h, ti)
                s = slots[ti]
                nk = s + 1
                for u in range(nk):
                    wait_slot(u)
                st = sts[ti % 2]
                qt = qh[h, ti].reshape(TILE, HEAD)
                dt = doh[h, ti].reshape(TILE, HEAD)
                m8 = [None] * GROUP
                for a in range(0, nk, 2):
                    n = min(2, nk - a)
                    kb = kv_slots(h, a, a + n, 0)
                    sc = mm(kb, qt, NT)
                    for j in range(n):
                        cap = caps[8 + ti] if a + j == s else caps[a + j]
                        for g in range(GROUP):
                            x = jnp.minimum(sc[j * SLOT:(j + 1) * SLOT, g * SLOT:(g + 1) * SLOT], cap)
                            st[(a + j) * SLOT:(a + j + 1) * SLOT, g * SLOT:(g + 1) * SLOT] = x
                            top = jnp.max(x.reshape(SLOT // 8, 8, SLOT), axis=0)
                            m8[g] = top if m8[g] is None else jnp.maximum(m8[g], top)
                m = [jnp.max(x, axis=0, keepdims=True) for x in m8]
                mc = [x * C2 for x in m]
                l8 = [None] * GROUP
                for a in range(nk):
                    for g in range(GROUP):
                        at = (slice(a * SLOT, (a + 1) * SLOT), slice(g * SLOT, (g + 1) * SLOT))
                        e = jnp.exp2(st[at] * C2 - mc[g])
                        st[at] = e
                        pb[at] = e.astype(BF16)
                        tot = jnp.sum(e.reshape(SLOT // 8, 8, SLOT), axis=0)
                        l8[g] = tot if l8[g] is None else l8[g] + tot
                ot = mm(vt[:, :nk * SLOT], pb[:nk * SLOT, :], NN)
                inv, dd = [], []
                oc, up = TILES[ti]
                for g in range(GROUP):
                    l = jnp.sum(l8[g], axis=0, keepdims=True)
                    has = m[g] > 0.5 * FILL
                    safe = jnp.where(has, l, 1.0)
                    i_l = jnp.where(has, 1.0 / safe, 0.0)
                    lse = jnp.where(has, m[g] * SCALE + jnp.log(safe), 0.0)
                    lse_st[oc, up, pl.ds(h * GROUP + g, 1), :] = lse
                    og = (ot[:, g * SLOT:(g + 1) * SLOT] * i_l).astype(BF16)
                    dog = jnp.transpose(dt[g * SLOT:(g + 1) * SLOT, :])
                    dd.append(jnp.sum(og.astype(F32) * dog.astype(F32), axis=0, keepdims=True))
                    inv.append(i_l)
                    o_st[h % 2, ti, g * SLOT:(g + 1) * SLOT, :] = jnp.transpose(og)

                state[ti] = [inv, dd, None]

            def backward(ti, part):
                inv, dd, dqt = state[ti]
                qt = qh[h, ti].reshape(TILE, HEAD)
                dt = doh[h, ti].reshape(TILE, HEAD)
                st = sts[ti % 2]
                runs = []
                for u in part:
                    if runs and runs[-1][1] == u and u - runs[-1][0] < 2:
                        runs[-1][1] = u + 1
                    else:
                        runs.append([u, u + 1])
                for a, b in runs:
                    n = b - a
                    vb = kv_slots(h, a, b, 1)
                    dp = mm(vb, dt, NT)
                    for j in range(n):
                        for g in range(GROUP):
                            at = (slice((a + j) * SLOT, (a + j + 1) * SLOT), slice(g * SLOT, (g + 1) * SLOT))
                            p = st[at] * inv[g]
                            pb[at] = p.astype(BF16)
                            ds = p * (dp[j * SLOT:(j + 1) * SLOT, g * SLOT:(g + 1) * SLOT] - dd[g])
                            db[at] = ds.astype(BF16)
                    dsb = db[a * SLOT:b * SLOT, :]
                    dv = mm(pb[a * SLOT:b * SLOT, :], dt, NN)
                    dk = mm(dsb, qt, NN) * SCALE
                    dq = mm(kt[:, a * SLOT:b * SLOT], dsb, NN)
                    dqt = dq if dqt is None else dqt + dq
                    for j in range(n):
                        u = a + j
                        new = (dk[j * SLOT:(j + 1) * SLOT], dv[j * SLOT:(j + 1) * SLOT])
                        for w in range(2):
                            dkv_acc[h, 2 * u + w] = dkv_acc[h, 2 * u + w] + new[w] if u in seen else new[w]
                        seen.add(u)
                state[ti][2] = dqt

            def finish(ti):
                dqt = state[ti][2]
                for g in range(GROUP):
                    dqg = (dqt[:, g * SLOT:(g + 1) * SLOT] * SCALE).astype(BF16)
                    dq_st[h % 2, ti, g * SLOT:(g + 1) * SLOT, :] = jnp.transpose(dqg)

            if ch == 0:
                for ti in (0, 1):
                    forward(ti)
                    backward(ti, range(slots[ti] + 1))
                    finish(ti)
                for ti in (2, 3):
                    forward(ti)
                    backward(ti, sent)
                for u in (2, 3, 4):
                    part_copy(h, u).start()
                for at in range(HC):
                    if SW[at] < 2:
                        pl.when(h == at)(part_copy(at, 5, 2 - SW[at]).start)
                for ti in (2, 3):
                    backward(ti, [u for u in range(slots[ti] + 1) if u not in sent])
                    finish(ti)
            else:
                for ti in range(4):
                    forward(ti)
                    backward(ti, range(slots[ti] + 1))
                    finish(ti)
            if ch == 1:
                point(h, 4)
            else:
                for ti in (2, 3):
                    dkv_put(h, ti, lambda w, ti=ti: dkv_acc[h, 2 * slots[ti] + w])
            for at in range(HC):
                pl.when(h == at)(functools.partial(near_run, ch, at, lambda cp: cp.start()))
            pl.when(h % 2 == 1)(lambda: res_put(h // 2))
            return 0

        lax.fori_loop(0, HC, head, 0)

        lse_out[:, own_heads, :] = lse_st[c]
        lse_far.start()

        if ch == 0:
            for h in range(HC):
                if SW[h]:
                    swap_copy(h).wait_recv()
                    for w in range(2 - SW[h], 2):
                        back_st[h, w] = (swap_in[h, w] + dkv_acc[h, 10 + w]).astype(BF16)
                    swap_back(h, c).start()

        def early(h, _):
            kv_push(h, 0, True).wait_send()
            for to in (1, 2):
                kv_push(h, to, ch == 1).wait_send()
            if ch == 0:
                for ti in (2, 3):
                    pl.when(c != TILES[ti][0])(dkv_copy(h, ti).wait_send)
                remote(dkv_st.at[h, 0], dkv_out.at[4 * pc + h, 1], dkv_ssem.at[h, 0], dkv_rsem.at[h, 1], partner).wait_recv()
            return 0
        lax.fori_loop(0, HC, early, 0)
        for h in range(HC):
            near_run(ch, h, lambda cp: cp.wait_send())
        push_q.wait_send()
        push_do.wait_send()
        for cp in push_val:
            cp.wait_send()
        for p in range(2):
            for which in range(2):
                stage, out = ((o_far, o_out), (dq_far, dq_out))[which]
                for ti in range(4):
                    pl.when(c != TILES[ti][0])(res_copy(p, ti, which).wait_send)
                for up in range(2):
                    dst = out.at[up, :, pl.ds(pl.multiple_of(16 * pc + 8 * p, 8), 8), :]
                    remote(stage.at[p, 0], dst, res_ssem.at[which, p, 0], res_rsem.at[which, p, up], partner).wait_recv()
        lse_far.wait_send()
        remote(lse_st.at[0], lse_out.at[:, oth_heads, :], lse_sem, lse_rsem, partner).wait_recv()

        def add_up(h, up, slot, n):
            if n == 0:
                return
            part_wait(4 * c + h, up, n)
            for w in range(n):
                dkv_out[4 * c + h, up, w] = (dkv_acc[h, 2 * slot + w] + cross_in[4 * c + h, up, w]).astype(BF16)
            near_wait(h, up, n)
            part_wait(4 * pc + h, up, n)
            for w in range(n):
                dkv_out[4 * pc + h, up, w] = (near_in[h, up, w] + cross_in[4 * pc + h, up, w]).astype(BF16)

        for h in range(HC):
            add_up(h, 0, 2 * ch + c, 2)
            if ch == 1:
                pl.when(c == 1)(functools.partial(add_up, h, 1, 4, 2))
                pl.when(c == 0)(functools.partial(add_up, h, 1, 5, 2 - SW[h]))

        for h in range(HC):
            for u in sent:
                n = 2 - SW[h] if u == 5 else 2
                if n:
                    part_copy(h, u, n).wait_send()
            if SW[h]:
                if ch == 0:
                    swap_back(h, c).wait_send()
                else:
                    swap_copy(h).wait_send()

        if ch == 1:
            @pl.when(c == 0)
            def _():
                for h in range(HC):
                    if SW[h]:
                        for core in range(2):
                            swap_back(h, core).wait_recv()

    pl.when(chip == 0)(functools.partial(run_chip, 0))
    pl.when(chip == 1)(functools.partial(run_chip, 1))


def attn_call(cu, valid, q, k, v, do):
    any_spec = pl.BlockSpec(memory_space=pl.ANY)
    dma = pltpu.SemaphoreType.DMA
    return pl.pallas_call(
        attn_kernel,
        out_shape=(
            pltpu.VMEM((2, SLOT, 32, HEAD), BF16),
            pltpu.VMEM((2, SLOT, 32, HEAD), BF16),
            pltpu.VMEM((8, 2, 2, SLOT, HEAD), BF16),
            pltpu.VMEM((2, 32, SLOT), F32),
            pltpu.SMEM((3,), jnp.int32),
        ),
        in_specs=[any_spec] * 6,
        out_specs=(pl.BlockSpec(memory_space=pltpu.VMEM),) * 4 + (pl.BlockSpec(memory_space=pltpu.SMEM),),
        scratch_shapes=[
            pltpu.VMEM((256, 16, HEAD), BF16),
            pltpu.VMEM((256, 16, HEAD), BF16),
            pltpu.VMEM((256, 16, HEAD), BF16),
            pltpu.VMEM((256, 16, HEAD), BF16),
            pltpu.VMEM((256, 8, HEAD), BF16),
            pltpu.VMEM((256, 8, HEAD), BF16),
            pltpu.VMEM((8, 2, 2, SLOT, HEAD), BF16),
            pltpu.VMEM((HC, 4, 2, 2, SLOT, HEAD), BF16),
            pltpu.VMEM((HEAD, 8 * SLOT), BF16),
            pltpu.VMEM((HEAD, 8 * SLOT), BF16),
            pltpu.VMEM((HC, 4, GROUP, SLOT, HEAD), BF16),
            pltpu.VMEM((HC, 4, GROUP, SLOT, HEAD), BF16),
            pltpu.VMEM((8 * SLOT, TILE), F32),
            pltpu.VMEM((8 * SLOT, TILE), F32),
            pltpu.VMEM((8 * SLOT, TILE), BF16),
            pltpu.VMEM((8 * SLOT, TILE), BF16),
            pltpu.VMEM((HC, 16, SLOT, HEAD), F32),
            pltpu.VMEM((8, 2, 2, SLOT, HEAD), F32),
            pltpu.VMEM((HC, 2, 2, SLOT, HEAD), F32),
            pltpu.VMEM((HC, 2, SLOT, HEAD), F32),
            pltpu.VMEM((2, 4, TILE, HEAD), BF16),
            pltpu.VMEM((2, 4, TILE, HEAD), BF16),
            pltpu.VMEM((2, 4, SLOT, 8, HEAD), BF16),
            pltpu.VMEM((2, 4, SLOT, 8, HEAD), BF16),
            pltpu.VMEM((HC, 4, 2, SLOT, HEAD), BF16),
            pltpu.VMEM((HC, 2, SLOT, HEAD), BF16),
            pltpu.VMEM((2, 2, 16, SLOT), F32),
            pltpu.VMEM((12, SLOT, SLOT), F32),
            pltpu.VMEM((4, 1, 2 * SLOT), jnp.int32),
            dma((6,)),
            dma((2,)), dma((2,)),
            dma((3,)), dma((4,)),
            dma((3, HC)), dma((HC, 4)),
            dma((HC, 4)), dma((8, 2)), dma((HC, 2)), dma((HC, 2)),
            dma((HC,)), dma((HC,)), dma((HC,)), dma((8,)),
            dma((2, 2, 4)), dma((2, 2, 2)),
            dma((HC, 4)), dma((HC, 2)),
            dma, dma,
        ],
        compiler_params=pltpu.CompilerParams(collective_id=0, has_side_effects=True, vmem_limit_bytes=61300000),
        name="attn",
    )(cu, valid, q, k, v, do)


def finish_kernel(o_in, dq_in, dkv_in, lse_in, cu, o_out, dq_out, dk_out, dv_out, lse_out, dk_t, dv_t, lse_t, sem, lse_sem):
    l0 = lax.shift_right_logical(cu[1], 3)
    rest = SLOT - l0

    def copies(i, x, out):
        runs = ((0, 0, 0, l0), (1, 0, l0, l0), (0, l0, 2 * l0, rest), (1, l0, SLOT + l0, rest))
        return [pltpu.make_async_copy(x.at[up, pl.ds(at, n)], out.at[pl.ds(to, n)], sem.at[i, j])
                for j, (up, at, to, n) in enumerate(runs)]

    moves = copies(0, o_in, o_out) + copies(1, dq_in, dq_out)
    for cp in moves:
        cp.start()

    for w, dst in ((0, dk_t), (1, dv_t)):
        for up in range(2):
            def body(i, _):
                at = pl.ds(pl.multiple_of(i * 16, 16), 16)
                dst[up, at] = jnp.transpose(dkv_in[:, up, w, at, :], (1, 0, 2))
                return 0
            lax.fori_loop(0, SLOT // 16, body, 0)
        more = copies(2 + w, dst, (dk_out, dv_out)[w])
        for cp in more:
            cp.start()
        moves += more

    row = lax.broadcasted_iota(jnp.int32, (2 * SLOT, SLOT), 0)
    col = lax.broadcasted_iota(jnp.int32, (2 * SLOT, SLOT), 1)
    acc = None
    for up in range(2):
        if up:
            src = jnp.where(col < l0, col + l0, col + SLOT)
        else:
            src = jnp.where(col < l0, col, col + l0)
        pick = jnp.where(row == src, 1.0, 0.0)
        part = lax.dot_general(lse_in[up], pick, NT, precision=lax.Precision.HIGHEST, preferred_element_type=F32)
        acc = part if acc is None else acc + part
    lse_t[...] = acc
    lse_move = pltpu.make_async_copy(lse_t, lse_out, lse_sem)
    lse_move.start()
    for cp in moves + [lse_move]:
        cp.wait()


def finish_call(o_t, dq_t, dkv_hm, lse_hm, cu):
    any_spec = pl.BlockSpec(memory_space=pl.ANY)
    vmem = pl.BlockSpec(memory_space=pltpu.VMEM)
    return pl.pallas_call(
        finish_kernel,
        out_shape=(
            jax.ShapeDtypeStruct((256, 32, HEAD), BF16),
            jax.ShapeDtypeStruct((256, 32, HEAD), BF16),
            jax.ShapeDtypeStruct((256, 8, HEAD), BF16),
            jax.ShapeDtypeStruct((256, 8, HEAD), BF16),
            jax.ShapeDtypeStruct((32, 256), F32),
        ),
        in_specs=[vmem] * 4 + [pl.BlockSpec(memory_space=pltpu.SMEM)],
        out_specs=(any_spec,) * 5,
        scratch_shapes=[
            pltpu.VMEM((2, SLOT, 8, HEAD), BF16),
            pltpu.VMEM((2, SLOT, 8, HEAD), BF16),
            pltpu.VMEM((32, 256), F32),
            pltpu.SemaphoreType.DMA((4, 4)),
            pltpu.SemaphoreType.DMA,
        ],
        compiler_params=pltpu.CompilerParams(vmem_limit_bytes=16 * 1024 * 1024),
        name="finish",
    )(o_t, dq_t, dkv_hm, lse_hm, cu)


def solution(mesh):
    tok_spec = P(("dp", "cp"), None, None)
    lse_spec = P(("dp", "cp"), None)

    def local(q, k, v, do, valid, cu):
        res = attn_call(cu, valid.reshape(1, 256), q, k, v, do)
        o, dq, dk, dv, lse = finish_call(*res)
        return o, lse.T, dq, dk, dv

    return jax.shard_map(local, mesh=mesh, in_specs=(tok_spec,) * 4 + (P(("dp", "cp")), P("dp")),
                         out_specs=(tok_spec, lse_spec, tok_spec, tok_spec, tok_spec), check_vma=False)
```

```python
import functools
import math

import jax
import jax.numpy as jnp
from jax import lax
from jax.experimental import pallas as pl
from jax.experimental.pallas import tpu as pltpu
from jax.sharding import PartitionSpec as P

MESH = pl.DeviceIdType.MESH
FILL = -1.0e30
BIG = 3.0e38
HEAD = 128
SLOT = 128
TILE = 512
GROUP = 4
HC = 4
SW = (2, 2, 1, 0)
SCALE = HEAD ** -0.5
C2 = SCALE * math.log2(math.e)
NT = (((1,), (1,)), ((), ()))
NN = (((1,), (0,)), ((), ()))
F32 = jnp.float32
BF16 = jnp.bfloat16

TILES = ((0, 0), (1, 0), (1, 1), (0, 1))


def slot_of(chip, ti):
    oc, up = TILES[ti]
    r = 2 * chip + oc
    return 7 - r if up else r


def mm(a, b, dims):
    return lax.dot_general(a, b, dims, preferred_element_type=F32)


def src_row(up, t, l0):
    if up:
        return jnp.where(t < l0, t + l0, t + SLOT)
    return jnp.where(t < l0, t, t + l0)


def attn_kernel(cu_hbm, valid, q, k, v, do, o_out, dq_out, dkv_out, lse_out, cu,
                raw_q, raw_do, far_q, far_do, raw_k, raw_v, kv_hm, kv_all, kt, vt, qh, doh, st0, st1, pb, db,
                dkv_acc, cross_in, near_in, swap_in, o_st, dq_st, o_far, dq_far, dkv_st, back_st, lse_st, caps, valid_all,
                in_sem, raw_ssem, raw_rsem, val_ssem, val_rsem, first_ssem, first_rsem, kv_ssem, kv_rsem,
                part_ssem, part_rsem, near_ssem, near_rsem, swap_ssem, swap_rsem, back_ssem, back_rsem, res_ssem, res_rsem, dkv_ssem, dkv_rsem, lse_sem, lse_rsem):
    r = lax.axis_index("cp")
    chip = r // 2
    c = r % 2
    pc = 1 - c
    partner = chip * 2 + pc
    cross = (1 - chip) * 2 + c
    cross_o = (1 - chip) * 2 + pc

    def remote(src, dst, ssem, rsem, dev):
        return pltpu.make_async_remote_copy(src_ref=src, dst_ref=dst, send_sem=ssem, recv_sem=rsem,
                                            device_id={"cp": dev}, device_id_type=MESH)

    own_heads = pl.ds(pl.multiple_of(16 * c, 16), 16)
    oth_heads = pl.ds(pl.multiple_of(16 * pc, 16), 16)
    ld_k = pltpu.make_async_copy(k, raw_k, in_sem.at[0])
    ld_v = pltpu.make_async_copy(v, raw_v, in_sem.at[1])
    ld_q = pltpu.make_async_copy(q.at[:, own_heads, :], raw_q, in_sem.at[2])
    ld_do = pltpu.make_async_copy(do.at[:, own_heads, :], raw_do, in_sem.at[3])
    ld_val = pltpu.make_async_copy(valid, valid_all.at[r], in_sem.at[4])
    ld_cu = pltpu.make_async_copy(cu_hbm, cu, in_sem.at[5])
    for cp in (ld_cu, ld_k, ld_v, ld_val):
        cp.start()

    barrier = pltpu.get_barrier_semaphore()
    for dev in (partner, cross, cross_o):
        pl.semaphore_signal(barrier, inc=1, device_id={"cp": dev}, device_id_type=MESH)
    pl.semaphore_wait(barrier, 3)
    ld_cu.wait()
    l0 = lax.shift_right_logical(cu[1], 3)

    peers = (partner, cross, cross_o)
    push_q = remote(q.at[:, oth_heads, :], far_q, raw_ssem.at[0], raw_rsem.at[0], partner)
    push_do = remote(do.at[:, oth_heads, :], far_do, raw_ssem.at[1], raw_rsem.at[1], partner)
    push_val = [remote(valid, valid_all.at[r], val_ssem.at[i], val_rsem.at[r], dev) for i, dev in enumerate(peers)]


    def kv_relayout(up):
        def body(i, _):
            t0 = i * 16
            for which, raw in ((0, raw_k), (1, raw_v)):
                rows = jnp.stack([raw[src_row(up, t0 + j, l0)] for j in range(16)])
                kv_hm[:, up, which, pl.ds(pl.multiple_of(t0, 16), 16), :] = jnp.transpose(rows, (1, 0, 2))
            return 0
        lax.fori_loop(0, SLOT // 16, body, 0)

    def kv_push(h, to, both):
        head = (4 * c if to == 1 else 4 * pc) + h
        dev = (partner, cross, cross_o)[to]
        ups = pl.ds(0, 2 if both else 1)
        return remote(kv_hm.at[head, ups], kv_all.at[h, r, ups], kv_ssem.at[to, h], kv_rsem.at[h, r], dev)

    def kv_first(to, up):
        head = 4 * c if to == 1 else 4 * pc
        at = pl.ds(up, 1)
        return remote(kv_hm.at[head, at], kv_all.at[0, r, at], first_ssem.at[to - 1, up], first_rsem.at[c, up],
                      (cross, cross_o)[to - 1])

    def kv_wait(h, owner, both):
        ups = pl.ds(0, 2 if both else 1)
        remote(kv_hm.at[0, ups], kv_all.at[h, owner, ups], kv_ssem.at[0, h], kv_rsem.at[h, owner], partner).wait_recv()

    def first_wait(owner):
        for up in range(2):
            at = pl.ds(up, 1)
            remote(kv_hm.at[0, at], kv_all.at[0, owner, at], first_ssem.at[0, up], first_rsem.at[owner - 2, up], partner).wait_recv()

    ld_k.wait()
    ld_v.wait()
    for cp in (ld_q, ld_do, push_q, push_do):
        cp.start()
    kv_relayout(0)

    def cross_send(ch, h):
        @pl.when(chip == ch)
        def _():
            for to in (1, 2):
                kv_push(h, to, ch == 1).start()

    cross_send(0, 0)

    def send_first(up):
        @pl.when(chip == 1)
        def _():
            for to in (1, 2):
                kv_first(to, up).start()

    send_first(0)
    kv_relayout(1)
    send_first(1)
    for h in range(HC):
        kv_push(h, 0, True).start()
    ld_val.wait()
    for cp in push_val:
        cp.start()

    def copy_own(h, _):
        for up in range(2):
            kv_all[h, r, up] = kv_hm[4 * c + h, up]
        return 0
    lax.fori_loop(0, HC, copy_own, 0)

    def q_relayout(oc, from_q, from_do):
        for up, ti in ((0, oc), (1, 3 - oc)):
            def body(i, _):
                t0 = i * 16
                at = pl.ds(pl.multiple_of(t0, 16), 16)
                for raw, dst in ((from_q, qh), (from_do, doh)):
                    rows = jnp.stack([raw[src_row(up, t0 + j, l0)] for j in range(16)])
                    dst[:, ti, :, at, :] = jnp.transpose(rows, (1, 0, 2)).reshape(HC, GROUP, 16, HEAD)
                return 0
            lax.fori_loop(0, SLOT // 16, body, 0)

    ld_q.wait()
    ld_do.wait()
    cross_send(0, 1)
    q_relayout(c, raw_q, raw_do)

    cross_send(0, 2)
    for i in range(3):
        remote(valid, valid_all.at[peers[i]], val_ssem.at[i], val_rsem.at[peers[i]], peers[i]).wait_recv()
    lane = lax.broadcasted_iota(jnp.int32, (SLOT, SLOT), 1)
    sub = lax.broadcasted_iota(jnp.int32, (SLOT, SLOT), 0)
    lane2 = lax.broadcasted_iota(jnp.int32, (SLOT, 2 * SLOT), 1)
    sub2 = lax.broadcasted_iota(jnp.int32, (SLOT, 2 * SLOT), 0)
    same_doc = (lane < l0) == (sub < l0)
    doc_f = jnp.where(lane < l0, 1.0, 0.0)
    doc_s = jnp.where(sub < l0, 1.0, 0.0)
    same_f = jnp.where(doc_f == doc_s, 1.0, 0.0)
    del same_doc

    def cap_body(s, _):
        owner = jnp.where(s < 4, s, 7 - s)
        off = jnp.where(s < 4, 0, 1)
        src_lo = jnp.where(sub2 < l0, sub2, sub2 + l0)
        src_hi = jnp.where(sub2 < l0, sub2 + l0, sub2 + SLOT)
        src = jnp.where(off == 1, src_hi, src_lo)
        row = jnp.broadcast_to(valid_all[owner].astype(F32), (SLOT, 2 * SLOT))
        ok = jnp.sum(jnp.where(src == lane2, row, 0.0), axis=1, keepdims=True)
        caps[s] = jnp.where(same_f * ok > 0.5, BIG, FILL)
        return 0
    lax.fori_loop(0, 8, cap_body, 0)
    for ti in range(4):
        oc, up = TILES[ti]
        s = (7 - (2 * chip + oc)) if up else 2 * chip + oc
        caps[8 + ti] = jnp.where(sub <= lane, caps[s], FILL)

    cross_send(0, 3)
    cross_send(1, 1)
    push_q.wait_recv()
    push_do.wait_recv()
    q_relayout(pc, far_q, far_do)

    def part_copy(h, u, n=2):
        up = int(u > 3)
        i = u if u < 2 else u - 2
        return remote(dkv_acc.at[h, pl.ds(2 * u, n)], cross_in.at[4 * c + h, up, pl.ds(0, n)], part_ssem.at[h, i],
                      part_rsem.at[4 * c + h, up], min(u, 7 - u))

    def part_wait(j, up, n=2):
        remote(dkv_acc.at[0, pl.ds(0, n)], cross_in.at[j, up, pl.ds(0, n)], part_ssem.at[0, 0],
               part_rsem.at[j, up], partner).wait_recv()

    def near_copy(h, up, slot, n=2):
        return remote(dkv_acc.at[h, pl.ds(2 * slot, n)], near_in.at[h, up, pl.ds(0, n)], near_ssem.at[h, up],
                      near_rsem.at[h, up], partner)

    def near_run(ch, h, act):
        act(near_copy(h, 0, 2 * ch + pc))
        if ch == 1:
            pl.when(c == 0)(lambda: act(near_copy(h, 1, 4)))
            if SW[h] < 2:
                pl.when(c == 1)(lambda: act(near_copy(h, 1, 5, 2 - SW[h])))

    def near_wait(h, up, n=2):
        near_copy(h, up, 0, n).wait_recv()

    def swap_copy(h):
        n = SW[h]
        return remote(dkv_acc.at[h, pl.ds(12 - n, n)], swap_in.at[h, pl.ds(2 - n, n)], swap_ssem.at[h], swap_rsem.at[h], cross)

    def swap_back(h, core):
        at = pl.ds(2 - SW[h], SW[h])
        j = 4 * core + h
        return remote(back_st.at[h, at], dkv_out.at[j, 1, at], back_ssem.at[h], back_rsem.at[j], 2)

    def res_copy(p, ti, which):
        stage, out = ((o_far, o_out), (dq_far, dq_out))[which]
        dst = out.at[TILES[ti][1], :, pl.ds(pl.multiple_of(16 * c + 8 * p, 8), 8), :]
        return remote(stage.at[p, ti], dst, res_ssem.at[which, p, ti], res_rsem.at[which, p, TILES[ti][1]], partner)

    def dkv_copy(h, ti):
        up = TILES[ti][1]
        return remote(dkv_st.at[h, ti], dkv_out.at[4 * c + h, up], dkv_ssem.at[h, ti], dkv_rsem.at[h, up], partner)

    def res_put(p):
        heads = pl.ds(pl.multiple_of(16 * c + 8 * p, 8), 8)
        for ti, (oc, up) in enumerate(TILES):
            def body(i, _, keep):
                at = pl.ds(pl.multiple_of(i * 16, 16), 16)
                for stage, far, out in ((o_st, o_far, o_out), (dq_st, dq_far, dq_out)):
                    x = jnp.concatenate([stage[e, ti, pl.ds(pl.multiple_of(g * SLOT + i * 16, 16), 16), :][None]
                                         for e in range(2) for g in range(GROUP)], axis=0)
                    y = jnp.transpose(x, (1, 0, 2))
                    if keep:
                        out[up, at, heads, :] = y
                    else:
                        far[p, ti, at, :, :] = y
                return 0

            @pl.when(c == oc)
            def _():
                lax.fori_loop(0, SLOT // 16, functools.partial(body, keep=True), 0)

            @pl.when(c != oc)
            def _():
                lax.fori_loop(0, SLOT // 16, functools.partial(body, keep=False), 0)
                for which in range(2):
                    res_copy(p, ti, which).start()

    def dkv_put(h, ti, parts):
        oc, up = TILES[ti]

        @pl.when(c == oc)
        def _():
            for w in range(2):
                dkv_out[4 * c + h, up, w] = parts(w).astype(BF16)

        @pl.when(c != oc)
        def _():
            for w in range(2):
                dkv_st[h, ti, w] = parts(w).astype(BF16)
            dkv_copy(h, ti).start()

    lse_far = remote(lse_st.at[pc], lse_out.at[:, own_heads, :], lse_sem, lse_rsem, partner)

    def kv_slot(h, s, which):
        return kv_all[h, min(s, 7 - s), int(s > 3), which]

    def kv_slots(h, a, b, which):
        return jnp.concatenate([kv_slot(h, s, which) for s in range(a, b)], axis=0)

    def run_chip(ch):
        slots = [slot_of(ch, ti) for ti in range(4)]
        sent = [0, 1] if ch == 1 else [2, 3, 4, 5]

        def transposes(s):
            for src, dst in ((0, kt), (1, vt)):
                dst[:, s * SLOT:(s + 1) * SLOT] = jnp.transpose(kv_slot(h_ref[0], s, src))

        h_ref = [None]
        sts = (st0, st1)

        def point(h, where):
            if ch == 0:
                return
            kv = {(0, 3): 2, (1, 2): 3}
            swaps = {(1, 4): (0, 1), (2, 4): (2,)}
            parts = {(2, 2): (0,), (2, 4): (1,), (3, 4): (2, 3)}
            for at in range(HC):
                if not any((at, where) in d for d in (kv, swaps, parts)):
                    continue

                @pl.when(h == at)
                def _():
                    if (at, where) in kv:
                        for to in (1, 2):
                            kv_push(kv[at, where], to, True).start()
                    for e in swaps.get((at, where), ()):
                        swap_copy(e).start()
                    for e in parts.get((at, where), ()):
                        for u in (0, 1):
                            part_copy(e, u).start()

        def head(h, _):
            h_ref[0] = h
            seen = set()
            ready = set()

            def wait_slot(s):
                if s in ready:
                    return
                if s in slots:
                    kv_wait(h, partner, True)
                    new = slots
                elif ch == 1:
                    for owner in (0, 1):
                        kv_wait(h, owner, False)
                    new = [0, 1]
                else:
                    for owner in (2, 3):
                        pl.when(h == 0)(functools.partial(first_wait, owner))
                        pl.when(h > 0)(functools.partial(kv_wait, h, owner, True))
                    new = [2, 3, 4, 5]
                for u in new:
                    ready.add(u)
                    transposes(u)

            state = {}

            def forward(ti):
                point(h, ti)
                s = slots[ti]
                nk = s + 1
                for u in range(nk):
                    wait_slot(u)
                st = sts[ti % 2]
                qt = qh[h, ti].reshape(TILE, HEAD)
                dt = doh[h, ti].reshape(TILE, HEAD)
                m8 = [None] * GROUP
                for a in range(0, nk, 2):
                    n = min(2, nk - a)
                    kb = kv_slots(h, a, a + n, 0)
                    sc = mm(kb, qt, NT)
                    for j in range(n):
                        cap = caps[8 + ti] if a + j == s else caps[a + j]
                        for g in range(GROUP):
                            x = jnp.minimum(sc[j * SLOT:(j + 1) * SLOT, g * SLOT:(g + 1) * SLOT], cap)
                            st[(a + j) * SLOT:(a + j + 1) * SLOT, g * SLOT:(g + 1) * SLOT] = x
                            top = jnp.max(x.reshape(SLOT // 8, 8, SLOT), axis=0)
                            m8[g] = top if m8[g] is None else jnp.maximum(m8[g], top)
                m = [jnp.max(x, axis=0, keepdims=True) for x in m8]
                mc = [x * C2 for x in m]
                l8 = [None] * GROUP
                for a in range(nk):
                    for g in range(GROUP):
                        at = (slice(a * SLOT, (a + 1) * SLOT), slice(g * SLOT, (g + 1) * SLOT))
                        e = jnp.exp2(st[at] * C2 - mc[g])
                        st[at] = e
                        pb[at] = e.astype(BF16)
                        tot = jnp.sum(e.reshape(SLOT // 8, 8, SLOT), axis=0)
                        l8[g] = tot if l8[g] is None else l8[g] + tot
                ot = mm(vt[:, :nk * SLOT], pb[:nk * SLOT, :], NN)
                inv, dd = [], []
                oc, up = TILES[ti]
                for g in range(GROUP):
                    l = jnp.sum(l8[g], axis=0, keepdims=True)
                    has = m[g] > 0.5 * FILL
                    safe = jnp.where(has, l, 1.0)
                    i_l = jnp.where(has, 1.0 / safe, 0.0)
                    lse = jnp.where(has, m[g] * SCALE + jnp.log(safe), 0.0)
                    lse_st[oc, up, pl.ds(h * GROUP + g, 1), :] = lse
                    og = (ot[:, g * SLOT:(g + 1) * SLOT] * i_l).astype(BF16)
                    dog = jnp.transpose(dt[g * SLOT:(g + 1) * SLOT, :])
                    dd.append(jnp.sum(og.astype(F32) * dog.astype(F32), axis=0, keepdims=True))
                    inv.append(i_l)
                    o_st[h % 2, ti, g * SLOT:(g + 1) * SLOT, :] = jnp.transpose(og)

                state[ti] = [inv, dd, None]

            def backward(ti, part):
                inv, dd, dqt = state[ti]
                qt = qh[h, ti].reshape(TILE, HEAD)
                dt = doh[h, ti].reshape(TILE, HEAD)
                st = sts[ti % 2]
                runs = []
                for u in part:
                    if runs and runs[-1][1] == u and u - runs[-1][0] < 2:
                        runs[-1][1] = u + 1
                    else:
                        runs.append([u, u + 1])
                for a, b in runs:
                    n = b - a
                    vb = kv_slots(h, a, b, 1)
                    dp = mm(vb, dt, NT)
                    for j in range(n):
                        for g in range(GROUP):
                            at = (slice((a + j) * SLOT, (a + j + 1) * SLOT), slice(g * SLOT, (g + 1) * SLOT))
                            p = st[at] * inv[g]
                            pb[at] = p.astype(BF16)
                            ds = p * (dp[j * SLOT:(j + 1) * SLOT, g * SLOT:(g + 1) * SLOT] - dd[g])
                            db[at] = ds.astype(BF16)
                    dsb = db[a * SLOT:b * SLOT, :]
                    dv = mm(pb[a * SLOT:b * SLOT, :], dt, NN)
                    dk = mm(dsb, qt, NN) * SCALE
                    dq = mm(kt[:, a * SLOT:b * SLOT], dsb, NN)
                    dqt = dq if dqt is None else dqt + dq
                    for j in range(n):
                        u = a + j
                        new = (dk[j * SLOT:(j + 1) * SLOT], dv[j * SLOT:(j + 1) * SLOT])
                        for w in range(2):
                            dkv_acc[h, 2 * u + w] = dkv_acc[h, 2 * u + w] + new[w] if u in seen else new[w]
                        seen.add(u)
                state[ti][2] = dqt

            def finish(ti):
                dqt = state[ti][2]
                for g in range(GROUP):
                    dqg = (dqt[:, g * SLOT:(g + 1) * SLOT] * SCALE).astype(BF16)
                    dq_st[h % 2, ti, g * SLOT:(g + 1) * SLOT, :] = jnp.transpose(dqg)

            if ch == 0:
                for ti in (0, 1):
                    forward(ti)
                    backward(ti, range(slots[ti] + 1))
                    finish(ti)
                for ti in (2, 3):
                    forward(ti)
                for ti in (2, 3):
                    backward(ti, [2, 3])
                for u in (2, 3):
                    part_copy(h, u).start()
                for ti in (2, 3):
                    backward(ti, [4, 5])
                part_copy(h, 4).start()
                for at in range(HC):
                    if SW[at] < 2:
                        pl.when(h == at)(part_copy(at, 5, 2 - SW[at]).start)
                for ti in (2, 3):
                    backward(ti, [u for u in range(slots[ti] + 1) if u not in sent])
                    finish(ti)
            else:
                for ti in range(4):
                    forward(ti)
                    backward(ti, range(slots[ti] + 1))
                    finish(ti)
            if ch == 1:
                point(h, 4)
            else:
                for ti in (2, 3):
                    dkv_put(h, ti, lambda w, ti=ti: dkv_acc[h, 2 * slots[ti] + w])
            for at in range(HC):
                pl.when(h == at)(functools.partial(near_run, ch, at, lambda cp: cp.start()))
            pl.when(h % 2 == 1)(lambda: res_put(h // 2))
            return 0

        lax.fori_loop(0, HC, head, 0)

        lse_out[:, own_heads, :] = lse_st[c]
        lse_far.start()

        if ch == 0:
            for h in range(HC):
                if SW[h]:
                    swap_copy(h).wait_recv()
                    for w in range(2 - SW[h], 2):
                        back_st[h, w] = (swap_in[h, w] + dkv_acc[h, 10 + w]).astype(BF16)
                    swap_back(h, c).start()

        def early(h, _):
            kv_push(h, 0, True).wait_send()
            for to in (1, 2):
                if ch == 0:
                    kv_push(h, to, False).wait_send()
                else:
                    pl.when(h > 0)(kv_push(h, to, True).wait_send)
            if ch == 0:
                for ti in (2, 3):
                    pl.when(c != TILES[ti][0])(dkv_copy(h, ti).wait_send)
                remote(dkv_st.at[h, 0], dkv_out.at[4 * pc + h, 1], dkv_ssem.at[h, 0], dkv_rsem.at[h, 1], partner).wait_recv()
            return 0
        lax.fori_loop(0, HC, early, 0)
        if ch == 1:
            for to in (1, 2):
                for up in range(2):
                    kv_first(to, up).wait_send()
        for h in range(HC):
            near_run(ch, h, lambda cp: cp.wait_send())
        push_q.wait_send()
        push_do.wait_send()
        for cp in push_val:
            cp.wait_send()
        for p in range(2):
            for which in range(2):
                stage, out = ((o_far, o_out), (dq_far, dq_out))[which]
                for ti in range(4):
                    pl.when(c != TILES[ti][0])(res_copy(p, ti, which).wait_send)
                for up in range(2):
                    dst = out.at[up, :, pl.ds(pl.multiple_of(16 * pc + 8 * p, 8), 8), :]
                    remote(stage.at[p, 0], dst, res_ssem.at[which, p, 0], res_rsem.at[which, p, up], partner).wait_recv()
        lse_far.wait_send()
        remote(lse_st.at[0], lse_out.at[:, oth_heads, :], lse_sem, lse_rsem, partner).wait_recv()

        def add_up(h, up, slot, n):
            if n == 0:
                return
            part_wait(4 * c + h, up, n)
            for w in range(n):
                dkv_out[4 * c + h, up, w] = (dkv_acc[h, 2 * slot + w] + cross_in[4 * c + h, up, w]).astype(BF16)
            near_wait(h, up, n)
            part_wait(4 * pc + h, up, n)
            for w in range(n):
                dkv_out[4 * pc + h, up, w] = (near_in[h, up, w] + cross_in[4 * pc + h, up, w]).astype(BF16)

        for h in range(HC):
            add_up(h, 0, 2 * ch + c, 2)
            if ch == 1:
                pl.when(c == 1)(functools.partial(add_up, h, 1, 4, 2))
                pl.when(c == 0)(functools.partial(add_up, h, 1, 5, 2 - SW[h]))

        for h in range(HC):
            for u in sent:
                n = 2 - SW[h] if u == 5 else 2
                if n:
                    part_copy(h, u, n).wait_send()
            if SW[h]:
                if ch == 0:
                    swap_back(h, c).wait_send()
                else:
                    swap_copy(h).wait_send()

        if ch == 1:
            @pl.when(c == 0)
            def _():
                for h in range(HC):
                    if SW[h]:
                        for core in range(2):
                            swap_back(h, core).wait_recv()

    pl.when(chip == 0)(functools.partial(run_chip, 0))
    pl.when(chip == 1)(functools.partial(run_chip, 1))


def attn_call(cu, valid, q, k, v, do):
    any_spec = pl.BlockSpec(memory_space=pl.ANY)
    dma = pltpu.SemaphoreType.DMA
    return pl.pallas_call(
        attn_kernel,
        out_shape=(
            pltpu.VMEM((2, SLOT, 32, HEAD), BF16),
            pltpu.VMEM((2, SLOT, 32, HEAD), BF16),
            pltpu.VMEM((8, 2, 2, SLOT, HEAD), BF16),
            pltpu.VMEM((2, 32, SLOT), F32),
            pltpu.SMEM((3,), jnp.int32),
        ),
        in_specs=[any_spec] * 6,
        out_specs=(pl.BlockSpec(memory_space=pltpu.VMEM),) * 4 + (pl.BlockSpec(memory_space=pltpu.SMEM),),
        scratch_shapes=[
            pltpu.VMEM((256, 16, HEAD), BF16),
            pltpu.VMEM((256, 16, HEAD), BF16),
            pltpu.VMEM((256, 16, HEAD), BF16),
            pltpu.VMEM((256, 16, HEAD), BF16),
            pltpu.VMEM((256, 8, HEAD), BF16),
            pltpu.VMEM((256, 8, HEAD), BF16),
            pltpu.VMEM((8, 2, 2, SLOT, HEAD), BF16),
            pltpu.VMEM((HC, 4, 2, 2, SLOT, HEAD), BF16),
            pltpu.VMEM((HEAD, 8 * SLOT), BF16),
            pltpu.VMEM((HEAD, 8 * SLOT), BF16),
            pltpu.VMEM((HC, 4, GROUP, SLOT, HEAD), BF16),
            pltpu.VMEM((HC, 4, GROUP, SLOT, HEAD), BF16),
            pltpu.VMEM((8 * SLOT, TILE), F32),
            pltpu.VMEM((8 * SLOT, TILE), F32),
            pltpu.VMEM((8 * SLOT, TILE), BF16),
            pltpu.VMEM((8 * SLOT, TILE), BF16),
            pltpu.VMEM((HC, 16, SLOT, HEAD), F32),
            pltpu.VMEM((8, 2, 2, SLOT, HEAD), F32),
            pltpu.VMEM((HC, 2, 2, SLOT, HEAD), F32),
            pltpu.VMEM((HC, 2, SLOT, HEAD), F32),
            pltpu.VMEM((2, 4, TILE, HEAD), BF16),
            pltpu.VMEM((2, 4, TILE, HEAD), BF16),
            pltpu.VMEM((2, 4, SLOT, 8, HEAD), BF16),
            pltpu.VMEM((2, 4, SLOT, 8, HEAD), BF16),
            pltpu.VMEM((HC, 4, 2, SLOT, HEAD), BF16),
            pltpu.VMEM((HC, 2, SLOT, HEAD), BF16),
            pltpu.VMEM((2, 2, 16, SLOT), F32),
            pltpu.VMEM((12, SLOT, SLOT), F32),
            pltpu.VMEM((4, 1, 2 * SLOT), jnp.int32),
            dma((6,)),
            dma((2,)), dma((2,)),
            dma((3,)), dma((4,)),
            dma((2, 2)), dma((2, 2)),
            dma((3, HC)), dma((HC, 4)),
            dma((HC, 4)), dma((8, 2)), dma((HC, 2)), dma((HC, 2)),
            dma((HC,)), dma((HC,)), dma((HC,)), dma((8,)),
            dma((2, 2, 4)), dma((2, 2, 2)),
            dma((HC, 4)), dma((HC, 2)),
            dma, dma,
        ],
        compiler_params=pltpu.CompilerParams(collective_id=0, has_side_effects=True, vmem_limit_bytes=61300000),
        name="attn",
    )(cu, valid, q, k, v, do)


def finish_kernel(o_in, dq_in, dkv_in, lse_in, cu, o_out, dq_out, dk_out, dv_out, lse_out, dk_t, dv_t, lse_t, sem, lse_sem):
    l0 = lax.shift_right_logical(cu[1], 3)
    rest = SLOT - l0

    def copies(i, x, out):
        runs = ((0, 0, 0, l0), (1, 0, l0, l0), (0, l0, 2 * l0, rest), (1, l0, SLOT + l0, rest))
        return [pltpu.make_async_copy(x.at[up, pl.ds(at, n)], out.at[pl.ds(to, n)], sem.at[i, j])
                for j, (up, at, to, n) in enumerate(runs)]

    moves = copies(0, o_in, o_out) + copies(1, dq_in, dq_out)
    for cp in moves:
        cp.start()

    for w, dst in ((0, dk_t), (1, dv_t)):
        for up in range(2):
            def body(i, _):
                at = pl.ds(pl.multiple_of(i * 16, 16), 16)
                dst[up, at] = jnp.transpose(dkv_in[:, up, w, at, :], (1, 0, 2))
                return 0
            lax.fori_loop(0, SLOT // 16, body, 0)
        more = copies(2 + w, dst, (dk_out, dv_out)[w])
        for cp in more:
            cp.start()
        moves += more

    row = lax.broadcasted_iota(jnp.int32, (2 * SLOT, SLOT), 0)
    col = lax.broadcasted_iota(jnp.int32, (2 * SLOT, SLOT), 1)
    acc = None
    for up in range(2):
        if up:
            src = jnp.where(col < l0, col + l0, col + SLOT)
        else:
            src = jnp.where(col < l0, col, col + l0)
        pick = jnp.where(row == src, 1.0, 0.0)
        part = lax.dot_general(lse_in[up], pick, NT, precision=lax.Precision.HIGHEST, preferred_element_type=F32)
        acc = part if acc is None else acc + part
    lse_t[...] = acc
    lse_move = pltpu.make_async_copy(lse_t, lse_out, lse_sem)
    lse_move.start()
    for cp in moves + [lse_move]:
        cp.wait()


def finish_call(o_t, dq_t, dkv_hm, lse_hm, cu):
    any_spec = pl.BlockSpec(memory_space=pl.ANY)
    vmem = pl.BlockSpec(memory_space=pltpu.VMEM)
    return pl.pallas_call(
        finish_kernel,
        out_shape=(
            jax.ShapeDtypeStruct((256, 32, HEAD), BF16),
            jax.ShapeDtypeStruct((256, 32, HEAD), BF16),
            jax.ShapeDtypeStruct((256, 8, HEAD), BF16),
            jax.ShapeDtypeStruct((256, 8, HEAD), BF16),
            jax.ShapeDtypeStruct((32, 256), F32),
        ),
        in_specs=[vmem] * 4 + [pl.BlockSpec(memory_space=pltpu.SMEM)],
        out_specs=(any_spec,) * 5,
        scratch_shapes=[
            pltpu.VMEM((2, SLOT, 8, HEAD), BF16),
            pltpu.VMEM((2, SLOT, 8, HEAD), BF16),
            pltpu.VMEM((32, 256), F32),
            pltpu.SemaphoreType.DMA((4, 4)),
            pltpu.SemaphoreType.DMA,
        ],
        compiler_params=pltpu.CompilerParams(vmem_limit_bytes=16 * 1024 * 1024),
        name="finish",
    )(o_t, dq_t, dkv_hm, lse_hm, cu)


def solution(mesh):
    tok_spec = P(("dp", "cp"), None, None)
    lse_spec = P(("dp", "cp"), None)

    def local(q, k, v, do, valid, cu):
        res = attn_call(cu, valid.reshape(1, 256), q, k, v, do)
        o, dq, dk, dv, lse = finish_call(*res)
        return o, lse.T, dq, dk, dv

    return jax.shard_map(local, mesh=mesh, in_specs=(tok_spec,) * 4 + (P(("dp", "cp")), P("dp")),
                         out_specs=(tok_spec, lse_spec, tok_spec, tok_spec, tok_spec), check_vma=False)
```

```python
import functools
import math

import jax
import jax.numpy as jnp
from jax import lax
from jax.experimental import pallas as pl
from jax.experimental.pallas import tpu as pltpu
from jax.sharding import PartitionSpec as P

MESH = pl.DeviceIdType.MESH
FILL = -1.0e30
BIG = 3.0e38
HEAD = 128
SLOT = 128
TILE = 512
GROUP = 4
HC = 4
SW = (2, 2, 2, 0)
SCALE = HEAD ** -0.5
C2 = SCALE * math.log2(math.e)
NT = (((1,), (1,)), ((), ()))
NN = (((1,), (0,)), ((), ()))
F32 = jnp.float32
BF16 = jnp.bfloat16

TILES = ((0, 0), (1, 0), (1, 1), (0, 1))


def slot_of(chip, ti):
    oc, up = TILES[ti]
    r = 2 * chip + oc
    return 7 - r if up else r


def mm(a, b, dims):
    return lax.dot_general(a, b, dims, preferred_element_type=F32)


def src_row(up, t, l0):
    if up:
        return jnp.where(t < l0, t + l0, t + SLOT)
    return jnp.where(t < l0, t, t + l0)


def attn_kernel(cu_hbm, valid, q, k, v, do, o_out, dq_out, dkv_out, lse_out, cu,
                raw_q, raw_do, far_q, far_do, raw_k, raw_v, kv_hm, kv_all, kt, vt, qh, doh, st0, st1, pb, db,
                dkv_acc, cross_in, near_in, swap_in, o_st, dq_st, o_far, dq_far, dkv_st, back_st, lse_st, caps, valid_all,
                in_sem, raw_ssem, raw_rsem, val_ssem, val_rsem, first_ssem, first_rsem, kv_ssem, kv_rsem,
                part_ssem, part_rsem, near_ssem, near_rsem, swap_ssem, swap_rsem, back_ssem, back_rsem, res_ssem, res_rsem, dkv_ssem, dkv_rsem, lse_sem, lse_rsem):
    r = lax.axis_index("cp")
    chip = r // 2
    c = r % 2
    pc = 1 - c
    partner = chip * 2 + pc
    cross = (1 - chip) * 2 + c
    cross_o = (1 - chip) * 2 + pc

    def remote(src, dst, ssem, rsem, dev):
        return pltpu.make_async_remote_copy(src_ref=src, dst_ref=dst, send_sem=ssem, recv_sem=rsem,
                                            device_id={"cp": dev}, device_id_type=MESH)

    own_heads = pl.ds(pl.multiple_of(16 * c, 16), 16)
    oth_heads = pl.ds(pl.multiple_of(16 * pc, 16), 16)
    ld_k = pltpu.make_async_copy(k, raw_k, in_sem.at[0])
    ld_v = pltpu.make_async_copy(v, raw_v, in_sem.at[1])
    ld_q = pltpu.make_async_copy(q.at[:, own_heads, :], raw_q, in_sem.at[2])
    ld_do = pltpu.make_async_copy(do.at[:, own_heads, :], raw_do, in_sem.at[3])
    ld_val = pltpu.make_async_copy(valid, valid_all.at[r], in_sem.at[4])
    ld_cu = pltpu.make_async_copy(cu_hbm, cu, in_sem.at[5])
    for cp in (ld_cu, ld_k, ld_v, ld_val):
        cp.start()

    barrier = pltpu.get_barrier_semaphore()
    for dev in (partner, cross, cross_o):
        pl.semaphore_signal(barrier, inc=1, device_id={"cp": dev}, device_id_type=MESH)
    pl.semaphore_wait(barrier, 3)
    ld_cu.wait()
    l0 = lax.shift_right_logical(cu[1], 3)

    peers = (partner, cross, cross_o)
    push_q = remote(q.at[:, oth_heads, :], far_q, raw_ssem.at[0], raw_rsem.at[0], partner)
    push_do = remote(do.at[:, oth_heads, :], far_do, raw_ssem.at[1], raw_rsem.at[1], partner)
    push_val = [remote(valid, valid_all.at[r], val_ssem.at[i], val_rsem.at[r], dev) for i, dev in enumerate(peers)]


    def kv_relayout(up):
        def body(i, _):
            t0 = i * 16
            for which, raw in ((0, raw_k), (1, raw_v)):
                rows = jnp.stack([raw[src_row(up, t0 + j, l0)] for j in range(16)])
                kv_hm[:, up, which, pl.ds(pl.multiple_of(t0, 16), 16), :] = jnp.transpose(rows, (1, 0, 2))
            return 0
        lax.fori_loop(0, SLOT // 16, body, 0)

    def kv_push(h, to, both):
        head = (4 * c if to == 1 else 4 * pc) + h
        dev = (partner, cross, cross_o)[to]
        ups = pl.ds(0, 2 if both else 1)
        return remote(kv_hm.at[head, ups], kv_all.at[h, r, ups], kv_ssem.at[to, h], kv_rsem.at[h, r], dev)

    def kv_first(to, up):
        head = 4 * c if to == 1 else 4 * pc
        at = pl.ds(up, 1)
        return remote(kv_hm.at[head, at], kv_all.at[0, r, at], first_ssem.at[to - 1, up], first_rsem.at[c, up],
                      (cross, cross_o)[to - 1])

    def kv_wait(h, owner, both):
        ups = pl.ds(0, 2 if both else 1)
        remote(kv_hm.at[0, ups], kv_all.at[h, owner, ups], kv_ssem.at[0, h], kv_rsem.at[h, owner], partner).wait_recv()

    def first_wait(owner):
        for up in range(2):
            at = pl.ds(up, 1)
            remote(kv_hm.at[0, at], kv_all.at[0, owner, at], first_ssem.at[0, up], first_rsem.at[owner - 2, up], partner).wait_recv()

    ld_k.wait()
    ld_v.wait()
    for cp in (ld_q, ld_do, push_q, push_do):
        cp.start()
    kv_relayout(0)

    def cross_send(ch, h):
        @pl.when(chip == ch)
        def _():
            for to in (1, 2):
                kv_push(h, to, ch == 1).start()

    cross_send(0, 0)

    def send_first(up):
        @pl.when(chip == 1)
        def _():
            for to in (1, 2):
                kv_first(to, up).start()

    send_first(0)
    kv_relayout(1)
    send_first(1)
    for h in range(HC):
        kv_push(h, 0, True).start()
    ld_val.wait()
    for cp in push_val:
        cp.start()

    def copy_own(h, _):
        for up in range(2):
            kv_all[h, r, up] = kv_hm[4 * c + h, up]
        return 0
    lax.fori_loop(0, HC, copy_own, 0)

    def q_relayout(oc, from_q, from_do):
        for up, ti in ((0, oc), (1, 3 - oc)):
            def body(i, _):
                t0 = i * 16
                at = pl.ds(pl.multiple_of(t0, 16), 16)
                for raw, dst in ((from_q, qh), (from_do, doh)):
                    rows = jnp.stack([raw[src_row(up, t0 + j, l0)] for j in range(16)])
                    dst[:, ti, :, at, :] = jnp.transpose(rows, (1, 0, 2)).reshape(HC, GROUP, 16, HEAD)
                return 0
            lax.fori_loop(0, SLOT // 16, body, 0)

    ld_q.wait()
    ld_do.wait()
    cross_send(0, 1)
    q_relayout(c, raw_q, raw_do)

    cross_send(0, 2)
    for i in range(3):
        remote(valid, valid_all.at[peers[i]], val_ssem.at[i], val_rsem.at[peers[i]], peers[i]).wait_recv()
    lane = lax.broadcasted_iota(jnp.int32, (SLOT, SLOT), 1)
    sub = lax.broadcasted_iota(jnp.int32, (SLOT, SLOT), 0)
    lane2 = lax.broadcasted_iota(jnp.int32, (SLOT, 2 * SLOT), 1)
    sub2 = lax.broadcasted_iota(jnp.int32, (SLOT, 2 * SLOT), 0)
    same_doc = (lane < l0) == (sub < l0)
    doc_f = jnp.where(lane < l0, 1.0, 0.0)
    doc_s = jnp.where(sub < l0, 1.0, 0.0)
    same_f = jnp.where(doc_f == doc_s, 1.0, 0.0)
    del same_doc

    def cap_body(s, _):
        owner = jnp.where(s < 4, s, 7 - s)
        off = jnp.where(s < 4, 0, 1)
        src_lo = jnp.where(sub2 < l0, sub2, sub2 + l0)
        src_hi = jnp.where(sub2 < l0, sub2 + l0, sub2 + SLOT)
        src = jnp.where(off == 1, src_hi, src_lo)
        row = jnp.broadcast_to(valid_all[owner].astype(F32), (SLOT, 2 * SLOT))
        ok = jnp.sum(jnp.where(src == lane2, row, 0.0), axis=1, keepdims=True)
        caps[s] = jnp.where(same_f * ok > 0.5, BIG, FILL)
        return 0
    lax.fori_loop(0, 8, cap_body, 0)
    for ti in range(4):
        oc, up = TILES[ti]
        s = (7 - (2 * chip + oc)) if up else 2 * chip + oc
        caps[8 + ti] = jnp.where(sub <= lane, caps[s], FILL)

    cross_send(0, 3)
    cross_send(1, 1)
    push_q.wait_recv()
    push_do.wait_recv()
    q_relayout(pc, far_q, far_do)

    def part_copy(h, u, n=2):
        up = int(u > 3)
        i = u if u < 2 else u - 2
        return remote(dkv_acc.at[h, pl.ds(2 * u, n)], cross_in.at[4 * c + h, up, pl.ds(0, n)], part_ssem.at[h, i],
                      part_rsem.at[4 * c + h, up], min(u, 7 - u))

    def part_wait(j, up, n=2):
        remote(dkv_acc.at[0, pl.ds(0, n)], cross_in.at[j, up, pl.ds(0, n)], part_ssem.at[0, 0],
               part_rsem.at[j, up], partner).wait_recv()

    def near_copy(h, up, slot, n=2):
        return remote(dkv_acc.at[h, pl.ds(2 * slot, n)], near_in.at[h, up, pl.ds(0, n)], near_ssem.at[h, up],
                      near_rsem.at[h, up], partner)

    def near_run(ch, h, act):
        act(near_copy(h, 0, 2 * ch + pc))
        if ch == 1:
            pl.when(c == 0)(lambda: act(near_copy(h, 1, 4)))
            if SW[h] < 2:
                pl.when(c == 1)(lambda: act(near_copy(h, 1, 5, 2 - SW[h])))

    def near_wait(h, up, n=2):
        near_copy(h, up, 0, n).wait_recv()

    def swap_copy(h):
        n = SW[h]
        return remote(dkv_acc.at[h, pl.ds(12 - n, n)], swap_in.at[h, pl.ds(2 - n, n)], swap_ssem.at[h], swap_rsem.at[h], cross)

    def swap_back(h, core):
        at = pl.ds(2 - SW[h], SW[h])
        j = 4 * core + h
        return remote(back_st.at[h, at], dkv_out.at[j, 1, at], back_ssem.at[h], back_rsem.at[j], 2)

    def res_copy(p, ti, which):
        stage, out = ((o_far, o_out), (dq_far, dq_out))[which]
        dst = out.at[TILES[ti][1], :, pl.ds(pl.multiple_of(16 * c + 8 * p, 8), 8), :]
        return remote(stage.at[p, ti], dst, res_ssem.at[which, p, ti], res_rsem.at[which, p, TILES[ti][1]], partner)

    def dkv_copy(h, ti):
        up = TILES[ti][1]
        return remote(dkv_st.at[h, ti], dkv_out.at[4 * c + h, up], dkv_ssem.at[h, ti], dkv_rsem.at[h, up], partner)

    def res_put(p):
        heads = pl.ds(pl.multiple_of(16 * c + 8 * p, 8), 8)
        for ti, (oc, up) in enumerate(TILES):
            def body(i, _, keep):
                at = pl.ds(pl.multiple_of(i * 16, 16), 16)
                for stage, far, out in ((o_st, o_far, o_out), (dq_st, dq_far, dq_out)):
                    x = jnp.concatenate([stage[e, ti, pl.ds(pl.multiple_of(g * SLOT + i * 16, 16), 16), :][None]
                                         for e in range(2) for g in range(GROUP)], axis=0)
                    y = jnp.transpose(x, (1, 0, 2))
                    if keep:
                        out[up, at, heads, :] = y
                    else:
                        far[p, ti, at, :, :] = y
                return 0

            @pl.when(c == oc)
            def _():
                lax.fori_loop(0, SLOT // 16, functools.partial(body, keep=True), 0)

            @pl.when(c != oc)
            def _():
                lax.fori_loop(0, SLOT // 16, functools.partial(body, keep=False), 0)
                for which in range(2):
                    res_copy(p, ti, which).start()

    def dkv_put(h, ti, parts):
        oc, up = TILES[ti]

        @pl.when(c == oc)
        def _():
            for w in range(2):
                dkv_out[4 * c + h, up, w] = parts(w).astype(BF16)

        @pl.when(c != oc)
        def _():
            for w in range(2):
                dkv_st[h, ti, w] = parts(w).astype(BF16)
            dkv_copy(h, ti).start()

    lse_far = remote(lse_st.at[pc], lse_out.at[:, own_heads, :], lse_sem, lse_rsem, partner)

    def kv_slot(h, s, which):
        return kv_all[h, min(s, 7 - s), int(s > 3), which]

    def kv_slots(h, a, b, which):
        return jnp.concatenate([kv_slot(h, s, which) for s in range(a, b)], axis=0)

    def run_chip(ch):
        slots = [slot_of(ch, ti) for ti in range(4)]
        sent = [0, 1] if ch == 1 else [2, 3, 4, 5]

        def transposes(s):
            for src, dst in ((0, kt), (1, vt)):
                dst[:, s * SLOT:(s + 1) * SLOT] = jnp.transpose(kv_slot(h_ref[0], s, src))

        h_ref = [None]
        sts = (st0, st1)

        def point(h, where):
            if ch == 0:
                return
            kv = {(0, 3): 2, (1, 2): 3}
            swaps = {(1, 4): (0, 1), (2, 4): (2,)}
            parts = {(2, 2): (0,), (2, 4): (1,), (3, 4): (2, 3)}
            for at in range(HC):
                if not any((at, where) in d for d in (kv, swaps, parts)):
                    continue

                @pl.when(h == at)
                def _():
                    if (at, where) in kv:
                        for to in (1, 2):
                            kv_push(kv[at, where], to, True).start()
                    for e in swaps.get((at, where), ()):
                        swap_copy(e).start()
                    for e in parts.get((at, where), ()):
                        for u in (0, 1):
                            part_copy(e, u).start()

        def head(h, _):
            h_ref[0] = h
            seen = set()
            ready = set()

            def wait_slot(s):
                if s in ready:
                    return
                if s in slots:
                    kv_wait(h, partner, True)
                    new = slots
                elif ch == 1:
                    for owner in (0, 1):
                        kv_wait(h, owner, False)
                    new = [0, 1]
                else:
                    for owner in (2, 3):
                        pl.when(h == 0)(functools.partial(first_wait, owner))
                        pl.when(h > 0)(functools.partial(kv_wait, h, owner, True))
                    new = [2, 3, 4, 5]
                for u in new:
                    ready.add(u)
                    transposes(u)

            state = {}

            def forward(ti):
                point(h, ti)
                s = slots[ti]
                nk = s + 1
                for u in range(nk):
                    wait_slot(u)
                st = sts[ti % 2]
                qt = qh[h, ti].reshape(TILE, HEAD)
                dt = doh[h, ti].reshape(TILE, HEAD)
                m8 = [None] * GROUP
                for a in range(0, nk, 2):
                    n = min(2, nk - a)
                    kb = kv_slots(h, a, a + n, 0)
                    sc = mm(kb, qt, NT)
                    for j in range(n):
                        cap = caps[8 + ti] if a + j == s else caps[a + j]
                        for g in range(GROUP):
                            x = jnp.minimum(sc[j * SLOT:(j + 1) * SLOT, g * SLOT:(g + 1) * SLOT], cap)
                            st[(a + j) * SLOT:(a + j + 1) * SLOT, g * SLOT:(g + 1) * SLOT] = x
                            top = jnp.max(x.reshape(SLOT // 8, 8, SLOT), axis=0)
                            m8[g] = top if m8[g] is None else jnp.maximum(m8[g], top)
                m = [jnp.max(x, axis=0, keepdims=True) for x in m8]
                mc = [x * C2 for x in m]
                l8 = [None] * GROUP
                for a in range(nk):
                    for g in range(GROUP):
                        at = (slice(a * SLOT, (a + 1) * SLOT), slice(g * SLOT, (g + 1) * SLOT))
                        e = jnp.exp2(st[at] * C2 - mc[g])
                        st[at] = e
                        pb[at] = e.astype(BF16)
                        tot = jnp.sum(e.reshape(SLOT // 8, 8, SLOT), axis=0)
                        l8[g] = tot if l8[g] is None else l8[g] + tot
                ot = mm(vt[:, :nk * SLOT], pb[:nk * SLOT, :], NN)
                inv, dd = [], []
                oc, up = TILES[ti]
                for g in range(GROUP):
                    l = jnp.sum(l8[g], axis=0, keepdims=True)
                    has = m[g] > 0.5 * FILL
                    safe = jnp.where(has, l, 1.0)
                    i_l = jnp.where(has, 1.0 / safe, 0.0)
                    lse = jnp.where(has, m[g] * SCALE + jnp.log(safe), 0.0)
                    lse_st[oc, up, pl.ds(h * GROUP + g, 1), :] = lse
                    og = (ot[:, g * SLOT:(g + 1) * SLOT] * i_l).astype(BF16)
                    dog = jnp.transpose(dt[g * SLOT:(g + 1) * SLOT, :])
                    dd.append(jnp.sum(og.astype(F32) * dog.astype(F32), axis=0, keepdims=True))
                    inv.append(i_l)
                    o_st[h % 2, ti, g * SLOT:(g + 1) * SLOT, :] = jnp.transpose(og)

                state[ti] = [inv, dd, None]

            def backward(ti, part):
                inv, dd, dqt = state[ti]
                qt = qh[h, ti].reshape(TILE, HEAD)
                dt = doh[h, ti].reshape(TILE, HEAD)
                st = sts[ti % 2]
                runs = []
                for u in part:
                    if runs and runs[-1][1] == u and u - runs[-1][0] < 2:
                        runs[-1][1] = u + 1
                    else:
                        runs.append([u, u + 1])
                for a, b in runs:
                    n = b - a
                    vb = kv_slots(h, a, b, 1)
                    dp = mm(vb, dt, NT)
                    for j in range(n):
                        for g in range(GROUP):
                            at = (slice((a + j) * SLOT, (a + j + 1) * SLOT), slice(g * SLOT, (g + 1) * SLOT))
                            p = st[at] * inv[g]
                            pb[at] = p.astype(BF16)
                            ds = p * (dp[j * SLOT:(j + 1) * SLOT, g * SLOT:(g + 1) * SLOT] - dd[g])
                            db[at] = ds.astype(BF16)
                    dsb = db[a * SLOT:b * SLOT, :]
                    dv = mm(pb[a * SLOT:b * SLOT, :], dt, NN)
                    dk = mm(dsb, qt, NN) * SCALE
                    dq = mm(kt[:, a * SLOT:b * SLOT], dsb, NN)
                    dqt = dq if dqt is None else dqt + dq
                    for j in range(n):
                        u = a + j
                        new = (dk[j * SLOT:(j + 1) * SLOT], dv[j * SLOT:(j + 1) * SLOT])
                        for w in range(2):
                            dkv_acc[h, 2 * u + w] = dkv_acc[h, 2 * u + w] + new[w] if u in seen else new[w]
                        seen.add(u)
                state[ti][2] = dqt

            def finish(ti):
                dqt = state[ti][2]
                for g in range(GROUP):
                    dqg = (dqt[:, g * SLOT:(g + 1) * SLOT] * SCALE).astype(BF16)
                    dq_st[h % 2, ti, g * SLOT:(g + 1) * SLOT, :] = jnp.transpose(dqg)

            if ch == 0:
                for ti in (0, 1):
                    forward(ti)
                    backward(ti, range(slots[ti] + 1))
                    finish(ti)
                for ti in (2, 3):
                    forward(ti)
                for ti in (2, 3):
                    backward(ti, [2, 3])
                for u in (2, 3):
                    part_copy(h, u).start()
                for ti in (2, 3):
                    backward(ti, [4, 5])
                part_copy(h, 4).start()
                for at in range(HC):
                    if SW[at] < 2:
                        pl.when(h == at)(part_copy(at, 5, 2 - SW[at]).start)
                for ti in (2, 3):
                    backward(ti, [u for u in range(slots[ti] + 1) if u not in sent])
                    finish(ti)
            else:
                for ti in range(4):
                    forward(ti)
                    backward(ti, range(slots[ti] + 1))
                    finish(ti)
            if ch == 1:
                point(h, 4)
            else:
                for ti in (2, 3):
                    dkv_put(h, ti, lambda w, ti=ti: dkv_acc[h, 2 * slots[ti] + w])
            for at in range(HC):
                pl.when(h == at)(functools.partial(near_run, ch, at, lambda cp: cp.start()))
            pl.when(h % 2 == 1)(lambda: res_put(h // 2))
            return 0

        lax.fori_loop(0, HC, head, 0)

        lse_out[:, own_heads, :] = lse_st[c]
        lse_far.start()

        if ch == 0:
            for h in range(HC):
                if SW[h]:
                    swap_copy(h).wait_recv()
                    for w in range(2 - SW[h], 2):
                        back_st[h, w] = (swap_in[h, w] + dkv_acc[h, 10 + w]).astype(BF16)
                    swap_back(h, c).start()

        def early(h, _):
            kv_push(h, 0, True).wait_send()
            for to in (1, 2):
                if ch == 0:
                    kv_push(h, to, False).wait_send()
                else:
                    pl.when(h > 0)(kv_push(h, to, True).wait_send)
            if ch == 0:
                for ti in (2, 3):
                    pl.when(c != TILES[ti][0])(dkv_copy(h, ti).wait_send)
                remote(dkv_st.at[h, 0], dkv_out.at[4 * pc + h, 1], dkv_ssem.at[h, 0], dkv_rsem.at[h, 1], partner).wait_recv()
            return 0
        lax.fori_loop(0, HC, early, 0)
        if ch == 1:
            for to in (1, 2):
                for up in range(2):
                    kv_first(to, up).wait_send()
        for h in range(HC):
            near_run(ch, h, lambda cp: cp.wait_send())
        push_q.wait_send()
        push_do.wait_send()
        for cp in push_val:
            cp.wait_send()
        for p in range(2):
            for which in range(2):
                stage, out = ((o_far, o_out), (dq_far, dq_out))[which]
                for ti in range(4):
                    pl.when(c != TILES[ti][0])(res_copy(p, ti, which).wait_send)
                for up in range(2):
                    dst = out.at[up, :, pl.ds(pl.multiple_of(16 * pc + 8 * p, 8), 8), :]
                    remote(stage.at[p, 0], dst, res_ssem.at[which, p, 0], res_rsem.at[which, p, up], partner).wait_recv()
        lse_far.wait_send()
        remote(lse_st.at[0], lse_out.at[:, oth_heads, :], lse_sem, lse_rsem, partner).wait_recv()

        def add_up(h, up, slot, n):
            if n == 0:
                return
            part_wait(4 * c + h, up, n)
            for w in range(n):
                dkv_out[4 * c + h, up, w] = (dkv_acc[h, 2 * slot + w] + cross_in[4 * c + h, up, w]).astype(BF16)
            near_wait(h, up, n)
            part_wait(4 * pc + h, up, n)
            for w in range(n):
                dkv_out[4 * pc + h, up, w] = (near_in[h, up, w] + cross_in[4 * pc + h, up, w]).astype(BF16)

        for h in range(HC):
            add_up(h, 0, 2 * ch + c, 2)
            if ch == 1:
                pl.when(c == 1)(functools.partial(add_up, h, 1, 4, 2))
                pl.when(c == 0)(functools.partial(add_up, h, 1, 5, 2 - SW[h]))

        for h in range(HC):
            for u in sent:
                n = 2 - SW[h] if u == 5 else 2
                if n:
                    part_copy(h, u, n).wait_send()
            if SW[h]:
                if ch == 0:
                    swap_back(h, c).wait_send()
                else:
                    swap_copy(h).wait_send()

        if ch == 1:
            @pl.when(c == 0)
            def _():
                for h in range(HC):
                    if SW[h]:
                        for core in range(2):
                            swap_back(h, core).wait_recv()

    pl.when(chip == 0)(functools.partial(run_chip, 0))
    pl.when(chip == 1)(functools.partial(run_chip, 1))


def attn_call(cu, valid, q, k, v, do):
    any_spec = pl.BlockSpec(memory_space=pl.ANY)
    dma = pltpu.SemaphoreType.DMA
    return pl.pallas_call(
        attn_kernel,
        out_shape=(
            pltpu.VMEM((2, SLOT, 32, HEAD), BF16),
            pltpu.VMEM((2, SLOT, 32, HEAD), BF16),
            pltpu.VMEM((8, 2, 2, SLOT, HEAD), BF16),
            pltpu.VMEM((2, 32, SLOT), F32),
            pltpu.SMEM((3,), jnp.int32),
        ),
        in_specs=[any_spec] * 6,
        out_specs=(pl.BlockSpec(memory_space=pltpu.VMEM),) * 4 + (pl.BlockSpec(memory_space=pltpu.SMEM),),
        scratch_shapes=[
            pltpu.VMEM((256, 16, HEAD), BF16),
            pltpu.VMEM((256, 16, HEAD), BF16),
            pltpu.VMEM((256, 16, HEAD), BF16),
            pltpu.VMEM((256, 16, HEAD), BF16),
            pltpu.VMEM((256, 8, HEAD), BF16),
            pltpu.VMEM((256, 8, HEAD), BF16),
            pltpu.VMEM((8, 2, 2, SLOT, HEAD), BF16),
            pltpu.VMEM((HC, 4, 2, 2, SLOT, HEAD), BF16),
            pltpu.VMEM((HEAD, 8 * SLOT), BF16),
            pltpu.VMEM((HEAD, 8 * SLOT), BF16),
            pltpu.VMEM((HC, 4, GROUP, SLOT, HEAD), BF16),
            pltpu.VMEM((HC, 4, GROUP, SLOT, HEAD), BF16),
            pltpu.VMEM((8 * SLOT, TILE), F32),
            pltpu.VMEM((8 * SLOT, TILE), F32),
            pltpu.VMEM((8 * SLOT, TILE), BF16),
            pltpu.VMEM((8 * SLOT, TILE), BF16),
            pltpu.VMEM((HC, 16, SLOT, HEAD), F32),
            pltpu.VMEM((8, 2, 2, SLOT, HEAD), F32),
            pltpu.VMEM((HC, 2, 2, SLOT, HEAD), F32),
            pltpu.VMEM((HC, 2, SLOT, HEAD), F32),
            pltpu.VMEM((2, 4, TILE, HEAD), BF16),
            pltpu.VMEM((2, 4, TILE, HEAD), BF16),
            pltpu.VMEM((2, 4, SLOT, 8, HEAD), BF16),
            pltpu.VMEM((2, 4, SLOT, 8, HEAD), BF16),
            pltpu.VMEM((HC, 4, 2, SLOT, HEAD), BF16),
            pltpu.VMEM((HC, 2, SLOT, HEAD), BF16),
            pltpu.VMEM((2, 2, 16, SLOT), F32),
            pltpu.VMEM((12, SLOT, SLOT), F32),
            pltpu.VMEM((4, 1, 2 * SLOT), jnp.int32),
            dma((6,)),
            dma((2,)), dma((2,)),
            dma((3,)), dma((4,)),
            dma((2, 2)), dma((2, 2)),
            dma((3, HC)), dma((HC, 4)),
            dma((HC, 4)), dma((8, 2)), dma((HC, 2)), dma((HC, 2)),
            dma((HC,)), dma((HC,)), dma((HC,)), dma((8,)),
            dma((2, 2, 4)), dma((2, 2, 2)),
            dma((HC, 4)), dma((HC, 2)),
            dma, dma,
        ],
        compiler_params=pltpu.CompilerParams(collective_id=0, has_side_effects=True, vmem_limit_bytes=61300000),
        name="attn",
    )(cu, valid, q, k, v, do)


def finish_kernel(o_in, dq_in, dkv_in, lse_in, cu, o_out, dq_out, dk_out, dv_out, lse_out, dk_t, dv_t, lse_t, sem, lse_sem):
    l0 = lax.shift_right_logical(cu[1], 3)
    rest = SLOT - l0

    def copies(i, x, out):
        runs = ((0, 0, 0, l0), (1, 0, l0, l0), (0, l0, 2 * l0, rest), (1, l0, SLOT + l0, rest))
        return [pltpu.make_async_copy(x.at[up, pl.ds(at, n)], out.at[pl.ds(to, n)], sem.at[i, j])
                for j, (up, at, to, n) in enumerate(runs)]

    moves = copies(0, o_in, o_out) + copies(1, dq_in, dq_out)
    for cp in moves:
        cp.start()

    for w, dst in ((0, dk_t), (1, dv_t)):
        for up in range(2):
            def body(i, _):
                at = pl.ds(pl.multiple_of(i * 16, 16), 16)
                dst[up, at] = jnp.transpose(dkv_in[:, up, w, at, :], (1, 0, 2))
                return 0
            lax.fori_loop(0, SLOT // 16, body, 0)
        more = copies(2 + w, dst, (dk_out, dv_out)[w])
        for cp in more:
            cp.start()
        moves += more

    row = lax.broadcasted_iota(jnp.int32, (2 * SLOT, SLOT), 0)
    col = lax.broadcasted_iota(jnp.int32, (2 * SLOT, SLOT), 1)
    acc = None
    for up in range(2):
        if up:
            src = jnp.where(col < l0, col + l0, col + SLOT)
        else:
            src = jnp.where(col < l0, col, col + l0)
        pick = jnp.where(row == src, 1.0, 0.0)
        part = lax.dot_general(lse_in[up], pick, NT, precision=lax.Precision.HIGHEST, preferred_element_type=F32)
        acc = part if acc is None else acc + part
    lse_t[...] = acc
    lse_move = pltpu.make_async_copy(lse_t, lse_out, lse_sem)
    lse_move.start()
    for cp in moves + [lse_move]:
        cp.wait()


def finish_call(o_t, dq_t, dkv_hm, lse_hm, cu):
    any_spec = pl.BlockSpec(memory_space=pl.ANY)
    vmem = pl.BlockSpec(memory_space=pltpu.VMEM)
    return pl.pallas_call(
        finish_kernel,
        out_shape=(
            jax.ShapeDtypeStruct((256, 32, HEAD), BF16),
            jax.ShapeDtypeStruct((256, 32, HEAD), BF16),
            jax.ShapeDtypeStruct((256, 8, HEAD), BF16),
            jax.ShapeDtypeStruct((256, 8, HEAD), BF16),
            jax.ShapeDtypeStruct((32, 256), F32),
        ),
        in_specs=[vmem] * 4 + [pl.BlockSpec(memory_space=pltpu.SMEM)],
        out_specs=(any_spec,) * 5,
        scratch_shapes=[
            pltpu.VMEM((2, SLOT, 8, HEAD), BF16),
            pltpu.VMEM((2, SLOT, 8, HEAD), BF16),
            pltpu.VMEM((32, 256), F32),
            pltpu.SemaphoreType.DMA((4, 4)),
            pltpu.SemaphoreType.DMA,
        ],
        compiler_params=pltpu.CompilerParams(vmem_limit_bytes=16 * 1024 * 1024),
        name="finish",
    )(o_t, dq_t, dkv_hm, lse_hm, cu)


def solution(mesh):
    tok_spec = P(("dp", "cp"), None, None)
    lse_spec = P(("dp", "cp"), None)

    def local(q, k, v, do, valid, cu):
        res = attn_call(cu, valid.reshape(1, 256), q, k, v, do)
        o, dq, dk, dv, lse = finish_call(*res)
        return o, lse.T, dq, dk, dv

    return jax.shard_map(local, mesh=mesh, in_specs=(tok_spec,) * 4 + (P(("dp", "cp")), P("dp")),
                         out_specs=(tok_spec, lse_spec, tok_spec, tok_spec, tok_spec), check_vma=False)
```

```python
import functools
import math

import jax
import jax.numpy as jnp
from jax import lax
from jax.experimental import pallas as pl
from jax.experimental.pallas import tpu as pltpu
from jax.sharding import PartitionSpec as P

MESH = pl.DeviceIdType.MESH
FILL = -1.0e30
BIG = 3.0e38
HEAD = 128
SLOT = 128
TILE = 512
GROUP = 4
HC = 4
SW = (2, 2, 2, 0)
SCALE = HEAD ** -0.5
C2 = SCALE * math.log2(math.e)
NT = (((1,), (1,)), ((), ()))
NN = (((1,), (0,)), ((), ()))
F32 = jnp.float32
BF16 = jnp.bfloat16

TILES = ((0, 0), (1, 0), (1, 1), (0, 1))


def slot_of(chip, ti):
    oc, up = TILES[ti]
    r = 2 * chip + oc
    return 7 - r if up else r


def mm(a, b, dims):
    return lax.dot_general(a, b, dims, preferred_element_type=F32)


def src_row(up, t, l0):
    if up:
        return jnp.where(t < l0, t + l0, t + SLOT)
    return jnp.where(t < l0, t, t + l0)


def attn_kernel(cu_hbm, valid, q, k, v, do, o_out, dq_out, dkv_out, lse_out, cu,
                raw_q, raw_do, far_q, far_do, raw_k, raw_v, kv_hm, kv_all, kt, vt, qh, doh, st0, st1, pb, db,
                dkv_acc, cross_in, swap_in, o_st, dq_st, o_far, dq_far, dkv_st, back_st, lse_st, caps, valid_all,
                in_sem, raw_ssem, raw_rsem, val_ssem, val_rsem, first_ssem, first_rsem, kv_ssem, kv_rsem,
                part_ssem, part_rsem, swap_ssem, swap_rsem, back_ssem, back_rsem, res_ssem, res_rsem, dkv_ssem, dkv_rsem, lse_sem, lse_rsem):
    r = lax.axis_index("cp")
    chip = r // 2
    c = r % 2
    pc = 1 - c
    partner = chip * 2 + pc
    cross = (1 - chip) * 2 + c
    cross_o = (1 - chip) * 2 + pc

    def remote(src, dst, ssem, rsem, dev):
        return pltpu.make_async_remote_copy(src_ref=src, dst_ref=dst, send_sem=ssem, recv_sem=rsem,
                                            device_id={"cp": dev}, device_id_type=MESH)

    own_heads = pl.ds(pl.multiple_of(16 * c, 16), 16)
    oth_heads = pl.ds(pl.multiple_of(16 * pc, 16), 16)
    ld_k = pltpu.make_async_copy(k, raw_k, in_sem.at[0])
    ld_v = pltpu.make_async_copy(v, raw_v, in_sem.at[1])
    ld_q = pltpu.make_async_copy(q.at[:, own_heads, :], raw_q, in_sem.at[2])
    ld_do = pltpu.make_async_copy(do.at[:, own_heads, :], raw_do, in_sem.at[3])
    ld_val = pltpu.make_async_copy(valid, valid_all.at[r], in_sem.at[4])
    ld_cu = pltpu.make_async_copy(cu_hbm, cu, in_sem.at[5])
    for cp in (ld_cu, ld_k, ld_v, ld_val):
        cp.start()

    barrier = pltpu.get_barrier_semaphore()
    for dev in (partner, cross, cross_o):
        pl.semaphore_signal(barrier, inc=1, device_id={"cp": dev}, device_id_type=MESH)
    pl.semaphore_wait(barrier, 3)
    ld_cu.wait()
    l0 = lax.shift_right_logical(cu[1], 3)

    peers = (partner, cross, cross_o)
    push_q = remote(q.at[:, oth_heads, :], far_q, raw_ssem.at[0], raw_rsem.at[0], partner)
    push_do = remote(do.at[:, oth_heads, :], far_do, raw_ssem.at[1], raw_rsem.at[1], partner)
    push_val = [remote(valid, valid_all.at[r], val_ssem.at[i], val_rsem.at[r], dev) for i, dev in enumerate(peers)]


    def kv_relayout(up):
        def body(i, _):
            t0 = i * 16
            for which, raw in ((0, raw_k), (1, raw_v)):
                rows = jnp.stack([raw[src_row(up, t0 + j, l0)] for j in range(16)])
                kv_hm[:, up, which, pl.ds(pl.multiple_of(t0, 16), 16), :] = jnp.transpose(rows, (1, 0, 2))
            return 0
        lax.fori_loop(0, SLOT // 16, body, 0)

    def kv_push(h, to, both):
        head = (4 * c if to == 1 else 4 * pc) + h
        dev = (partner, cross, cross_o)[to]
        ups = pl.ds(0, 2 if both else 1)
        return remote(kv_hm.at[head, ups], kv_all.at[h, r, ups], kv_ssem.at[to, h], kv_rsem.at[h, r], dev)

    def kv_first(to, up):
        head = 4 * c if to == 1 else 4 * pc
        at = pl.ds(up, 1)
        return remote(kv_hm.at[head, at], kv_all.at[0, r, at], first_ssem.at[to - 1, up], first_rsem.at[c, up],
                      (cross, cross_o)[to - 1])

    def kv_wait(h, owner, both):
        ups = pl.ds(0, 2 if both else 1)
        remote(kv_hm.at[0, ups], kv_all.at[h, owner, ups], kv_ssem.at[0, h], kv_rsem.at[h, owner], partner).wait_recv()

    def first_wait(owner):
        for up in range(2):
            at = pl.ds(up, 1)
            remote(kv_hm.at[0, at], kv_all.at[0, owner, at], first_ssem.at[0, up], first_rsem.at[owner - 2, up], partner).wait_recv()

    ld_k.wait()
    ld_v.wait()
    for cp in (ld_q, ld_do, push_q, push_do):
        cp.start()
    kv_relayout(0)

    def cross_send(ch, h):
        @pl.when(chip == ch)
        def _():
            for to in (1, 2):
                kv_push(h, to, ch == 1).start()

    cross_send(0, 0)

    def send_first(up):
        @pl.when(chip == 1)
        def _():
            for to in (1, 2):
                kv_first(to, up).start()

    send_first(0)
    kv_relayout(1)
    send_first(1)
    for h in range(HC):
        kv_push(h, 0, True).start()
    ld_val.wait()
    for cp in push_val:
        cp.start()

    def copy_own(h, _):
        for up in range(2):
            kv_all[h, r, up] = kv_hm[4 * c + h, up]
        return 0
    lax.fori_loop(0, HC, copy_own, 0)

    def q_relayout(oc, from_q, from_do):
        for up, ti in ((0, oc), (1, 3 - oc)):
            def body(i, _):
                t0 = i * 16
                at = pl.ds(pl.multiple_of(t0, 16), 16)
                for raw, dst in ((from_q, qh), (from_do, doh)):
                    rows = jnp.stack([raw[src_row(up, t0 + j, l0)] for j in range(16)])
                    dst[:, ti, :, at, :] = jnp.transpose(rows, (1, 0, 2)).reshape(HC, GROUP, 16, HEAD)
                return 0
            lax.fori_loop(0, SLOT // 16, body, 0)

    ld_q.wait()
    ld_do.wait()
    cross_send(0, 1)
    q_relayout(c, raw_q, raw_do)

    cross_send(0, 2)
    for i in range(3):
        remote(valid, valid_all.at[peers[i]], val_ssem.at[i], val_rsem.at[peers[i]], peers[i]).wait_recv()
    lane = lax.broadcasted_iota(jnp.int32, (SLOT, SLOT), 1)
    sub = lax.broadcasted_iota(jnp.int32, (SLOT, SLOT), 0)
    lane2 = lax.broadcasted_iota(jnp.int32, (SLOT, 2 * SLOT), 1)
    sub2 = lax.broadcasted_iota(jnp.int32, (SLOT, 2 * SLOT), 0)
    same_doc = (lane < l0) == (sub < l0)
    doc_f = jnp.where(lane < l0, 1.0, 0.0)
    doc_s = jnp.where(sub < l0, 1.0, 0.0)
    same_f = jnp.where(doc_f == doc_s, 1.0, 0.0)
    del same_doc

    def cap_body(s, _):
        owner = jnp.where(s < 4, s, 7 - s)
        off = jnp.where(s < 4, 0, 1)
        src_lo = jnp.where(sub2 < l0, sub2, sub2 + l0)
        src_hi = jnp.where(sub2 < l0, sub2 + l0, sub2 + SLOT)
        src = jnp.where(off == 1, src_hi, src_lo)
        row = jnp.broadcast_to(valid_all[owner].astype(F32), (SLOT, 2 * SLOT))
        ok = jnp.sum(jnp.where(src == lane2, row, 0.0), axis=1, keepdims=True)
        caps[s] = jnp.where(same_f * ok > 0.5, BIG, FILL)
        return 0
    lax.fori_loop(0, 8, cap_body, 0)
    for ti in range(4):
        oc, up = TILES[ti]
        s = (7 - (2 * chip + oc)) if up else 2 * chip + oc
        caps[8 + ti] = jnp.where(sub <= lane, caps[s], FILL)

    cross_send(0, 3)
    cross_send(1, 1)
    push_q.wait_recv()
    push_do.wait_recv()
    q_relayout(pc, far_q, far_do)

    def part_copy(h, i, first, n):
        return remote(dkv_acc.at[h, pl.ds(first, n)], cross_in.at[h, pl.ds(4 * i, n)], part_ssem.at[h, i],
                      part_rsem.at[h, i], cross)

    def part_list(ch, h):
        if ch == 1:
            return [part_copy(h, 0, 0, 4)]
        return [part_copy(h, 0, 4, 4), part_copy(h, 1, 8, 4 - SW[h])]

    def swap_copy(h):
        n = SW[h]
        return remote(dkv_acc.at[h, pl.ds(12 - n, n)], swap_in.at[h, pl.ds(2 - n, n)], swap_ssem.at[h], swap_rsem.at[h], cross)

    def swap_back(h, core):
        at = pl.ds(2 - SW[h], SW[h])
        j = 4 * core + h
        return remote(back_st.at[h, at], dkv_out.at[j, 1, at], back_ssem.at[h], back_rsem.at[j], 2)

    def res_copy(p, ti, which):
        stage, out = ((o_far, o_out), (dq_far, dq_out))[which]
        dst = out.at[TILES[ti][1], :, pl.ds(pl.multiple_of(16 * c + 8 * p, 8), 8), :]
        return remote(stage.at[p, ti], dst, res_ssem.at[which, p, ti], res_rsem.at[which, p, TILES[ti][1]], partner)

    def dkv_copy(h, ti, n=2, j=None):
        up = TILES[ti][1]
        at = pl.ds(0, n)
        return remote(dkv_st.at[h, ti, at], dkv_out.at[4 * c + h if j is None else j, up, at], dkv_ssem.at[h, ti],
                      dkv_rsem.at[h, up], partner)

    def res_put(p):
        heads = pl.ds(pl.multiple_of(16 * c + 8 * p, 8), 8)
        for ti, (oc, up) in enumerate(TILES):
            def body(i, _, keep):
                at = pl.ds(pl.multiple_of(i * 16, 16), 16)
                for stage, far, out in ((o_st, o_far, o_out), (dq_st, dq_far, dq_out)):
                    x = jnp.concatenate([stage[e, ti, pl.ds(pl.multiple_of(g * SLOT + i * 16, 16), 16), :][None]
                                         for e in range(2) for g in range(GROUP)], axis=0)
                    y = jnp.transpose(x, (1, 0, 2))
                    if keep:
                        out[up, at, heads, :] = y
                    else:
                        far[p, ti, at, :, :] = y
                return 0

            @pl.when(c == oc)
            def _():
                lax.fori_loop(0, SLOT // 16, functools.partial(body, keep=True), 0)

            @pl.when(c != oc)
            def _():
                lax.fori_loop(0, SLOT // 16, functools.partial(body, keep=False), 0)
                for which in range(2):
                    res_copy(p, ti, which).start()

    def dkv_put(h, ti, parts, n=2):
        oc, up = TILES[ti]

        @pl.when(c == oc)
        def _():
            for w in range(n):
                dkv_out[4 * c + h, up, w] = parts(w).astype(BF16)

        @pl.when(c != oc)
        def _():
            for w in range(n):
                dkv_st[h, ti, w] = parts(w).astype(BF16)
            dkv_copy(h, ti, n).start()

    lse_far = remote(lse_st.at[pc], lse_out.at[:, own_heads, :], lse_sem, lse_rsem, partner)

    def kv_slot(h, s, which):
        return kv_all[h, min(s, 7 - s), int(s > 3), which]

    def kv_slots(h, a, b, which):
        return jnp.concatenate([kv_slot(h, s, which) for s in range(a, b)], axis=0)

    def run_chip(ch):
        slots = [slot_of(ch, ti) for ti in range(4)]
        sent = [0, 1] if ch == 1 else [2, 3, 4, 5]

        def transposes(s):
            for src, dst in ((0, kt), (1, vt)):
                dst[:, s * SLOT:(s + 1) * SLOT] = jnp.transpose(kv_slot(h_ref[0], s, src))

        h_ref = [None]
        sts = (st0, st1)

        def point(h, where):
            if ch == 0:
                return
            kv = {(0, 3): 2, (1, 2): 3}
            swaps = {(1, 4): (0, 1), (2, 4): (2,)}
            parts = {(2, 2): (0,), (2, 4): (1,), (3, 4): (2, 3)}
            for at in range(HC):
                if not any((at, where) in d for d in (kv, swaps, parts)):
                    continue

                @pl.when(h == at)
                def _():
                    if (at, where) in kv:
                        for to in (1, 2):
                            kv_push(kv[at, where], to, True).start()
                    for e in swaps.get((at, where), ()):
                        swap_copy(e).start()
                    for e in parts.get((at, where), ()):
                        part_list(1, e)[0].start()

        def head(h, _):
            h_ref[0] = h
            seen = set()
            ready = set()

            def wait_slot(s):
                if s in ready:
                    return
                if s in slots:
                    kv_wait(h, partner, True)
                    new = slots
                elif ch == 1:
                    for owner in (0, 1):
                        kv_wait(h, owner, False)
                    new = [0, 1]
                else:
                    for owner in (2, 3):
                        pl.when(h == 0)(functools.partial(first_wait, owner))
                        pl.when(h > 0)(functools.partial(kv_wait, h, owner, True))
                    new = [2, 3, 4, 5]
                for u in new:
                    ready.add(u)
                    transposes(u)

            state = {}

            def forward(ti):
                point(h, ti)
                s = slots[ti]
                nk = s + 1
                for u in range(nk):
                    wait_slot(u)
                st = sts[ti % 2]
                qt = qh[h, ti].reshape(TILE, HEAD)
                dt = doh[h, ti].reshape(TILE, HEAD)
                m8 = [None] * GROUP
                for a in range(0, nk, 2):
                    n = min(2, nk - a)
                    kb = kv_slots(h, a, a + n, 0)
                    sc = mm(kb, qt, NT)
                    for j in range(n):
                        cap = caps[8 + ti] if a + j == s else caps[a + j]
                        for g in range(GROUP):
                            x = jnp.minimum(sc[j * SLOT:(j + 1) * SLOT, g * SLOT:(g + 1) * SLOT], cap)
                            st[(a + j) * SLOT:(a + j + 1) * SLOT, g * SLOT:(g + 1) * SLOT] = x
                            top = jnp.max(x.reshape(SLOT // 8, 8, SLOT), axis=0)
                            m8[g] = top if m8[g] is None else jnp.maximum(m8[g], top)
                m = [jnp.max(x, axis=0, keepdims=True) for x in m8]
                mc = [x * C2 for x in m]
                l8 = [None] * GROUP
                for a in range(nk):
                    for g in range(GROUP):
                        at = (slice(a * SLOT, (a + 1) * SLOT), slice(g * SLOT, (g + 1) * SLOT))
                        e = jnp.exp2(st[at] * C2 - mc[g])
                        st[at] = e
                        pb[at] = e.astype(BF16)
                        tot = jnp.sum(e.reshape(SLOT // 8, 8, SLOT), axis=0)
                        l8[g] = tot if l8[g] is None else l8[g] + tot
                ot = mm(vt[:, :nk * SLOT], pb[:nk * SLOT, :], NN)
                inv, dd = [], []
                oc, up = TILES[ti]
                for g in range(GROUP):
                    l = jnp.sum(l8[g], axis=0, keepdims=True)
                    has = m[g] > 0.5 * FILL
                    safe = jnp.where(has, l, 1.0)
                    i_l = jnp.where(has, 1.0 / safe, 0.0)
                    lse = jnp.where(has, m[g] * SCALE + jnp.log(safe), 0.0)
                    lse_st[oc, up, pl.ds(h * GROUP + g, 1), :] = lse
                    og = (ot[:, g * SLOT:(g + 1) * SLOT] * i_l).astype(BF16)
                    dog = jnp.transpose(dt[g * SLOT:(g + 1) * SLOT, :])
                    dd.append(jnp.sum(og.astype(F32) * dog.astype(F32), axis=0, keepdims=True))
                    inv.append(i_l)
                    o_st[h % 2, ti, g * SLOT:(g + 1) * SLOT, :] = jnp.transpose(og)

                state[ti] = [inv, dd, None]

            def backward(ti, part):
                inv, dd, dqt = state[ti]
                qt = qh[h, ti].reshape(TILE, HEAD)
                dt = doh[h, ti].reshape(TILE, HEAD)
                st = sts[ti % 2]
                runs = []
                for u in part:
                    if runs and runs[-1][1] == u and u - runs[-1][0] < 2:
                        runs[-1][1] = u + 1
                    else:
                        runs.append([u, u + 1])
                for a, b in runs:
                    n = b - a
                    vb = kv_slots(h, a, b, 1)
                    dp = mm(vb, dt, NT)
                    for j in range(n):
                        for g in range(GROUP):
                            at = (slice((a + j) * SLOT, (a + j + 1) * SLOT), slice(g * SLOT, (g + 1) * SLOT))
                            p = st[at] * inv[g]
                            pb[at] = p.astype(BF16)
                            ds = p * (dp[j * SLOT:(j + 1) * SLOT, g * SLOT:(g + 1) * SLOT] - dd[g])
                            db[at] = ds.astype(BF16)
                    dsb = db[a * SLOT:b * SLOT, :]
                    dv = mm(pb[a * SLOT:b * SLOT, :], dt, NN)
                    dk = mm(dsb, qt, NN) * SCALE
                    dq = mm(kt[:, a * SLOT:b * SLOT], dsb, NN)
                    dqt = dq if dqt is None else dqt + dq
                    for j in range(n):
                        u = a + j
                        new = (dk[j * SLOT:(j + 1) * SLOT], dv[j * SLOT:(j + 1) * SLOT])
                        for w in range(2):
                            dkv_acc[h, 2 * u + w] = dkv_acc[h, 2 * u + w] + new[w] if u in seen else new[w]
                        seen.add(u)
                state[ti][2] = dqt

            def finish(ti):
                dqt = state[ti][2]
                for g in range(GROUP):
                    dqg = (dqt[:, g * SLOT:(g + 1) * SLOT] * SCALE).astype(BF16)
                    dq_st[h % 2, ti, g * SLOT:(g + 1) * SLOT, :] = jnp.transpose(dqg)

            if ch == 0:
                for ti in (0, 1):
                    forward(ti)
                    backward(ti, range(slots[ti] + 1))
                    finish(ti)
                for ti in (2, 3):
                    forward(ti)
                for ti in (2, 3):
                    backward(ti, [2, 3])
                part_copy(h, 0, 4, 4).start()
                for ti in (2, 3):
                    backward(ti, [4, 5])
                for at in range(HC):
                    pl.when(h == at)(part_copy(at, 1, 8, 4 - SW[at]).start)
                for ti in (2, 3):
                    backward(ti, [u for u in range(slots[ti] + 1) if u not in sent])
                    finish(ti)
            else:
                for ti in range(4):
                    forward(ti)
                    backward(ti, range(slots[ti] + 1))
                    finish(ti)
            if ch == 1:
                point(h, 4)
            else:
                for ti in (2, 3):
                    dkv_put(h, ti, lambda w, ti=ti: dkv_acc[h, 2 * slots[ti] + w])
            pl.when(h % 2 == 1)(lambda: res_put(h // 2))
            return 0

        lax.fori_loop(0, HC, head, 0)

        lse_out[:, own_heads, :] = lse_st[c]
        lse_far.start()

        if ch == 0:
            for h in range(HC):
                if SW[h]:
                    swap_copy(h).wait_recv()
                    for w in range(2 - SW[h], 2):
                        back_st[h, w] = (swap_in[h, w] + dkv_acc[h, 10 + w]).astype(BF16)
                    swap_back(h, c).start()

        def early(h, _):
            kv_push(h, 0, True).wait_send()
            for to in (1, 2):
                if ch == 0:
                    kv_push(h, to, False).wait_send()
                else:
                    pl.when(h > 0)(kv_push(h, to, True).wait_send)
            if ch == 0:
                for ti in (2, 3):
                    pl.when(c != TILES[ti][0])(dkv_copy(h, ti).wait_send)
                remote(dkv_st.at[h, 0], dkv_out.at[4 * pc + h, 1], dkv_ssem.at[h, 0], dkv_rsem.at[h, 1], partner).wait_recv()
            return 0
        lax.fori_loop(0, HC, early, 0)
        if ch == 1:
            for to in (1, 2):
                for up in range(2):
                    kv_first(to, up).wait_send()
        push_q.wait_send()
        push_do.wait_send()
        for cp in push_val:
            cp.wait_send()
        for p in range(2):
            for which in range(2):
                stage, out = ((o_far, o_out), (dq_far, dq_out))[which]
                for ti in range(4):
                    pl.when(c != TILES[ti][0])(res_copy(p, ti, which).wait_send)
                for up in range(2):
                    dst = out.at[up, :, pl.ds(pl.multiple_of(16 * pc + 8 * p, 8), 8), :]
                    remote(stage.at[p, 0], dst, res_ssem.at[which, p, 0], res_rsem.at[which, p, up], partner).wait_recv()
        lse_far.wait_send()
        remote(lse_st.at[0], lse_out.at[:, oth_heads, :], lse_sem, lse_rsem, partner).wait_recv()

        kept = [(i, ti) for i, ti in enumerate([0, 1] if ch == 0 else [0, 1, 2, 3])]
        for h in range(HC):
            for i, cp in enumerate(part_list(1 - ch, h)):
                cp.wait_recv()
                for k, ti in kept[2 * i:2 * i + 2]:
                    u = slots[ti]
                    n = 2 - SW[h] if u == 5 else 2
                    if n:
                        dkv_put(h, ti, lambda w, k=k, u=u: dkv_acc[h, 2 * u + w] + cross_in[h, 2 * k + w], n)
        for h in range(HC):
            for k, ti in kept:
                n = 2 - SW[h] if slots[ti] == 5 else 2
                if n:
                    pl.when(c != TILES[ti][0])(dkv_copy(h, ti, n).wait_send)
                    pl.when(c == TILES[ti][0])(dkv_copy(h, ti, n, 4 * pc + h).wait_recv)

        for h in range(HC):
            for cp in part_list(ch, h):
                cp.wait_send()
            if SW[h]:
                if ch == 0:
                    swap_back(h, c).wait_send()
                else:
                    swap_copy(h).wait_send()

        if ch == 1:
            @pl.when(c == 0)
            def _():
                for h in range(HC):
                    if SW[h]:
                        for core in range(2):
                            swap_back(h, core).wait_recv()

    pl.when(chip == 0)(functools.partial(run_chip, 0))
    pl.when(chip == 1)(functools.partial(run_chip, 1))


def attn_call(cu, valid, q, k, v, do):
    any_spec = pl.BlockSpec(memory_space=pl.ANY)
    dma = pltpu.SemaphoreType.DMA
    return pl.pallas_call(
        attn_kernel,
        out_shape=(
            pltpu.VMEM((2, SLOT, 32, HEAD), BF16),
            pltpu.VMEM((2, SLOT, 32, HEAD), BF16),
            pltpu.VMEM((8, 2, 2, SLOT, HEAD), BF16),
            pltpu.VMEM((2, 32, SLOT), F32),
            pltpu.SMEM((3,), jnp.int32),
        ),
        in_specs=[any_spec] * 6,
        out_specs=(pl.BlockSpec(memory_space=pltpu.VMEM),) * 4 + (pl.BlockSpec(memory_space=pltpu.SMEM),),
        scratch_shapes=[
            pltpu.VMEM((256, 16, HEAD), BF16),
            pltpu.VMEM((256, 16, HEAD), BF16),
            pltpu.VMEM((256, 16, HEAD), BF16),
            pltpu.VMEM((256, 16, HEAD), BF16),
            pltpu.VMEM((256, 8, HEAD), BF16),
            pltpu.VMEM((256, 8, HEAD), BF16),
            pltpu.VMEM((8, 2, 2, SLOT, HEAD), BF16),
            pltpu.VMEM((HC, 4, 2, 2, SLOT, HEAD), BF16),
            pltpu.VMEM((HEAD, 8 * SLOT), BF16),
            pltpu.VMEM((HEAD, 8 * SLOT), BF16),
            pltpu.VMEM((HC, 4, GROUP, SLOT, HEAD), BF16),
            pltpu.VMEM((HC, 4, GROUP, SLOT, HEAD), BF16),
            pltpu.VMEM((8 * SLOT, TILE), F32),
            pltpu.VMEM((8 * SLOT, TILE), F32),
            pltpu.VMEM((8 * SLOT, TILE), BF16),
            pltpu.VMEM((8 * SLOT, TILE), BF16),
            pltpu.VMEM((HC, 16, SLOT, HEAD), F32),
            pltpu.VMEM((HC, 8, SLOT, HEAD), F32),
            pltpu.VMEM((HC, 2, SLOT, HEAD), F32),
            pltpu.VMEM((2, 4, TILE, HEAD), BF16),
            pltpu.VMEM((2, 4, TILE, HEAD), BF16),
            pltpu.VMEM((2, 4, SLOT, 8, HEAD), BF16),
            pltpu.VMEM((2, 4, SLOT, 8, HEAD), BF16),
            pltpu.VMEM((HC, 4, 2, SLOT, HEAD), BF16),
            pltpu.VMEM((HC, 2, SLOT, HEAD), BF16),
            pltpu.VMEM((2, 2, 16, SLOT), F32),
            pltpu.VMEM((12, SLOT, SLOT), F32),
            pltpu.VMEM((4, 1, 2 * SLOT), jnp.int32),
            dma((6,)),
            dma((2,)), dma((2,)),
            dma((3,)), dma((4,)),
            dma((2, 2)), dma((2, 2)),
            dma((3, HC)), dma((HC, 4)),
            dma((HC, 2)), dma((HC, 2)),
            dma((HC,)), dma((HC,)), dma((HC,)), dma((8,)),
            dma((2, 2, 4)), dma((2, 2, 2)),
            dma((HC, 4)), dma((HC, 2)),
            dma, dma,
        ],
        compiler_params=pltpu.CompilerParams(collective_id=0, has_side_effects=True, vmem_limit_bytes=61300000),
        name="attn",
    )(cu, valid, q, k, v, do)


def finish_kernel(o_in, dq_in, dkv_in, lse_in, cu, o_out, dq_out, dk_out, dv_out, lse_out, dk_t, dv_t, lse_t, sem, lse_sem):
    l0 = lax.shift_right_logical(cu[1], 3)
    rest = SLOT - l0

    def copies(i, x, out):
        runs = ((0, 0, 0, l0), (1, 0, l0, l0), (0, l0, 2 * l0, rest), (1, l0, SLOT + l0, rest))
        return [pltpu.make_async_copy(x.at[up, pl.ds(at, n)], out.at[pl.ds(to, n)], sem.at[i, j])
                for j, (up, at, to, n) in enumerate(runs)]

    moves = copies(0, o_in, o_out) + copies(1, dq_in, dq_out)
    for cp in moves:
        cp.start()

    for w, dst in ((0, dk_t), (1, dv_t)):
        for up in range(2):
            def body(i, _):
                at = pl.ds(pl.multiple_of(i * 16, 16), 16)
                dst[up, at] = jnp.transpose(dkv_in[:, up, w, at, :], (1, 0, 2))
                return 0
            lax.fori_loop(0, SLOT // 16, body, 0)
        more = copies(2 + w, dst, (dk_out, dv_out)[w])
        for cp in more:
            cp.start()
        moves += more

    row = lax.broadcasted_iota(jnp.int32, (2 * SLOT, SLOT), 0)
    col = lax.broadcasted_iota(jnp.int32, (2 * SLOT, SLOT), 1)
    acc = None
    for up in range(2):
        if up:
            src = jnp.where(col < l0, col + l0, col + SLOT)
        else:
            src = jnp.where(col < l0, col, col + l0)
        pick = jnp.where(row == src, 1.0, 0.0)
        part = lax.dot_general(lse_in[up], pick, NT, precision=lax.Precision.HIGHEST, preferred_element_type=F32)
        acc = part if acc is None else acc + part
    lse_t[...] = acc
    lse_move = pltpu.make_async_copy(lse_t, lse_out, lse_sem)
    lse_move.start()
    for cp in moves + [lse_move]:
        cp.wait()


def finish_call(o_t, dq_t, dkv_hm, lse_hm, cu):
    any_spec = pl.BlockSpec(memory_space=pl.ANY)
    vmem = pl.BlockSpec(memory_space=pltpu.VMEM)
    return pl.pallas_call(
        finish_kernel,
        out_shape=(
            jax.ShapeDtypeStruct((256, 32, HEAD), BF16),
            jax.ShapeDtypeStruct((256, 32, HEAD), BF16),
            jax.ShapeDtypeStruct((256, 8, HEAD), BF16),
            jax.ShapeDtypeStruct((256, 8, HEAD), BF16),
            jax.ShapeDtypeStruct((32, 256), F32),
        ),
        in_specs=[vmem] * 4 + [pl.BlockSpec(memory_space=pltpu.SMEM)],
        out_specs=(any_spec,) * 5,
        scratch_shapes=[
            pltpu.VMEM((2, SLOT, 8, HEAD), BF16),
            pltpu.VMEM((2, SLOT, 8, HEAD), BF16),
            pltpu.VMEM((32, 256), F32),
            pltpu.SemaphoreType.DMA((4, 4)),
            pltpu.SemaphoreType.DMA,
        ],
        compiler_params=pltpu.CompilerParams(vmem_limit_bytes=16 * 1024 * 1024),
        name="finish",
    )(o_t, dq_t, dkv_hm, lse_hm, cu)


def solution(mesh):
    tok_spec = P(("dp", "cp"), None, None)
    lse_spec = P(("dp", "cp"), None)

    def local(q, k, v, do, valid, cu):
        res = attn_call(cu, valid.reshape(1, 256), q, k, v, do)
        o, dq, dk, dv, lse = finish_call(*res)
        return o, lse.T, dq, dk, dv

    return jax.shard_map(local, mesh=mesh, in_specs=(tok_spec,) * 4 + (P(("dp", "cp")), P("dp")),
                         out_specs=(tok_spec, lse_spec, tok_spec, tok_spec, tok_spec), check_vma=False)
```

```python
import functools
import math

import jax
import jax.numpy as jnp
from jax import lax
from jax.experimental import pallas as pl
from jax.experimental.pallas import tpu as pltpu
from jax.sharding import PartitionSpec as P

MESH = pl.DeviceIdType.MESH
FILL = -1.0e30
BIG = 3.0e38
HEAD = 128
SLOT = 128
TILE = 512
GROUP = 4
HC = 4
SW = (2, 2, 2, 0)
SCALE = HEAD ** -0.5
C2 = SCALE * math.log2(math.e)
NT = (((1,), (1,)), ((), ()))
NN = (((1,), (0,)), ((), ()))
F32 = jnp.float32
BF16 = jnp.bfloat16

TILES = ((0, 0), (1, 0), (1, 1), (0, 1))


def slot_of(chip, ti):
    oc, up = TILES[ti]
    r = 2 * chip + oc
    return 7 - r if up else r


def mm(a, b, dims):
    return lax.dot_general(a, b, dims, preferred_element_type=F32)


def src_row(up, t, l0):
    if up:
        return jnp.where(t < l0, t + l0, t + SLOT)
    return jnp.where(t < l0, t, t + l0)


def attn_kernel(cu_hbm, valid, q, k, v, do, o_out, dq_out, dkv_out, lse_out, cu,
                raw_q, raw_do, far_q, far_do, raw_k, raw_v, kv_hm, kv_all, kt, vt, qh, doh, st0, st1, pb, db,
                dkv_acc, cross_in, near_in, swap_in, o_st, dq_st, o_far, dq_far, dkv_st, back_st, lse_st, caps, valid_all,
                in_sem, raw_ssem, raw_rsem, val_ssem, val_rsem, first_ssem, first_rsem, kv_ssem, kv_rsem,
                part_ssem, part_rsem, near_ssem, near_rsem, swap_ssem, swap_rsem, back_ssem, back_rsem, res_ssem, res_rsem, dkv_ssem, dkv_rsem, lse_sem, lse_rsem):
    r = lax.axis_index("cp")
    chip = r // 2
    c = r % 2
    pc = 1 - c
    partner = chip * 2 + pc
    cross = (1 - chip) * 2 + c
    cross_o = (1 - chip) * 2 + pc

    def remote(src, dst, ssem, rsem, dev):
        return pltpu.make_async_remote_copy(src_ref=src, dst_ref=dst, send_sem=ssem, recv_sem=rsem,
                                            device_id={"cp": dev}, device_id_type=MESH)

    own_heads = pl.ds(pl.multiple_of(16 * c, 16), 16)
    oth_heads = pl.ds(pl.multiple_of(16 * pc, 16), 16)
    ld_k = pltpu.make_async_copy(k, raw_k, in_sem.at[0])
    ld_v = pltpu.make_async_copy(v, raw_v, in_sem.at[1])
    ld_q = pltpu.make_async_copy(q.at[:, own_heads, :], raw_q, in_sem.at[2])
    ld_do = pltpu.make_async_copy(do.at[:, own_heads, :], raw_do, in_sem.at[3])
    ld_val = pltpu.make_async_copy(valid, valid_all.at[r], in_sem.at[4])
    ld_cu = pltpu.make_async_copy(cu_hbm, cu, in_sem.at[5])
    for cp in (ld_cu, ld_k, ld_v, ld_val):
        cp.start()

    barrier = pltpu.get_barrier_semaphore()
    for dev in (partner, cross, cross_o):
        pl.semaphore_signal(barrier, inc=1, device_id={"cp": dev}, device_id_type=MESH)
    ld_cu.wait()
    l0 = lax.shift_right_logical(cu[1], 3)

    peers = (partner, cross, cross_o)
    push_q = remote(q.at[:, oth_heads, :], far_q, raw_ssem.at[0], raw_rsem.at[0], partner)
    push_do = remote(do.at[:, oth_heads, :], far_do, raw_ssem.at[1], raw_rsem.at[1], partner)
    push_val = [remote(valid, valid_all.at[r], val_ssem.at[i], val_rsem.at[r], dev) for i, dev in enumerate(peers)]


    def kv_relayout(up):
        def body(i, _):
            t0 = i * 16
            for which, raw in ((0, raw_k), (1, raw_v)):
                rows = jnp.stack([raw[src_row(up, t0 + j, l0)] for j in range(16)])
                kv_hm[:, up, which, pl.ds(pl.multiple_of(t0, 16), 16), :] = jnp.transpose(rows, (1, 0, 2))
            return 0
        lax.fori_loop(0, SLOT // 16, body, 0)

    def kv_push(h, to, both):
        head = (4 * c if to == 1 else 4 * pc) + h
        dev = (partner, cross, cross_o)[to]
        ups = pl.ds(0, 2 if both else 1)
        return remote(kv_hm.at[head, ups], kv_all.at[h, r, ups], kv_ssem.at[to, h], kv_rsem.at[h, r], dev)

    def kv_first(to, up):
        head = 4 * c if to == 1 else 4 * pc
        at = pl.ds(up, 1)
        return remote(kv_hm.at[head, at], kv_all.at[0, r, at], first_ssem.at[to - 1, up], first_rsem.at[c, up],
                      (cross, cross_o)[to - 1])

    def kv_wait(h, owner, both):
        ups = pl.ds(0, 2 if both else 1)
        remote(kv_hm.at[0, ups], kv_all.at[h, owner, ups], kv_ssem.at[0, h], kv_rsem.at[h, owner], partner).wait_recv()

    def first_wait(owner):
        for up in range(2):
            at = pl.ds(up, 1)
            remote(kv_hm.at[0, at], kv_all.at[0, owner, at], first_ssem.at[0, up], first_rsem.at[owner - 2, up], partner).wait_recv()

    ld_k.wait()
    ld_v.wait()
    kv_relayout(0)
    pl.semaphore_wait(barrier, 3)

    def cross_send(ch, h):
        @pl.when(chip == ch)
        def _():
            for to in (1, 2):
                kv_push(h, to, ch == 1).start()

    cross_send(0, 0)

    def send_first(up):
        @pl.when(chip == 1)
        def _():
            for to in (1, 2):
                kv_first(to, up).start()

    send_first(0)
    for cp in (ld_q, ld_do, push_q, push_do):
        cp.start()
    kv_relayout(1)
    send_first(1)
    for h in range(HC):
        kv_push(h, 0, True).start()
    ld_val.wait()
    for cp in push_val:
        cp.start()

    def copy_own(h, _):
        for up in range(2):
            kv_all[h, r, up] = kv_hm[4 * c + h, up]
        return 0
    lax.fori_loop(0, HC, copy_own, 0)

    def q_relayout(oc, from_q, from_do):
        for up, ti in ((0, oc), (1, 3 - oc)):
            def body(i, _):
                t0 = i * 16
                at = pl.ds(pl.multiple_of(t0, 16), 16)
                for raw, dst in ((from_q, qh), (from_do, doh)):
                    rows = jnp.stack([raw[src_row(up, t0 + j, l0)] for j in range(16)])
                    dst[:, ti, :, at, :] = jnp.transpose(rows, (1, 0, 2)).reshape(HC, GROUP, 16, HEAD)
                return 0
            lax.fori_loop(0, SLOT // 16, body, 0)

    ld_q.wait()
    ld_do.wait()
    cross_send(0, 1)
    q_relayout(c, raw_q, raw_do)

    cross_send(0, 2)
    for i in range(3):
        remote(valid, valid_all.at[peers[i]], val_ssem.at[i], val_rsem.at[peers[i]], peers[i]).wait_recv()
    lane = lax.broadcasted_iota(jnp.int32, (SLOT, SLOT), 1)
    sub = lax.broadcasted_iota(jnp.int32, (SLOT, SLOT), 0)
    lane2 = lax.broadcasted_iota(jnp.int32, (SLOT, 2 * SLOT), 1)
    sub2 = lax.broadcasted_iota(jnp.int32, (SLOT, 2 * SLOT), 0)
    same_doc = (lane < l0) == (sub < l0)
    doc_f = jnp.where(lane < l0, 1.0, 0.0)
    doc_s = jnp.where(sub < l0, 1.0, 0.0)
    same_f = jnp.where(doc_f == doc_s, 1.0, 0.0)
    del same_doc

    def cap_body(s, _):
        owner = jnp.where(s < 4, s, 7 - s)
        off = jnp.where(s < 4, 0, 1)
        src_lo = jnp.where(sub2 < l0, sub2, sub2 + l0)
        src_hi = jnp.where(sub2 < l0, sub2 + l0, sub2 + SLOT)
        src = jnp.where(off == 1, src_hi, src_lo)
        row = jnp.broadcast_to(valid_all[owner].astype(F32), (SLOT, 2 * SLOT))
        ok = jnp.sum(jnp.where(src == lane2, row, 0.0), axis=1, keepdims=True)
        caps[s] = jnp.where(same_f * ok > 0.5, BIG, FILL)
        return 0
    lax.fori_loop(0, 8, cap_body, 0)
    for ti in range(4):
        oc, up = TILES[ti]
        s = (7 - (2 * chip + oc)) if up else 2 * chip + oc
        caps[8 + ti] = jnp.where(sub <= lane, caps[s], FILL)

    cross_send(0, 3)
    cross_send(1, 1)
    push_q.wait_recv()
    push_do.wait_recv()
    q_relayout(pc, far_q, far_do)

    def part_copy(h, u, n=2):
        up = int(u > 3)
        return remote(dkv_acc.at[h, pl.ds(2 * u, n)], cross_in.at[4 * c + h, up, pl.ds(0, n)], part_ssem,
                      part_rsem.at[4 * c + h, up], min(u, 7 - u))

    def part_wait(j, up, n=2):
        remote(dkv_acc.at[0, pl.ds(0, n)], cross_in.at[j, up, pl.ds(0, n)], part_ssem,
               part_rsem.at[j, up], partner).wait_recv()

    def near_copy(h, up, slot, n=2):
        return remote(dkv_acc.at[h, pl.ds(2 * slot, n)], near_in.at[h, up, pl.ds(0, n)], near_ssem.at[h, up],
                      near_rsem.at[h, up], partner)

    def near_run(ch, h, act):
        act(near_copy(h, 0, 2 * ch + pc))
        if ch == 1:
            pl.when(c == 0)(lambda: act(near_copy(h, 1, 4)))
            if SW[h] < 2:
                pl.when(c == 1)(lambda: act(near_copy(h, 1, 5, 2 - SW[h])))

    def near_wait(h, up, n=2):
        near_copy(h, up, 0, n).wait_recv()

    def swap_copy(h):
        n = SW[h]
        return remote(dkv_acc.at[h, pl.ds(12 - n, n)], swap_in.at[h, pl.ds(2 - n, n)], swap_ssem.at[h], swap_rsem.at[h], cross)

    def swap_back(h, core):
        at = pl.ds(2 - SW[h], SW[h])
        j = 4 * core + h
        return remote(back_st.at[h, at], dkv_out.at[j, 1, at], back_ssem.at[h], back_rsem.at[j], 2)

    def res_copy(p, ti, which):
        stage, out = ((o_far, o_out), (dq_far, dq_out))[which]
        dst = out.at[TILES[ti][1], :, pl.ds(pl.multiple_of(16 * c + 8 * p, 8), 8), :]
        return remote(stage.at[p, ti], dst, res_ssem.at[which, p, ti], res_rsem.at[which, p, TILES[ti][1]], partner)

    def dkv_copy(h, ti):
        up = TILES[ti][1]
        return remote(dkv_st.at[h, ti], dkv_out.at[4 * c + h, up], dkv_ssem.at[h, ti], dkv_rsem.at[h, up], partner)

    def res_put(p):
        heads = pl.ds(pl.multiple_of(16 * c + 8 * p, 8), 8)
        for ti, (oc, up) in enumerate(TILES):
            def body(i, _, keep):
                at = pl.ds(pl.multiple_of(i * 16, 16), 16)
                for stage, far, out in ((o_st, o_far, o_out), (dq_st, dq_far, dq_out)):
                    x = jnp.concatenate([stage[e, ti, pl.ds(pl.multiple_of(g * SLOT + i * 16, 16), 16), :][None]
                                         for e in range(2) for g in range(GROUP)], axis=0)
                    y = jnp.transpose(x, (1, 0, 2))
                    if keep:
                        out[up, at, heads, :] = y
                    else:
                        far[p, ti, at, :, :] = y
                return 0

            @pl.when(c == oc)
            def _():
                lax.fori_loop(0, SLOT // 16, functools.partial(body, keep=True), 0)

            @pl.when(c != oc)
            def _():
                lax.fori_loop(0, SLOT // 16, functools.partial(body, keep=False), 0)
                for which in range(2):
                    res_copy(p, ti, which).start()

    def dkv_put(h, ti, parts):
        oc, up = TILES[ti]

        @pl.when(c == oc)
        def _():
            for w in range(2):
                dkv_out[4 * c + h, up, w] = parts(w).astype(BF16)

        @pl.when(c != oc)
        def _():
            for w in range(2):
                dkv_st[h, ti, w] = parts(w).astype(BF16)
            dkv_copy(h, ti).start()

    lse_far = remote(lse_st.at[pc], lse_out.at[:, own_heads, :], lse_sem, lse_rsem, partner)

    def kv_slot(h, s, which):
        return kv_all[h, min(s, 7 - s), int(s > 3), which]

    def kv_slots(h, a, b, which):
        return jnp.concatenate([kv_slot(h, s, which) for s in range(a, b)], axis=0)

    def run_chip(ch):
        slots = [slot_of(ch, ti) for ti in range(4)]
        sent = [0, 1] if ch == 1 else [2, 3, 4, 5]

        def transposes(s):
            for src, dst in ((0, kt), (1, vt)):
                dst[:, s * SLOT:(s + 1) * SLOT] = jnp.transpose(kv_slot(h_ref[0], s, src))

        h_ref = [None]
        sts = (st0, st1)

        def point(h, where):
            if ch == 0:
                return
            kv = {(0, 3): 2, (1, 2): 3}
            swaps = {(1, 4): (0, 1), (2, 4): (2,)}
            parts = {(2, 2): (0,), (2, 4): (1,), (3, 4): (2, 3)}
            for at in range(HC):
                if not any((at, where) in d for d in (kv, swaps, parts)):
                    continue

                @pl.when(h == at)
                def _():
                    if (at, where) in kv:
                        for to in (1, 2):
                            kv_push(kv[at, where], to, True).start()
                    for e in swaps.get((at, where), ()):
                        swap_copy(e).start()
                    for e in parts.get((at, where), ()):
                        for u in (0, 1):
                            part_copy(e, u).start()

        def head(h, _):
            h_ref[0] = h
            seen = set()
            ready = set()

            def wait_slot(s):
                if s in ready:
                    return
                if s in slots:
                    kv_wait(h, partner, True)
                    new = slots
                elif ch == 1:
                    for owner in (0, 1):
                        kv_wait(h, owner, False)
                    new = [0, 1]
                else:
                    for owner in (2, 3):
                        pl.when(h == 0)(functools.partial(first_wait, owner))
                        pl.when(h > 0)(functools.partial(kv_wait, h, owner, True))
                    new = [2, 3, 4, 5]
                for u in new:
                    ready.add(u)
                    transposes(u)

            state = {}

            def forward(ti):
                point(h, ti)
                s = slots[ti]
                nk = s + 1
                for u in range(nk):
                    wait_slot(u)
                st = sts[ti % 2]
                qt = qh[h, ti].reshape(TILE, HEAD)
                dt = doh[h, ti].reshape(TILE, HEAD)
                m8 = [None] * GROUP
                for a in range(0, nk, 2):
                    n = min(2, nk - a)
                    kb = kv_slots(h, a, a + n, 0)
                    sc = mm(kb, qt, NT)
                    for j in range(n):
                        cap = caps[8 + ti] if a + j == s else caps[a + j]
                        for g in range(GROUP):
                            x = jnp.minimum(sc[j * SLOT:(j + 1) * SLOT, g * SLOT:(g + 1) * SLOT], cap)
                            st[(a + j) * SLOT:(a + j + 1) * SLOT, g * SLOT:(g + 1) * SLOT] = x
                            top = jnp.max(x.reshape(SLOT // 8, 8, SLOT), axis=0)
                            m8[g] = top if m8[g] is None else jnp.maximum(m8[g], top)
                m = [jnp.max(x, axis=0, keepdims=True) for x in m8]
                mc = [x * C2 for x in m]
                l8 = [None] * GROUP
                for a in range(nk):
                    for g in range(GROUP):
                        at = (slice(a * SLOT, (a + 1) * SLOT), slice(g * SLOT, (g + 1) * SLOT))
                        e = jnp.exp2(st[at] * C2 - mc[g])
                        st[at] = e
                        pb[at] = e.astype(BF16)
                        tot = jnp.sum(e.reshape(SLOT // 8, 8, SLOT), axis=0)
                        l8[g] = tot if l8[g] is None else l8[g] + tot
                ot = mm(vt[:, :nk * SLOT], pb[:nk * SLOT, :], NN)
                inv, dd = [], []
                oc, up = TILES[ti]
                for g in range(GROUP):
                    l = jnp.sum(l8[g], axis=0, keepdims=True)
                    has = m[g] > 0.5 * FILL
                    safe = jnp.where(has, l, 1.0)
                    i_l = jnp.where(has, 1.0 / safe, 0.0)
                    lse = jnp.where(has, m[g] * SCALE + jnp.log(safe), 0.0)
                    lse_st[oc, up, pl.ds(h * GROUP + g, 1), :] = lse
                    og = (ot[:, g * SLOT:(g + 1) * SLOT] * i_l).astype(BF16)
                    dog = jnp.transpose(dt[g * SLOT:(g + 1) * SLOT, :])
                    dd.append(jnp.sum(og.astype(F32) * dog.astype(F32), axis=0, keepdims=True))
                    inv.append(i_l)
                    o_st[h % 2, ti, g * SLOT:(g + 1) * SLOT, :] = jnp.transpose(og)

                state[ti] = [inv, dd, None]

            def backward(ti, part):
                inv, dd, dqt = state[ti]
                qt = qh[h, ti].reshape(TILE, HEAD)
                dt = doh[h, ti].reshape(TILE, HEAD)
                st = sts[ti % 2]
                runs = []
                for u in part:
                    if runs and runs[-1][1] == u and u - runs[-1][0] < 2:
                        runs[-1][1] = u + 1
                    else:
                        runs.append([u, u + 1])
                for a, b in runs:
                    n = b - a
                    vb = kv_slots(h, a, b, 1)
                    dp = mm(vb, dt, NT)
                    for j in range(n):
                        for g in range(GROUP):
                            at = (slice((a + j) * SLOT, (a + j + 1) * SLOT), slice(g * SLOT, (g + 1) * SLOT))
                            p = st[at] * inv[g]
                            pb[at] = p.astype(BF16)
                            ds = p * (dp[j * SLOT:(j + 1) * SLOT, g * SLOT:(g + 1) * SLOT] - dd[g])
                            db[at] = ds.astype(BF16)
                    dsb = db[a * SLOT:b * SLOT, :]
                    dv = mm(pb[a * SLOT:b * SLOT, :], dt, NN)
                    dk = mm(dsb, qt, NN) * SCALE
                    dq = mm(kt[:, a * SLOT:b * SLOT], dsb, NN)
                    dqt = dq if dqt is None else dqt + dq
                    for j in range(n):
                        u = a + j
                        new = (dk[j * SLOT:(j + 1) * SLOT], dv[j * SLOT:(j + 1) * SLOT])
                        for w in range(2):
                            dkv_acc[h, 2 * u + w] = dkv_acc[h, 2 * u + w] + new[w] if u in seen else new[w]
                        seen.add(u)
                state[ti][2] = dqt

            def finish(ti):
                dqt = state[ti][2]
                for g in range(GROUP):
                    dqg = (dqt[:, g * SLOT:(g + 1) * SLOT] * SCALE).astype(BF16)
                    dq_st[h % 2, ti, g * SLOT:(g + 1) * SLOT, :] = jnp.transpose(dqg)

            if ch == 0:
                for ti in (0, 1):
                    forward(ti)
                    backward(ti, range(slots[ti] + 1))
                    finish(ti)
                for ti in (2, 3):
                    forward(ti)
                for ti in (2, 3):
                    backward(ti, [2, 3])
                for u in (2, 3):
                    part_copy(h, u).start()
                for ti in (2, 3):
                    backward(ti, [4, 5])
                part_copy(h, 4).start()
                for at in range(HC):
                    if SW[at] < 2:
                        pl.when(h == at)(part_copy(at, 5, 2 - SW[at]).start)
                for ti in (2, 3):
                    backward(ti, [u for u in range(slots[ti] + 1) if u not in sent])
                    finish(ti)
            else:
                for ti in range(4):
                    forward(ti)
                    backward(ti, range(slots[ti] + 1))
                    finish(ti)
            if ch == 1:
                point(h, 4)
            else:
                for ti in (2, 3):
                    dkv_put(h, ti, lambda w, ti=ti: dkv_acc[h, 2 * slots[ti] + w])
            for at in range(HC):
                pl.when(h == at)(functools.partial(near_run, ch, at, lambda cp: cp.start()))
            pl.when(h % 2 == 1)(lambda: res_put(h // 2))
            return 0

        lax.fori_loop(0, HC, head, 0)

        lse_out[:, own_heads, :] = lse_st[c]
        lse_far.start()

        if ch == 0:
            for h in range(HC):
                if SW[h]:
                    swap_copy(h).wait_recv()
                    for w in range(2 - SW[h], 2):
                        back_st[h, w] = (swap_in[h, w] + dkv_acc[h, 10 + w]).astype(BF16)
                    swap_back(h, c).start()

        def early(h, _):
            kv_push(h, 0, True).wait_send()
            for to in (1, 2):
                if ch == 0:
                    kv_push(h, to, False).wait_send()
                else:
                    pl.when(h > 0)(kv_push(h, to, True).wait_send)
            if ch == 0:
                for ti in (2, 3):
                    pl.when(c != TILES[ti][0])(dkv_copy(h, ti).wait_send)
                remote(dkv_st.at[h, 0], dkv_out.at[4 * pc + h, 1], dkv_ssem.at[h, 0], dkv_rsem.at[h, 1], partner).wait_recv()
            return 0
        lax.fori_loop(0, HC, early, 0)
        if ch == 1:
            for to in (1, 2):
                for up in range(2):
                    kv_first(to, up).wait_send()
        for h in range(HC):
            near_run(ch, h, lambda cp: cp.wait_send())
        push_q.wait_send()
        push_do.wait_send()
        for cp in push_val:
            cp.wait_send()
        for p in range(2):
            for which in range(2):
                stage, out = ((o_far, o_out), (dq_far, dq_out))[which]
                for ti in range(4):
                    pl.when(c != TILES[ti][0])(res_copy(p, ti, which).wait_send)
                for up in range(2):
                    dst = out.at[up, :, pl.ds(pl.multiple_of(16 * pc + 8 * p, 8), 8), :]
                    remote(stage.at[p, 0], dst, res_ssem.at[which, p, 0], res_rsem.at[which, p, up], partner).wait_recv()
        lse_far.wait_send()
        remote(lse_st.at[0], lse_out.at[:, oth_heads, :], lse_sem, lse_rsem, partner).wait_recv()

        def add_up(h, up, slot, n):
            if n == 0:
                return
            part_wait(4 * c + h, up, n)
            for w in range(n):
                dkv_out[4 * c + h, up, w] = (dkv_acc[h, 2 * slot + w] + cross_in[4 * c + h, up, w]).astype(BF16)
            near_wait(h, up, n)
            part_wait(4 * pc + h, up, n)
            for w in range(n):
                dkv_out[4 * pc + h, up, w] = (near_in[h, up, w] + cross_in[4 * pc + h, up, w]).astype(BF16)

        for h in range(HC):
            add_up(h, 0, 2 * ch + c, 2)
            if ch == 1:
                pl.when(c == 1)(functools.partial(add_up, h, 1, 4, 2))
                pl.when(c == 0)(functools.partial(add_up, h, 1, 5, 2 - SW[h]))

        units = HC * 4 if ch == 1 else HC * 8 - sum(SW)
        rows = next(a for a in (1, 2, 3, 4) if units % a == 0 and units // a <= 16)
        block = dkv_acc.at[pl.ds(0, rows), pl.ds(0, units // rows)]
        remote(block, block, part_ssem, part_rsem.at[0, 0], partner).wait_send()
        for h in range(HC):
            if SW[h]:
                if ch == 0:
                    swap_back(h, c).wait_send()
                else:
                    swap_copy(h).wait_send()

        if ch == 1:
            @pl.when(c == 0)
            def _():
                for h in range(HC):
                    if SW[h]:
                        for core in range(2):
                            swap_back(h, core).wait_recv()

    pl.when(chip == 0)(functools.partial(run_chip, 0))
    pl.when(chip == 1)(functools.partial(run_chip, 1))


def attn_call(cu, valid, q, k, v, do):
    any_spec = pl.BlockSpec(memory_space=pl.ANY)
    dma = pltpu.SemaphoreType.DMA
    return pl.pallas_call(
        attn_kernel,
        out_shape=(
            pltpu.VMEM((2, SLOT, 32, HEAD), BF16),
            pltpu.VMEM((2, SLOT, 32, HEAD), BF16),
            pltpu.VMEM((8, 2, 2, SLOT, HEAD), BF16),
            pltpu.VMEM((2, 32, SLOT), F32),
            pltpu.SMEM((3,), jnp.int32),
        ),
        in_specs=[any_spec] * 6,
        out_specs=(pl.BlockSpec(memory_space=pltpu.VMEM),) * 4 + (pl.BlockSpec(memory_space=pltpu.SMEM),),
        scratch_shapes=[
            pltpu.VMEM((256, 16, HEAD), BF16),
            pltpu.VMEM((256, 16, HEAD), BF16),
            pltpu.VMEM((256, 16, HEAD), BF16),
            pltpu.VMEM((256, 16, HEAD), BF16),
            pltpu.VMEM((256, 8, HEAD), BF16),
            pltpu.VMEM((256, 8, HEAD), BF16),
            pltpu.VMEM((8, 2, 2, SLOT, HEAD), BF16),
            pltpu.VMEM((HC, 4, 2, 2, SLOT, HEAD), BF16),
            pltpu.VMEM((HEAD, 8 * SLOT), BF16),
            pltpu.VMEM((HEAD, 8 * SLOT), BF16),
            pltpu.VMEM((HC, 4, GROUP, SLOT, HEAD), BF16),
            pltpu.VMEM((HC, 4, GROUP, SLOT, HEAD), BF16),
            pltpu.VMEM((8 * SLOT, TILE), F32),
            pltpu.VMEM((8 * SLOT, TILE), F32),
            pltpu.VMEM((8 * SLOT, TILE), BF16),
            pltpu.VMEM((8 * SLOT, TILE), BF16),
            pltpu.VMEM((HC, 16, SLOT, HEAD), F32),
            pltpu.VMEM((8, 2, 2, SLOT, HEAD), F32),
            pltpu.VMEM((HC, 2, 2, SLOT, HEAD), F32),
            pltpu.VMEM((HC, 2, SLOT, HEAD), F32),
            pltpu.VMEM((2, 4, TILE, HEAD), BF16),
            pltpu.VMEM((2, 4, TILE, HEAD), BF16),
            pltpu.VMEM((2, 4, SLOT, 8, HEAD), BF16),
            pltpu.VMEM((2, 4, SLOT, 8, HEAD), BF16),
            pltpu.VMEM((HC, 4, 2, SLOT, HEAD), BF16),
            pltpu.VMEM((HC, 2, SLOT, HEAD), BF16),
            pltpu.VMEM((2, 2, 16, SLOT), F32),
            pltpu.VMEM((12, SLOT, SLOT), F32),
            pltpu.VMEM((4, 1, 2 * SLOT), jnp.int32),
            dma((6,)),
            dma((2,)), dma((2,)),
            dma((3,)), dma((4,)),
            dma((2, 2)), dma((2, 2)),
            dma((3, HC)), dma((HC, 4)),
            dma, dma((8, 2)), dma((HC, 2)), dma((HC, 2)),
            dma((HC,)), dma((HC,)), dma((HC,)), dma((8,)),
            dma((2, 2, 4)), dma((2, 2, 2)),
            dma((HC, 4)), dma((HC, 2)),
            dma, dma,
        ],
        compiler_params=pltpu.CompilerParams(collective_id=0, has_side_effects=True, vmem_limit_bytes=61300000),
        name="attn",
    )(cu, valid, q, k, v, do)


def finish_kernel(o_in, dq_in, dkv_in, lse_in, cu, o_out, dq_out, dk_out, dv_out, lse_out, dk_t, dv_t, lse_t, sem, lse_sem):
    l0 = lax.shift_right_logical(cu[1], 3)
    rest = SLOT - l0

    def copies(i, x, out):
        runs = ((0, 0, 0, l0), (1, 0, l0, l0), (0, l0, 2 * l0, rest), (1, l0, SLOT + l0, rest))
        return [pltpu.make_async_copy(x.at[up, pl.ds(at, n)], out.at[pl.ds(to, n)], sem.at[i, j])
                for j, (up, at, to, n) in enumerate(runs)]

    moves = copies(0, o_in, o_out) + copies(1, dq_in, dq_out)
    for cp in moves:
        cp.start()

    for w, dst in ((0, dk_t), (1, dv_t)):
        for up in range(2):
            def body(i, _):
                at = pl.ds(pl.multiple_of(i * 16, 16), 16)
                dst[up, at] = jnp.transpose(dkv_in[:, up, w, at, :], (1, 0, 2))
                return 0
            lax.fori_loop(0, SLOT // 16, body, 0)
        more = copies(2 + w, dst, (dk_out, dv_out)[w])
        for cp in more:
            cp.start()
        moves += more

    row = lax.broadcasted_iota(jnp.int32, (2 * SLOT, SLOT), 0)
    col = lax.broadcasted_iota(jnp.int32, (2 * SLOT, SLOT), 1)
    acc = None
    for up in range(2):
        if up:
            src = jnp.where(col < l0, col + l0, col + SLOT)
        else:
            src = jnp.where(col < l0, col, col + l0)
        pick = jnp.where(row == src, 1.0, 0.0)
        part = lax.dot_general(lse_in[up], pick, NT, precision=lax.Precision.HIGHEST, preferred_element_type=F32)
        acc = part if acc is None else acc + part
    lse_t[...] = acc
    lse_move = pltpu.make_async_copy(lse_t, lse_out, lse_sem)
    lse_move.start()
    for cp in moves + [lse_move]:
        cp.wait()


def finish_call(o_t, dq_t, dkv_hm, lse_hm, cu):
    any_spec = pl.BlockSpec(memory_space=pl.ANY)
    vmem = pl.BlockSpec(memory_space=pltpu.VMEM)
    return pl.pallas_call(
        finish_kernel,
        out_shape=(
            jax.ShapeDtypeStruct((256, 32, HEAD), BF16),
            jax.ShapeDtypeStruct((256, 32, HEAD), BF16),
            jax.ShapeDtypeStruct((256, 8, HEAD), BF16),
            jax.ShapeDtypeStruct((256, 8, HEAD), BF16),
            jax.ShapeDtypeStruct((32, 256), F32),
        ),
        in_specs=[vmem] * 4 + [pl.BlockSpec(memory_space=pltpu.SMEM)],
        out_specs=(any_spec,) * 5,
        scratch_shapes=[
            pltpu.VMEM((2, SLOT, 8, HEAD), BF16),
            pltpu.VMEM((2, SLOT, 8, HEAD), BF16),
            pltpu.VMEM((32, 256), F32),
            pltpu.SemaphoreType.DMA((4, 4)),
            pltpu.SemaphoreType.DMA,
        ],
        compiler_params=pltpu.CompilerParams(vmem_limit_bytes=16 * 1024 * 1024),
        name="finish",
    )(o_t, dq_t, dkv_hm, lse_hm, cu)


def solution(mesh):
    tok_spec = P(("dp", "cp"), None, None)
    lse_spec = P(("dp", "cp"), None)

    def local(q, k, v, do, valid, cu):
        res = attn_call(cu, valid.reshape(1, 256), q, k, v, do)
        o, dq, dk, dv, lse = finish_call(*res)
        return o, lse.T, dq, dk, dv

    return jax.shard_map(local, mesh=mesh, in_specs=(tok_spec,) * 4 + (P(("dp", "cp")), P("dp")),
                         out_specs=(tok_spec, lse_spec, tok_spec, tok_spec, tok_spec), check_vma=False)
```

```python
import functools
import math

import jax
import jax.numpy as jnp
from jax import lax
from jax.experimental import pallas as pl
from jax.experimental.pallas import tpu as pltpu
from jax.sharding import PartitionSpec as P

MESH = pl.DeviceIdType.MESH
FILL = -1.0e30
BIG = 3.0e38
HEAD = 128
SLOT = 128
TILE = 512
GROUP = 4
HC = 4
SW = (2, 2, 2, 0)
SCALE = HEAD ** -0.5
C2 = SCALE * math.log2(math.e)
NT = (((1,), (1,)), ((), ()))
NN = (((1,), (0,)), ((), ()))
F32 = jnp.float32
BF16 = jnp.bfloat16

TILES = ((0, 0), (1, 0), (1, 1), (0, 1))


def slot_of(chip, ti):
    oc, up = TILES[ti]
    r = 2 * chip + oc
    return 7 - r if up else r


def mm(a, b, dims):
    return lax.dot_general(a, b, dims, preferred_element_type=F32)


def src_row(up, t, l0):
    if up:
        return jnp.where(t < l0, t + l0, t + SLOT)
    return jnp.where(t < l0, t, t + l0)


def attn_kernel(cu_hbm, valid, q, k, v, do, o_out, dq_out, dkv_out, lse_out, cu,
                raw_q, raw_do, far_q, far_do, raw_k, raw_v, kv_hm, kv_all, kt, vt, qh, doh, st0, st1, pb, db,
                dkv_acc, cross_in, near_in, swap_in, o_st, dq_st, o_far, dq_far, dkv_st, back_st, lse_st, caps, valid_all,
                in_sem, raw_ssem, raw_rsem, val_ssem, val_rsem, first_ssem, first_rsem, kv_ssem, kv_rsem,
                part_ssem, part_rsem, near_ssem, near_rsem, swap_ssem, swap_rsem, back_ssem, back_rsem, res_ssem, res_rsem, dkv_ssem, dkv_rsem, lse_sem, lse_rsem):
    r = lax.axis_index("cp")
    chip = r // 2
    c = r % 2
    pc = 1 - c
    partner = chip * 2 + pc
    cross = (1 - chip) * 2 + c
    cross_o = (1 - chip) * 2 + pc

    def remote(src, dst, ssem, rsem, dev):
        return pltpu.make_async_remote_copy(src_ref=src, dst_ref=dst, send_sem=ssem, recv_sem=rsem,
                                            device_id={"cp": dev}, device_id_type=MESH)

    own_heads = pl.ds(pl.multiple_of(16 * c, 16), 16)
    oth_heads = pl.ds(pl.multiple_of(16 * pc, 16), 16)
    ld_k = pltpu.make_async_copy(k, raw_k, in_sem.at[0])
    ld_v = pltpu.make_async_copy(v, raw_v, in_sem.at[1])
    ld_q = pltpu.make_async_copy(q.at[:, own_heads, :], raw_q, in_sem.at[2])
    ld_do = pltpu.make_async_copy(do.at[:, own_heads, :], raw_do, in_sem.at[3])
    ld_val = pltpu.make_async_copy(valid, valid_all.at[r], in_sem.at[4])
    ld_cu = pltpu.make_async_copy(cu_hbm, cu, in_sem.at[5])
    for cp in (ld_cu, ld_k, ld_v, ld_val):
        cp.start()

    barrier = pltpu.get_barrier_semaphore()
    for dev in (partner, cross, cross_o):
        pl.semaphore_signal(barrier, inc=1, device_id={"cp": dev}, device_id_type=MESH)
    ld_cu.wait()
    l0 = lax.shift_right_logical(cu[1], 3)

    peers = (partner, cross, cross_o)
    push_q = remote(q.at[:, oth_heads, :], far_q, raw_ssem.at[0], raw_rsem.at[0], partner)
    push_do = remote(do.at[:, oth_heads, :], far_do, raw_ssem.at[1], raw_rsem.at[1], partner)
    push_val = [remote(valid, valid_all.at[r], val_ssem.at[i], val_rsem.at[r], dev) for i, dev in enumerate(peers)]


    def kv_relayout(up):
        def body(i, _):
            t0 = i * 16
            for which, raw in ((0, raw_k), (1, raw_v)):
                rows = jnp.stack([raw[src_row(up, t0 + j, l0)] for j in range(16)])
                kv_hm[:, up, which, pl.ds(pl.multiple_of(t0, 16), 16), :] = jnp.transpose(rows, (1, 0, 2))
            return 0
        lax.fori_loop(0, SLOT // 16, body, 0)

    def kv_push(h, to, both):
        head = (4 * c if to == 1 else 4 * pc) + h
        dev = (partner, cross, cross_o)[to]
        ups = pl.ds(0, 2 if both else 1)
        return remote(kv_hm.at[head, ups], kv_all.at[h, r, ups], kv_ssem.at[to, h], kv_rsem.at[h, r], dev)

    def kv_first(to, up):
        head = 4 * c if to == 1 else 4 * pc
        at = pl.ds(up, 1)
        return remote(kv_hm.at[head, at], kv_all.at[0, r, at], first_ssem.at[to - 1, up], first_rsem.at[c, up],
                      (cross, cross_o)[to - 1])

    def kv_wait(h, owner, both):
        ups = pl.ds(0, 2 if both else 1)
        remote(kv_hm.at[0, ups], kv_all.at[h, owner, ups], kv_ssem.at[0, h], kv_rsem.at[h, owner], partner).wait_recv()

    def first_wait(owner):
        for up in range(2):
            at = pl.ds(up, 1)
            remote(kv_hm.at[0, at], kv_all.at[0, owner, at], first_ssem.at[0, up], first_rsem.at[owner - 2, up], partner).wait_recv()

    ld_k.wait()
    ld_v.wait()
    kv_relayout(0)
    pl.semaphore_wait(barrier, 3)

    def cross_send(ch, h):
        @pl.when(chip == ch)
        def _():
            for to in (1, 2):
                kv_push(h, to, ch == 1).start()

    cross_send(0, 0)

    def send_first(up):
        @pl.when(chip == 1)
        def _():
            for to in (1, 2):
                kv_first(to, up).start()

    send_first(0)
    for cp in (ld_q, ld_do, push_q, push_do):
        cp.start()
    kv_relayout(1)
    send_first(1)
    for h in range(HC):
        kv_push(h, 0, True).start()
    ld_val.wait()
    for cp in push_val:
        cp.start()

    def copy_own(h, _):
        for up in range(2):
            kv_all[h, r, up] = kv_hm[4 * c + h, up]
        return 0
    lax.fori_loop(0, HC, copy_own, 0)

    def q_relayout(oc, from_q, from_do):
        for up, ti in ((0, oc), (1, 3 - oc)):
            def body(i, _):
                t0 = i * 16
                at = pl.ds(pl.multiple_of(t0, 16), 16)
                for raw, dst in ((from_q, qh), (from_do, doh)):
                    rows = jnp.stack([raw[src_row(up, t0 + j, l0)] for j in range(16)])
                    dst[:, ti, :, at, :] = jnp.transpose(rows, (1, 0, 2)).reshape(HC, GROUP, 16, HEAD)
                return 0
            lax.fori_loop(0, SLOT // 16, body, 0)

    ld_q.wait()
    ld_do.wait()
    cross_send(0, 1)
    q_relayout(c, raw_q, raw_do)

    cross_send(0, 2)
    for i in range(3):
        remote(valid, valid_all.at[peers[i]], val_ssem.at[i], val_rsem.at[peers[i]], peers[i]).wait_recv()
    lane = lax.broadcasted_iota(jnp.int32, (SLOT, SLOT), 1)
    sub = lax.broadcasted_iota(jnp.int32, (SLOT, SLOT), 0)
    lane2 = lax.broadcasted_iota(jnp.int32, (SLOT, 2 * SLOT), 1)
    sub2 = lax.broadcasted_iota(jnp.int32, (SLOT, 2 * SLOT), 0)
    same_doc = (lane < l0) == (sub < l0)
    doc_f = jnp.where(lane < l0, 1.0, 0.0)
    doc_s = jnp.where(sub < l0, 1.0, 0.0)
    same_f = jnp.where(doc_f == doc_s, 1.0, 0.0)
    del same_doc

    def cap_body(s, _):
        owner = jnp.where(s < 4, s, 7 - s)
        off = jnp.where(s < 4, 0, 1)
        src_lo = jnp.where(sub2 < l0, sub2, sub2 + l0)
        src_hi = jnp.where(sub2 < l0, sub2 + l0, sub2 + SLOT)
        src = jnp.where(off == 1, src_hi, src_lo)
        row = jnp.broadcast_to(valid_all[owner].astype(F32), (SLOT, 2 * SLOT))
        ok = jnp.sum(jnp.where(src == lane2, row, 0.0), axis=1, keepdims=True)
        caps[s] = jnp.where(same_f * ok > 0.5, BIG, FILL)
        return 0
    lax.fori_loop(0, 8, cap_body, 0)
    for ti in range(4):
        oc, up = TILES[ti]
        s = (7 - (2 * chip + oc)) if up else 2 * chip + oc
        caps[8 + ti] = jnp.where(sub <= lane, caps[s], FILL)

    cross_send(0, 3)
    cross_send(1, 1)
    push_q.wait_recv()
    push_do.wait_recv()
    q_relayout(pc, far_q, far_do)

    def part_copy(h, u, n=2):
        up = int(u > 3)
        return remote(dkv_acc.at[h, pl.ds(2 * u, n)], cross_in.at[4 * c + h, up, pl.ds(0, n)], part_ssem,
                      part_rsem.at[4 * c + h, up], min(u, 7 - u))

    def part_wait(j, up, n=2):
        remote(dkv_acc.at[0, pl.ds(0, n)], cross_in.at[j, up, pl.ds(0, n)], part_ssem,
               part_rsem.at[j, up], partner).wait_recv()

    def near_copy(h, up, slot, n=2):
        return remote(dkv_acc.at[h, pl.ds(2 * slot, n)], near_in.at[h, up, pl.ds(0, n)], near_ssem.at[h, up],
                      near_rsem.at[h, up], partner)

    def near_run(ch, h, act):
        act(near_copy(h, 0, 2 * ch + pc))
        if ch == 1:
            pl.when(c == 0)(lambda: act(near_copy(h, 1, 4)))
            if SW[h] < 2:
                pl.when(c == 1)(lambda: act(near_copy(h, 1, 5, 2 - SW[h])))

    def near_wait(h, up, n=2):
        near_copy(h, up, 0, n).wait_recv()

    def swap_copy(h):
        n = SW[h]
        return remote(dkv_acc.at[h, pl.ds(12 - n, n)], swap_in.at[h, pl.ds(2 - n, n)], swap_ssem.at[h], swap_rsem.at[h], cross)

    def swap_back(h, core):
        at = pl.ds(2 - SW[h], SW[h])
        j = 4 * core + h
        return remote(back_st.at[h, at], dkv_out.at[j, 1, at], back_ssem.at[h], back_rsem.at[j], 2)

    def res_copy(p, ti, which):
        stage, out = ((o_far, o_out), (dq_far, dq_out))[which]
        dst = out.at[TILES[ti][1], :, pl.ds(pl.multiple_of(16 * c + 8 * p, 8), 8), :]
        return remote(stage.at[p, ti], dst, res_ssem.at[which, p, ti], res_rsem.at[which, p, TILES[ti][1]], partner)

    def dkv_copy(h, ti):
        up = TILES[ti][1]
        return remote(dkv_st.at[h, ti], dkv_out.at[4 * c + h, up], dkv_ssem.at[h, ti], dkv_rsem.at[h, up], partner)

    def res_put(p):
        heads = pl.ds(pl.multiple_of(16 * c + 8 * p, 8), 8)
        for ti, (oc, up) in enumerate(TILES):
            def body(i, _, keep):
                at = pl.ds(pl.multiple_of(i * 16, 16), 16)
                for stage, far, out in ((o_st, o_far, o_out), (dq_st, dq_far, dq_out)):
                    x = jnp.concatenate([stage[e, ti, pl.ds(pl.multiple_of(g * SLOT + i * 16, 16), 16), :][None]
                                         for e in range(2) for g in range(GROUP)], axis=0)
                    y = jnp.transpose(x, (1, 0, 2))
                    if keep:
                        out[up, at, heads, :] = y
                    else:
                        far[p, ti, at, :, :] = y
                return 0

            @pl.when(c == oc)
            def _():
                lax.fori_loop(0, SLOT // 16, functools.partial(body, keep=True), 0)

            @pl.when(c != oc)
            def _():
                lax.fori_loop(0, SLOT // 16, functools.partial(body, keep=False), 0)
                for which in range(2):
                    res_copy(p, ti, which).start()

    def dkv_put(h, ti, parts):
        oc, up = TILES[ti]

        @pl.when(c == oc)
        def _():
            for w in range(2):
                dkv_out[4 * c + h, up, w] = parts(w).astype(BF16)

        @pl.when(c != oc)
        def _():
            for w in range(2):
                dkv_st[h, ti, w] = parts(w).astype(BF16)
            dkv_copy(h, ti).start()

    lse_far = remote(lse_st.at[pc], lse_out.at[:, own_heads, :], lse_sem, lse_rsem, partner)

    def kv_slot(h, s, which):
        return kv_all[h, min(s, 7 - s), int(s > 3), which]

    def kv_slots(h, a, b, which):
        return jnp.concatenate([kv_slot(h, s, which) for s in range(a, b)], axis=0)

    def run_chip(ch):
        slots = [slot_of(ch, ti) for ti in range(4)]
        sent = [0, 1] if ch == 1 else [2, 3, 4, 5]

        def transposes(s):
            for src, dst in ((0, kt), (1, vt)):
                dst[:, s * SLOT:(s + 1) * SLOT] = jnp.transpose(kv_slot(h_ref[0], s, src))

        h_ref = [None]
        sts = (st0, st1)

        def point(h, where):
            if ch == 0:
                return
            kv = {(0, 3): 2, (1, 2): 3}
            swaps = {(1, 4): (0, 1), (2, 4): (2,)}
            parts = {(2, 2): (0,), (2, 4): (1,), (3, 4): (2, 3)}
            for at in range(HC):
                if not any((at, where) in d for d in (kv, swaps, parts)):
                    continue

                @pl.when(h == at)
                def _():
                    if (at, where) in kv:
                        for to in (1, 2):
                            kv_push(kv[at, where], to, True).start()
                    for e in swaps.get((at, where), ()):
                        swap_copy(e).start()
                    for e in parts.get((at, where), ()):
                        for u in (0, 1):
                            part_copy(e, u).start()

        def head(h, _):
            h_ref[0] = h
            seen = set()
            ready = set()

            def wait_slot(s):
                if s in ready:
                    return
                if s in slots:
                    kv_wait(h, partner, True)
                    new = slots
                elif ch == 1:
                    for owner in (0, 1):
                        kv_wait(h, owner, False)
                    new = [0, 1]
                else:
                    for owner in (2, 3):
                        pl.when(h == 0)(functools.partial(first_wait, owner))
                        pl.when(h > 0)(functools.partial(kv_wait, h, owner, True))
                    new = [2, 3, 4, 5]
                for u in new:
                    ready.add(u)
                    transposes(u)

            state = {}

            def forward(ti):
                point(h, ti)
                s = slots[ti]
                nk = s + 1
                for u in range(nk):
                    wait_slot(u)
                st = sts[ti % 2]
                qt = qh[h, ti].reshape(TILE, HEAD)
                dt = doh[h, ti].reshape(TILE, HEAD)
                m8 = [None] * GROUP
                for a in range(0, nk, 2):
                    n = min(2, nk - a)
                    kb = kv_slots(h, a, a + n, 0)
                    sc = mm(kb, qt, NT)
                    for j in range(n):
                        cap = caps[8 + ti] if a + j == s else caps[a + j]
                        for g in range(GROUP):
                            x = jnp.minimum(sc[j * SLOT:(j + 1) * SLOT, g * SLOT:(g + 1) * SLOT], cap)
                            st[(a + j) * SLOT:(a + j + 1) * SLOT, g * SLOT:(g + 1) * SLOT] = x
                            top = jnp.max(x.reshape(SLOT // 8, 8, SLOT), axis=0)
                            m8[g] = top if m8[g] is None else jnp.maximum(m8[g], top)
                m = [jnp.max(x, axis=0, keepdims=True) for x in m8]
                mc = [x * C2 for x in m]
                l8 = [None] * GROUP
                for a in range(nk):
                    for g in range(GROUP):
                        at = (slice(a * SLOT, (a + 1) * SLOT), slice(g * SLOT, (g + 1) * SLOT))
                        e = jnp.exp2(st[at] * C2 - mc[g])
                        st[at] = e
                        pb[at] = e.astype(BF16)
                        tot = jnp.sum(e.reshape(SLOT // 8, 8, SLOT), axis=0)
                        l8[g] = tot if l8[g] is None else l8[g] + tot
                ot = mm(vt[:, :nk * SLOT], pb[:nk * SLOT, :], NN)
                inv, dd = [], []
                oc, up = TILES[ti]
                for g in range(GROUP):
                    l = jnp.sum(l8[g], axis=0, keepdims=True)
                    has = m[g] > 0.5 * FILL
                    safe = jnp.where(has, l, 1.0)
                    i_l = jnp.where(has, 1.0 / safe, 0.0)
                    lse = jnp.where(has, m[g] * SCALE + jnp.log(safe), 0.0)
                    lse_st[oc, up, pl.ds(h * GROUP + g, 1), :] = lse
                    og = (ot[:, g * SLOT:(g + 1) * SLOT] * i_l).astype(BF16)
                    dog = jnp.transpose(dt[g * SLOT:(g + 1) * SLOT, :])
                    dd.append(jnp.sum(og.astype(F32) * dog.astype(F32), axis=0, keepdims=True))
                    inv.append(i_l)
                    o_st[h % 2, ti, g * SLOT:(g + 1) * SLOT, :] = jnp.transpose(og)

                state[ti] = [inv, dd, None]

            def backward(ti, part):
                inv, dd, dqt = state[ti]
                qt = qh[h, ti].reshape(TILE, HEAD)
                dt = doh[h, ti].reshape(TILE, HEAD)
                st = sts[ti % 2]
                runs = []
                for u in part:
                    if runs and runs[-1][1] == u and u - runs[-1][0] < 2:
                        runs[-1][1] = u + 1
                    else:
                        runs.append([u, u + 1])
                for a, b in runs:
                    n = b - a
                    vb = kv_slots(h, a, b, 1)
                    dp = mm(vb, dt, NT)
                    for j in range(n):
                        for g in range(GROUP):
                            at = (slice((a + j) * SLOT, (a + j + 1) * SLOT), slice(g * SLOT, (g + 1) * SLOT))
                            p = st[at] * inv[g]
                            pb[at] = p.astype(BF16)
                            ds = p * (dp[j * SLOT:(j + 1) * SLOT, g * SLOT:(g + 1) * SLOT] - dd[g])
                            db[at] = ds.astype(BF16)
                    dsb = db[a * SLOT:b * SLOT, :]
                    dv = mm(pb[a * SLOT:b * SLOT, :], dt, NN)
                    dk = mm(dsb, qt, NN) * SCALE
                    dq = mm(kt[:, a * SLOT:b * SLOT], dsb, NN)
                    dqt = dq if dqt is None else dqt + dq
                    for j in range(n):
                        u = a + j
                        new = (dk[j * SLOT:(j + 1) * SLOT], dv[j * SLOT:(j + 1) * SLOT])
                        for w in range(2):
                            dkv_acc[h, 2 * u + w] = dkv_acc[h, 2 * u + w] + new[w] if u in seen else new[w]
                        seen.add(u)
                state[ti][2] = dqt

            def finish(ti):
                dqt = state[ti][2]
                for g in range(GROUP):
                    dqg = (dqt[:, g * SLOT:(g + 1) * SLOT] * SCALE).astype(BF16)
                    dq_st[h % 2, ti, g * SLOT:(g + 1) * SLOT, :] = jnp.transpose(dqg)

            if ch == 0:
                for ti in (0, 1):
                    forward(ti)
                    backward(ti, range(slots[ti] + 1))
                    finish(ti)
                for ti in (2, 3):
                    forward(ti)
                for ti in (2, 3):
                    backward(ti, [2, 3])
                for u in (2, 3):
                    part_copy(h, u).start()
                for ti in (2, 3):
                    backward(ti, [4, 5])
                part_copy(h, 4).start()
                for at in range(HC):
                    if SW[at] < 2:
                        pl.when(h == at)(part_copy(at, 5, 2 - SW[at]).start)
                for ti in (2, 3):
                    backward(ti, [u for u in range(slots[ti] + 1) if u not in sent])
                    finish(ti)
            else:
                for ti in range(4):
                    forward(ti)
                    backward(ti, range(slots[ti] + 1))
                    finish(ti)
            if ch == 1:
                point(h, 4)
            else:
                for ti in (2, 3):
                    dkv_put(h, ti, lambda w, ti=ti: dkv_acc[h, 2 * slots[ti] + w])
            for at in range(HC):
                pl.when(h == at)(functools.partial(near_run, ch, at, lambda cp: cp.start()))
            pl.when(h % 2 == 1)(lambda: res_put(h // 2))
            return 0

        lax.fori_loop(0, HC, head, 0)

        lse_out[:, own_heads, :] = lse_st[c]
        lse_far.start()

        if ch == 0:
            for h in range(HC):
                if SW[h]:
                    swap_copy(h).wait_recv()
                    for w in range(2 - SW[h], 2):
                        back_st[h, w] = (swap_in[h, w] + dkv_acc[h, 10 + w]).astype(BF16)
                    swap_back(h, c).start()

        def early(h, _):
            kv_push(h, 0, True).wait_send()
            for to in (1, 2):
                if ch == 0:
                    kv_push(h, to, False).wait_send()
                else:
                    pl.when(h > 0)(kv_push(h, to, True).wait_send)
            if ch == 0:
                for ti in (2, 3):
                    pl.when(c != TILES[ti][0])(dkv_copy(h, ti).wait_send)
                remote(dkv_st.at[h, 0], dkv_out.at[4 * pc + h, 1], dkv_ssem.at[h, 0], dkv_rsem.at[h, 1], partner).wait_recv()
            return 0
        lax.fori_loop(0, HC, early, 0)
        if ch == 1:
            for to in (1, 2):
                for up in range(2):
                    kv_first(to, up).wait_send()
        for h in range(HC):
            near_run(ch, h, lambda cp: cp.wait_send())
            near_wait(h, 0)
            if ch == 1:
                pl.when(c == 1)(functools.partial(near_wait, h, 1))
                if SW[h] < 2:
                    pl.when(c == 0)(functools.partial(near_wait, h, 1, 2 - SW[h]))
        push_q.wait_send()
        push_do.wait_send()
        for cp in push_val:
            cp.wait_send()
        for p in range(2):
            for which in range(2):
                stage, out = ((o_far, o_out), (dq_far, dq_out))[which]
                for ti in range(4):
                    pl.when(c != TILES[ti][0])(res_copy(p, ti, which).wait_send)
                for up in range(2):
                    dst = out.at[up, :, pl.ds(pl.multiple_of(16 * pc + 8 * p, 8), 8), :]
                    remote(stage.at[p, 0], dst, res_ssem.at[which, p, 0], res_rsem.at[which, p, up], partner).wait_recv()
        lse_far.wait_send()
        remote(lse_st.at[0], lse_out.at[:, oth_heads, :], lse_sem, lse_rsem, partner).wait_recv()

        def add_up(h, up, slot, n):
            if n == 0:
                return
            part_wait(4 * c + h, up, n)
            for w in range(n):
                dkv_out[4 * c + h, up, w] = (dkv_acc[h, 2 * slot + w] + cross_in[4 * c + h, up, w]).astype(BF16)
            part_wait(4 * pc + h, up, n)
            for w in range(n):
                dkv_out[4 * pc + h, up, w] = (near_in[h, up, w] + cross_in[4 * pc + h, up, w]).astype(BF16)

        for h in range(HC):
            add_up(h, 0, 2 * ch + c, 2)
            if ch == 1:
                pl.when(c == 1)(functools.partial(add_up, h, 1, 4, 2))
                pl.when(c == 0)(functools.partial(add_up, h, 1, 5, 2 - SW[h]))

        units = HC * 4 if ch == 1 else HC * 8 - sum(SW)
        rows = next(a for a in (1, 2, 3, 4) if units % a == 0 and units // a <= 16)
        block = dkv_acc.at[pl.ds(0, rows), pl.ds(0, units // rows)]
        remote(block, block, part_ssem, part_rsem.at[0, 0], partner).wait_send()
        for h in range(HC):
            if SW[h]:
                if ch == 0:
                    swap_back(h, c).wait_send()
                else:
                    swap_copy(h).wait_send()

        if ch == 1:
            @pl.when(c == 0)
            def _():
                for h in range(HC):
                    if SW[h]:
                        for core in range(2):
                            swap_back(h, core).wait_recv()

    pl.when(chip == 0)(functools.partial(run_chip, 0))
    pl.when(chip == 1)(functools.partial(run_chip, 1))


def attn_call(cu, valid, q, k, v, do):
    any_spec = pl.BlockSpec(memory_space=pl.ANY)
    dma = pltpu.SemaphoreType.DMA
    return pl.pallas_call(
        attn_kernel,
        out_shape=(
            pltpu.VMEM((2, SLOT, 32, HEAD), BF16),
            pltpu.VMEM((2, SLOT, 32, HEAD), BF16),
            pltpu.VMEM((8, 2, 2, SLOT, HEAD), BF16),
            pltpu.VMEM((2, 32, SLOT), F32),
            pltpu.SMEM((3,), jnp.int32),
        ),
        in_specs=[any_spec] * 6,
        out_specs=(pl.BlockSpec(memory_space=pltpu.VMEM),) * 4 + (pl.BlockSpec(memory_space=pltpu.SMEM),),
        scratch_shapes=[
            pltpu.VMEM((256, 16, HEAD), BF16),
            pltpu.VMEM((256, 16, HEAD), BF16),
            pltpu.VMEM((256, 16, HEAD), BF16),
            pltpu.VMEM((256, 16, HEAD), BF16),
            pltpu.VMEM((256, 8, HEAD), BF16),
            pltpu.VMEM((256, 8, HEAD), BF16),
            pltpu.VMEM((8, 2, 2, SLOT, HEAD), BF16),
            pltpu.VMEM((HC, 4, 2, 2, SLOT, HEAD), BF16),
            pltpu.VMEM((HEAD, 8 * SLOT), BF16),
            pltpu.VMEM((HEAD, 8 * SLOT), BF16),
            pltpu.VMEM((HC, 4, GROUP, SLOT, HEAD), BF16),
            pltpu.VMEM((HC, 4, GROUP, SLOT, HEAD), BF16),
            pltpu.VMEM((8 * SLOT, TILE), F32),
            pltpu.VMEM((8 * SLOT, TILE), F32),
            pltpu.VMEM((8 * SLOT, TILE), BF16),
            pltpu.VMEM((8 * SLOT, TILE), BF16),
            pltpu.VMEM((HC, 16, SLOT, HEAD), F32),
            pltpu.VMEM((8, 2, 2, SLOT, HEAD), F32),
            pltpu.VMEM((HC, 2, 2, SLOT, HEAD), F32),
            pltpu.VMEM((HC, 2, SLOT, HEAD), F32),
            pltpu.VMEM((2, 4, TILE, HEAD), BF16),
            pltpu.VMEM((2, 4, TILE, HEAD), BF16),
            pltpu.VMEM((2, 4, SLOT, 8, HEAD), BF16),
            pltpu.VMEM((2, 4, SLOT, 8, HEAD), BF16),
            pltpu.VMEM((HC, 4, 2, SLOT, HEAD), BF16),
            pltpu.VMEM((HC, 2, SLOT, HEAD), BF16),
            pltpu.VMEM((2, 2, 16, SLOT), F32),
            pltpu.VMEM((12, SLOT, SLOT), F32),
            pltpu.VMEM((4, 1, 2 * SLOT), jnp.int32),
            dma((6,)),
            dma((2,)), dma((2,)),
            dma((3,)), dma((4,)),
            dma((2, 2)), dma((2, 2)),
            dma((3, HC)), dma((HC, 4)),
            dma, dma((8, 2)), dma((HC, 2)), dma((HC, 2)),
            dma((HC,)), dma((HC,)), dma((HC,)), dma((8,)),
            dma((2, 2, 4)), dma((2, 2, 2)),
            dma((HC, 4)), dma((HC, 2)),
            dma, dma,
        ],
        compiler_params=pltpu.CompilerParams(collective_id=0, has_side_effects=True, vmem_limit_bytes=61300000),
        name="attn",
    )(cu, valid, q, k, v, do)


def finish_kernel(o_in, dq_in, dkv_in, lse_in, cu, o_out, dq_out, dk_out, dv_out, lse_out, dk_t, dv_t, lse_t, sem, lse_sem):
    l0 = lax.shift_right_logical(cu[1], 3)
    rest = SLOT - l0

    def copies(i, x, out):
        runs = ((0, 0, 0, l0), (1, 0, l0, l0), (0, l0, 2 * l0, rest), (1, l0, SLOT + l0, rest))
        return [pltpu.make_async_copy(x.at[up, pl.ds(at, n)], out.at[pl.ds(to, n)], sem.at[i])
                for up, at, to, n in runs]

    for cp in copies(0, o_in, o_out) + copies(1, dq_in, dq_out):
        cp.start()

    for w, dst in ((0, dk_t), (1, dv_t)):
        for up in range(2):
            def body(i, _):
                at = pl.ds(pl.multiple_of(i * 16, 16), 16)
                dst[up, at] = jnp.transpose(dkv_in[:, up, w, at, :], (1, 0, 2))
                return 0
            lax.fori_loop(0, SLOT // 16, body, 0)
        for cp in copies(2 + w, dst, (dk_out, dv_out)[w]):
            cp.start()

    row = lax.broadcasted_iota(jnp.int32, (2 * SLOT, SLOT), 0)
    col = lax.broadcasted_iota(jnp.int32, (2 * SLOT, SLOT), 1)
    acc = None
    for up in range(2):
        if up:
            src = jnp.where(col < l0, col + l0, col + SLOT)
        else:
            src = jnp.where(col < l0, col, col + l0)
        pick = jnp.where(row == src, 1.0, 0.0)
        part = lax.dot_general(lse_in[up], pick, NT, precision=lax.Precision.HIGHEST, preferred_element_type=F32)
        acc = part if acc is None else acc + part
    lse_t[...] = acc
    lse_move = pltpu.make_async_copy(lse_t, lse_out, lse_sem)
    lse_move.start()
    for i, out in enumerate((o_out, dq_out, dk_out, dv_out)):
        pltpu.make_async_copy(out, out, sem.at[i]).wait()
    lse_move.wait()


def finish_call(o_t, dq_t, dkv_hm, lse_hm, cu):
    any_spec = pl.BlockSpec(memory_space=pl.ANY)
    vmem = pl.BlockSpec(memory_space=pltpu.VMEM)
    return pl.pallas_call(
        finish_kernel,
        out_shape=(
            jax.ShapeDtypeStruct((256, 32, HEAD), BF16),
            jax.ShapeDtypeStruct((256, 32, HEAD), BF16),
            jax.ShapeDtypeStruct((256, 8, HEAD), BF16),
            jax.ShapeDtypeStruct((256, 8, HEAD), BF16),
            jax.ShapeDtypeStruct((32, 256), F32),
        ),
        in_specs=[vmem] * 4 + [pl.BlockSpec(memory_space=pltpu.SMEM)],
        out_specs=(any_spec,) * 5,
        scratch_shapes=[
            pltpu.VMEM((2, SLOT, 8, HEAD), BF16),
            pltpu.VMEM((2, SLOT, 8, HEAD), BF16),
            pltpu.VMEM((32, 256), F32),
            pltpu.SemaphoreType.DMA((4,)),
            pltpu.SemaphoreType.DMA,
        ],
        compiler_params=pltpu.CompilerParams(vmem_limit_bytes=16 * 1024 * 1024),
        name="finish",
    )(o_t, dq_t, dkv_hm, lse_hm, cu)


def solution(mesh):
    tok_spec = P(("dp", "cp"), None, None)
    lse_spec = P(("dp", "cp"), None)

    def local(q, k, v, do, valid, cu):
        res = attn_call(cu, valid.reshape(1, 256), q, k, v, do)
        o, dq, dk, dv, lse = finish_call(*res)
        return o, lse.T, dq, dk, dv

    return jax.shard_map(local, mesh=mesh, in_specs=(tok_spec,) * 4 + (P(("dp", "cp")), P("dp")),
                         out_specs=(tok_spec, lse_spec, tok_spec, tok_spec, tok_spec), check_vma=False)
```

```python
import functools
import math

import jax
import jax.numpy as jnp
from jax import lax
from jax.experimental import pallas as pl
from jax.experimental.pallas import tpu as pltpu
from jax.sharding import PartitionSpec as P

MESH = pl.DeviceIdType.MESH
FILL = -1.0e30
BIG = 3.0e38
HEAD = 128
SLOT = 128
TILE = 512
GROUP = 4
HC = 4
SW = (2, 2, 2, 0)
SCALE = HEAD ** -0.5
C2 = SCALE * math.log2(math.e)
NT = (((1,), (1,)), ((), ()))
NN = (((1,), (0,)), ((), ()))
F32 = jnp.float32
BF16 = jnp.bfloat16

TILES = ((0, 0), (1, 0), (1, 1), (0, 1))


def slot_of(chip, ti):
    oc, up = TILES[ti]
    r = 2 * chip + oc
    return 7 - r if up else r


def mm(a, b, dims):
    return lax.dot_general(a, b, dims, preferred_element_type=F32)


def src_row(up, t, l0):
    if up:
        return jnp.where(t < l0, t + l0, t + SLOT)
    return jnp.where(t < l0, t, t + l0)


def attn_kernel(cu_hbm, valid, q, k, v, do, o_out, dq_out, dkv_out, lse_out, cu,
                raw_q, raw_do, far_q, far_do, raw_k, raw_v, kv_hm, kv_all, kt, vt, qh, doh, st0, st1, pb, db,
                dkv_acc, cross_in, near_in, swap_in, o_st, dq_st, o_far, dq_far, dkv_st, back_st, lse_st, caps, valid_all,
                in_sem, raw_ssem, raw_rsem, val_ssem, val_rsem, first_ssem, first_rsem, kv_ssem, kv_rsem,
                part_ssem, part_rsem, near_ssem, near_rsem, swap_ssem, swap_rsem, back_ssem, back_rsem, res_ssem, res_rsem, dkv_ssem, dkv_rsem, lse_sem, lse_rsem):
    r = lax.axis_index("cp")
    chip = r // 2
    c = r % 2
    pc = 1 - c
    partner = chip * 2 + pc
    cross = (1 - chip) * 2 + c
    cross_o = (1 - chip) * 2 + pc

    def remote(src, dst, ssem, rsem, dev):
        return pltpu.make_async_remote_copy(src_ref=src, dst_ref=dst, send_sem=ssem, recv_sem=rsem,
                                            device_id={"cp": dev}, device_id_type=MESH)

    own_heads = pl.ds(pl.multiple_of(16 * c, 16), 16)
    oth_heads = pl.ds(pl.multiple_of(16 * pc, 16), 16)
    ld_k = pltpu.make_async_copy(k, raw_k, in_sem.at[0])
    ld_v = pltpu.make_async_copy(v, raw_v, in_sem.at[1])
    ld_q = pltpu.make_async_copy(q.at[:, own_heads, :], raw_q, in_sem.at[2])
    ld_do = pltpu.make_async_copy(do.at[:, own_heads, :], raw_do, in_sem.at[3])
    ld_val = pltpu.make_async_copy(valid, valid_all.at[r], in_sem.at[4])
    ld_cu = pltpu.make_async_copy(cu_hbm, cu, in_sem.at[5])
    for cp in (ld_cu, ld_k, ld_v, ld_val):
        cp.start()

    barrier = pltpu.get_barrier_semaphore()
    for dev in (partner, cross, cross_o):
        pl.semaphore_signal(barrier, inc=1, device_id={"cp": dev}, device_id_type=MESH)
    ld_cu.wait()
    l0 = lax.shift_right_logical(cu[1], 3)

    peers = (partner, cross, cross_o)
    push_q = remote(q.at[:, oth_heads, :], far_q, raw_ssem.at[0], raw_rsem.at[0], partner)
    push_do = remote(do.at[:, oth_heads, :], far_do, raw_ssem.at[1], raw_rsem.at[1], partner)
    push_val = [remote(valid, valid_all.at[r], val_ssem.at[i], val_rsem.at[r], dev) for i, dev in enumerate(peers)]


    def kv_relayout(up):
        def body(i, _):
            t0 = i * 16
            for which, raw in ((0, raw_k), (1, raw_v)):
                rows = jnp.stack([raw[src_row(up, t0 + j, l0)] for j in range(16)])
                kv_hm[:, up, which, pl.ds(pl.multiple_of(t0, 16), 16), :] = jnp.transpose(rows, (1, 0, 2))
            return 0
        lax.fori_loop(0, SLOT // 16, body, 0)

    def kv_push(h, to, both):
        head = (4 * c if to == 1 else 4 * pc) + h
        dev = (partner, cross, cross_o)[to]
        ups = pl.ds(0, 2 if both else 1)
        return remote(kv_hm.at[head, ups], kv_all.at[h, r, ups], kv_ssem.at[to, h], kv_rsem.at[h, r], dev)

    def kv_first(to, up):
        head = 4 * c if to == 1 else 4 * pc
        at = pl.ds(up, 1)
        return remote(kv_hm.at[head, at], kv_all.at[0, r, at], first_ssem.at[to - 1, up], first_rsem.at[c, up],
                      (cross, cross_o)[to - 1])

    def kv_wait(h, owner, both):
        ups = pl.ds(0, 2 if both else 1)
        remote(kv_hm.at[0, ups], kv_all.at[h, owner, ups], kv_ssem.at[0, h], kv_rsem.at[h, owner], partner).wait_recv()

    def first_wait(owner):
        for up in range(2):
            at = pl.ds(up, 1)
            remote(kv_hm.at[0, at], kv_all.at[0, owner, at], first_ssem.at[0, up], first_rsem.at[owner - 2, up], partner).wait_recv()

    ld_k.wait()
    ld_v.wait()
    kv_relayout(0)
    pl.semaphore_wait(barrier, 3)

    def cross_send(ch, h):
        @pl.when(chip == ch)
        def _():
            for to in (1, 2):
                kv_push(h, to, ch == 1).start()

    cross_send(0, 0)

    def send_first(up):
        @pl.when(chip == 1)
        def _():
            for to in (1, 2):
                kv_first(to, up).start()

    send_first(0)
    for cp in (ld_q, ld_do, push_q, push_do):
        cp.start()
    kv_relayout(1)
    send_first(1)
    for h in range(HC):
        kv_push(h, 0, True).start()
    ld_val.wait()
    for cp in push_val:
        cp.start()

    def copy_own(h, _):
        for up in range(2):
            kv_all[h, r, up] = kv_hm[4 * c + h, up]
        return 0
    lax.fori_loop(0, HC, copy_own, 0)

    def q_relayout(oc, from_q, from_do):
        for up, ti in ((0, oc), (1, 3 - oc)):
            def body(i, _):
                t0 = i * 16
                at = pl.ds(pl.multiple_of(t0, 16), 16)
                for raw, dst in ((from_q, qh), (from_do, doh)):
                    rows = jnp.stack([raw[src_row(up, t0 + j, l0)] for j in range(16)])
                    dst[:, ti, :, at, :] = jnp.transpose(rows, (1, 0, 2)).reshape(HC, GROUP, 16, HEAD)
                return 0
            lax.fori_loop(0, SLOT // 16, body, 0)

    ld_q.wait()
    ld_do.wait()
    cross_send(0, 1)
    q_relayout(c, raw_q, raw_do)

    cross_send(0, 2)
    for i in range(3):
        remote(valid, valid_all.at[peers[i]], val_ssem.at[i], val_rsem.at[peers[i]], peers[i]).wait_recv()
    lane = lax.broadcasted_iota(jnp.int32, (SLOT, SLOT), 1)
    sub = lax.broadcasted_iota(jnp.int32, (SLOT, SLOT), 0)
    lane2 = lax.broadcasted_iota(jnp.int32, (SLOT, 2 * SLOT), 1)
    sub2 = lax.broadcasted_iota(jnp.int32, (SLOT, 2 * SLOT), 0)
    same_doc = (lane < l0) == (sub < l0)
    doc_f = jnp.where(lane < l0, 1.0, 0.0)
    doc_s = jnp.where(sub < l0, 1.0, 0.0)
    same_f = jnp.where(doc_f == doc_s, 1.0, 0.0)
    del same_doc

    def cap_body(s, _):
        owner = jnp.where(s < 4, s, 7 - s)
        off = jnp.where(s < 4, 0, 1)
        src_lo = jnp.where(sub2 < l0, sub2, sub2 + l0)
        src_hi = jnp.where(sub2 < l0, sub2 + l0, sub2 + SLOT)
        src = jnp.where(off == 1, src_hi, src_lo)
        row = jnp.broadcast_to(valid_all[owner].astype(F32), (SLOT, 2 * SLOT))
        ok = jnp.sum(jnp.where(src == lane2, row, 0.0), axis=1, keepdims=True)
        caps[s] = jnp.where(same_f * ok > 0.5, BIG, FILL)
        return 0
    lax.fori_loop(0, 8, cap_body, 0)
    for ti in range(4):
        oc, up = TILES[ti]
        s = (7 - (2 * chip + oc)) if up else 2 * chip + oc
        caps[8 + ti] = jnp.where(sub <= lane, caps[s], FILL)

    cross_send(0, 3)
    cross_send(1, 1)
    push_q.wait_recv()
    push_do.wait_recv()
    q_relayout(pc, far_q, far_do)

    def part_copy(h, u, n=2):
        up = int(u > 3)
        return remote(dkv_acc.at[h, pl.ds(2 * u, n)], cross_in.at[4 * c + h, up, pl.ds(0, n)], part_ssem,
                      part_rsem.at[4 * c + h, up], min(u, 7 - u))

    def part_wait(j, up, n=2):
        remote(dkv_acc.at[0, pl.ds(0, n)], cross_in.at[j, up, pl.ds(0, n)], part_ssem,
               part_rsem.at[j, up], partner).wait_recv()

    def near_copy(h, up, slot, n=2):
        return remote(dkv_acc.at[h, pl.ds(2 * slot, n)], near_in.at[h, up, pl.ds(0, n)], near_ssem.at[h, up],
                      near_rsem.at[h, up], partner)

    def near_run(ch, h, act):
        act(near_copy(h, 0, 2 * ch + pc))
        if ch == 1:
            pl.when(c == 0)(lambda: act(near_copy(h, 1, 4)))
            if SW[h] < 2:
                pl.when(c == 1)(lambda: act(near_copy(h, 1, 5, 2 - SW[h])))

    def near_wait(h, up, n=2):
        near_copy(h, up, 0, n).wait_recv()

    def swap_copy(h):
        n = SW[h]
        return remote(dkv_acc.at[h, pl.ds(12 - n, n)], swap_in.at[h, pl.ds(2 - n, n)], swap_ssem.at[h], swap_rsem.at[h], cross)

    def swap_back(h, core):
        at = pl.ds(2 - SW[h], SW[h])
        j = 4 * core + h
        return remote(back_st.at[h, at], dkv_out.at[j, 1, at], back_ssem.at[h], back_rsem.at[j], 2)

    def res_copy(p, ti, which):
        stage, out = ((o_far, o_out), (dq_far, dq_out))[which]
        dst = out.at[TILES[ti][1], :, pl.ds(pl.multiple_of(16 * c + 8 * p, 8), 8), :]
        return remote(stage.at[p, ti], dst, res_ssem.at[which, p, ti], res_rsem.at[which, p, TILES[ti][1]], partner)

    def dkv_copy(h, ti):
        up = TILES[ti][1]
        return remote(dkv_st.at[h, ti], dkv_out.at[4 * c + h, up], dkv_ssem.at[h, ti], dkv_rsem.at[h, up], partner)

    def res_put(p):
        heads = pl.ds(pl.multiple_of(16 * c + 8 * p, 8), 8)
        for ti, (oc, up) in enumerate(TILES):
            def body(i, _, keep):
                at = pl.ds(pl.multiple_of(i * 16, 16), 16)
                for stage, far, out in ((o_st, o_far, o_out), (dq_st, dq_far, dq_out)):
                    x = jnp.concatenate([stage[e, ti, pl.ds(pl.multiple_of(g * SLOT + i * 16, 16), 16), :][None]
                                         for e in range(2) for g in range(GROUP)], axis=0)
                    y = jnp.transpose(x, (1, 0, 2))
                    if keep:
                        out[up, at, heads, :] = y
                    else:
                        far[p, ti, at, :, :] = y
                return 0

            @pl.when(c == oc)
            def _():
                lax.fori_loop(0, SLOT // 16, functools.partial(body, keep=True), 0)

            @pl.when(c != oc)
            def _():
                lax.fori_loop(0, SLOT // 16, functools.partial(body, keep=False), 0)
                for which in range(2):
                    res_copy(p, ti, which).start()

    def dkv_put(h, ti, parts):
        oc, up = TILES[ti]

        @pl.when(c == oc)
        def _():
            for w in range(2):
                dkv_out[4 * c + h, up, w] = parts(w).astype(BF16)

        @pl.when(c != oc)
        def _():
            for w in range(2):
                dkv_st[h, ti, w] = parts(w).astype(BF16)
            dkv_copy(h, ti).start()

    lse_far = remote(lse_st.at[pc], lse_out.at[:, own_heads, :], lse_sem, lse_rsem, partner)

    def kv_slot(h, s, which):
        return kv_all[h, min(s, 7 - s), int(s > 3), which]

    def kv_slots(h, a, b, which):
        return jnp.concatenate([kv_slot(h, s, which) for s in range(a, b)], axis=0)

    def run_chip(ch):
        slots = [slot_of(ch, ti) for ti in range(4)]
        sent = [0, 1] if ch == 1 else [2, 3, 4, 5]

        def transposes(s):
            for src, dst in ((0, kt), (1, vt)):
                dst[:, s * SLOT:(s + 1) * SLOT] = jnp.transpose(kv_slot(h_ref[0], s, src))

        h_ref = [None]
        sts = (st0, st1)

        def point(h, where):
            if ch == 0:
                return
            kv = {(0, 1): 2, (0, 4): 3}
            swaps = {(1, 2): (0,), (1, 4): (1,), (2, 4): (2,)}
            parts = {(2, 2): (0,), (2, 4): (1,), (3, 4): (2, 3)}
            for at in range(HC):
                if not any((at, where) in d for d in (kv, swaps, parts)):
                    continue

                @pl.when(h == at)
                def _():
                    if (at, where) in kv:
                        for to in (1, 2):
                            kv_push(kv[at, where], to, True).start()
                    for e in swaps.get((at, where), ()):
                        swap_copy(e).start()
                    for e in parts.get((at, where), ()):
                        for u in (0, 1):
                            part_copy(e, u).start()

        def head(h, _):
            h_ref[0] = h
            seen = set()
            ready = set()

            def wait_slot(s):
                if s in ready:
                    return
                if s in slots:
                    kv_wait(h, partner, True)
                    new = slots
                elif ch == 1:
                    for owner in (0, 1):
                        kv_wait(h, owner, False)
                    new = [0, 1]
                else:
                    for owner in (2, 3):
                        pl.when(h == 0)(functools.partial(first_wait, owner))
                        pl.when(h > 0)(functools.partial(kv_wait, h, owner, True))
                    new = [2, 3, 4, 5]
                for u in new:
                    ready.add(u)
                    transposes(u)

            state = {}

            def forward(ti):
                point(h, ti)
                s = slots[ti]
                nk = s + 1
                for u in range(nk):
                    wait_slot(u)
                st = sts[ti % 2]
                qt = qh[h, ti].reshape(TILE, HEAD)
                dt = doh[h, ti].reshape(TILE, HEAD)
                m8 = [None] * GROUP
                for a in range(0, nk, 2):
                    n = min(2, nk - a)
                    kb = kv_slots(h, a, a + n, 0)
                    sc = mm(kb, qt, NT)
                    for j in range(n):
                        cap = caps[8 + ti] if a + j == s else caps[a + j]
                        for g in range(GROUP):
                            x = jnp.minimum(sc[j * SLOT:(j + 1) * SLOT, g * SLOT:(g + 1) * SLOT], cap)
                            st[(a + j) * SLOT:(a + j + 1) * SLOT, g * SLOT:(g + 1) * SLOT] = x
                            top = jnp.max(x.reshape(SLOT // 8, 8, SLOT), axis=0)
                            m8[g] = top if m8[g] is None else jnp.maximum(m8[g], top)
                m = [jnp.max(x, axis=0, keepdims=True) for x in m8]
                mc = [x * C2 for x in m]
                l8 = [None] * GROUP
                for a in range(nk):
                    for g in range(GROUP):
                        at = (slice(a * SLOT, (a + 1) * SLOT), slice(g * SLOT, (g + 1) * SLOT))
                        e = jnp.exp2(st[at] * C2 - mc[g])
                        st[at] = e
                        pb[at] = e.astype(BF16)
                        tot = jnp.sum(e.reshape(SLOT // 8, 8, SLOT), axis=0)
                        l8[g] = tot if l8[g] is None else l8[g] + tot
                ot = mm(vt[:, :nk * SLOT], pb[:nk * SLOT, :], NN)
                inv, dd = [], []
                oc, up = TILES[ti]
                for g in range(GROUP):
                    l = jnp.sum(l8[g], axis=0, keepdims=True)
                    has = m[g] > 0.5 * FILL
                    safe = jnp.where(has, l, 1.0)
                    i_l = jnp.where(has, 1.0 / safe, 0.0)
                    lse = jnp.where(has, m[g] * SCALE + jnp.log(safe), 0.0)
                    lse_st[oc, up, pl.ds(h * GROUP + g, 1), :] = lse
                    og = (ot[:, g * SLOT:(g + 1) * SLOT] * i_l).astype(BF16)
                    dog = jnp.transpose(dt[g * SLOT:(g + 1) * SLOT, :])
                    dd.append(jnp.sum(og.astype(F32) * dog.astype(F32), axis=0, keepdims=True))
                    inv.append(i_l)
                    o_st[h % 2, ti, g * SLOT:(g + 1) * SLOT, :] = jnp.transpose(og)

                state[ti] = [inv, dd, None]

            def backward(ti, part):
                inv, dd, dqt = state[ti]
                qt = qh[h, ti].reshape(TILE, HEAD)
                dt = doh[h, ti].reshape(TILE, HEAD)
                st = sts[ti % 2]
                runs = []
                for u in part:
                    if runs and runs[-1][1] == u and u - runs[-1][0] < 2:
                        runs[-1][1] = u + 1
                    else:
                        runs.append([u, u + 1])
                for a, b in runs:
                    n = b - a
                    vb = kv_slots(h, a, b, 1)
                    dp = mm(vb, dt, NT)
                    for j in range(n):
                        for g in range(GROUP):
                            at = (slice((a + j) * SLOT, (a + j + 1) * SLOT), slice(g * SLOT, (g + 1) * SLOT))
                            p = st[at] * inv[g]
                            pb[at] = p.astype(BF16)
                            ds = p * (dp[j * SLOT:(j + 1) * SLOT, g * SLOT:(g + 1) * SLOT] - dd[g])
                            db[at] = ds.astype(BF16)
                    dsb = db[a * SLOT:b * SLOT, :]
                    dv = mm(pb[a * SLOT:b * SLOT, :], dt, NN)
                    dk = mm(dsb, qt, NN) * SCALE
                    dq = mm(kt[:, a * SLOT:b * SLOT], dsb, NN)
                    dqt = dq if dqt is None else dqt + dq
                    for j in range(n):
                        u = a + j
                        new = (dk[j * SLOT:(j + 1) * SLOT], dv[j * SLOT:(j + 1) * SLOT])
                        for w in range(2):
                            dkv_acc[h, 2 * u + w] = dkv_acc[h, 2 * u + w] + new[w] if u in seen else new[w]
                        seen.add(u)
                state[ti][2] = dqt

            def finish(ti):
                dqt = state[ti][2]
                for g in range(GROUP):
                    dqg = (dqt[:, g * SLOT:(g + 1) * SLOT] * SCALE).astype(BF16)
                    dq_st[h % 2, ti, g * SLOT:(g + 1) * SLOT, :] = jnp.transpose(dqg)

            if ch == 0:
                for ti in (0, 1):
                    forward(ti)
                    backward(ti, range(slots[ti] + 1))
                    finish(ti)
                for ti in (2, 3):
                    forward(ti)
                for ti in (2, 3):
                    backward(ti, [2, 3])
                for u in (2, 3):
                    part_copy(h, u).start()
                for ti in (2, 3):
                    backward(ti, [4, 5])
                part_copy(h, 4).start()
                for at in range(HC):
                    if SW[at] < 2:
                        pl.when(h == at)(part_copy(at, 5, 2 - SW[at]).start)
                for ti in (2, 3):
                    backward(ti, [u for u in range(slots[ti] + 1) if u not in sent])
                    finish(ti)
            else:
                for ti in range(4):
                    forward(ti)
                    backward(ti, range(slots[ti] + 1))
                    finish(ti)
            if ch == 1:
                point(h, 4)
            else:
                for ti in (2, 3):
                    dkv_put(h, ti, lambda w, ti=ti: dkv_acc[h, 2 * slots[ti] + w])
            for at in range(HC):
                pl.when(h == at)(functools.partial(near_run, ch, at, lambda cp: cp.start()))
            pl.when(h % 2 == 1)(lambda: res_put(h // 2))
            return 0

        lax.fori_loop(0, HC, head, 0)

        lse_out[:, own_heads, :] = lse_st[c]
        lse_far.start()

        if ch == 0:
            for h in range(HC):
                if SW[h]:
                    swap_copy(h).wait_recv()
                    for w in range(2 - SW[h], 2):
                        back_st[h, w] = (swap_in[h, w] + dkv_acc[h, 10 + w]).astype(BF16)
                    swap_back(h, c).start()

        def early(h, _):
            kv_push(h, 0, True).wait_send()
            for to in (1, 2):
                if ch == 0:
                    kv_push(h, to, False).wait_send()
                else:
                    pl.when(h > 0)(kv_push(h, to, True).wait_send)
            if ch == 0:
                for ti in (2, 3):
                    pl.when(c != TILES[ti][0])(dkv_copy(h, ti).wait_send)
                remote(dkv_st.at[h, 0], dkv_out.at[4 * pc + h, 1], dkv_ssem.at[h, 0], dkv_rsem.at[h, 1], partner).wait_recv()
            return 0
        lax.fori_loop(0, HC, early, 0)
        if ch == 1:
            for to in (1, 2):
                for up in range(2):
                    kv_first(to, up).wait_send()
        for h in range(HC):
            near_run(ch, h, lambda cp: cp.wait_send())
            near_wait(h, 0)
            if ch == 1:
                pl.when(c == 1)(functools.partial(near_wait, h, 1))
                if SW[h] < 2:
                    pl.when(c == 0)(functools.partial(near_wait, h, 1, 2 - SW[h]))
        push_q.wait_send()
        push_do.wait_send()
        for cp in push_val:
            cp.wait_send()
        for p in range(2):
            for which in range(2):
                stage, out = ((o_far, o_out), (dq_far, dq_out))[which]
                for ti in range(4):
                    pl.when(c != TILES[ti][0])(res_copy(p, ti, which).wait_send)
                for up in range(2):
                    dst = out.at[up, :, pl.ds(pl.multiple_of(16 * pc + 8 * p, 8), 8), :]
                    remote(stage.at[p, 0], dst, res_ssem.at[which, p, 0], res_rsem.at[which, p, up], partner).wait_recv()
        lse_far.wait_send()
        remote(lse_st.at[0], lse_out.at[:, oth_heads, :], lse_sem, lse_rsem, partner).wait_recv()

        def add_up(h, up, slot, n):
            if n == 0:
                return
            part_wait(4 * c + h, up, n)
            for w in range(n):
                dkv_out[4 * c + h, up, w] = (dkv_acc[h, 2 * slot + w] + cross_in[4 * c + h, up, w]).astype(BF16)
            part_wait(4 * pc + h, up, n)
            for w in range(n):
                dkv_out[4 * pc + h, up, w] = (near_in[h, up, w] + cross_in[4 * pc + h, up, w]).astype(BF16)

        for h in range(HC):
            add_up(h, 0, 2 * ch + c, 2)
            if ch == 1:
                pl.when(c == 1)(functools.partial(add_up, h, 1, 4, 2))
                pl.when(c == 0)(functools.partial(add_up, h, 1, 5, 2 - SW[h]))

        units = HC * 4 if ch == 1 else HC * 8 - sum(SW)
        rows = next(a for a in (1, 2, 3, 4) if units % a == 0 and units // a <= 16)
        block = dkv_acc.at[pl.ds(0, rows), pl.ds(0, units // rows)]
        remote(block, block, part_ssem, part_rsem.at[0, 0], partner).wait_send()
        for h in range(HC):
            if SW[h]:
                if ch == 0:
                    swap_back(h, c).wait_send()
                else:
                    swap_copy(h).wait_send()

        if ch == 1:
            @pl.when(c == 0)
            def _():
                for h in range(HC):
                    if SW[h]:
                        for core in range(2):
                            swap_back(h, core).wait_recv()

    pl.when(chip == 0)(functools.partial(run_chip, 0))
    pl.when(chip == 1)(functools.partial(run_chip, 1))


def attn_call(cu, valid, q, k, v, do):
    any_spec = pl.BlockSpec(memory_space=pl.ANY)
    dma = pltpu.SemaphoreType.DMA
    return pl.pallas_call(
        attn_kernel,
        out_shape=(
            pltpu.VMEM((2, SLOT, 32, HEAD), BF16),
            pltpu.VMEM((2, SLOT, 32, HEAD), BF16),
            pltpu.VMEM((8, 2, 2, SLOT, HEAD), BF16),
            pltpu.VMEM((2, 32, SLOT), F32),
            pltpu.SMEM((3,), jnp.int32),
        ),
        in_specs=[any_spec] * 6,
        out_specs=(pl.BlockSpec(memory_space=pltpu.VMEM),) * 4 + (pl.BlockSpec(memory_space=pltpu.SMEM),),
        scratch_shapes=[
            pltpu.VMEM((256, 16, HEAD), BF16),
            pltpu.VMEM((256, 16, HEAD), BF16),
            pltpu.VMEM((256, 16, HEAD), BF16),
            pltpu.VMEM((256, 16, HEAD), BF16),
            pltpu.VMEM((256, 8, HEAD), BF16),
            pltpu.VMEM((256, 8, HEAD), BF16),
            pltpu.VMEM((8, 2, 2, SLOT, HEAD), BF16),
            pltpu.VMEM((HC, 4, 2, 2, SLOT, HEAD), BF16),
            pltpu.VMEM((HEAD, 8 * SLOT), BF16),
            pltpu.VMEM((HEAD, 8 * SLOT), BF16),
            pltpu.VMEM((HC, 4, GROUP, SLOT, HEAD), BF16),
            pltpu.VMEM((HC, 4, GROUP, SLOT, HEAD), BF16),
            pltpu.VMEM((8 * SLOT, TILE), F32),
            pltpu.VMEM((8 * SLOT, TILE), F32),
            pltpu.VMEM((8 * SLOT, TILE), BF16),
            pltpu.VMEM((8 * SLOT, TILE), BF16),
            pltpu.VMEM((HC, 16, SLOT, HEAD), F32),
            pltpu.VMEM((8, 2, 2, SLOT, HEAD), F32),
            pltpu.VMEM((HC, 2, 2, SLOT, HEAD), F32),
            pltpu.VMEM((HC, 2, SLOT, HEAD), F32),
            pltpu.VMEM((2, 4, TILE, HEAD), BF16),
            pltpu.VMEM((2, 4, TILE, HEAD), BF16),
            pltpu.VMEM((2, 4, SLOT, 8, HEAD), BF16),
            pltpu.VMEM((2, 4, SLOT, 8, HEAD), BF16),
            pltpu.VMEM((HC, 4, 2, SLOT, HEAD), BF16),
            pltpu.VMEM((HC, 2, SLOT, HEAD), BF16),
            pltpu.VMEM((2, 2, 16, SLOT), F32),
            pltpu.VMEM((12, SLOT, SLOT), F32),
            pltpu.VMEM((4, 1, 2 * SLOT), jnp.int32),
            dma((6,)),
            dma((2,)), dma((2,)),
            dma((3,)), dma((4,)),
            dma((2, 2)), dma((2, 2)),
            dma((3, HC)), dma((HC, 4)),
            dma, dma((8, 2)), dma((HC, 2)), dma((HC, 2)),
            dma((HC,)), dma((HC,)), dma((HC,)), dma((8,)),
            dma((2, 2, 4)), dma((2, 2, 2)),
            dma((HC, 4)), dma((HC, 2)),
            dma, dma,
        ],
        compiler_params=pltpu.CompilerParams(collective_id=0, has_side_effects=True, vmem_limit_bytes=61300000),
        name="attn",
    )(cu, valid, q, k, v, do)


def finish_kernel(o_in, dq_in, dkv_in, lse_in, cu, o_out, dq_out, dk_out, dv_out, lse_out, dk_t, dv_t, lse_t, sem, lse_sem):
    l0 = lax.shift_right_logical(cu[1], 3)
    rest = SLOT - l0

    def copies(i, x, out):
        runs = ((0, 0, 0, l0), (1, 0, l0, l0), (0, l0, 2 * l0, rest), (1, l0, SLOT + l0, rest))
        return [pltpu.make_async_copy(x.at[up, pl.ds(at, n)], out.at[pl.ds(to, n)], sem.at[i])
                for up, at, to, n in runs]

    for cp in copies(0, o_in, o_out) + copies(1, dq_in, dq_out):
        cp.start()

    for w, dst in ((0, dk_t), (1, dv_t)):
        for up in range(2):
            def body(i, _):
                at = pl.ds(pl.multiple_of(i * 16, 16), 16)
                dst[up, at] = jnp.transpose(dkv_in[:, up, w, at, :], (1, 0, 2))
                return 0
            lax.fori_loop(0, SLOT // 16, body, 0)
        for cp in copies(2 + w, dst, (dk_out, dv_out)[w]):
            cp.start()

    row = lax.broadcasted_iota(jnp.int32, (2 * SLOT, SLOT), 0)
    col = lax.broadcasted_iota(jnp.int32, (2 * SLOT, SLOT), 1)
    acc = None
    for up in range(2):
        if up:
            src = jnp.where(col < l0, col + l0, col + SLOT)
        else:
            src = jnp.where(col < l0, col, col + l0)
        pick = jnp.where(row == src, 1.0, 0.0)
        part = lax.dot_general(lse_in[up], pick, NT, precision=lax.Precision.HIGHEST, preferred_element_type=F32)
        acc = part if acc is None else acc + part
    lse_t[...] = acc
    lse_move = pltpu.make_async_copy(lse_t, lse_out, lse_sem)
    lse_move.start()
    for i, out in enumerate((o_out, dq_out, dk_out, dv_out)):
        pltpu.make_async_copy(out, out, sem.at[i]).wait()
    lse_move.wait()


def finish_call(o_t, dq_t, dkv_hm, lse_hm, cu):
    any_spec = pl.BlockSpec(memory_space=pl.ANY)
    vmem = pl.BlockSpec(memory_space=pltpu.VMEM)
    return pl.pallas_call(
        finish_kernel,
        out_shape=(
            jax.ShapeDtypeStruct((256, 32, HEAD), BF16),
            jax.ShapeDtypeStruct((256, 32, HEAD), BF16),
            jax.ShapeDtypeStruct((256, 8, HEAD), BF16),
            jax.ShapeDtypeStruct((256, 8, HEAD), BF16),
            jax.ShapeDtypeStruct((32, 256), F32),
        ),
        in_specs=[vmem] * 4 + [pl.BlockSpec(memory_space=pltpu.SMEM)],
        out_specs=(any_spec,) * 5,
        scratch_shapes=[
            pltpu.VMEM((2, SLOT, 8, HEAD), BF16),
            pltpu.VMEM((2, SLOT, 8, HEAD), BF16),
            pltpu.VMEM((32, 256), F32),
            pltpu.SemaphoreType.DMA((4,)),
            pltpu.SemaphoreType.DMA,
        ],
        compiler_params=pltpu.CompilerParams(vmem_limit_bytes=16 * 1024 * 1024),
        name="finish",
    )(o_t, dq_t, dkv_hm, lse_hm, cu)


def solution(mesh):
    tok_spec = P(("dp", "cp"), None, None)
    lse_spec = P(("dp", "cp"), None)

    def local(q, k, v, do, valid, cu):
        res = attn_call(cu, valid.reshape(1, 256), q, k, v, do)
        o, dq, dk, dv, lse = finish_call(*res)
        return o, lse.T, dq, dk, dv

    return jax.shard_map(local, mesh=mesh, in_specs=(tok_spec,) * 4 + (P(("dp", "cp")), P("dp")),
                         out_specs=(tok_spec, lse_spec, tok_spec, tok_spec, tok_spec), check_vma=False)
```

```python
import functools
import math

import jax
import jax.numpy as jnp
from jax import lax
from jax.experimental import pallas as pl
from jax.experimental.pallas import tpu as pltpu
from jax.sharding import PartitionSpec as P

MESH = pl.DeviceIdType.MESH
FILL = -1.0e30
BIG = 3.0e38
HEAD = 128
SLOT = 128
TILE = 512
GROUP = 4
HC = 4
SW = (2, 2, 2, 0)
SCALE = HEAD ** -0.5
C2 = SCALE * math.log2(math.e)
NT = (((1,), (1,)), ((), ()))
NN = (((1,), (0,)), ((), ()))
F32 = jnp.float32
BF16 = jnp.bfloat16

TILES = ((0, 0), (1, 0), (1, 1), (0, 1))


def slot_of(chip, ti):
    oc, up = TILES[ti]
    r = 2 * chip + oc
    return 7 - r if up else r


def mm(a, b, dims):
    return lax.dot_general(a, b, dims, preferred_element_type=F32)


def src_row(up, t, l0):
    if up:
        return jnp.where(t < l0, t + l0, t + SLOT)
    return jnp.where(t < l0, t, t + l0)


def attn_kernel(cu_hbm, valid, q, k, v, do, o_out, dq_out, dkv_out, lse_out, cu,
                raw_q, raw_do, far_q, far_do, raw_k, raw_v, kv_hm, kv_all, kt, vt, qh, doh, st0, st1, pb, db,
                dkv_acc, cross_in, near_in, swap_in, o_st, dq_st, o_far, dq_far, dkv_st, back_st, lse_st, caps, valid_all,
                in_sem, raw_ssem, raw_rsem, val_ssem, val_rsem, first_ssem, first_rsem, kv_ssem, kv_rsem,
                part_ssem, part_rsem, near_ssem, near_rsem, swap_ssem, swap_rsem, back_ssem, back_rsem, res_ssem, res_rsem, dkv_ssem, dkv_rsem, lse_sem, lse_rsem):
    r = lax.axis_index("cp")
    chip = r // 2
    c = r % 2
    pc = 1 - c
    partner = chip * 2 + pc
    cross = (1 - chip) * 2 + c
    cross_o = (1 - chip) * 2 + pc

    def remote(src, dst, ssem, rsem, dev):
        return pltpu.make_async_remote_copy(src_ref=src, dst_ref=dst, send_sem=ssem, recv_sem=rsem,
                                            device_id={"cp": dev}, device_id_type=MESH)

    own_heads = pl.ds(pl.multiple_of(16 * c, 16), 16)
    oth_heads = pl.ds(pl.multiple_of(16 * pc, 16), 16)
    ld_k = pltpu.make_async_copy(k, raw_k, in_sem.at[0])
    ld_v = pltpu.make_async_copy(v, raw_v, in_sem.at[1])
    ld_q = pltpu.make_async_copy(q.at[:, own_heads, :], raw_q, in_sem.at[2])
    ld_do = pltpu.make_async_copy(do.at[:, own_heads, :], raw_do, in_sem.at[3])
    ld_val = pltpu.make_async_copy(valid, valid_all.at[r], in_sem.at[4])
    ld_cu = pltpu.make_async_copy(cu_hbm, cu, in_sem.at[5])
    for cp in (ld_cu, ld_k, ld_v, ld_val):
        cp.start()

    barrier = pltpu.get_barrier_semaphore()
    for dev in (partner, cross, cross_o):
        pl.semaphore_signal(barrier, inc=1, device_id={"cp": dev}, device_id_type=MESH)
    ld_cu.wait()
    l0 = lax.shift_right_logical(cu[1], 3)

    peers = (partner, cross, cross_o)
    push_q = remote(q.at[:, oth_heads, :], far_q, raw_ssem.at[0], raw_rsem.at[0], partner)
    push_do = remote(do.at[:, oth_heads, :], far_do, raw_ssem.at[1], raw_rsem.at[1], partner)
    push_val = [remote(valid, valid_all.at[r], val_ssem.at[i], val_rsem.at[r], dev) for i, dev in enumerate(peers)]


    def kv_relayout(up):
        def body(i, _):
            t0 = i * 16
            for which, raw in ((0, raw_k), (1, raw_v)):
                rows = jnp.stack([raw[src_row(up, t0 + j, l0)] for j in range(16)])
                kv_hm[:, up, which, pl.ds(pl.multiple_of(t0, 16), 16), :] = jnp.transpose(rows, (1, 0, 2))
            return 0
        lax.fori_loop(0, SLOT // 16, body, 0)

    def kv_push(h, to, both):
        head = (4 * c if to == 1 else 4 * pc) + h
        dev = (partner, cross, cross_o)[to]
        ups = pl.ds(0, 2 if both else 1)
        return remote(kv_hm.at[head, ups], kv_all.at[h, r, ups], kv_ssem.at[to, h], kv_rsem.at[h, r], dev)

    def kv_first(to, up):
        head = 4 * c if to == 1 else 4 * pc
        at = pl.ds(up, 1)
        return remote(kv_hm.at[head, at], kv_all.at[0, r, at], first_ssem.at[to - 1, up], first_rsem.at[c, up],
                      (cross, cross_o)[to - 1])

    def kv_wait(h, owner, both):
        ups = pl.ds(0, 2 if both else 1)
        remote(kv_hm.at[0, ups], kv_all.at[h, owner, ups], kv_ssem.at[0, h], kv_rsem.at[h, owner], partner).wait_recv()

    def first_wait(owner):
        for up in range(2):
            at = pl.ds(up, 1)
            remote(kv_hm.at[0, at], kv_all.at[0, owner, at], first_ssem.at[0, up], first_rsem.at[owner - 2, up], partner).wait_recv()

    ld_k.wait()
    ld_v.wait()
    kv_relayout(0)
    pl.semaphore_wait(barrier, 3)

    def cross_send(ch, h):
        @pl.when(chip == ch)
        def _():
            for to in (1, 2):
                kv_push(h, to, ch == 1).start()

    cross_send(0, 0)

    def send_first(up):
        @pl.when(chip == 1)
        def _():
            for to in (1, 2):
                kv_first(to, up).start()

    send_first(0)
    kv_relayout(1)
    send_first(1)
    for cp in (ld_q, ld_do, push_q, push_do):
        cp.start()
    for h in range(HC):
        kv_push(h, 0, True).start()
    ld_val.wait()
    for cp in push_val:
        cp.start()

    def copy_own(h, _):
        for up in range(2):
            kv_all[h, r, up] = kv_hm[4 * c + h, up]
        return 0
    lax.fori_loop(0, HC, copy_own, 0)

    def q_relayout(oc, from_q, from_do):
        for up, ti in ((0, oc), (1, 3 - oc)):
            def body(i, _):
                t0 = i * 16
                at = pl.ds(pl.multiple_of(t0, 16), 16)
                for raw, dst in ((from_q, qh), (from_do, doh)):
                    rows = jnp.stack([raw[src_row(up, t0 + j, l0)] for j in range(16)])
                    dst[:, ti, :, at, :] = jnp.transpose(rows, (1, 0, 2)).reshape(HC, GROUP, 16, HEAD)
                return 0
            lax.fori_loop(0, SLOT // 16, body, 0)

    ld_q.wait()
    ld_do.wait()
    cross_send(0, 1)
    q_relayout(c, raw_q, raw_do)

    cross_send(0, 2)
    for i in range(3):
        remote(valid, valid_all.at[peers[i]], val_ssem.at[i], val_rsem.at[peers[i]], peers[i]).wait_recv()
    lane = lax.broadcasted_iota(jnp.int32, (SLOT, SLOT), 1)
    sub = lax.broadcasted_iota(jnp.int32, (SLOT, SLOT), 0)
    lane2 = lax.broadcasted_iota(jnp.int32, (SLOT, 2 * SLOT), 1)
    sub2 = lax.broadcasted_iota(jnp.int32, (SLOT, 2 * SLOT), 0)
    same_doc = (lane < l0) == (sub < l0)
    doc_f = jnp.where(lane < l0, 1.0, 0.0)
    doc_s = jnp.where(sub < l0, 1.0, 0.0)
    same_f = jnp.where(doc_f == doc_s, 1.0, 0.0)
    del same_doc

    def cap_body(s, _):
        owner = jnp.where(s < 4, s, 7 - s)
        off = jnp.where(s < 4, 0, 1)
        src_lo = jnp.where(sub2 < l0, sub2, sub2 + l0)
        src_hi = jnp.where(sub2 < l0, sub2 + l0, sub2 + SLOT)
        src = jnp.where(off == 1, src_hi, src_lo)
        row = jnp.broadcast_to(valid_all[owner].astype(F32), (SLOT, 2 * SLOT))
        ok = jnp.sum(jnp.where(src == lane2, row, 0.0), axis=1, keepdims=True)
        caps[s] = jnp.where(same_f * ok > 0.5, BIG, FILL)
        return 0
    lax.fori_loop(0, 8, cap_body, 0)
    for ti in range(4):
        oc, up = TILES[ti]
        s = (7 - (2 * chip + oc)) if up else 2 * chip + oc
        caps[8 + ti] = jnp.where(sub <= lane, caps[s], FILL)

    cross_send(0, 3)
    cross_send(1, 1)
    push_q.wait_recv()
    push_do.wait_recv()
    q_relayout(pc, far_q, far_do)

    def part_copy(h, u, n=2):
        up = int(u > 3)
        return remote(dkv_acc.at[h, pl.ds(2 * u, n)], cross_in.at[4 * c + h, up, pl.ds(0, n)], part_ssem,
                      part_rsem.at[4 * c + h, up], min(u, 7 - u))

    def part_wait(j, up, n=2):
        remote(dkv_acc.at[0, pl.ds(0, n)], cross_in.at[j, up, pl.ds(0, n)], part_ssem,
               part_rsem.at[j, up], partner).wait_recv()

    def near_copy(h, up, slot, n=2):
        return remote(dkv_acc.at[h, pl.ds(2 * slot, n)], near_in.at[h, up, pl.ds(0, n)], near_ssem.at[h, up],
                      near_rsem.at[h, up], partner)

    def near_run(ch, h, act):
        act(near_copy(h, 0, 2 * ch + pc))
        if ch == 1:
            pl.when(c == 0)(lambda: act(near_copy(h, 1, 4)))
            if SW[h] < 2:
                pl.when(c == 1)(lambda: act(near_copy(h, 1, 5, 2 - SW[h])))

    def near_wait(h, up, n=2):
        near_copy(h, up, 0, n).wait_recv()

    def swap_copy(h):
        n = SW[h]
        return remote(dkv_acc.at[h, pl.ds(12 - n, n)], swap_in.at[h, pl.ds(2 - n, n)], swap_ssem.at[h], swap_rsem.at[h], cross)

    def swap_back(h, core):
        at = pl.ds(2 - SW[h], SW[h])
        j = 4 * core + h
        return remote(back_st.at[h, at], dkv_out.at[j, 1, at], back_ssem.at[h], back_rsem.at[j], 2)

    def res_copy(p, ti, which):
        stage, out = ((o_far, o_out), (dq_far, dq_out))[which]
        dst = out.at[TILES[ti][1], :, pl.ds(pl.multiple_of(16 * c + 8 * p, 8), 8), :]
        return remote(stage.at[p, ti], dst, res_ssem.at[which, p, ti], res_rsem.at[which, p, TILES[ti][1]], partner)

    def dkv_copy(h, ti):
        up = TILES[ti][1]
        return remote(dkv_st.at[h, ti], dkv_out.at[4 * c + h, up], dkv_ssem.at[h, ti], dkv_rsem.at[h, up], partner)

    def res_put(p):
        heads = pl.ds(pl.multiple_of(16 * c + 8 * p, 8), 8)
        for ti, (oc, up) in enumerate(TILES):
            def body(i, _, keep):
                at = pl.ds(pl.multiple_of(i * 16, 16), 16)
                for stage, far, out in ((o_st, o_far, o_out), (dq_st, dq_far, dq_out)):
                    x = jnp.concatenate([stage[e, ti, pl.ds(pl.multiple_of(g * SLOT + i * 16, 16), 16), :][None]
                                         for e in range(2) for g in range(GROUP)], axis=0)
                    y = jnp.transpose(x, (1, 0, 2))
                    if keep:
                        out[up, at, heads, :] = y
                    else:
                        far[p, ti, at, :, :] = y
                return 0

            @pl.when(c == oc)
            def _():
                lax.fori_loop(0, SLOT // 16, functools.partial(body, keep=True), 0)

            @pl.when(c != oc)
            def _():
                lax.fori_loop(0, SLOT // 16, functools.partial(body, keep=False), 0)
                for which in range(2):
                    res_copy(p, ti, which).start()

    def dkv_put(h, ti, parts):
        oc, up = TILES[ti]

        @pl.when(c == oc)
        def _():
            for w in range(2):
                dkv_out[4 * c + h, up, w] = parts(w).astype(BF16)

        @pl.when(c != oc)
        def _():
            for w in range(2):
                dkv_st[h, ti, w] = parts(w).astype(BF16)
            dkv_copy(h, ti).start()

    lse_far = remote(lse_st.at[pc], lse_out.at[:, own_heads, :], lse_sem, lse_rsem, partner)

    def kv_slot(h, s, which):
        return kv_all[h, min(s, 7 - s), int(s > 3), which]

    def kv_slots(h, a, b, which):
        return jnp.concatenate([kv_slot(h, s, which) for s in range(a, b)], axis=0)

    def run_chip(ch):
        slots = [slot_of(ch, ti) for ti in range(4)]
        sent = [0, 1] if ch == 1 else [2, 3, 4, 5]

        def transposes(s):
            for src, dst in ((0, kt), (1, vt)):
                dst[:, s * SLOT:(s + 1) * SLOT] = jnp.transpose(kv_slot(h_ref[0], s, src))

        h_ref = [None]
        sts = (st0, st1)

        def point(h, where):
            if ch == 0:
                return
            kv = {(0, 1): 2, (0, 4): 3}
            swaps = {(1, 2): (0,), (1, 4): (1,), (2, 4): (2,)}
            parts = {(2, 2): (0,), (2, 4): (1,), (3, 4): (2, 3)}
            for at in range(HC):
                if not any((at, where) in d for d in (kv, swaps, parts)):
                    continue

                @pl.when(h == at)
                def _():
                    if (at, where) in kv:
                        for to in (1, 2):
                            kv_push(kv[at, where], to, True).start()
                    for e in swaps.get((at, where), ()):
                        swap_copy(e).start()
                    for e in parts.get((at, where), ()):
                        for u in (0, 1):
                            part_copy(e, u).start()

        def head(h, _):
            h_ref[0] = h
            seen = set()
            ready = set()

            def wait_slot(s):
                if s in ready:
                    return
                if s in slots:
                    kv_wait(h, partner, True)
                    new = slots
                elif ch == 1:
                    for owner in (0, 1):
                        kv_wait(h, owner, False)
                    new = [0, 1]
                else:
                    for owner in (2, 3):
                        pl.when(h == 0)(functools.partial(first_wait, owner))
                        pl.when(h > 0)(functools.partial(kv_wait, h, owner, True))
                    new = [2, 3, 4, 5]
                for u in new:
                    ready.add(u)
                    transposes(u)

            state = {}

            def forward(ti):
                point(h, ti)
                s = slots[ti]
                nk = s + 1
                for u in range(nk):
                    wait_slot(u)
                st = sts[ti % 2]
                qt = qh[h, ti].reshape(TILE, HEAD)
                dt = doh[h, ti].reshape(TILE, HEAD)
                m8 = [None] * GROUP
                for a in range(0, nk, 2):
                    n = min(2, nk - a)
                    kb = kv_slots(h, a, a + n, 0)
                    sc = mm(kb, qt, NT)
                    for j in range(n):
                        cap = caps[8 + ti] if a + j == s else caps[a + j]
                        for g in range(GROUP):
                            x = jnp.minimum(sc[j * SLOT:(j + 1) * SLOT, g * SLOT:(g + 1) * SLOT], cap)
                            st[(a + j) * SLOT:(a + j + 1) * SLOT, g * SLOT:(g + 1) * SLOT] = x
                            top = jnp.max(x.reshape(SLOT // 8, 8, SLOT), axis=0)
                            m8[g] = top if m8[g] is None else jnp.maximum(m8[g], top)
                m = [jnp.max(x, axis=0, keepdims=True) for x in m8]
                mc = [x * C2 for x in m]
                l8 = [None] * GROUP
                for a in range(nk):
                    for g in range(GROUP):
                        at = (slice(a * SLOT, (a + 1) * SLOT), slice(g * SLOT, (g + 1) * SLOT))
                        e = jnp.exp2(st[at] * C2 - mc[g])
                        st[at] = e
                        pb[at] = e.astype(BF16)
                        tot = jnp.sum(e.reshape(SLOT // 8, 8, SLOT), axis=0)
                        l8[g] = tot if l8[g] is None else l8[g] + tot
                ot = mm(vt[:, :nk * SLOT], pb[:nk * SLOT, :], NN)
                inv, dd = [], []
                oc, up = TILES[ti]
                for g in range(GROUP):
                    l = jnp.sum(l8[g], axis=0, keepdims=True)
                    has = m[g] > 0.5 * FILL
                    safe = jnp.where(has, l, 1.0)
                    i_l = jnp.where(has, 1.0 / safe, 0.0)
                    lse = jnp.where(has, m[g] * SCALE + jnp.log(safe), 0.0)
                    lse_st[oc, up, pl.ds(h * GROUP + g, 1), :] = lse
                    og = (ot[:, g * SLOT:(g + 1) * SLOT] * i_l).astype(BF16)
                    dog = jnp.transpose(dt[g * SLOT:(g + 1) * SLOT, :])
                    dd.append(jnp.sum(og.astype(F32) * dog.astype(F32), axis=0, keepdims=True))
                    inv.append(i_l)
                    o_st[h % 2, ti, g * SLOT:(g + 1) * SLOT, :] = jnp.transpose(og)

                state[ti] = [inv, dd, None]

            def backward(ti, part):
                inv, dd, dqt = state[ti]
                qt = qh[h, ti].reshape(TILE, HEAD)
                dt = doh[h, ti].reshape(TILE, HEAD)
                st = sts[ti % 2]
                runs = []
                for u in part:
                    if runs and runs[-1][1] == u and u - runs[-1][0] < 2:
                        runs[-1][1] = u + 1
                    else:
                        runs.append([u, u + 1])
                for a, b in runs:
                    n = b - a
                    vb = kv_slots(h, a, b, 1)
                    dp = mm(vb, dt, NT)
                    for j in range(n):
                        for g in range(GROUP):
                            at = (slice((a + j) * SLOT, (a + j + 1) * SLOT), slice(g * SLOT, (g + 1) * SLOT))
                            p = st[at] * inv[g]
                            pb[at] = p.astype(BF16)
                            ds = p * (dp[j * SLOT:(j + 1) * SLOT, g * SLOT:(g + 1) * SLOT] - dd[g])
                            db[at] = ds.astype(BF16)
                    dsb = db[a * SLOT:b * SLOT, :]
                    dv = mm(pb[a * SLOT:b * SLOT, :], dt, NN)
                    dk = mm(dsb, qt, NN) * SCALE
                    dq = mm(kt[:, a * SLOT:b * SLOT], dsb, NN)
                    dqt = dq if dqt is None else dqt + dq
                    for j in range(n):
                        u = a + j
                        new = (dk[j * SLOT:(j + 1) * SLOT], dv[j * SLOT:(j + 1) * SLOT])
                        for w in range(2):
                            dkv_acc[h, 2 * u + w] = dkv_acc[h, 2 * u + w] + new[w] if u in seen else new[w]
                        seen.add(u)
                state[ti][2] = dqt

            def finish(ti):
                dqt = state[ti][2]
                for g in range(GROUP):
                    dqg = (dqt[:, g * SLOT:(g + 1) * SLOT] * SCALE).astype(BF16)
                    dq_st[h % 2, ti, g * SLOT:(g + 1) * SLOT, :] = jnp.transpose(dqg)

            if ch == 0:
                for ti in (0, 1):
                    forward(ti)
                    backward(ti, range(slots[ti] + 1))
                    finish(ti)
                for ti in (2, 3):
                    forward(ti)
                for ti in (2, 3):
                    backward(ti, [2, 3])
                for u in (2, 3):
                    part_copy(h, u).start()
                for ti in (2, 3):
                    backward(ti, [4, 5])
                part_copy(h, 4).start()
                for at in range(HC):
                    if SW[at] < 2:
                        pl.when(h == at)(part_copy(at, 5, 2 - SW[at]).start)
                for ti in (2, 3):
                    backward(ti, [u for u in range(slots[ti] + 1) if u not in sent])
                    finish(ti)
            else:
                for ti in range(4):
                    forward(ti)
                    backward(ti, range(slots[ti] + 1))
                    finish(ti)
            if ch == 1:
                point(h, 4)
            else:
                for ti in (2, 3):
                    dkv_put(h, ti, lambda w, ti=ti: dkv_acc[h, 2 * slots[ti] + w])
            for at in range(HC):
                pl.when(h == at)(functools.partial(near_run, ch, at, lambda cp: cp.start()))
            pl.when(h % 2 == 1)(lambda: res_put(h // 2))
            return 0

        lax.fori_loop(0, HC, head, 0)

        lse_out[:, own_heads, :] = lse_st[c]
        lse_far.start()

        if ch == 0:
            for h in range(HC):
                if SW[h]:
                    swap_copy(h).wait_recv()
                    for w in range(2 - SW[h], 2):
                        back_st[h, w] = (swap_in[h, w] + dkv_acc[h, 10 + w]).astype(BF16)
                    swap_back(h, c).start()

        def early(h, _):
            kv_push(h, 0, True).wait_send()
            for to in (1, 2):
                if ch == 0:
                    kv_push(h, to, False).wait_send()
                else:
                    pl.when(h > 0)(kv_push(h, to, True).wait_send)
            if ch == 0:
                for ti in (2, 3):
                    pl.when(c != TILES[ti][0])(dkv_copy(h, ti).wait_send)
                remote(dkv_st.at[h, 0], dkv_out.at[4 * pc + h, 1], dkv_ssem.at[h, 0], dkv_rsem.at[h, 1], partner).wait_recv()
            return 0
        lax.fori_loop(0, HC, early, 0)
        if ch == 1:
            for to in (1, 2):
                for up in range(2):
                    kv_first(to, up).wait_send()
        for h in range(HC):
            near_run(ch, h, lambda cp: cp.wait_send())
            near_wait(h, 0)
            if ch == 1:
                pl.when(c == 1)(functools.partial(near_wait, h, 1))
                if SW[h] < 2:
                    pl.when(c == 0)(functools.partial(near_wait, h, 1, 2 - SW[h]))
        push_q.wait_send()
        push_do.wait_send()
        for cp in push_val:
            cp.wait_send()
        for p in range(2):
            for which in range(2):
                stage, out = ((o_far, o_out), (dq_far, dq_out))[which]
                for ti in range(4):
                    pl.when(c != TILES[ti][0])(res_copy(p, ti, which).wait_send)
                for up in range(2):
                    dst = out.at[up, :, pl.ds(pl.multiple_of(16 * pc + 8 * p, 8), 8), :]
                    remote(stage.at[p, 0], dst, res_ssem.at[which, p, 0], res_rsem.at[which, p, up], partner).wait_recv()
        lse_far.wait_send()
        remote(lse_st.at[0], lse_out.at[:, oth_heads, :], lse_sem, lse_rsem, partner).wait_recv()

        def add_up(h, up, slot, n):
            if n == 0:
                return
            part_wait(4 * c + h, up, n)
            for w in range(n):
                dkv_out[4 * c + h, up, w] = (dkv_acc[h, 2 * slot + w] + cross_in[4 * c + h, up, w]).astype(BF16)
            part_wait(4 * pc + h, up, n)
            for w in range(n):
                dkv_out[4 * pc + h, up, w] = (near_in[h, up, w] + cross_in[4 * pc + h, up, w]).astype(BF16)

        for h in range(HC):
            add_up(h, 0, 2 * ch + c, 2)
            if ch == 1:
                pl.when(c == 1)(functools.partial(add_up, h, 1, 4, 2))
                pl.when(c == 0)(functools.partial(add_up, h, 1, 5, 2 - SW[h]))

        units = HC * 4 if ch == 1 else HC * 8 - sum(SW)
        rows = next(a for a in (1, 2, 3, 4) if units % a == 0 and units // a <= 16)
        block = dkv_acc.at[pl.ds(0, rows), pl.ds(0, units // rows)]
        remote(block, block, part_ssem, part_rsem.at[0, 0], partner).wait_send()
        for h in range(HC):
            if SW[h]:
                if ch == 0:
                    swap_back(h, c).wait_send()
                else:
                    swap_copy(h).wait_send()

        if ch == 1:
            @pl.when(c == 0)
            def _():
                for h in range(HC):
                    if SW[h]:
                        for core in range(2):
                            swap_back(h, core).wait_recv()

    pl.when(chip == 0)(functools.partial(run_chip, 0))
    pl.when(chip == 1)(functools.partial(run_chip, 1))


def attn_call(cu, valid, q, k, v, do):
    any_spec = pl.BlockSpec(memory_space=pl.ANY)
    dma = pltpu.SemaphoreType.DMA
    return pl.pallas_call(
        attn_kernel,
        out_shape=(
            pltpu.VMEM((2, SLOT, 32, HEAD), BF16),
            pltpu.VMEM((2, SLOT, 32, HEAD), BF16),
            pltpu.VMEM((8, 2, 2, SLOT, HEAD), BF16),
            pltpu.VMEM((2, 32, SLOT), F32),
            pltpu.SMEM((3,), jnp.int32),
        ),
        in_specs=[any_spec] * 6,
        out_specs=(pl.BlockSpec(memory_space=pltpu.VMEM),) * 4 + (pl.BlockSpec(memory_space=pltpu.SMEM),),
        scratch_shapes=[
            pltpu.VMEM((256, 16, HEAD), BF16),
            pltpu.VMEM((256, 16, HEAD), BF16),
            pltpu.VMEM((256, 16, HEAD), BF16),
            pltpu.VMEM((256, 16, HEAD), BF16),
            pltpu.VMEM((256, 8, HEAD), BF16),
            pltpu.VMEM((256, 8, HEAD), BF16),
            pltpu.VMEM((8, 2, 2, SLOT, HEAD), BF16),
            pltpu.VMEM((HC, 4, 2, 2, SLOT, HEAD), BF16),
            pltpu.VMEM((HEAD, 8 * SLOT), BF16),
            pltpu.VMEM((HEAD, 8 * SLOT), BF16),
            pltpu.VMEM((HC, 4, GROUP, SLOT, HEAD), BF16),
            pltpu.VMEM((HC, 4, GROUP, SLOT, HEAD), BF16),
            pltpu.VMEM((8 * SLOT, TILE), F32),
            pltpu.VMEM((8 * SLOT, TILE), F32),
            pltpu.VMEM((8 * SLOT, TILE), BF16),
            pltpu.VMEM((8 * SLOT, TILE), BF16),
            pltpu.VMEM((HC, 16, SLOT, HEAD), F32),
            pltpu.VMEM((8, 2, 2, SLOT, HEAD), F32),
            pltpu.VMEM((HC, 2, 2, SLOT, HEAD), F32),
            pltpu.VMEM((HC, 2, SLOT, HEAD), F32),
            pltpu.VMEM((2, 4, TILE, HEAD), BF16),
            pltpu.VMEM((2, 4, TILE, HEAD), BF16),
            pltpu.VMEM((2, 4, SLOT, 8, HEAD), BF16),
            pltpu.VMEM((2, 4, SLOT, 8, HEAD), BF16),
            pltpu.VMEM((HC, 4, 2, SLOT, HEAD), BF16),
            pltpu.VMEM((HC, 2, SLOT, HEAD), BF16),
            pltpu.VMEM((2, 2, 16, SLOT), F32),
            pltpu.VMEM((12, SLOT, SLOT), F32),
            pltpu.VMEM((4, 1, 2 * SLOT), jnp.int32),
            dma((6,)),
            dma((2,)), dma((2,)),
            dma((3,)), dma((4,)),
            dma((2, 2)), dma((2, 2)),
            dma((3, HC)), dma((HC, 4)),
            dma, dma((8, 2)), dma((HC, 2)), dma((HC, 2)),
            dma((HC,)), dma((HC,)), dma((HC,)), dma((8,)),
            dma((2, 2, 4)), dma((2, 2, 2)),
            dma((HC, 4)), dma((HC, 2)),
            dma, dma,
        ],
        compiler_params=pltpu.CompilerParams(collective_id=0, has_side_effects=True, vmem_limit_bytes=61300000),
        name="attn",
    )(cu, valid, q, k, v, do)


def finish_kernel(o_in, dq_in, dkv_in, lse_in, cu, o_out, dq_out, dk_out, dv_out, lse_out, dk_t, dv_t, lse_t, sem, lse_sem):
    l0 = lax.shift_right_logical(cu[1], 3)
    rest = SLOT - l0

    def copies(i, x, out):
        runs = ((0, 0, 0, l0), (1, 0, l0, l0), (0, l0, 2 * l0, rest), (1, l0, SLOT + l0, rest))
        return [pltpu.make_async_copy(x.at[up, pl.ds(at, n)], out.at[pl.ds(to, n)], sem.at[i])
                for up, at, to, n in runs]

    for cp in copies(0, o_in, o_out) + copies(1, dq_in, dq_out):
        cp.start()

    for w, dst in ((0, dk_t), (1, dv_t)):
        for up in range(2):
            def body(i, _):
                at = pl.ds(pl.multiple_of(i * 16, 16), 16)
                dst[up, at] = jnp.transpose(dkv_in[:, up, w, at, :], (1, 0, 2))
                return 0
            lax.fori_loop(0, SLOT // 16, body, 0)
        for cp in copies(2 + w, dst, (dk_out, dv_out)[w]):
            cp.start()

    row = lax.broadcasted_iota(jnp.int32, (2 * SLOT, SLOT), 0)
    col = lax.broadcasted_iota(jnp.int32, (2 * SLOT, SLOT), 1)
    acc = None
    for up in range(2):
        if up:
            src = jnp.where(col < l0, col + l0, col + SLOT)
        else:
            src = jnp.where(col < l0, col, col + l0)
        pick = jnp.where(row == src, 1.0, 0.0)
        part = lax.dot_general(lse_in[up], pick, NT, precision=lax.Precision.HIGHEST, preferred_element_type=F32)
        acc = part if acc is None else acc + part
    lse_t[...] = acc
    lse_move = pltpu.make_async_copy(lse_t, lse_out, lse_sem)
    lse_move.start()
    for i, out in enumerate((o_out, dq_out, dk_out, dv_out)):
        pltpu.make_async_copy(out, out, sem.at[i]).wait()
    lse_move.wait()


def finish_call(o_t, dq_t, dkv_hm, lse_hm, cu):
    any_spec = pl.BlockSpec(memory_space=pl.ANY)
    vmem = pl.BlockSpec(memory_space=pltpu.VMEM)
    return pl.pallas_call(
        finish_kernel,
        out_shape=(
            jax.ShapeDtypeStruct((256, 32, HEAD), BF16),
            jax.ShapeDtypeStruct((256, 32, HEAD), BF16),
            jax.ShapeDtypeStruct((256, 8, HEAD), BF16),
            jax.ShapeDtypeStruct((256, 8, HEAD), BF16),
            jax.ShapeDtypeStruct((32, 256), F32),
        ),
        in_specs=[vmem] * 4 + [pl.BlockSpec(memory_space=pltpu.SMEM)],
        out_specs=(any_spec,) * 5,
        scratch_shapes=[
            pltpu.VMEM((2, SLOT, 8, HEAD), BF16),
            pltpu.VMEM((2, SLOT, 8, HEAD), BF16),
            pltpu.VMEM((32, 256), F32),
            pltpu.SemaphoreType.DMA((4,)),
            pltpu.SemaphoreType.DMA,
        ],
        compiler_params=pltpu.CompilerParams(vmem_limit_bytes=16 * 1024 * 1024),
        name="finish",
    )(o_t, dq_t, dkv_hm, lse_hm, cu)


def solution(mesh):
    tok_spec = P(("dp", "cp"), None, None)
    lse_spec = P(("dp", "cp"), None)

    def local(q, k, v, do, valid, cu):
        res = attn_call(cu, valid.reshape(1, 256), q, k, v, do)
        o, dq, dk, dv, lse = finish_call(*res)
        return o, lse.T, dq, dk, dv

    return jax.shard_map(local, mesh=mesh, in_specs=(tok_spec,) * 4 + (P(("dp", "cp")), P("dp")),
                         out_specs=(tok_spec, lse_spec, tok_spec, tok_spec, tok_spec), check_vma=False)
```
